32 devices in a mesh: row: 4 (over x, core), col: 8 (over z, y).
Axes of the slice: x: 2, y: 2, z: 4, core: 2. Of those that a mesh axis runs over, the one named last changes fastest.
Arguments:
- inputs: bfloat16 [8, 512, 2048], P('col', 'row'), may hold values from -6 to 6
- segment_ids: int32 [8, 512], P('col'), may hold values from 0 to 2, never falling along the last dimension, each value on 1 to 256 neighbouring positions
- routes: int32 [8, 512, 6], P('col', 'row'), may hold values from 0 to 63, all different within a row; in each aligned block of 128 rows (0 to 127, 128 to 255, ..., all dimensions but the last counted through in order) at most 16 rows name the same one
- first_gain: float32 [2048], replicated, may hold values from 0.5 to 1.5
- query_weight: bfloat16 [2048, 3072], P('col', 'row'), may hold values from -0.13258252 to 0.13258252
- latent_down: bfloat16 [2048, 576], P('col'), may hold values from -0.13258252 to 0.13258252
- latent_gain: float32 [512], replicated, may hold values from 0.5 to 1.5
- latent_up: bfloat16 [512, 4096], P('col', 'row'), may hold values from -0.25 to 0.25
- output_weight: bfloat16 [2048, 2048], P('row', 'col'), may hold values from -0.375 to 0.375
- second_gain: float32 [2048], replicated, may hold values from 0.5 to 1.5
- router_weight: bfloat16 [2048, 64], replicated, may hold values from -0.25 to 0.25
- shared_gate: bfloat16 [2048, 2816], P('col', 'row'), may hold values from -0.125 to 0.125
- shared_up: bfloat16 [2048, 2816], P('col', 'row'), may hold values from -0.125 to 0.125
- shared_down: bfloat16 [2816, 2048], P('row', 'col'), may hold values from -0.15625 to 0.15625
- expert_gate: bfloat16 [64, 2048, 1408], P('col', None, 'row'), may hold values from -0.125 to 0.125
- expert_up: bfloat16 [64, 2048, 1408], P('col', None, 'row'), may hold values from -0.125 to 0.125
- expert_down: bfloat16 [64, 1408, 2048], P('col', 'row'), may hold values from -0.21875 to 0.21875
- cotangent: float32 [8, 512, 2048], P('col', 'row'), may hold values from -6 to 6
Outputs:
- layer_out: bfloat16 [8, 512, 2048], P('col', 'row')
- input_grad: float32 [8, 512, 2048], P('col', 'row')
- first_gain_grad: float32 [2048], replicated
- query_grad: float32 [2048, 3072], P('col', 'row')
- latent_down_grad: float32 [2048, 576], P('col')
- latent_gain_grad: float32 [512], replicated
- latent_up_grad: float32 [512, 4096], P('col', 'row')
- output_grad: float32 [2048, 2048], P('row', 'col')
- second_gain_grad: float32 [2048], replicated
- router_grad: float32 [2048, 64], replicated
- shared_gate_grad: float32 [2048, 2816], P('col', 'row')
- shared_up_grad: float32 [2048, 2816], P('col', 'row')
- shared_down_grad: float32 [2816, 2048], P('row', 'col')
- expert_gate_grad: float32 [64, 2048, 1408], P('col', None, 'row')
- expert_up_grad: float32 [64, 2048, 1408], P('col', None, 'row')
- expert_down_grad: float32 [64, 1408, 2048], P('col', 'row')
The draws below stay inside these ranges and needn't reach their ends.
Inputs may be any that keep to these rules, and one draw needn't show every extreme that they name: `segment_ids`: within a sequence the segment numbers never fall; a segment spans at most one half of 512 positions, and some segment spans exactly that many. `routes`: each token names 6 different experts. Among the 128 tokens of one device no expert is named more than 16 times, a bound that some block reaches.
All inputs are finite; a program needn't handle non-finite values.
Results may differ from the reference program's by a relative error of at most 0.03.
Values may be sent and summed in bfloat16 or wider, within the bound.
A program may use at most 448 MiB of HBM per device.

```python
import math
import jax
import jax.numpy as jnp
import numpy as np
from jax import lax

D = 2048
H = 16
NOPE = 128
ROPE = 64
LATENT = 512
VD = 128
EXPERTS = 64
TOPK = 6
FF = 1408
SHARED = 2816
LENGTH = 512
TOK_DEV = 128
SEQS = 8
MOST = 16
N_ROW = 4
N_COL = 8


def weight_base(key, salt, column_count):
    random_part = jnp.clip(jax.random.normal(jax.random.fold_in(key, salt), (D, column_count), jnp.float32), -6.0, 6.0)
    return random_part * D ** (-0.5)


def draw_inputs(key, part):
    random_part = jnp.clip(jax.random.normal(jax.random.fold_in(key, 11), (SEQS, LENGTH, D), jnp.float32), -6.0, 6.0)
    return random_part.astype(jnp.bfloat16)


def draw_query_weight(key, part):
    column_count = H * (NOPE + ROPE)
    result_block = weight_base(key, 21, column_count)
    return result_block.astype(jnp.bfloat16)


def draw_latent_down(key, part):
    column_count = LATENT + ROPE
    result_block = weight_base(key, 31, column_count)
    return result_block.astype(jnp.bfloat16)


def level_of(own_key, dims, cuts, smallest, high):
    level = 1.0
    for dim, shards_of in cuts:
        heights = jax.random.uniform(jax.random.fold_in(jax.random.fold_in(own_key, 6), dim), (shards_of,), jnp.float32, smallest / len(cuts), high / len(cuts))
        level = level * jnp.repeat(jnp.exp(heights), dims[dim] // shards_of).reshape((-1,) + (1,) * (len(dims) - 1 - dim))
    return level


def length_profile(amount, total, most, slope):
    loads = [(1 << 20) // math.isqrt(rank ** slope) + 1 for rank in range(2, amount + 1)]
    surplus, counts = total - most - (amount - 1), [1] * (amount - 1)
    while surplus > 0:
        candidates = [i for i in range(amount - 1) if counts[i] < most]
        pool, left = sum([loads[i] for i in candidates]), surplus
        for i in candidates:
            more = min(most - counts[i], max(1, left * loads[i] // pool), surplus)
            counts[i] = counts[i] + more
            surplus = surplus - more
    return np.array([most] + counts)


def uneven_parts(stream_key, number_of, total, reach, lean):
    if number_of == 2:
        one = jax.random.randint(stream_key, (), max(1, total - reach), min(reach, total - 1) + 1)
        return jnp.stack([one, total - one])
    tallies = jnp.asarray(length_profile(number_of, total, reach, lean), jnp.int32)
    couples = (number_of - 1) // 2
    donor, taker = tallies[1:1 + 2 * couples:2], tallies[2:2 + 2 * couples:2]
    margin = jnp.minimum(donor - 1, reach - taker)
    passed = jax.random.randint(jax.random.fold_in(stream_key, 1), (couples,), 0, 1 << 20) % (margin + 1)
    tallies = tallies.at[1:1 + 2 * couples:2].set(donor - passed).at[2:2 + 2 * couples:2].set(taker + passed)
    return tallies[jax.random.permutation(jax.random.fold_in(stream_key, 2), number_of)]


def assign_block(stream_key, own, number, rows, number_of, top, most, lean):
    sequence = jax.random.permutation(stream_key, number_of)
    packed, ordinary = portions_of(number_of, rows * top, most, lean, True), portions_of(number_of, rows * top, most, lean, False)
    places = jnp.arange(number_of)

    def named(lengths, offset_by):
        used = int((lengths > 0).sum())
        fixed = max(1, used // 4)
        shifted = fixed + (places - fixed + offset_by * (used - fixed)) % max(1, number_of - fixed)
        return jnp.zeros((number_of,), jnp.int32).at[sequence[jnp.where(places < fixed, places, shifted)]].set(jnp.asarray(lengths, jnp.int32))

    lengths = jnp.where(number % 4 == 0, named(packed, number // 4), named(ordinary, number - number // 4 - 1))
    mixed = jax.random.permutation(jax.random.fold_in(own, 3), number_of)
    source_of, taker = mixed[0:number_of // 2 * 2:2], mixed[1:number_of // 2 * 2:2]
    slack = jnp.minimum(lengths[source_of] - 1, most - lengths[taker]) // 2
    slack = jnp.where((source_of == sequence[0]) | (taker == sequence[0]) | (lengths[taker] == 0), 0, jnp.maximum(slack, 0))
    shifted = jax.random.randint(jax.random.fold_in(own, 4), (number_of // 2,), 0, 1 << 20) % (slack + 1)
    lengths = lengths.at[source_of].add(-shifted).at[taker].add(shifted)
    members = jnp.searchsorted(jnp.cumsum(lengths), jnp.arange(rows * top), side="right").astype(jnp.int32)
    table = members.reshape(top, rows).T
    table = table[jax.random.permutation(jax.random.fold_in(own, 1), rows)]
    offset_by = jax.random.randint(jax.random.fold_in(own, 2), (rows, 1), 0, top)
    return jnp.take_along_axis(table, (jnp.arange(top)[None, :] + offset_by) % top, axis=1)


def portions_of(number_of, total, reach, slope, full):
    portions = [(1 << 20) // math.isqrt(rank ** slope) + 1 for rank in range(1, number_of + 1)]
    largest = reach if full else min(reach, max(-(-total // number_of), total * portions[0] // sum(portions)))
    least = 1 if total - largest >= number_of - 1 else 0
    counts, spare = [largest] + [least] * (number_of - 1), total - largest - least * (number_of - 1)
    while spare > 0:
        candidates = [i for i in range(1, number_of) if counts[i] < largest] or [i for i in range(1, number_of) if counts[i] < reach]
        pool, left = sum([portions[i] for i in candidates]), spare
        for i in candidates:
            addition = min(reach - counts[i], max(1, left * portions[i] // pool), spare)
            counts[i] = counts[i] + addition
            spare = spare - addition
    return np.array(counts)


def normal_values(key, extent, scale, bound, pieces=(), kind=jnp.bfloat16):
    level = level_of(key, extent, pieces, -0.22, 0.18) if pieces else 1.0
    entries = jax.random.normal(key, extent, jnp.float32) * scale * level
    return jnp.minimum(jnp.maximum(entries, -bound), bound).astype(kind)


def setup_inputs(seed: int = 0) -> dict:
    splits = jax.random.split(jax.random.key(seed), 19)
    inputs = draw_inputs(jax.random.fold_in(splits[18], 71), 0)
    segment_ids = jax.vmap(lambda own: jnp.searchsorted(jnp.cumsum(uneven_parts(own, 3, LENGTH, LENGTH // 2, 1)), jnp.arange(LENGTH), side="right"))(jax.random.split(splits[1], SEQS)).reshape((SEQS, LENGTH)).astype(jnp.int32)
    routes_keys = jax.random.split(jax.random.fold_in(splits[2], 1), SEQS * LENGTH // TOK_DEV)
    routes_turns = jax.random.permutation(jax.random.fold_in(splits[2], 3), SEQS * LENGTH // TOK_DEV)
    routes = jax.vmap(lambda own, number: assign_block(jax.random.fold_in(splits[2], 2), own, number, TOK_DEV, EXPERTS, TOPK, MOST, 1))(routes_keys, routes_turns).reshape((SEQS, LENGTH, TOPK))
    first_gain = jnp.clip(1.0 + 0.1 * jax.random.normal(splits[3], (D,), jnp.float32), 0.5, 1.5)
    query_weight = draw_query_weight(jax.random.fold_in(splits[18], 71), 0)
    latent_down = draw_latent_down(jax.random.fold_in(splits[18], 71), 0)
    latent_gain = jnp.clip(1.0 + 0.1 * jax.random.normal(splits[6], (LATENT,), jnp.float32), 0.5, 1.5)
    latent_up = normal_values(splits[7], (LATENT, H * (NOPE + VD)), LATENT ** -0.5, 0.25, ((0, 8), (1, 4)))
    output_weight = normal_values(splits[8], (H * VD, D), (H * VD // 8) ** -0.5, 0.375, ((0, 4), (1, 8)))
    second_gain = jnp.clip(1.0 + 0.1 * jax.random.normal(splits[9], (D,), jnp.float32), 0.5, 1.5)
    router_weight = normal_values(splits[10], (D, EXPERTS), (D // 4) ** -0.5, 0.25)
    shared_gate = normal_values(splits[11], (D, SHARED), D ** -0.5, 0.125, ((0, 8), (1, 4)))
    shared_up = normal_values(splits[12], (D, SHARED), D ** -0.5, 0.125, ((0, 8), (1, 4)))
    shared_down = normal_values(splits[13], (SHARED, D), (SHARED // 2) ** -0.5, 0.15625, ((0, 4), (1, 8)))
    expert_gate = normal_values(splits[14], (EXPERTS, D, FF), D ** -0.5, 0.125, ((0, 8), (2, 4)))
    expert_up = normal_values(splits[15], (EXPERTS, D, FF), D ** -0.5, 0.125, ((0, 8), (2, 4)))
    expert_down = normal_values(splits[16], (EXPERTS, FF, D), (FF // 2) ** -0.5, 0.21875, ((0, 8), (1, 4)))
    cotangent = normal_values(splits[17], (SEQS, LENGTH, D), 1.0, 6.0, ((0, 8), (1, 4)), jnp.float32)
    return {"inputs": inputs, "segment_ids": segment_ids, "routes": routes, "first_gain": first_gain, "query_weight": query_weight, "latent_down": latent_down, "latent_gain": latent_gain, "latent_up": latent_up, "output_weight": output_weight, "second_gain": second_gain, "router_weight": router_weight, "shared_gate": shared_gate, "shared_up": shared_up, "shared_down": shared_down, "expert_gate": expert_gate, "expert_up": expert_up, "expert_down": expert_down, "cotangent": cotangent}


EPS = 1e-06

def matmul(left_side, right_side):
    return jnp.dot(left_side, right_side, preferred_element_type=jnp.float32)

def rounded(values):
    return lax.optimization_barrier(values.astype(jnp.bfloat16))

def rms_scale(values):
    return lax.rsqrt(lax.optimization_barrier(jnp.mean(values * values, axis=-1, keepdims=True)) + EPS)

def rms_back(values, scaling, gradient):
    return scaling * gradient - values * scaling ** 3 * lax.optimization_barrier(jnp.mean(gradient * values, axis=-1, keepdims=True))

def silu_parts(preact):
    logistic = jax.nn.sigmoid(preact)
    return (preact * logistic, logistic * (1.0 + preact * (1.0 - logistic)))

def angle_tables(length):
    halfway = ROPE // 2
    frequency = 10000.0 ** (-2.0 * jnp.arange(halfway, dtype=jnp.float32) / ROPE)
    angles = jnp.arange(length, dtype=jnp.float32)[:, None] * frequency[None, :]
    return (jnp.cos(angles), jnp.sin(angles))

def rotate(values, cosine_in, sine_in):
    halfway = values.shape[-1] // 2
    leading = values[..., :halfway]
    trailing = values[..., halfway:]
    return jnp.concatenate([leading * cosine_in - trailing * sine_in, leading * sine_in + trailing * cosine_in], axis=-1)

def unrotate(values, cosine_in, sine_in):
    halfway = values.shape[-1] // 2
    leading = values[..., :halfway]
    trailing = values[..., halfway:]
    return jnp.concatenate([leading * cosine_in + trailing * sine_in, trailing * cosine_in - leading * sine_in], axis=-1)

def reference(inputs, segment_ids, routes, first_gain, query_weight, latent_down, latent_gain, latent_up, output_weight, second_gain, router_weight, shared_gate, shared_up, shared_down, expert_gate, expert_up, expert_down, cotangent):
    seq_count, length, width = inputs.shape
    tokens = seq_count * length
    experts = expert_gate.shape[0]
    qk_dim = NOPE + ROPE
    softmax_scale = qk_dim ** (-0.5)
    cosine_table, sine_table = angle_tables(length)
    stream = inputs.reshape(tokens, width).astype(jnp.float32)
    scale_one = rms_scale(stream)
    normed_one = (stream * scale_one * first_gain).astype(jnp.bfloat16)
    query_raw = matmul(normed_one, query_weight).reshape(seq_count, length, H, qk_dim)
    queries = rounded(jnp.concatenate([query_raw[..., :NOPE], rotate(query_raw[..., NOPE:], cosine_table[:, None, :], sine_table[:, None, :])], axis=-1))
    latent_all = matmul(normed_one, latent_down)
    latent = latent_all[:, :LATENT]
    scale_latent = rms_scale(latent)
    latent_normed = (latent * scale_latent * latent_gain).astype(jnp.bfloat16)
    keyval = matmul(latent_normed, latent_up).reshape(seq_count, length, H, NOPE + VD)
    key_rope = rotate(latent_all[:, LATENT:].reshape(seq_count, length, ROPE), cosine_table, sine_table)
    attn_keys = rounded(jnp.concatenate([keyval[..., :NOPE], jnp.broadcast_to(key_rope[:, :, None, :], (seq_count, length, H, ROPE))], axis=-1))
    values = rounded(keyval[..., NOPE:])
    causal = jnp.arange(length)[:, None] >= jnp.arange(length)[None, :]

    def score_block(query_seq, keys_seq, segments):
        allowed = causal & (segments[:, None] == segments[None, :])
        scores = jnp.einsum('qhd,khd->hqk', query_seq.astype(jnp.float32), keys_seq.astype(jnp.float32)) * softmax_scale
        return jnp.where(allowed[None], scores, -1e+30)

    def attend(operands):
        query_seq, keys_seq, values_seq, segments = operands
        scores = score_block(query_seq, keys_seq, segments)
        highest = lax.optimization_barrier(jnp.max(scores, axis=-1, keepdims=True))
        log_total = highest + jnp.log(lax.optimization_barrier(jnp.sum(jnp.exp(scores - highest), axis=-1, keepdims=True)))
        attn_probs = rounded(jnp.exp(scores - log_total))
        attended = rounded(jnp.einsum('hqk,khd->qhd', attn_probs.astype(jnp.float32), values_seq.astype(jnp.float32)))
        return (attended, log_total)
    heads_out, log_totals = lax.map(attend, (queries, attn_keys, values, segment_ids))
    heads_flat = heads_out.reshape(tokens, H * VD)
    residual = stream + matmul(heads_flat, output_weight)
    scale_two = rms_scale(residual)
    normed_two = (residual * scale_two * second_gain).astype(jnp.bfloat16)
    logits = matmul(normed_two, router_weight)
    flat_routes = routes.reshape(tokens, TOPK)
    expert_ids = jnp.arange(experts)
    chosen = flat_routes[:, :, None] == expert_ids[None, None, :]
    picked = lax.optimization_barrier(jnp.sum(jnp.where(chosen, logits[:, None, :], 0.0), axis=-1))
    gate_probs = jax.nn.softmax(picked, axis=-1)
    shared_pre = matmul(normed_two, shared_gate)
    shared_lin = matmul(normed_two, shared_up)
    shared_act, shared_slope = silu_parts(shared_pre)
    shared_hidden = (shared_act * shared_lin).astype(jnp.bfloat16)
    shared_out = matmul(shared_hidden, shared_down)
    per_token = lax.optimization_barrier(jnp.sum(chosen.astype(jnp.int32), axis=1))
    earlier = jnp.cumsum(per_token, axis=0) - per_token
    slot_rank = lax.optimization_barrier(jnp.sum(jnp.where(chosen, earlier[:, None, :], 0), axis=-1)).astype(jnp.int32)
    capacity = N_ROW * N_COL * MOST
    token_ids = jnp.broadcast_to(jnp.arange(tokens, dtype=jnp.int32)[:, None], (tokens, TOPK))
    slot_table = jnp.full((experts, capacity), tokens, jnp.int32).at[flat_routes.reshape(-1), slot_rank.reshape(-1)].set(token_ids.reshape(-1))
    gate_table = jnp.zeros((tokens + 1, experts), jnp.float32).at[token_ids.reshape(-1), flat_routes.reshape(-1)].set(gate_probs.reshape(-1))
    normed_pad = jnp.concatenate([normed_two, jnp.zeros((1, width), jnp.bfloat16)], axis=0)

    def expert_forward(operands):
        slot_rows, gate_block, up_block, down_block = operands
        rows_in = normed_pad[slot_rows]
        activated, derivative = silu_parts(matmul(rows_in, gate_block))
        hidden = (activated * matmul(rows_in, up_block)).astype(jnp.bfloat16)
        return rounded(matmul(hidden, down_block))
    expert_out = lax.map(expert_forward, (slot_table, expert_gate, expert_up, expert_down))
    chosen_out = expert_out[flat_routes, slot_rank]
    routed = jnp.zeros((tokens, width), jnp.float32)
    for pick_index in range(TOPK):
        routed = routed + gate_probs[:, pick_index, None] * chosen_out[:, pick_index].astype(jnp.float32)
    result = residual + shared_out + routed
    layer_out = result.astype(jnp.bfloat16).reshape(seq_count, length, width)
    grad_out = cotangent.reshape(tokens, width)
    gate_grad = jnp.stack([lax.optimization_barrier(jnp.sum(grad_out * chosen_out[:, pick_index].astype(jnp.float32), axis=-1)) for pick_index in range(TOPK)], axis=1)
    picked_grad = gate_probs * (gate_grad - lax.optimization_barrier(jnp.sum(gate_probs * gate_grad, axis=-1, keepdims=True)))
    logit_grad = lax.optimization_barrier(jnp.sum(jnp.where(chosen, picked_grad[:, :, None], 0.0), axis=1)).astype(jnp.bfloat16)
    router_grad = matmul(normed_two.T, logit_grad)
    grad_pad = jnp.concatenate([grad_out, jnp.zeros((1, width), jnp.float32)], axis=0)

    def expert_backward(operands):
        slot_rows, column, gate_block, up_block, down_block = operands
        rows_in = normed_pad[slot_rows]
        gate_pre = matmul(rows_in, gate_block)
        up_lin = matmul(rows_in, up_block)
        activated, derivative = silu_parts(gate_pre)
        hidden = (activated * up_lin).astype(jnp.bfloat16)
        scaled_grad = (gate_table[slot_rows, column][:, None] * grad_pad[slot_rows]).astype(jnp.bfloat16)
        hidden_grad = matmul(scaled_grad, down_block.T)
        down_wgrad = matmul(hidden.T, scaled_grad)
        pre_grad = (hidden_grad * up_lin * derivative).astype(jnp.bfloat16)
        lin_grad = (hidden_grad * activated).astype(jnp.bfloat16)
        gate_wgrad = matmul(rows_in.T, pre_grad)
        up_wgrad = matmul(rows_in.T, lin_grad)
        rows_grad = rounded(matmul(pre_grad, gate_block.T) + matmul(lin_grad, up_block.T))
        return (gate_wgrad, up_wgrad, down_wgrad, rows_grad)
    expert_gate_grad, expert_up_grad, expert_down_grad, slot_grads = lax.map(expert_backward, (slot_table, jnp.arange(experts), expert_gate, expert_up, expert_down))
    chosen_grad = slot_grads[flat_routes, slot_rank]
    normed_two_grad = matmul(logit_grad, router_weight.T)
    for pick_index in range(TOPK):
        normed_two_grad = normed_two_grad + chosen_grad[:, pick_index].astype(jnp.float32)
    grad_b16 = grad_out.astype(jnp.bfloat16)
    shared_down_grad = matmul(shared_hidden.T, grad_b16)
    shared_hidden_grad = matmul(grad_b16, shared_down.T)
    shared_pre_grad = (shared_hidden_grad * shared_lin * shared_slope).astype(jnp.bfloat16)
    shared_lin_grad = (shared_hidden_grad * shared_act).astype(jnp.bfloat16)
    shared_gate_grad = matmul(normed_two.T, shared_pre_grad)
    shared_up_grad = matmul(normed_two.T, shared_lin_grad)
    normed_two_grad = normed_two_grad + matmul(shared_pre_grad, shared_gate.T) + matmul(shared_lin_grad, shared_up.T)
    second_gain_grad = lax.optimization_barrier(jnp.sum(normed_two_grad * residual * scale_two, axis=0))
    residual_grad = grad_out + rms_back(residual, scale_two, normed_two_grad * second_gain)
    attn_grad = residual_grad.astype(jnp.bfloat16)
    output_grad = matmul(heads_flat.T, attn_grad)
    heads_grad = rounded(matmul(attn_grad, output_weight.T)).reshape(seq_count, length, H, VD)

    def attend_back(operands):
        query_seq, keys_seq, values_seq, segments, attended, log_total, upstream = operands
        scores = score_block(query_seq, keys_seq, segments)
        recomputed = jnp.exp(scores - log_total)
        upstream_f = upstream.astype(jnp.float32)
        delta_rows = lax.optimization_barrier(jnp.sum(upstream_f * attended.astype(jnp.float32), axis=-1))
        prob_grad = jnp.einsum('qhd,khd->hqk', upstream_f, values_seq.astype(jnp.float32))
        score_grad = rounded(recomputed * (prob_grad - delta_rows.T[:, :, None]) * softmax_scale).astype(jnp.float32)
        queries_grad = jnp.einsum('hqk,khd->qhd', score_grad, keys_seq.astype(jnp.float32))
        key_grad = jnp.einsum('hqk,qhd->khd', score_grad, query_seq.astype(jnp.float32))
        value_grad = jnp.einsum('hqk,qhd->khd', rounded(recomputed).astype(jnp.float32), upstream_f)
        return (queries_grad, key_grad, value_grad)
    queries_grad, key_grad, value_grad = lax.map(attend_back, (queries, attn_keys, values, segment_ids, heads_out, log_totals, heads_grad))
    query_full = jnp.concatenate([queries_grad[..., :NOPE], unrotate(queries_grad[..., NOPE:], cosine_table[:, None, :], sine_table[:, None, :])], axis=-1).astype(jnp.bfloat16).reshape(tokens, H * qk_dim)
    query_grad = matmul(normed_one.T, query_full)
    keyval_grad = jnp.concatenate([key_grad[..., :NOPE], value_grad], axis=-1).astype(jnp.bfloat16).reshape(tokens, H * (NOPE + VD))
    latent_up_grad = matmul(latent_normed.T, keyval_grad)
    latent_normed_grad = matmul(keyval_grad, latent_up.T)
    latent_gain_grad = lax.optimization_barrier(jnp.sum(latent_normed_grad * latent * scale_latent, axis=0))
    rope_grad = unrotate(lax.optimization_barrier(jnp.sum(key_grad[..., NOPE:], axis=2)), cosine_table, sine_table).reshape(tokens, ROPE)
    latent_grad = rms_back(latent, scale_latent, latent_normed_grad * latent_gain)
    down_grad_in = jnp.concatenate([latent_grad, rope_grad], axis=-1).astype(jnp.bfloat16)
    latent_down_grad = matmul(normed_one.T, down_grad_in)
    normed_one_grad = matmul(query_full, query_weight.T) + matmul(down_grad_in, latent_down.T)
    first_gain_grad = lax.optimization_barrier(jnp.sum(normed_one_grad * stream * scale_one, axis=0))
    input_grad = (residual_grad + rms_back(stream, scale_one, normed_one_grad * first_gain)).reshape(seq_count, length, width)
    return (layer_out, input_grad, first_gain_grad, query_grad, latent_down_grad, latent_gain_grad, latent_up_grad, output_grad, second_gain_grad, router_grad, shared_gate_grad, shared_up_grad, shared_down_grad, expert_gate_grad, expert_up_grad, expert_down_grad)
```

```python
import functools

import jax
import jax.numpy as jnp
from jax import lax
from jax.experimental import pallas as pl
from jax.experimental.pallas import tpu as pltpu
from jax.sharding import PartitionSpec as P

NOPE = 128
ROPE = 64
LATENT = 512
VD = 128
TOPK = 6


EPS = 1e-06
ROWS_CONTRACT = (((0,), (0,)), ((), ()))
COLS_CONTRACT = (((1,), (1,)), ((), ()))


def matmul(left_side, right_side):
    return jnp.dot(left_side, right_side, preferred_element_type=jnp.float32)


def inner_rows(left_side, right_side):
    return lax.dot_general(left_side, right_side, ROWS_CONTRACT, preferred_element_type=jnp.float32)


def outer_cols(left_side, right_side):
    return lax.dot_general(left_side, right_side, COLS_CONTRACT, preferred_element_type=jnp.float32)


def rms_scale(values):
    return lax.rsqrt(jnp.mean(values * values, axis=-1, keepdims=True) + EPS)


def rms_back(values, scaling, gradient):
    return scaling * gradient - values * scaling**3 * jnp.mean(
        gradient * values, axis=-1, keepdims=True
    )


def silu_parts(preact):
    logistic = jax.nn.sigmoid(preact)
    return (preact * logistic, logistic * (1.0 + preact * (1.0 - logistic)))


def angle_tables(length):
    halfway = ROPE // 2
    frequency = 10000.0 ** (-2.0 * jnp.arange(halfway, dtype=jnp.float32) / ROPE)
    angles = jnp.arange(length, dtype=jnp.float32)[:, None] * frequency[None, :]
    return (jnp.cos(angles), jnp.sin(angles))


def rotate(values, cosine_in, sine_in):
    halfway = values.shape[-1] // 2
    leading = values[..., :halfway]
    trailing = values[..., halfway:]
    return jnp.concatenate(
        [leading * cosine_in - trailing * sine_in, leading * sine_in + trailing * cosine_in],
        axis=-1,
    )


def unrotate(values, cosine_in, sine_in):
    halfway = values.shape[-1] // 2
    leading = values[..., :halfway]
    trailing = values[..., halfway:]
    return jnp.concatenate(
        [leading * cosine_in + trailing * sine_in, trailing * cosine_in - leading * sine_in],
        axis=-1,
    )


F32 = jnp.float32
BF16 = jnp.bfloat16
EVERY = ("col", "row")
VMEM_LIMIT = 63 * 1024 * 1024


def token_rows(values):
    return lax.all_gather(values, "row", axis=0, tiled=True)


def every_token(values):
    return lax.all_gather(values, EVERY, axis=0, tiled=True)


def row_total(partial_value):
    return lax.psum_scatter(
        partial_value.astype(BF16), "row", scatter_dimension=0, tiled=True
    ).astype(F32)


def every_total(partial_value):
    return lax.psum_scatter(partial_value, EVERY, scatter_dimension=0, tiled=True).astype(F32)


def col_gather(values):
    return lax.all_gather(values, "col", axis=0, tiled=True)


def col_total(partial_value, dim):
    return lax.psum_scatter(
        partial_value.astype(BF16), "col", scatter_dimension=dim, tiled=True
    ).astype(F32)


MESH_ID = pl.DeviceIdType.MESH


def places():
    row, col = lax.axis_index("row"), lax.axis_index("col")
    return row // 2, lax.rem(row, 2), col // 2, lax.rem(col, 2)


def to_place(wide, core, line, side):
    return {"row": wide * 2 + core, "col": line * 2 + side}


def greet(partners, everyone):
    barrier = pltpu.get_barrier_semaphore()
    if everyone:
        n_row, n_col = lax.axis_size("row"), lax.axis_size("col")
        total = n_row * n_col
        me = lax.axis_index("col") * n_row + lax.axis_index("row")

        @pl.loop(1, total)
        def _(step):
            other = lax.rem(me + step, total)
            pl.semaphore_signal(
                barrier,
                inc=1,
                device_id={"row": lax.rem(other, n_row), "col": other // n_row},
                device_id_type=MESH_ID,
            )

        pl.semaphore_wait(barrier, total - 1)
        return
    for there, partner in partners:

        @pl.when(there)
        def _(partner=partner):
            pl.semaphore_signal(barrier, inc=1, device_id=partner, device_id_type=MESH_ID)

    for there, partner in partners:

        @pl.when(there)
        def _():
            pl.semaphore_wait(barrier, 1)


def remote(src, dst, send_sem, recv_sem, partner):
    return pltpu.make_async_remote_copy(
        src_ref=src,
        dst_ref=dst,
        send_sem=send_sem,
        recv_sem=recv_sem,
        device_id=partner,
        device_id_type=MESH_ID,
    )


def small_exchange(small_ref, small_out, send_sem, recv_sem, personal):
    n_row = lax.axis_size("row")
    total = n_row * lax.axis_size("col")
    me = lax.axis_index("col") * n_row + lax.axis_index("row")

    def copy(other, slot):
        return remote(
            small_ref.at[other] if personal else small_ref,
            small_out.at[slot],
            send_sem.at[other],
            recv_sem.at[slot],
            {"row": lax.rem(other, n_row), "col": other // n_row},
        )

    def start():
        @pl.loop(1, total)
        def _(step):
            copy(lax.rem(me + step, total), me).start()

        small_out[me] = small_ref[me] if personal else small_ref[...]

    def finish():
        @pl.loop(1, total)
        def _(step):
            other = lax.rem(me + step, total)
            copy(other, other).wait_recv()
            copy(other, me).wait_send()

    return start, finish


def line_order(lines):
    order = []
    for step in range((lines + 1) // 2):
        order.append(step)
        if lines - 1 - step != step:
            order.append(lines - 1 - step)
    return order


def scatter_body(lines, count, small, *refs):
    bigs, refs = refs[:count], refs[count:]
    if small:
        small_ref, refs = refs[0], refs[1:]
    outs, refs = refs[:count], refs[count:]
    if small:
        small_out, refs = refs[0], refs[1:]
    own, core_in, wide_in, side_in, up_in, down_in = refs[:6]
    load_sem, core_send, core_recv, wide_send, wide_recv, side_send, side_recv = refs[6:13]
    up_send, up_recv, down_send, down_recv = refs[13:17]
    wide, core, line, side = places()
    tokens = own.shape[1]
    half = tokens // 2
    core_mate = to_place(wide, 1 - core, line, side)
    wide_mate = to_place(1 - wide, core, line, side)
    side_mate = to_place(wide, core, line, 1 - side)
    above = to_place(wide, core, line + 1, side)
    below = to_place(wide, core, line - 1, side)
    has_above = line < lines - 1
    has_below = line > 0
    greet(
        [
            (core >= 0, core_mate),
            (core >= 0, wide_mate),
            (core >= 0, side_mate),
            (has_above, above),
            (has_below, below),
        ],
        small,
    )
    parts = [pl.ds(0, half), pl.ds(half, half)]

    def at(a, l, s, w):
        return ((a * lines + l) * 2 + s) * 2 + w

    def core_copy(a, i):
        n = a * 4 * lines + i
        return remote(
            bigs[a].at[pl.ds((2 * i + 1 - core) * tokens, tokens)],
            core_in.at[n],
            core_send.at[n],
            core_recv.at[n],
            core_mate,
        )

    def load(a, i):
        n = a * 4 * lines + i
        return pltpu.make_async_copy(
            bigs[a].at[pl.ds((2 * i + core) * tokens, tokens)], own.at[n], load_sem.at[n]
        )

    def wide_one(a, l, s):
        n = (a * lines + l) * 3 + s
        return remote(
            own.at[at(a, l, s, 1 - wide), parts[0]],
            wide_in.at[n],
            wide_send.at[n],
            wide_recv.at[n],
            wide_mate,
        )

    def side_one(a, l, w):
        n = (a * lines + l) * 3 + w
        return remote(
            own.at[at(a, l, 1 - side, w), parts[1]],
            side_in.at[n],
            side_send.at[n],
            side_recv.at[n],
            side_mate,
        )

    def side_two(a, l):
        n = (a * lines + l) * 3 + 2
        return remote(
            own.at[at(a, l, 1 - side, wide), parts[0]],
            side_in.at[n],
            side_send.at[n],
            side_recv.at[n],
            side_mate,
        )

    def wide_two(a, l):
        n = (a * lines + l) * 3 + 2
        return remote(
            own.at[at(a, l, side, 1 - wide), parts[1]],
            wide_in.at[n],
            wide_send.at[n],
            wide_recv.at[n],
            wide_mate,
        )

    def up_copy(a, l, h):
        n = (a * lines + l) * 2 + h
        return remote(
            own.at[at(a, l, side, wide), parts[h]],
            up_in.at[n],
            up_send.at[n],
            up_recv.at[n],
            above,
        )

    def down_copy(a, l, h):
        n = (a * lines + l) * 2 + h
        return remote(
            own.at[at(a, l, side, wide), parts[h]],
            down_in.at[n],
            down_send.at[n],
            down_recv.at[n],
            below,
        )

    def add(i, rows, other):
        own[i, rows] = (own[i, rows].astype(F32) + other[...].astype(F32)).astype(BF16)

    items = [(a, l) for a in range(count) for l in line_order(lines)]
    for a, l in items:
        for j in range(4):
            core_copy(a, l * 4 + j).start()
            load(a, l * 4 + j).start()
    if small:
        small_start, small_finish = small_exchange(small_ref, small_out, *refs[17:19], True)
        small_start()

    def stage_one(a, l):
        for j in range(4):
            i = l * 4 + j
            load(a, i).wait()
            core_copy(a, i).wait_recv()
            add(a * 4 * lines + i, pl.ds(0, tokens), core_in.at[a * 4 * lines + i])
        for j in range(2):
            wide_one(a, l, j).start()
            side_one(a, l, j).start()

    def stage_two(a, l):
        n = (a * lines + l) * 3
        for j in range(2):
            s = 1 - side if j == 0 else side
            wide_one(a, l, s).wait_recv()
            add(at(a, l, s, wide), parts[0], wide_in.at[n + s])
            if j == 0:
                side_two(a, l).start()
            w = 1 - wide if j == 0 else wide
            side_one(a, l, w).wait_recv()
            add(at(a, l, side, w), parts[1], side_in.at[n + w])
            if j == 0:
                wide_two(a, l).start()

    def stage_three(a, l):
        n = (a * lines + l) * 3 + 2
        i = at(a, l, side, wide)
        for h in range(2):
            if h == 0:
                side_two(a, l).wait_recv()
                add(i, parts[0], side_in.at[n])
            else:
                wide_two(a, l).wait_recv()
                add(i, parts[1], wide_in.at[n])

            @pl.when(jnp.logical_and(line == 0, l > 0))
            def _(h=h):
                up_copy(a, l, h).start()

            @pl.when(jnp.logical_and(line == lines - 1, l < lines - 1))
            def _(h=h):
                down_copy(a, l, h).start()

    def stage_four(a, l):
        i = at(a, l, side, wide)
        for h in range(2):

            @pl.when(jnp.logical_and(has_below, line <= l))
            def _(h=h):
                up_copy(a, l, h).wait_recv()
                add(i, parts[h], up_in.at[(a * lines + l) * 2 + h])

            @pl.when(jnp.logical_and(has_above, line >= l))
            def _(h=h):
                down_copy(a, l, h).wait_recv()
                add(i, parts[h], down_in.at[(a * lines + l) * 2 + h])

            @pl.when(jnp.logical_and(jnp.logical_and(has_below, has_above), line < l))
            def _(h=h):
                up_copy(a, l, h).start()

            @pl.when(jnp.logical_and(jnp.logical_and(has_below, has_above), line > l))
            def _(h=h):
                down_copy(a, l, h).start()

    for step in range(len(items) + 3):
        if step < len(items):
            stage_one(*items[step])
        if 0 <= step - 1 < len(items):
            stage_two(*items[step - 1])
        if 0 <= step - 2 < len(items):
            stage_three(*items[step - 2])
        if 0 <= step - 3 < len(items):
            stage_four(*items[step - 3])
    for a in range(count):
        outs[a][...] = own[at(a, line, side, wide)].astype(F32)
    if small:
        small_finish()
    for a, l in items:
        for j in range(4):
            core_copy(a, l * 4 + j).wait_send()
        for j in range(2):
            wide_one(a, l, j).wait_send()
            side_one(a, l, j).wait_send()
        side_two(a, l).wait_send()
        wide_two(a, l).wait_send()
        for h in range(2):

            @pl.when(jnp.logical_and(has_above, line < l))
            def _(h=h):
                up_copy(a, l, h).wait_send()

            @pl.when(jnp.logical_and(has_below, line > l))
            def _(h=h):
                down_copy(a, l, h).wait_send()


def kernel_total(partials, small_value, number):
    n_row, n_col = lax.axis_size("row"), lax.axis_size("col")
    lines, count = n_col // 2, len(partials)
    width = partials[0].shape[1]
    tokens = partials[0].shape[0] // (n_row * n_col)
    small = small_value is not None
    out_shape = [jax.ShapeDtypeStruct((tokens, width), F32)] * count
    in_specs = [pl.BlockSpec(memory_space=pl.ANY)] * count
    operands = list(partials)
    if small:
        in_specs.append(pl.BlockSpec(memory_space=pltpu.VMEM))
        out_shape.append(jax.ShapeDtypeStruct(small_value.shape, small_value.dtype))
        operands.append(small_value)
    dma = pltpu.SemaphoreType.DMA
    scratch = [
        pltpu.VMEM((count * 4 * lines, tokens, width), BF16),
        pltpu.VMEM((count * 4 * lines, tokens, width), BF16),
        pltpu.VMEM((count * 3 * lines, tokens // 2, width), BF16),
        pltpu.VMEM((count * 3 * lines, tokens // 2, width), BF16),
        pltpu.VMEM((count * 2 * lines, tokens // 2, width), BF16),
        pltpu.VMEM((count * 2 * lines, tokens // 2, width), BF16),
        *[dma((count * 4 * lines,))] * 3,
        *[dma((count * 3 * lines,))] * 4,
        *[dma((count * 2 * lines,))] * 4,
    ]
    if small:
        scratch += [dma((n_row * n_col,))] * 2
    return pl.pallas_call(
        functools.partial(scatter_body, lines, count, small),
        out_shape=out_shape,
        in_specs=in_specs,
        out_specs=[pl.BlockSpec(memory_space=pltpu.VMEM)] * len(out_shape),
        scratch_shapes=scratch,
        compiler_params=pltpu.CompilerParams(
            collective_id=number, has_side_effects=True, vmem_limit_bytes=VMEM_LIMIT
        ),
        name=f"scatter_{number}",
    )(*operands)


def gather_body(lines, small, *refs):
    own_ref, refs = refs[0], refs[1:]
    if small:
        small_ref, refs = refs[0], refs[1:]
    out_ref, refs = refs[0], refs[1:]
    if small:
        small_out, refs = refs[0], refs[1:]
    local_sem, core_send, core_recv, wide_send, wide_recv, side_send, side_recv = refs[:7]
    up_send, up_recv, down_send, down_recv = refs[7:11]
    wide, core, line, side = places()
    tokens = own_ref.shape[0]
    half = tokens // 2
    core_mate = to_place(wide, 1 - core, line, side)
    wide_mate = to_place(1 - wide, core, line, side)
    side_mate = to_place(wide, core, line, 1 - side)
    above = to_place(wide, core, line + 1, side)
    below = to_place(wide, core, line - 1, side)
    has_above = line < lines - 1
    has_below = line > 0
    greet(
        [
            (core >= 0, core_mate),
            (core >= 0, wide_mate),
            (core >= 0, side_mate),
            (has_above, above),
            (has_below, below),
        ],
        small,
    )

    def spot(l, s, w, k, h):
        return out_ref.at[pl.ds((((l * 2 + s) * 2 + w) * 2 + k) * tokens + h * half, half)]

    def source(l, s, w, h, here):
        return own_ref.at[pl.ds(h * half, half)] if here else spot(l, s, w, core, h)

    def core_copy(l, s, w, h, here=False):
        n = ((l * 2 + s) * 2 + w) * 2 + h
        return remote(
            source(l, s, w, h, here),
            spot(l, s, w, core, h),
            core_send.at[n],
            core_recv.at[n],
            core_mate,
        )

    def wide_copy(l, s, h, here=False):
        n = l * 3 + (2 if h else s)
        return remote(
            source(l, s, wide, h, here),
            spot(l, s, wide, core, h),
            wide_send.at[n],
            wide_recv.at[n],
            wide_mate,
        )

    def side_copy(l, w, h, here=False):
        n = l * 3 + (w if h else 2)
        return remote(
            source(l, side, w, h, here),
            spot(l, side, w, core, h),
            side_send.at[n],
            side_recv.at[n],
            side_mate,
        )

    def up_copy(l, h, here=False):
        n = l * 2 + h
        return remote(
            source(l, side, wide, h, here),
            spot(l, side, wide, core, h),
            up_send.at[n],
            up_recv.at[n],
            above,
        )

    def down_copy(l, h, here=False):
        n = l * 2 + h
        return remote(
            source(l, side, wide, h, here),
            spot(l, side, wide, core, h),
            down_send.at[n],
            down_recv.at[n],
            below,
        )

    def local(h):
        return pltpu.make_async_copy(
            own_ref.at[pl.ds(h * half, half)], spot(line, side, wide, core, h), local_sem.at[h]
        )

    def spread(l, h, here=False):
        if h == 0:
            side_copy(l, wide, 0, here).start()
            wide_copy(l, side, 0, here).start()
        else:
            wide_copy(l, side, 1, here).start()
            side_copy(l, wide, 1, here).start()
        core_copy(l, side, wide, h, here).start()

    def second(l):
        side_copy(l, wide, 0).wait_recv()
        wide_copy(l, 1 - side, 0).start()
        core_copy(l, 1 - side, wide, 0).start()
        wide_copy(l, side, 1).wait_recv()
        side_copy(l, 1 - wide, 1).start()
        core_copy(l, side, 1 - wide, 1).start()

    def third(l):
        for j in range(2):
            s = 1 - side if j else side
            wide_copy(l, s, 0).wait_recv()
            core_copy(l, s, 1 - wide, 0).start()
            w = 1 - wide if j else wide
            side_copy(l, w, 1).wait_recv()
            core_copy(l, 1 - side, w, 1).start()

    for h in range(2):

        @pl.when(has_above)
        def _(h=h):
            up_copy(line, h, True).start()

        @pl.when(has_below)
        def _(h=h):
            down_copy(line, h, True).start()

        spread(line, h, True)
    if small:
        small_start, small_finish = small_exchange(small_ref, small_out, *refs[11:13], False)
        small_start()
    for h in range(2):
        local(h).start()

    def from_line(dist, up):
        l = line - dist if up else line + dist
        there = l >= 0 if up else l < lines
        further = has_above if up else has_below
        copy = up_copy if up else down_copy

        @pl.when(there)
        def _():
            for h in range(2):
                copy(l, h).wait_recv()

                @pl.when(further)
                def _(h=h):
                    copy(l, h).start()

                spread(l, h)

    def stage(action, dist):
        if dist == 0:
            action(line)
            return

        @pl.when(line - dist >= 0)
        def _():
            action(line - dist)

        @pl.when(line + dist < lines)
        def _():
            action(line + dist)

    for dist in range(1, lines + 2):
        if dist < lines:
            from_line(dist, True)
            from_line(dist, False)
        if dist - 1 < lines:
            stage(second, dist - 1)
        if 0 <= dist - 2 < lines:
            stage(third, dist - 2)
    if small:
        small_finish()
    for h in range(2):
        local(h).wait()
    for l in range(lines):
        for s in range(2):
            for w in range(2):
                for h in range(2):
                    core_copy(l, s, w, h).wait_recv()
                    core_copy(l, s, w, h).wait_send()
        for j in range(2):
            wide_copy(l, j, 0).wait_send()
            side_copy(l, j, 1).wait_send()
        wide_copy(l, side, 1).wait_send()
        side_copy(l, wide, 0).wait_send()
        for h in range(2):

            @pl.when(jnp.logical_and(has_above, line >= l))
            def _(h=h):
                up_copy(l, h).wait_send()

            @pl.when(jnp.logical_and(has_below, line <= l))
            def _(h=h):
                down_copy(l, h).wait_send()


def kernel_gather(own, small_value, number):
    n_row, n_col = lax.axis_size("row"), lax.axis_size("col")
    lines, total = n_col // 2, n_row * n_col
    tokens, width = own.shape
    small = small_value is not None
    out_shape = [jax.ShapeDtypeStruct((total * tokens, width), own.dtype)]
    in_specs = [pl.BlockSpec(memory_space=pltpu.VMEM)]
    out_specs = [pl.BlockSpec(memory_space=pl.ANY)]
    operands = [own]
    if small:
        in_specs.append(pl.BlockSpec(memory_space=pltpu.VMEM))
        out_specs.append(pl.BlockSpec(memory_space=pltpu.VMEM))
        out_shape.append(jax.ShapeDtypeStruct((total, *small_value.shape), small_value.dtype))
        operands.append(small_value)
    dma = pltpu.SemaphoreType.DMA
    scratch = [
        dma((2,)),
        *[dma((8 * lines,))] * 2,
        *[dma((3 * lines,))] * 4,
        *[dma((2 * lines,))] * 4,
    ]
    if small:
        scratch += [dma((total,))] * 2
    return pl.pallas_call(
        functools.partial(gather_body, lines, small),
        out_shape=out_shape,
        in_specs=in_specs,
        out_specs=out_specs,
        scratch_shapes=scratch,
        compiler_params=pltpu.CompilerParams(collective_id=number, has_side_effects=True),
        name=f"gather_{number}",
    )(*operands)


def kernel_fits(rows, width, count):
    n_row, n_col = lax.axis_size("row"), lax.axis_size("col")
    tokens = rows // (n_row * n_col)
    held = count * n_col * 2 * width * tokens * 13 // 4
    return n_row == 4 and n_col % 2 == 0 and tokens % 32 == 0 and held < 58 * 1024 * 1024


def small_body(personal, value_ref, out_ref, send_sem, recv_sem):
    greet([], True)
    start, finish = small_exchange(value_ref, out_ref, send_sem, recv_sem, personal)
    start()
    finish()


def kernel_small(value, personal, number):
    total = lax.axis_size("row") * lax.axis_size("col")
    shape = value.shape if personal else (total, *value.shape)
    dma = pltpu.SemaphoreType.DMA
    return pl.pallas_call(
        functools.partial(small_body, personal),
        out_shape=jax.ShapeDtypeStruct(shape, value.dtype),
        in_specs=[pl.BlockSpec(memory_space=pltpu.VMEM)],
        out_specs=pl.BlockSpec(memory_space=pltpu.VMEM),
        scratch_shapes=[dma((total,)), dma((total,))],
        compiler_params=pltpu.CompilerParams(collective_id=number, has_side_effects=True),
        name=f"small_{number}",
    )(value)


def gather_every(own, small_value, number):
    total = lax.axis_size("row") * lax.axis_size("col")
    if kernel_fits(total * own.shape[0], own.shape[1], 1):
        return kernel_gather(own, small_value, number)
    return every_token(own), every_token(small_value[None])


def total_every(partials, small_value, number):
    if kernel_fits(partials[0].shape[0], partials[0].shape[1], len(partials)):
        return kernel_total(partials, small_value, number)
    exchanged = lax.all_to_all(small_value, EVERY, split_axis=0, concat_axis=0, tiled=True)
    return *[every_total(p) for p in partials], exchanged


def padded_rows(values):
    return jnp.pad(values, ((0, -values.shape[0] % 8), (0, 0)))


def masked_scores(queries, attn_keys, allowed, softmax_scale):
    scores = (
        jnp.einsum("qhd,khd->hqk", queries, attn_keys, preferred_element_type=jnp.float32)
        * softmax_scale
    )
    return jnp.where(allowed[None], scores, -1e30)


def select_body(group, capacity, place_ref, rows_ref, slots_ref):
    tokens = place_ref.shape[2]
    for block in range(group):
        picked = matmul(place_ref[block], rows_ref[block * tokens : (block + 1) * tokens, :])
        slots_ref[:, block] = picked.astype(BF16).reshape(-1, capacity, picked.shape[-1])


def select_rows(place, rows, capacity):
    blocks, slots, tokens = place.shape
    width = rows.shape[1]
    local_experts = slots // capacity
    group = 4 if blocks % 4 == 0 else 1
    out = pl.pallas_call(
        functools.partial(select_body, group, capacity),
        grid=(blocks // group,),
        in_specs=[
            pl.BlockSpec((group, slots, tokens), lambda i: (i, 0, 0)),
            pl.BlockSpec((group * tokens, width), lambda i: (i, 0)),
        ],
        out_specs=pl.BlockSpec((local_experts, group, capacity, width), lambda i: (0, i, 0, 0)),
        out_shape=jax.ShapeDtypeStruct((local_experts, blocks, capacity, width), BF16),
        compiler_params=pltpu.CompilerParams(vmem_limit_bytes=VMEM_LIMIT),
        cost_estimate=pl.CostEstimate(
            flops=2 * blocks * slots * tokens * width,
            bytes_accessed=4 * blocks * tokens * width,
            transcendentals=0,
        ),
        name="select_rows",
    )(place, rows)
    return out.reshape(local_experts, blocks * capacity, width)


def experts_body(
    x_ref, g_ref, gate_ref, wg_ref, wu_ref, wd_ref, y_ref, r_ref, dg_ref, du_ref, dd_ref, gg_ref
):
    first = pl.program_id(1) == 0
    x = x_ref[0]
    g = g_ref[0]
    gate = gate_ref[0]
    pre = outer_cols(x, wg_ref[0])
    lin = outer_cols(x, wu_ref[0])
    back = outer_cols(g, wd_ref[0])
    act, slope = silu_parts(pre)
    hidden = act * lin
    gg_ref[0] = jnp.sum(hidden * back, axis=-1, keepdims=True)
    hidden = (hidden * gate).astype(BF16)
    back = back * gate
    pre_grad = (back * lin * slope).astype(BF16)
    lin_grad = (back * act).astype(BF16)
    width = x_ref.shape[2]
    chunk = 512 if width % 512 == 0 else width
    for start in range(0, width, chunk):
        cols = slice(start, start + chunk)
        y_ref[0, :, cols] = matmul(hidden, wd_ref[0, :, cols]).astype(BF16)
        r_ref[0, :, cols] = (
            matmul(pre_grad, wg_ref[0, :, cols]) + matmul(lin_grad, wu_ref[0, :, cols])
        ).astype(BF16)
        d_gate = inner_rows(pre_grad, x_ref[0, :, cols])
        d_up = inner_rows(lin_grad, x_ref[0, :, cols])
        d_down = inner_rows(hidden, g_ref[0, :, cols])

        @pl.when(first)
        def _():
            dg_ref[0, :, cols] = d_gate
            du_ref[0, :, cols] = d_up
            dd_ref[0, :, cols] = d_down

        @pl.when(jnp.logical_not(first))
        def _():
            dg_ref[0, :, cols] += d_gate
            du_ref[0, :, cols] += d_up
            dd_ref[0, :, cols] += d_down


def run_experts(x_slots, g_slots, gates, w_gate, w_up, w_down):
    count, rows, width = x_slots.shape
    hidden = w_down.shape[1]
    chunk = 512 if rows % 512 == 0 else rows
    row_block = pl.BlockSpec((1, chunk, width), lambda e, r: (e, r, 0))
    col_block = pl.BlockSpec((1, chunk, 1), lambda e, r: (e, r, 0))
    out_block = pl.BlockSpec((1, hidden, width), lambda e, r: (e, 0, 0))
    y, r, d_gate, d_up, d_down, dots = pl.pallas_call(
        experts_body,
        grid=(count, rows // chunk),
        in_specs=[row_block, row_block, col_block, out_block, out_block, out_block],
        out_specs=[row_block, row_block, out_block, out_block, out_block, col_block],
        out_shape=[
            jax.ShapeDtypeStruct((count, rows, width), BF16),
            jax.ShapeDtypeStruct((count, rows, width), BF16),
            jax.ShapeDtypeStruct((count, hidden, width), F32),
            jax.ShapeDtypeStruct((count, hidden, width), F32),
            jax.ShapeDtypeStruct((count, hidden, width), F32),
            jax.ShapeDtypeStruct((count, rows, 1), F32),
        ],
        compiler_params=pltpu.CompilerParams(vmem_limit_bytes=VMEM_LIMIT),
        cost_estimate=pl.CostEstimate(
            flops=18 * count * rows * width * hidden,
            bytes_accessed=count * (8 * rows * width + 18 * width * hidden),
            transcendentals=count * rows * hidden,
        ),
        name="run_experts",
    )(x_slots, g_slots, gates, w_gate.transpose(0, 2, 1), w_up.transpose(0, 2, 1), w_down)
    return y, r, d_gate.transpose(0, 2, 1), d_up.transpose(0, 2, 1), d_down, dots


def combine_body(group, place_ref, slots_ref, extra_ref, weight_ref, out_ref):
    tokens = place_ref.shape[2]
    width = out_ref.shape[1]
    for block in range(group):
        rows = slice(block * tokens, (block + 1) * tokens)
        total = inner_rows(place_ref[block], slots_ref[:, block].reshape(-1, width))
        total += matmul(extra_ref[rows, :], weight_ref[...])
        out_ref[rows, :] = total.astype(BF16)


def combine_rows(place, slots, extra, weight, capacity):
    blocks, slot_count, tokens = place.shape
    local_experts, _, width = slots.shape
    group = 4 if blocks % 4 == 0 else 1
    inner = extra.shape[1]
    return pl.pallas_call(
        functools.partial(combine_body, group),
        grid=(blocks // group,),
        in_specs=[
            pl.BlockSpec((group, slot_count, tokens), lambda i: (i, 0, 0)),
            pl.BlockSpec((local_experts, group, capacity, width), lambda i: (0, i, 0, 0)),
            pl.BlockSpec((group * tokens, inner), lambda i: (i, 0)),
            pl.BlockSpec((inner, width), lambda i: (0, 0)),
        ],
        out_specs=pl.BlockSpec((group * tokens, width), lambda i: (i, 0)),
        out_shape=jax.ShapeDtypeStruct((blocks * tokens, width), BF16),
        compiler_params=pltpu.CompilerParams(vmem_limit_bytes=VMEM_LIMIT),
        cost_estimate=pl.CostEstimate(
            flops=2 * blocks * tokens * (slot_count + inner) * width,
            bytes_accessed=4 * blocks * tokens * width,
            transcendentals=0,
        ),
        name="combine_rows",
    )(place, slots.reshape(local_experts, blocks, capacity, width), extra, weight)


def on_device(
    inputs,
    segment_ids,
    routes,
    first_gain,
    query_weight,
    latent_down,
    latent_gain,
    latent_up,
    output_weight,
    second_gain,
    router_weight,
    shared_gate,
    shared_up,
    shared_down,
    expert_gate,
    expert_up,
    expert_down,
    cotangent,
):
    n_row = lax.axis_size("row")
    n_col = lax.axis_size("col")
    blocks = n_row * n_col
    own_row = lax.axis_index("row")
    own_col = lax.axis_index("col")
    own_rows = inputs.shape[1]
    width = inputs.shape[2]
    experts = router_weight.shape[1]
    local_experts = expert_gate.shape[0]
    capacity = max(2, own_rows // 8)
    stream = inputs.reshape(own_rows, width).astype(F32)
    grad_out = cotangent.reshape(own_rows, width)
    own_routes = routes.reshape(own_rows, TOPK)
    segments = segment_ids.reshape(-1)
    length = segments.shape[0]
    own_start = own_row * own_rows
    qk_dim = NOPE + ROPE
    softmax_scale = qk_dim ** (-0.5)
    cosine_table, sine_table = angle_tables(length)

    scale_one = rms_scale(stream)
    normed_one = (stream * scale_one * first_gain).astype(BF16)
    seq_normed = token_rows(normed_one)
    down_cols = latent_down.shape[1] // n_row
    own_down = lax.dynamic_slice_in_dim(latent_down, own_row * down_cols, down_cols, 1)
    query_cols = query_weight.shape[1]
    query_down = col_gather(jnp.concatenate([query_weight, own_down], axis=1))
    query_all = query_down[:, :query_cols]
    down_all = query_down[:, query_cols:]
    expand_all = col_gather(latent_up)
    output_all = lax.all_gather(output_weight, "col", axis=1, tiled=True)

    all_routes = kernel_small(padded_rows(own_routes.astype(F32).T), False, 1)
    all_routes = all_routes[:, :TOPK].astype(jnp.int32)
    grad_all = every_token(grad_out.astype(BF16))
    local_ids = own_col * local_experts + jnp.arange(local_experts)
    named = all_routes[:, :, None, :] == local_ids[None, None, :, None]
    chosen_here = jnp.max(named.astype(BF16), axis=1)
    before = (jnp.arange(own_rows)[:, None] < jnp.arange(own_rows)[None, :]).astype(BF16)
    rank = matmul(chosen_here.reshape(-1, own_rows), before).reshape(chosen_here.shape)
    slot_of = jnp.where(chosen_here > 0, rank.astype(jnp.int32), -1)
    placed = slot_of[:, :, None, :] == jnp.arange(capacity)[None, None, :, None]
    place = placed.astype(BF16).reshape(blocks, local_experts * capacity, own_rows)
    grad_slots = select_rows(place, grad_all, capacity)

    shared_cols = shared_gate.shape[1] // n_col
    shared_send = jnp.stack([shared_gate.T, shared_up.T, shared_down], axis=0)
    depth = shared_send.shape[2]
    shared_send = (
        shared_send.reshape(3, n_col, shared_cols, depth)
        .transpose(1, 0, 2, 3)
        .reshape(n_col, 3 * shared_cols, depth)
    )
    shared_own = (
        lax.all_to_all(shared_send, "col", split_axis=0, concat_axis=0, tiled=True)
        .transpose(1, 0, 2)
        .reshape(3, shared_cols, width)
    )
    gate_up_own = shared_own[:2].reshape(2 * shared_cols, width)
    down_own = shared_own[2]

    heads_local = query_cols // qk_dim
    query_raw = matmul(seq_normed, query_all).reshape(length, heads_local, qk_dim)
    queries = jnp.concatenate(
        [
            query_raw[..., :NOPE],
            rotate(query_raw[..., NOPE:], cosine_table[:, None, :], sine_table[:, None, :]),
        ],
        axis=-1,
    ).astype(BF16)
    latent_all = lax.all_gather(matmul(seq_normed, down_all), "row", axis=1, tiled=True)
    latent = latent_all[:, :LATENT]
    scale_latent = rms_scale(latent)
    latent_normed = (latent * scale_latent * latent_gain).astype(BF16)
    keyval = matmul(latent_normed, expand_all).reshape(length, heads_local, NOPE + VD)
    key_rope = rotate(latent_all[:, LATENT:], cosine_table, sine_table)
    attn_keys = jnp.concatenate(
        [keyval[..., :NOPE], jnp.broadcast_to(key_rope[:, None, :], (length, heads_local, ROPE))],
        axis=-1,
    ).astype(BF16)
    values = keyval[..., NOPE:].astype(BF16)
    positions = jnp.arange(length)
    allowed = (positions[:, None] >= positions[None, :]) & (segments[:, None] == segments[None, :])
    scores = masked_scores(queries, attn_keys, allowed, softmax_scale)
    highest = jnp.max(scores, axis=-1, keepdims=True)
    log_total = highest + jnp.log(jnp.sum(jnp.exp(scores - highest), axis=-1, keepdims=True))
    attn_probs = jnp.exp(scores - log_total).astype(BF16)
    heads_out = (
        jnp.einsum("hqk,khd->qhd", attn_probs, values, preferred_element_type=jnp.float32)
        .astype(BF16)
        .reshape(length, heads_local * VD)
    )
    residual = stream + row_total(matmul(heads_out, output_all))

    scale_two = rms_scale(residual)
    normed_two = (residual * scale_two * second_gain).astype(BF16)
    logits = matmul(normed_two, router_weight)
    expert_ids = jnp.arange(experts)
    chosen = own_routes[:, :, None] == expert_ids[None, None, :]
    picked = jnp.sum(jnp.where(chosen, logits[:, None, :], 0.0), axis=-1)
    gate_probs = jax.nn.softmax(picked, axis=-1)

    all_normed, all_gates = gather_every(normed_two, padded_rows(gate_probs.T), 2)
    all_gates = all_gates[:, :TOPK]
    gate_here = jnp.sum(jnp.where(named, all_gates[:, :, None, :], 0.0), axis=1)
    slot_gate = jnp.sum(jnp.where(placed, gate_here[:, :, None, :], 0.0), axis=-1)
    slot_gate = slot_gate.transpose(1, 0, 2).reshape(local_experts, blocks * capacity, 1)
    normed_slots = select_rows(place, all_normed, capacity)
    out_slots, rows_slots, expert_gate_grad, expert_up_grad, expert_down_grad, slot_dot = (
        run_experts(normed_slots, grad_slots, slot_gate, expert_gate, expert_up, expert_down)
    )

    shared_both = outer_cols(all_normed, gate_up_own)
    shared_act, shared_slope = silu_parts(shared_both[:, :shared_cols])
    shared_lin = shared_both[:, shared_cols:]
    shared_hidden = (shared_act * shared_lin).astype(BF16)
    shared_hidden_grad = outer_cols(grad_all, down_own)
    shared_both_grad = jnp.concatenate(
        [
            (shared_hidden_grad * shared_lin * shared_slope).astype(BF16),
            (shared_hidden_grad * shared_act).astype(BF16),
        ],
        axis=1,
    )
    slot_dot = slot_dot.reshape(local_experts, blocks, capacity).transpose(1, 0, 2)
    token_dot = jnp.sum(jnp.where(placed, slot_dot[:, :, :, None], 0.0), axis=2)
    out_total, rows_total, token_dot = total_every(
        [
            combine_rows(place, out_slots, shared_hidden, down_own, capacity),
            combine_rows(place, rows_slots, shared_both_grad, gate_up_own, capacity),
        ],
        token_dot,
        3,
    )
    layer_out = (residual + out_total).astype(BF16).reshape(1, own_rows, width)
    gate_up_part = inner_rows(shared_both_grad, all_normed)
    down_part = inner_rows(shared_hidden, grad_all)
    shared_back = jnp.concatenate([gate_up_part, down_part], axis=0).astype(BF16)
    shared_back = (
        shared_back.reshape(3 * shared_cols, n_col, depth).transpose(1, 0, 2)
    )
    shared_back = lax.all_to_all(shared_back, "col", split_axis=0, concat_axis=0, tiled=True)
    shared_back = (
        shared_back.reshape(n_col, 3, shared_cols, depth)
        .transpose(1, 0, 2, 3)
        .reshape(3, n_col * shared_cols, depth)
        .astype(F32)
    )
    shared_gate_grad = shared_back[0].T
    shared_up_grad = shared_back[1].T
    shared_down_grad = shared_back[2]

    token_dot = jnp.sum(token_dot.reshape(n_col, n_row, local_experts, own_rows), axis=1)
    token_dot = token_dot.reshape(experts, own_rows).T
    gate_grad = jnp.sum(jnp.where(chosen, token_dot[:, None, :], 0.0), axis=-1)
    picked_grad = gate_probs * (gate_grad - jnp.sum(gate_probs * gate_grad, axis=-1, keepdims=True))
    logit_grad = jnp.sum(jnp.where(chosen, picked_grad[:, :, None], 0.0), axis=1).astype(BF16)
    all_logit_grad = kernel_small(logit_grad, False, 4).reshape(-1, experts)
    router_grad = inner_rows(all_normed, all_logit_grad)

    normed_two_grad = rows_total + outer_cols(logit_grad, router_weight)
    second_gain_part = jnp.sum(normed_two_grad * residual * scale_two, axis=0)
    residual_grad = grad_out + rms_back(residual, scale_two, normed_two_grad * second_gain)

    seq_resid = token_rows(residual_grad.astype(BF16))
    output_part = inner_rows(heads_out, seq_resid)
    heads_grad = outer_cols(seq_resid, output_all).astype(BF16).reshape(length, heads_local, VD)
    recomputed = jnp.exp(masked_scores(queries, attn_keys, allowed, softmax_scale) - log_total)
    delta_rows = jnp.sum(
        heads_grad.astype(F32) * heads_out.reshape(length, heads_local, VD).astype(F32),
        axis=-1,
    )
    prob_grad = jnp.einsum("qhd,khd->hqk", heads_grad, values, preferred_element_type=jnp.float32)
    score_grad = (recomputed * (prob_grad - delta_rows.T[:, :, None]) * softmax_scale).astype(BF16)
    queries_grad = jnp.einsum(
        "hqk,khd->qhd", score_grad, attn_keys, preferred_element_type=jnp.float32
    )
    key_grad = jnp.einsum("hqk,qhd->khd", score_grad, queries, preferred_element_type=jnp.float32)
    value_grad = jnp.einsum(
        "hqk,qhd->khd",
        recomputed.astype(BF16),
        heads_grad,
        preferred_element_type=jnp.float32,
    )
    query_full = (
        jnp.concatenate(
            [
                queries_grad[..., :NOPE],
                unrotate(
                    queries_grad[..., NOPE:], cosine_table[:, None, :], sine_table[:, None, :]
                ),
            ],
            axis=-1,
        )
        .astype(BF16)
        .reshape(length, heads_local * qk_dim)
    )
    keyval_grad = (
        jnp.concatenate([key_grad[..., :NOPE], value_grad], axis=-1)
        .astype(BF16)
        .reshape(length, heads_local * (NOPE + VD))
    )
    expand_part = inner_rows(latent_normed, keyval_grad)
    latent_normed_part = outer_cols(keyval_grad, expand_all)
    rope_part = jnp.sum(key_grad[..., NOPE:], axis=1)
    latent_normed_grad, rope_raw = (
        lax.psum(latent_normed_part.astype(BF16), "row").astype(F32),
        lax.psum(rope_part.astype(BF16), "row").astype(F32),
    )
    rope_grad = unrotate(rope_raw, cosine_table, sine_table)
    latent_gain_part = jnp.sum(
        lax.dynamic_slice_in_dim(
            latent_normed_grad * latent * scale_latent, own_start, own_rows, 0
        ),
        axis=0,
    )
    latent_grad = rms_back(latent, scale_latent, latent_normed_grad * latent_gain)
    down_grad_in = jnp.concatenate([latent_grad, rope_grad], axis=-1).astype(BF16)
    own_down_grad = lax.dynamic_slice_in_dim(down_grad_in, own_row * down_cols, down_cols, 1)
    both_grad = jnp.concatenate([query_full, own_down_grad], axis=1)
    normed_one_grad = row_total(outer_cols(both_grad, query_down))
    first_gain_part = jnp.sum(normed_one_grad * stream * scale_one, axis=0)
    input_grad = (
        residual_grad + rms_back(stream, scale_one, normed_one_grad * first_gain)
    ).reshape(1, own_rows, width)

    output_grad = col_total(output_part, 1)
    latent_up_grad = col_total(expand_part, 0)
    both_total = col_total(inner_rows(seq_normed, both_grad), 0)
    query_grad = both_total[:, :query_cols]
    latent_down_grad = lax.all_gather(
        both_total[:, query_cols:].astype(BF16), "row", axis=1, tiled=True
    ).astype(F32)
    gains = jnp.concatenate([first_gain_part, latent_gain_part, second_gain_part])
    gains = padded_rows(gains.reshape(-1, LATENT // 4))
    gains = jnp.sum(kernel_small(gains, False, 5), axis=0).reshape(-1)
    first_gain_grad = gains[:width]
    latent_gain_grad = gains[width : width + LATENT]
    second_gain_grad = gains[width + LATENT : 2 * width + LATENT]
    return (
        layer_out,
        input_grad,
        first_gain_grad,
        query_grad,
        latent_down_grad,
        latent_gain_grad,
        latent_up_grad,
        output_grad,
        second_gain_grad,
        router_grad,
        shared_gate_grad,
        shared_up_grad,
        shared_down_grad,
        expert_gate_grad,
        expert_up_grad,
        expert_down_grad,
    )


def solution(mesh):
    return jax.shard_map(
        on_device,
        mesh=mesh,
        in_specs=(
            P("col", "row", None),
            P("col", None),
            P("col", "row", None),
            P(),
            P("col", "row"),
            P("col", None),
            P(),
            P("col", "row"),
            P("row", "col"),
            P(),
            P(),
            P("col", "row"),
            P("col", "row"),
            P("row", "col"),
            P("col", None, "row"),
            P("col", None, "row"),
            P("col", "row", None),
            P("col", "row", None),
        ),
        out_specs=(
            P("col", "row", None),
            P("col", "row", None),
            P(),
            P("col", "row"),
            P("col", None),
            P(),
            P("col", "row"),
            P("row", "col"),
            P(),
            P(),
            P("col", "row"),
            P("col", "row"),
            P("row", "col"),
            P("col", None, "row"),
            P("col", None, "row"),
            P("col", "row", None),
        ),
        check_vma=False,
    )
```

```python
import functools

import jax
import jax.numpy as jnp
from jax import lax
from jax.experimental import pallas as pl
from jax.experimental.pallas import tpu as pltpu
from jax.sharding import PartitionSpec as P

NOPE = 128
ROPE = 64
LATENT = 512
VD = 128
TOPK = 6


EPS = 1e-06
ROWS_CONTRACT = (((0,), (0,)), ((), ()))
COLS_CONTRACT = (((1,), (1,)), ((), ()))


def matmul(left_side, right_side):
    return jnp.dot(left_side, right_side, preferred_element_type=jnp.float32)


def inner_rows(left_side, right_side):
    return lax.dot_general(left_side, right_side, ROWS_CONTRACT, preferred_element_type=jnp.float32)


def outer_cols(left_side, right_side):
    return lax.dot_general(left_side, right_side, COLS_CONTRACT, preferred_element_type=jnp.float32)


def rms_scale(values):
    return lax.rsqrt(jnp.mean(values * values, axis=-1, keepdims=True) + EPS)


def rms_back(values, scaling, gradient):
    return scaling * gradient - values * scaling**3 * jnp.mean(
        gradient * values, axis=-1, keepdims=True
    )


def silu_parts(preact):
    logistic = jax.nn.sigmoid(preact)
    return (preact * logistic, logistic * (1.0 + preact * (1.0 - logistic)))


def angle_tables(length):
    halfway = ROPE // 2
    frequency = 10000.0 ** (-2.0 * jnp.arange(halfway, dtype=jnp.float32) / ROPE)
    angles = jnp.arange(length, dtype=jnp.float32)[:, None] * frequency[None, :]
    return (jnp.cos(angles), jnp.sin(angles))


def rotate(values, cosine_in, sine_in):
    halfway = values.shape[-1] // 2
    leading = values[..., :halfway]
    trailing = values[..., halfway:]
    return jnp.concatenate(
        [leading * cosine_in - trailing * sine_in, leading * sine_in + trailing * cosine_in],
        axis=-1,
    )


def unrotate(values, cosine_in, sine_in):
    halfway = values.shape[-1] // 2
    leading = values[..., :halfway]
    trailing = values[..., halfway:]
    return jnp.concatenate(
        [leading * cosine_in + trailing * sine_in, trailing * cosine_in - leading * sine_in],
        axis=-1,
    )


F32 = jnp.float32
BF16 = jnp.bfloat16
EVERY = ("col", "row")
VMEM_LIMIT = 63 * 1024 * 1024


def token_rows(values):
    return lax.all_gather(values, "row", axis=0, tiled=True)


def every_token(values):
    return lax.all_gather(values, EVERY, axis=0, tiled=True)


def row_total(partial_value):
    return lax.psum_scatter(
        partial_value.astype(BF16), "row", scatter_dimension=0, tiled=True
    ).astype(F32)


def every_total(partial_value):
    return lax.psum_scatter(partial_value, EVERY, scatter_dimension=0, tiled=True).astype(F32)


def col_gather(values):
    return lax.all_gather(values, "col", axis=0, tiled=True)


def col_total(partial_value, dim):
    return lax.psum_scatter(
        partial_value.astype(BF16), "col", scatter_dimension=dim, tiled=True
    ).astype(F32)


MESH_ID = pl.DeviceIdType.MESH


def places():
    row, col = lax.axis_index("row"), lax.axis_index("col")
    return row // 2, lax.rem(row, 2), col // 2, lax.rem(col, 2)


def to_place(wide, core, line, side):
    return {"row": wide * 2 + core, "col": line * 2 + side}


def greet(partners, everyone):
    barrier = pltpu.get_barrier_semaphore()
    if everyone:
        n_row, n_col = lax.axis_size("row"), lax.axis_size("col")
        total = n_row * n_col
        me = lax.axis_index("col") * n_row + lax.axis_index("row")

        @pl.loop(1, total)
        def _(step):
            other = lax.rem(me + step, total)
            pl.semaphore_signal(
                barrier,
                inc=1,
                device_id={"row": lax.rem(other, n_row), "col": other // n_row},
                device_id_type=MESH_ID,
            )

        pl.semaphore_wait(barrier, total - 1)
        return
    for there, partner in partners:

        @pl.when(there)
        def _(partner=partner):
            pl.semaphore_signal(barrier, inc=1, device_id=partner, device_id_type=MESH_ID)

    pl.semaphore_wait(barrier, sum(jnp.int32(there) for there, _ in partners))


def remote(src, dst, send_sem, recv_sem, partner):
    return pltpu.make_async_remote_copy(
        src_ref=src,
        dst_ref=dst,
        send_sem=send_sem,
        recv_sem=recv_sem,
        device_id=partner,
        device_id_type=MESH_ID,
    )


def small_exchange(small_ref, small_out, send_sem, recv_sem, personal):
    n_row = lax.axis_size("row")
    total = n_row * lax.axis_size("col")
    me = lax.axis_index("col") * n_row + lax.axis_index("row")

    def copy(other, slot):
        return remote(
            small_ref.at[other] if personal else small_ref,
            small_out.at[slot],
            send_sem.at[other],
            recv_sem.at[slot],
            {"row": lax.rem(other, n_row), "col": other // n_row},
        )

    def start():
        @pl.loop(1, total)
        def _(step):
            copy(lax.rem(me + step, total), me).start()

        small_out[me] = small_ref[me] if personal else small_ref[...]

    def finish():
        @pl.loop(1, total)
        def _(step):
            other = lax.rem(me + step, total)
            copy(other, other).wait_recv()
            copy(other, me).wait_send()

    return start, finish


def line_order(lines):
    order = []
    for step in range((lines + 1) // 2):
        order.append(step)
        if lines - 1 - step != step:
            order.append(lines - 1 - step)
    return order


def scatter_body(lines, count, small, *refs):
    bigs, refs = refs[:count], refs[count:]
    if small:
        small_ref, refs = refs[0], refs[1:]
    outs, refs = refs[:count], refs[count:]
    if small:
        small_out, refs = refs[0], refs[1:]
    own, core_in, wide_in, side_in, up_in, down_in = refs[:6]
    load_sem, core_send, core_recv, wide_send, wide_recv, side_send, side_recv = refs[6:13]
    up_send, up_recv, down_send, down_recv = refs[13:17]
    wide, core, line, side = places()
    tokens = own.shape[1]
    half = tokens // 2
    core_mate = to_place(wide, 1 - core, line, side)
    wide_mate = to_place(1 - wide, core, line, side)
    side_mate = to_place(wide, core, line, 1 - side)
    above = to_place(wide, core, line + 1, side)
    below = to_place(wide, core, line - 1, side)
    has_above = line < lines - 1
    has_below = line > 0
    greet(
        [
            (core >= 0, core_mate),
            (core >= 0, wide_mate),
            (core >= 0, side_mate),
            (has_above, above),
            (has_below, below),
        ],
        small,
    )
    parts = [pl.ds(0, half), pl.ds(half, half)]

    def at(a, l, s, w):
        return ((a * lines + l) * 2 + s) * 2 + w

    def core_copy(a, i):
        n = a * 4 * lines + i
        return remote(
            bigs[a].at[pl.ds((2 * i + 1 - core) * tokens, tokens)],
            core_in.at[n],
            core_send.at[n],
            core_recv.at[n],
            core_mate,
        )

    def load(a, i):
        n = a * 4 * lines + i
        return pltpu.make_async_copy(
            bigs[a].at[pl.ds((2 * i + core) * tokens, tokens)], own.at[n], load_sem.at[n]
        )

    def wide_one(a, l, s):
        n = (a * lines + l) * 3 + s
        return remote(
            own.at[at(a, l, s, 1 - wide), parts[0]],
            wide_in.at[n],
            wide_send.at[n],
            wide_recv.at[n],
            wide_mate,
        )

    def side_one(a, l, w):
        n = (a * lines + l) * 3 + w
        return remote(
            own.at[at(a, l, 1 - side, w), parts[1]],
            side_in.at[n],
            side_send.at[n],
            side_recv.at[n],
            side_mate,
        )

    def side_two(a, l):
        n = (a * lines + l) * 3 + 2
        return remote(
            own.at[at(a, l, 1 - side, wide), parts[0]],
            side_in.at[n],
            side_send.at[n],
            side_recv.at[n],
            side_mate,
        )

    def wide_two(a, l):
        n = (a * lines + l) * 3 + 2
        return remote(
            own.at[at(a, l, side, 1 - wide), parts[1]],
            wide_in.at[n],
            wide_send.at[n],
            wide_recv.at[n],
            wide_mate,
        )

    def up_copy(a, l, h):
        n = (a * lines + l) * 2 + h
        return remote(
            own.at[at(a, l, side, wide), parts[h]],
            up_in.at[n],
            up_send.at[n],
            up_recv.at[n],
            above,
        )

    def down_copy(a, l, h):
        n = (a * lines + l) * 2 + h
        return remote(
            own.at[at(a, l, side, wide), parts[h]],
            down_in.at[n],
            down_send.at[n],
            down_recv.at[n],
            below,
        )

    def add(i, rows, other):
        own[i, rows] = (own[i, rows].astype(F32) + other[...].astype(F32)).astype(BF16)

    items = [(a, l) for a in range(count) for l in line_order(lines)]
    for a, l in items:
        for j in range(4):
            core_copy(a, l * 4 + j).start()
            load(a, l * 4 + j).start()
    if small:
        small_start, small_finish = small_exchange(small_ref, small_out, *refs[17:19], True)
        small_start()

    def stage_one(a, l):
        for j in range(4):
            i = l * 4 + j
            load(a, i).wait()
            core_copy(a, i).wait_recv()
            add(a * 4 * lines + i, pl.ds(0, tokens), core_in.at[a * 4 * lines + i])
        for j in range(2):
            wide_one(a, l, j).start()
            side_one(a, l, j).start()

    def stage_two(a, l):
        n = (a * lines + l) * 3
        for j in range(2):
            s = 1 - side if j == 0 else side
            wide_one(a, l, s).wait_recv()
            add(at(a, l, s, wide), parts[0], wide_in.at[n + s])
            if j == 0:
                side_two(a, l).start()
            w = 1 - wide if j == 0 else wide
            side_one(a, l, w).wait_recv()
            add(at(a, l, side, w), parts[1], side_in.at[n + w])
            if j == 0:
                wide_two(a, l).start()

    def stage_three(a, l):
        n = (a * lines + l) * 3 + 2
        i = at(a, l, side, wide)
        for h in range(2):
            if h == 0:
                side_two(a, l).wait_recv()
                add(i, parts[0], side_in.at[n])
            else:
                wide_two(a, l).wait_recv()
                add(i, parts[1], wide_in.at[n])

            @pl.when(jnp.logical_and(line == 0, l > 0))
            def _(h=h):
                up_copy(a, l, h).start()

            @pl.when(jnp.logical_and(line == lines - 1, l < lines - 1))
            def _(h=h):
                down_copy(a, l, h).start()

    def onward(a, l, up):
        @pl.when(jnp.logical_and(has_below, has_above))
        def _():
            copy, arrived = (up_copy, up_in) if up else (down_copy, down_in)
            for h in range(2):
                copy(a, l, h).wait_recv()
                add(at(a, l, side, wide), parts[h], arrived.at[(a * lines + l) * 2 + h])
                copy(a, l, h).start()

    def passing(a, j):
        high, low = lines - 1 - j, j
        lower_half = line * 2 < lines

        def go(up, when):
            l = high if up else low
            beyond = line < l if up else line > l

            @pl.when(jnp.logical_and(when, beyond))
            def _():
                onward(a, l, up)

        go(True, lower_half)
        go(False, lower_half)
        go(False, jnp.logical_not(lower_half))
        go(True, jnp.logical_not(lower_half))

    def final(a):
        for h in range(2):

            @pl.when(has_below)
            def _(h=h):
                up_copy(a, line, h).wait_recv()
                add(at(a, line, side, wide), parts[h], up_in.at[(a * lines + line) * 2 + h])

            @pl.when(has_above)
            def _(h=h):
                down_copy(a, line, h).wait_recv()
                add(at(a, line, side, wide), parts[h], down_in.at[(a * lines + line) * 2 + h])

        outs[a][...] = own[at(a, line, side, wide)].astype(F32)

    passes = {}
    for a in range(count):
        for j in range(lines - 1):
            after = a * lines + min(2 * j + 2, lines - 1) + 3
            passes.setdefault(after, []).append(functools.partial(passing, a, j))
        passes.setdefault(a * lines + lines + 3, []).append(functools.partial(final, a))
    for step in range(len(items) + 4):
        if step < len(items):
            stage_one(*items[step])
        if 0 <= step - 1 < len(items):
            stage_two(*items[step - 1])
        if 0 <= step - 2 < len(items):
            stage_three(*items[step - 2])
        for action in passes.get(step, []):
            action()
    if small:
        small_finish()
    for a, l in items:
        for j in range(4):
            core_copy(a, l * 4 + j).wait_send()
        for j in range(2):
            wide_one(a, l, j).wait_send()
            side_one(a, l, j).wait_send()
        side_two(a, l).wait_send()
        wide_two(a, l).wait_send()
        for h in range(2):

            @pl.when(jnp.logical_and(has_above, line < l))
            def _(h=h):
                up_copy(a, l, h).wait_send()

            @pl.when(jnp.logical_and(has_below, line > l))
            def _(h=h):
                down_copy(a, l, h).wait_send()


def kernel_total(partials, small_value, number):
    n_row, n_col = lax.axis_size("row"), lax.axis_size("col")
    lines, count = n_col // 2, len(partials)
    width = partials[0].shape[1]
    tokens = partials[0].shape[0] // (n_row * n_col)
    small = small_value is not None
    out_shape = [jax.ShapeDtypeStruct((tokens, width), F32)] * count
    in_specs = [pl.BlockSpec(memory_space=pl.ANY)] * count
    operands = list(partials)
    if small:
        in_specs.append(pl.BlockSpec(memory_space=pltpu.VMEM))
        out_shape.append(jax.ShapeDtypeStruct(small_value.shape, small_value.dtype))
        operands.append(small_value)
    dma = pltpu.SemaphoreType.DMA
    scratch = [
        pltpu.VMEM((count * 4 * lines, tokens, width), BF16),
        pltpu.VMEM((count * 4 * lines, tokens, width), BF16),
        pltpu.VMEM((count * 3 * lines, tokens // 2, width), BF16),
        pltpu.VMEM((count * 3 * lines, tokens // 2, width), BF16),
        pltpu.VMEM((count * 2 * lines, tokens // 2, width), BF16),
        pltpu.VMEM((count * 2 * lines, tokens // 2, width), BF16),
        *[dma((count * 4 * lines,))] * 3,
        *[dma((count * 3 * lines,))] * 4,
        *[dma((count * 2 * lines,))] * 4,
    ]
    if small:
        scratch += [dma((n_row * n_col,))] * 2
    return pl.pallas_call(
        functools.partial(scatter_body, lines, count, small),
        out_shape=out_shape,
        in_specs=in_specs,
        out_specs=[pl.BlockSpec(memory_space=pltpu.VMEM)] * len(out_shape),
        scratch_shapes=scratch,
        compiler_params=pltpu.CompilerParams(
            collective_id=number, has_side_effects=True, vmem_limit_bytes=VMEM_LIMIT
        ),
        name=f"scatter_{number}",
    )(*operands)


def gather_body(lines, small, *refs):
    own_ref, refs = refs[0], refs[1:]
    if small:
        small_ref, refs = refs[0], refs[1:]
    out_ref, refs = refs[0], refs[1:]
    if small:
        small_out, refs = refs[0], refs[1:]
    local_sem, core_send, core_recv, wide_send, wide_recv, side_send, side_recv = refs[:7]
    up_send, up_recv, down_send, down_recv = refs[7:11]
    wide, core, line, side = places()
    tokens = own_ref.shape[0]
    half = tokens // 2
    core_mate = to_place(wide, 1 - core, line, side)
    wide_mate = to_place(1 - wide, core, line, side)
    side_mate = to_place(wide, core, line, 1 - side)
    above = to_place(wide, core, line + 1, side)
    below = to_place(wide, core, line - 1, side)
    has_above = line < lines - 1
    has_below = line > 0
    greet(
        [
            (core >= 0, core_mate),
            (core >= 0, wide_mate),
            (core >= 0, side_mate),
            (has_above, above),
            (has_below, below),
        ],
        small,
    )

    def spot(l, s, w, k, h):
        return out_ref.at[pl.ds((((l * 2 + s) * 2 + w) * 2 + k) * tokens + h * half, half)]

    def source(l, s, w, h, here):
        return own_ref.at[pl.ds(h * half, half)] if here else spot(l, s, w, core, h)

    def core_copy(l, s, w, h, here=False):
        n = ((l * 2 + s) * 2 + w) * 2 + h
        return remote(
            source(l, s, w, h, here),
            spot(l, s, w, core, h),
            core_send.at[n],
            core_recv.at[n],
            core_mate,
        )

    def wide_copy(l, s, h, here=False):
        n = l * 3 + (2 if h else s)
        return remote(
            source(l, s, wide, h, here),
            spot(l, s, wide, core, h),
            wide_send.at[n],
            wide_recv.at[n],
            wide_mate,
        )

    def side_copy(l, w, h, here=False):
        n = l * 3 + (w if h else 2)
        return remote(
            source(l, side, w, h, here),
            spot(l, side, w, core, h),
            side_send.at[n],
            side_recv.at[n],
            side_mate,
        )

    def up_copy(l, h, here=False):
        n = l * 2 + h
        return remote(
            source(l, side, wide, h, here),
            spot(l, side, wide, core, h),
            up_send.at[n],
            up_recv.at[n],
            above,
        )

    def down_copy(l, h, here=False):
        n = l * 2 + h
        return remote(
            source(l, side, wide, h, here),
            spot(l, side, wide, core, h),
            down_send.at[n],
            down_recv.at[n],
            below,
        )

    def local(h):
        return pltpu.make_async_copy(
            own_ref.at[pl.ds(h * half, half)], spot(line, side, wide, core, h), local_sem.at[h]
        )

    def spread(l, h, here=False):
        if h == 0:
            side_copy(l, wide, 0, here).start()
            wide_copy(l, side, 0, here).start()
        else:
            wide_copy(l, side, 1, here).start()
            side_copy(l, wide, 1, here).start()
        core_copy(l, side, wide, h, here).start()

    def second(l):
        side_copy(l, wide, 0).wait_recv()
        wide_copy(l, 1 - side, 0).start()
        core_copy(l, 1 - side, wide, 0).start()
        wide_copy(l, side, 1).wait_recv()
        side_copy(l, 1 - wide, 1).start()
        core_copy(l, side, 1 - wide, 1).start()

    def third(l):
        for j in range(2):
            s = 1 - side if j else side
            wide_copy(l, s, 0).wait_recv()
            core_copy(l, s, 1 - wide, 0).start()
            w = 1 - wide if j else wide
            side_copy(l, w, 1).wait_recv()
            core_copy(l, 1 - side, w, 1).start()

    for h in range(2):

        @pl.when(has_above)
        def _(h=h):
            up_copy(line, h, True).start()

        @pl.when(has_below)
        def _(h=h):
            down_copy(line, h, True).start()

        spread(line, h, True)
    if small:
        small_start, small_finish = small_exchange(small_ref, small_out, *refs[11:13], False)
        small_start()
    for h in range(2):
        local(h).start()

    def from_line(dist, up):
        l = line - dist if up else line + dist
        there = l >= 0 if up else l < lines
        further = has_above if up else has_below
        copy = up_copy if up else down_copy

        @pl.when(there)
        def _():
            for h in range(2):
                copy(l, h).wait_recv()

                @pl.when(further)
                def _(h=h):
                    copy(l, h).start()

                spread(l, h)

    def stage(action, dist):
        if dist == 0:
            action(line)
            return

        @pl.when(line - dist >= 0)
        def _():
            action(line - dist)

        @pl.when(line + dist < lines)
        def _():
            action(line + dist)

    for dist in range(1, lines + 2):
        if dist < lines:
            from_line(dist, True)
            from_line(dist, False)
        if dist - 1 < lines:
            stage(second, dist - 1)
        if 0 <= dist - 2 < lines:
            stage(third, dist - 2)
    if small:
        small_finish()
    for h in range(2):
        local(h).wait()
    for l in range(lines):
        for s in range(2):
            for w in range(2):
                for h in range(2):
                    core_copy(l, s, w, h).wait_recv()
                    core_copy(l, s, w, h).wait_send()
        for j in range(2):
            wide_copy(l, j, 0).wait_send()
            side_copy(l, j, 1).wait_send()
        wide_copy(l, side, 1).wait_send()
        side_copy(l, wide, 0).wait_send()
        for h in range(2):

            @pl.when(jnp.logical_and(has_above, line >= l))
            def _(h=h):
                up_copy(l, h).wait_send()

            @pl.when(jnp.logical_and(has_below, line <= l))
            def _(h=h):
                down_copy(l, h).wait_send()


def kernel_gather(own, small_value, number):
    n_row, n_col = lax.axis_size("row"), lax.axis_size("col")
    lines, total = n_col // 2, n_row * n_col
    tokens, width = own.shape
    small = small_value is not None
    out_shape = [jax.ShapeDtypeStruct((total * tokens, width), own.dtype)]
    in_specs = [pl.BlockSpec(memory_space=pltpu.VMEM)]
    out_specs = [pl.BlockSpec(memory_space=pl.ANY)]
    operands = [own]
    if small:
        in_specs.append(pl.BlockSpec(memory_space=pltpu.VMEM))
        out_specs.append(pl.BlockSpec(memory_space=pltpu.VMEM))
        out_shape.append(jax.ShapeDtypeStruct((total, *small_value.shape), small_value.dtype))
        operands.append(small_value)
    dma = pltpu.SemaphoreType.DMA
    scratch = [
        dma((2,)),
        *[dma((8 * lines,))] * 2,
        *[dma((3 * lines,))] * 4,
        *[dma((2 * lines,))] * 4,
    ]
    if small:
        scratch += [dma((total,))] * 2
    return pl.pallas_call(
        functools.partial(gather_body, lines, small),
        out_shape=out_shape,
        in_specs=in_specs,
        out_specs=out_specs,
        scratch_shapes=scratch,
        compiler_params=pltpu.CompilerParams(collective_id=number, has_side_effects=True),
        name=f"gather_{number}",
    )(*operands)


def kernel_fits(rows, width, count):
    n_row, n_col = lax.axis_size("row"), lax.axis_size("col")
    tokens = rows // (n_row * n_col)
    held = count * n_col * 2 * width * tokens * 13 // 4
    return n_row == 4 and n_col % 2 == 0 and tokens % 32 == 0 and held < 58 * 1024 * 1024


def row_mates(wide, core, line, side):
    return to_place(wide, 1 - core, line, side), to_place(1 - wide, core, line, side)


def strip(ref, dim, index, size):
    start = pl.multiple_of(index * size, size)
    return ref.at[pl.ds(start, size)] if dim == 0 else ref.at[:, pl.ds(start, size)]


def mixed_gather_body(lines, dims, flips, small, *refs):
    count = len(dims)
    cols, row_ref, refs = refs[:count], refs[count], refs[count + 1 :]
    if small:
        small_ref, refs = refs[0], refs[1:]
    col_outs, row_out, refs = refs[:count], refs[count], refs[count + 1 :]
    if small:
        small_out, refs = refs[0], refs[1:]
    local_sem, core_send, core_recv, wide_send, wide_recv = refs[:5]
    refs = refs[5:]
    if count:
        side_send, side_recv, up_send, up_recv, down_send, down_recv = refs[:6]
        refs = refs[6:]
    wide, core, line, side = places()
    core_mate, wide_mate = row_mates(wide, core, line, side)
    side_mate = to_place(wide, core, line, 1 - side)
    above = to_place(wide, core, line + 1, side)
    below = to_place(wide, core, line - 1, side)
    has_above = line < lines - 1
    has_below = line > 0
    partners = [(core >= 0, core_mate), (core >= 0, wide_mate)]
    if count:
        partners += [(core >= 0, side_mate), (has_above, above), (has_below, below)]
    greet(partners, small)

    def spot(m, l, s):
        size = cols[m].shape[dims[m]]
        return strip(col_outs[m], dims[m], l * 2 + s, size)

    def line_copy(m, l, s, up, here=False):
        n = (m * lines + l) * 2 + s
        return remote(
            cols[m] if here else spot(m, l, s),
            spot(m, l, s),
            (up_send if up else down_send).at[n],
            (up_recv if up else down_recv).at[n],
            above if up else below,
        )

    def side_copy(m, l, here=False):
        n = m * lines + l
        return remote(
            cols[m] if here else spot(m, l, side),
            spot(m, l, side),
            side_send.at[n],
            side_recv.at[n],
            side_mate,
        )

    tokens = row_ref.shape[0]

    def row_spot(w, k):
        return strip(row_out, 0, w * 2 + k, tokens)

    def core_copy(n):
        src = row_ref if n == 0 else row_spot(1 - wide, core)
        dst = row_spot(wide if n == 0 else 1 - wide, core)
        return remote(src, dst, core_send.at[n], core_recv.at[n], core_mate)

    def to_line(m, s, here):
        @pl.when(has_above)
        def _():
            line_copy(m, line, s, True, here).start()

        @pl.when(has_below)
        def _():
            line_copy(m, line, s, False, here).start()

    wide_copy = remote(row_ref, row_spot(wide, core), wide_send.at[0], wide_recv.at[0], wide_mate)
    wide_copy.start()
    core_copy(0).start()
    for m in range(count):

        to_line(m, side, True)
        side_copy(m, line, True).start()
    if small:
        small_start, small_finish = small_exchange(small_ref, small_out, *refs[:2], False)
        small_start()
    local = [pltpu.make_async_copy(row_ref, row_spot(wide, core), local_sem.at[count])]
    for m in range(count):
        local.append(pltpu.make_async_copy(cols[m], spot(m, line, side), local_sem.at[m]))
    for copy in local:
        copy.start()

    def from_line(m, dist, up):
        l = line - dist if up else line + dist

        @pl.when(l >= 0 if up else l < lines)
        def _():
            for s in (side, 1 - side) if flips[m] else (side,):
                line_copy(m, l, s, up).wait_recv()

                @pl.when(has_above if up else has_below)
                def _(s=s):
                    line_copy(m, l, s, up).start()

            if not flips[m]:
                side_copy(m, l).start()

    for m in range(count):
        if flips[m]:
            side_copy(m, line).wait_recv()
            to_line(m, 1 - side, False)

    def pass_on():
        wide_copy.wait_recv()
        core_copy(1).start()

    if lines == 1 or not count:
        pass_on()
    for dist in range(1, lines if count else 1):
        for m in range(count):
            from_line(m, dist, True)
            from_line(m, dist, False)
        if dist == 1:
            pass_on()
    if small:
        small_finish()
    for copy in local:
        copy.wait()
    wide_copy.wait_send()
    for n in range(2):
        core_copy(n).wait()
    for m in range(count):
        if flips[m]:
            side_copy(m, line).wait_send()
        for l in range(lines):
            if not flips[m]:
                side_copy(m, l).wait()
            for s in range(2) if flips[m] else (side,):

                @pl.when(jnp.logical_and(has_above, line >= l))
                def _(m=m, l=l, s=s):
                    line_copy(m, l, s, True).wait_send()

                @pl.when(jnp.logical_and(has_below, line <= l))
                def _(m=m, l=l, s=s):
                    line_copy(m, l, s, False).wait_send()


def mixed_gather(col_values, dims, flips, row_value, small_value, number):
    n_row, n_col = lax.axis_size("row"), lax.axis_size("col")
    lines, count, small = n_col // 2, len(dims), small_value is not None
    tokens, width = row_value.shape
    hbm, vmem = pl.BlockSpec(memory_space=pl.ANY), pl.BlockSpec(memory_space=pltpu.VMEM)
    out_shape = []
    for value, dim in zip(col_values, dims):
        shape = list(value.shape)
        shape[dim] *= n_col
        out_shape.append(jax.ShapeDtypeStruct(tuple(shape), value.dtype))
    out_shape.append(jax.ShapeDtypeStruct((n_row * tokens, width), row_value.dtype))
    operands = [*col_values, row_value]
    in_specs, out_specs = [hbm] * count + [vmem], [hbm] * (count + 1)
    dma = pltpu.SemaphoreType.DMA
    scratch = [dma((count + 1,)), dma((2,)), dma((2,)), dma((1,)), dma((1,))]
    if count:
        scratch += [dma((count * lines,))] * 2 + [dma((2 * count * lines,))] * 4
    if small:
        operands.append(small_value)
        in_specs.append(vmem)
        out_specs.append(vmem)
        out_shape.append(
            jax.ShapeDtypeStruct((n_row * n_col, *small_value.shape), small_value.dtype)
        )
        scratch += [dma((n_row * n_col,))] * 2
    return pl.pallas_call(
        functools.partial(mixed_gather_body, lines, tuple(dims), tuple(flips), small),
        out_shape=out_shape,
        in_specs=in_specs,
        out_specs=out_specs,
        scratch_shapes=scratch,
        compiler_params=pltpu.CompilerParams(collective_id=number, has_side_effects=True),
        name=f"mixed_gather_{number}",
    )(*operands)


def mixed_total_body(lines, dims, flips, *refs):
    count = len(dims)
    cols, row_ref, refs = refs[:count], refs[count], refs[count + 1 :]
    col_outs, row_out, refs = refs[:count], refs[count], refs[count + 1 :]
    row_own, row_core, row_wide, refs = refs[0], refs[1], refs[2], refs[3:]
    owns, refs = refs[:count], refs[count:]
    side_ins, refs = refs[:count], refs[count:]
    up_ins, refs = refs[:count], refs[count:]
    down_ins, refs = refs[:count], refs[count:]
    row_load, core_send, core_recv, wide_send, wide_recv = refs[:5]
    if count:
        load_sem, side_send, side_recv, up_send, up_recv, down_send, down_recv = refs[5:12]
    wide, core, line, side = places()
    core_mate, wide_mate = row_mates(wide, core, line, side)
    side_mate = to_place(wide, core, line, 1 - side)
    above = to_place(wide, core, line + 1, side)
    below = to_place(wide, core, line - 1, side)
    has_above = line < lines - 1
    has_below = line > 0
    partners = [(core >= 0, core_mate), (core >= 0, wide_mate)]
    if count:
        partners += [(core >= 0, side_mate), (has_above, above), (has_below, below)]
    greet(partners, False)
    tokens = row_out.shape[0]

    def core_copy(w):
        return remote(
            strip(row_ref, 0, w * 2 + 1 - core, tokens),
            row_core.at[w],
            core_send.at[w],
            core_recv.at[w],
            core_mate,
        )

    def row_loaded(w):
        return pltpu.make_async_copy(
            strip(row_ref, 0, w * 2 + core, tokens), row_own.at[w], row_load.at[w]
        )

    wide_copy = remote(row_own.at[1 - wide], row_wide, wide_send.at[0], wide_recv.at[0], wide_mate)

    def source(m, l, s):
        return strip(cols[m], dims[m], l * 2 + s, col_outs[m].shape[dims[m]])

    def side_copy(m, l):
        n = m * lines + l
        return remote(
            owns[m].at[l, 1 - side] if flips[m] else source(m, l, 1 - side),
            side_ins[m].at[0 if flips[m] else l],
            side_send.at[n],
            side_recv.at[n],
            side_mate,
        )

    def own_at(m, l, s):
        return owns[m].at[l, s] if flips[m] else owns[m].at[l]

    def loaded(m, l, s):
        return pltpu.make_async_copy(
            source(m, l, s), own_at(m, l, s), load_sem.at[(m * lines + l) * 2 + s]
        )

    def line_copy(m, l, s, up):
        n = (m * lines + l) * 2 + s
        into = (up_ins if up else down_ins)[m]
        return remote(
            own_at(m, l, s),
            into.at[l, s] if flips[m] else into.at[l],
            (up_send if up else down_send).at[n],
            (up_recv if up else down_recv).at[n],
            above if up else below,
        )

    def sides(m):
        return (1 - side, side) if flips[m] else (side,)

    for w in range(2):
        core_copy(w).start()
        row_loaded(w).start()
    items = [(m, l) for l in (line_order(lines) if count else []) for m in range(count)]
    for m, l in items:
        for s in sides(m):
            loaded(m, l, s).start()
        if not flips[m]:
            side_copy(m, l).start()
    for j in range(2):
        w = wide if j else 1 - wide
        row_loaded(w).wait()
        core_copy(w).wait_recv()
        row_own[w] = (row_own[w].astype(F32) + row_core[w].astype(F32)).astype(BF16)
        if j == 0:
            wide_copy.start()

    def add(m, l, s, other):
        mine = own_at(m, l, s)
        mine[...] = (mine[...].astype(F32) + other.astype(F32)).astype(BF16)

    def near(m, l):
        for s in sides(m):
            loaded(m, l, s).wait()
            if not flips[m]:
                side_copy(m, l).wait_recv()
                add(m, l, s, side_ins[m][l])

            @pl.when(jnp.logical_and(line == 0, l > 0))
            def _(s=s):
                line_copy(m, l, s, True).start()

            @pl.when(jnp.logical_and(line == lines - 1, l < lines - 1))
            def _(s=s):
                line_copy(m, l, s, False).start()

    def onward(m, l, up):
        @pl.when(jnp.logical_and(has_below, has_above))
        def _():
            for s in sides(m):
                where = (l, s) if flips[m] else (l,)
                line_copy(m, l, s, up).wait_recv()
                add(m, l, s, (up_ins if up else down_ins)[m][where])
                line_copy(m, l, s, up).start()

    def passing(m, j):
        high, low = lines - 1 - j, j
        lower_half = line * 2 < lines

        def go(up, when):
            l = high if up else low
            beyond = line < l if up else line > l

            @pl.when(jnp.logical_and(when, beyond))
            def _():
                onward(m, l, up)

        go(True, lower_half)
        go(False, lower_half)
        go(False, jnp.logical_not(lower_half))
        go(True, jnp.logical_not(lower_half))

    def final(m):
        for s in sides(m):
            where = (line, s) if flips[m] else (line,)

            @pl.when(has_below)
            def _(s=s, where=where):
                line_copy(m, line, s, True).wait_recv()
                add(m, line, s, up_ins[m][where])

            @pl.when(has_above)
            def _(s=s, where=where):
                line_copy(m, line, s, False).wait_recv()
                add(m, line, s, down_ins[m][where])

        if flips[m]:
            side_copy(m, line).start()

    flipped = [m for m in range(count) if flips[m]]
    straight = [m for m in range(count) if not flips[m]]
    order = line_order(lines)
    for l in order:
        for m in flipped:
            near(m, l)
    if count:
        for step in range(lines + 2):
            if step < lines:
                for m in straight:
                    near(m, order[step])
            if step < lines - 1:
                for m in flipped:
                    passing(m, step)
            if step == lines - 1:
                for m in flipped:
                    final(m)
            if 2 <= step < lines + 1:
                for m in straight:
                    passing(m, step - 2)
            if step == lines + 1:
                for m in straight:
                    final(m)
    wide_copy.wait()
    row_out[...] = row_own[wide].astype(F32) + row_wide[...].astype(F32)
    for w in range(2):
        core_copy(w).wait_send()
    for m in range(count):
        if flips[m]:
            side_copy(m, line).wait()
            add(m, line, side, side_ins[m][0])
        col_outs[m][...] = own_at(m, line, side)[...].astype(F32)
        for l in range(lines):
            if not flips[m]:
                side_copy(m, l).wait_send()
            for s in sides(m):

                @pl.when(jnp.logical_and(has_above, line < l))
                def _(m=m, l=l, s=s):
                    line_copy(m, l, s, True).wait_send()

                @pl.when(jnp.logical_and(has_below, line > l))
                def _(m=m, l=l, s=s):
                    line_copy(m, l, s, False).wait_send()


def mixed_total(col_values, dims, flips, row_value, number):
    n_row, n_col = lax.axis_size("row"), lax.axis_size("col")
    lines, count = n_col // 2, len(dims)
    tokens, width = row_value.shape[0] // n_row, row_value.shape[1]
    hbm, vmem = pl.BlockSpec(memory_space=pl.ANY), pl.BlockSpec(memory_space=pltpu.VMEM)
    blocks = []
    for value, dim in zip(col_values, dims):
        shape = list(value.shape)
        shape[dim] //= n_col
        blocks.append(tuple(shape))
    dma = pltpu.SemaphoreType.DMA
    scratch = [
        pltpu.VMEM((2, tokens, width), BF16),
        pltpu.VMEM((2, tokens, width), BF16),
        pltpu.VMEM((tokens, width), BF16),
    ]
    doubled = [(lines, 2) if flip else (lines,) for flip in flips]
    side_held = [(1,) if flip else (lines,) for flip in flips]
    for lead in (doubled, side_held, doubled, doubled):
        scratch += [pltpu.VMEM((*d, *shape), BF16) for d, shape in zip(lead, blocks)]
    scratch += [dma((2,)), dma((2,)), dma((2,)), dma((1,)), dma((1,))]
    if count:
        scratch += [dma((2 * count * lines,))] + [dma((count * lines,))] * 2
        scratch += [dma((2 * count * lines,))] * 4
    return pl.pallas_call(
        functools.partial(mixed_total_body, lines, tuple(dims), tuple(flips)),
        out_shape=[jax.ShapeDtypeStruct(shape, F32) for shape in blocks]
        + [jax.ShapeDtypeStruct((tokens, width), F32)],
        in_specs=[hbm] * (count + 1),
        out_specs=[vmem] * (count + 1),
        scratch_shapes=scratch,
        compiler_params=pltpu.CompilerParams(
            collective_id=number, has_side_effects=True, vmem_limit_bytes=VMEM_LIMIT
        ),
        name=f"mixed_total_{number}",
    )(*col_values, row_value)


def small_body(personal, value_ref, out_ref, send_sem, recv_sem):
    greet([], True)
    start, finish = small_exchange(value_ref, out_ref, send_sem, recv_sem, personal)
    start()
    finish()


def kernel_small(value, personal, number):
    total = lax.axis_size("row") * lax.axis_size("col")
    shape = value.shape if personal else (total, *value.shape)
    dma = pltpu.SemaphoreType.DMA
    return pl.pallas_call(
        functools.partial(small_body, personal),
        out_shape=jax.ShapeDtypeStruct(shape, value.dtype),
        in_specs=[pl.BlockSpec(memory_space=pltpu.VMEM)],
        out_specs=pl.BlockSpec(memory_space=pltpu.VMEM),
        scratch_shapes=[dma((total,)), dma((total,))],
        compiler_params=pltpu.CompilerParams(collective_id=number, has_side_effects=True),
        name=f"small_{number}",
    )(value)


def gather_every(own, small_value, number):
    total = lax.axis_size("row") * lax.axis_size("col")
    if kernel_fits(total * own.shape[0], own.shape[1], 1):
        return kernel_gather(own, small_value, number)
    return every_token(own), every_token(small_value[None])


def total_every(partials, small_value, number):
    if kernel_fits(partials[0].shape[0], partials[0].shape[1], len(partials)):
        return kernel_total(partials, small_value, number)
    exchanged = lax.all_to_all(small_value, EVERY, split_axis=0, concat_axis=0, tiled=True)
    return *[every_total(p) for p in partials], exchanged


def mixed_fits(col_values):
    n_row, lines = lax.axis_size("row"), lax.axis_size("col") // 2
    return n_row == 4 and (not col_values or (lax.axis_size("col") % 2 == 0 and lines <= 8))


def gather_mixed(col_values, dims, flips, row_value, small_value, number):
    if mixed_fits(col_values):
        return mixed_gather(col_values, dims, flips, row_value, small_value, number)
    cols = [lax.all_gather(v, "col", axis=d, tiled=True) for v, d in zip(col_values, dims)]
    return *cols, token_rows(row_value), every_token(small_value[None])


def total_mixed(col_values, dims, flips, row_value, number):
    if mixed_fits(col_values):
        return mixed_total(col_values, dims, flips, row_value, number)
    return *[col_total(v, d) for v, d in zip(col_values, dims)], row_total(row_value)


def padded_rows(values):
    return jnp.pad(values, ((0, -values.shape[0] % 8), (0, 0)))


def masked_scores(queries, attn_keys, allowed, softmax_scale):
    scores = (
        jnp.einsum("qhd,khd->hqk", queries, attn_keys, preferred_element_type=jnp.float32)
        * softmax_scale
    )
    return jnp.where(allowed[None], scores, -1e30)


def select_body(group, capacity, place_ref, rows_ref, slots_ref):
    tokens = place_ref.shape[2]
    for block in range(group):
        picked = matmul(place_ref[block], rows_ref[block * tokens : (block + 1) * tokens, :])
        slots_ref[:, block] = picked.astype(BF16).reshape(-1, capacity, picked.shape[-1])


def select_rows(place, rows, capacity):
    blocks, slots, tokens = place.shape
    width = rows.shape[1]
    local_experts = slots // capacity
    group = 4 if blocks % 4 == 0 else 1
    out = pl.pallas_call(
        functools.partial(select_body, group, capacity),
        grid=(blocks // group,),
        in_specs=[
            pl.BlockSpec((group, slots, tokens), lambda i: (i, 0, 0)),
            pl.BlockSpec((group * tokens, width), lambda i: (i, 0)),
        ],
        out_specs=pl.BlockSpec((local_experts, group, capacity, width), lambda i: (0, i, 0, 0)),
        out_shape=jax.ShapeDtypeStruct((local_experts, blocks, capacity, width), BF16),
        compiler_params=pltpu.CompilerParams(vmem_limit_bytes=VMEM_LIMIT),
        cost_estimate=pl.CostEstimate(
            flops=2 * blocks * slots * tokens * width,
            bytes_accessed=4 * blocks * tokens * width,
            transcendentals=0,
        ),
        name="select_rows",
    )(place, rows)
    return out.reshape(local_experts, blocks * capacity, width)


def experts_body(
    x_ref, g_ref, gate_ref, wg_ref, wu_ref, wd_ref, y_ref, r_ref, dg_ref, du_ref, dd_ref, gg_ref
):
    first = pl.program_id(1) == 0
    x = x_ref[0]
    g = g_ref[0]
    gate = gate_ref[0]
    pre = outer_cols(x, wg_ref[0])
    lin = outer_cols(x, wu_ref[0])
    back = outer_cols(g, wd_ref[0])
    act, slope = silu_parts(pre)
    hidden = act * lin
    gg_ref[0] = jnp.sum(hidden * back, axis=-1, keepdims=True)
    hidden = (hidden * gate).astype(BF16)
    back = back * gate
    pre_grad = (back * lin * slope).astype(BF16)
    lin_grad = (back * act).astype(BF16)
    width = x_ref.shape[2]
    chunk = 512 if width % 512 == 0 else width
    for start in range(0, width, chunk):
        cols = slice(start, start + chunk)
        y_ref[0, :, cols] = matmul(hidden, wd_ref[0, :, cols]).astype(BF16)
        r_ref[0, :, cols] = (
            matmul(pre_grad, wg_ref[0, :, cols]) + matmul(lin_grad, wu_ref[0, :, cols])
        ).astype(BF16)
        d_gate = inner_rows(pre_grad, x_ref[0, :, cols])
        d_up = inner_rows(lin_grad, x_ref[0, :, cols])
        d_down = inner_rows(hidden, g_ref[0, :, cols])

        @pl.when(first)
        def _():
            dg_ref[0, :, cols] = d_gate
            du_ref[0, :, cols] = d_up
            dd_ref[0, :, cols] = d_down

        @pl.when(jnp.logical_not(first))
        def _():
            dg_ref[0, :, cols] += d_gate
            du_ref[0, :, cols] += d_up
            dd_ref[0, :, cols] += d_down


def run_experts(x_slots, g_slots, gates, w_gate, w_up, w_down):
    count, rows, width = x_slots.shape
    hidden = w_down.shape[1]
    chunk = 512 if rows % 512 == 0 else rows
    row_block = pl.BlockSpec((1, chunk, width), lambda e, r: (e, r, 0))
    col_block = pl.BlockSpec((1, chunk, 1), lambda e, r: (e, r, 0))
    out_block = pl.BlockSpec((1, hidden, width), lambda e, r: (e, 0, 0))
    y, r, d_gate, d_up, d_down, dots = pl.pallas_call(
        experts_body,
        grid=(count, rows // chunk),
        in_specs=[row_block, row_block, col_block, out_block, out_block, out_block],
        out_specs=[row_block, row_block, out_block, out_block, out_block, col_block],
        out_shape=[
            jax.ShapeDtypeStruct((count, rows, width), BF16),
            jax.ShapeDtypeStruct((count, rows, width), BF16),
            jax.ShapeDtypeStruct((count, hidden, width), F32),
            jax.ShapeDtypeStruct((count, hidden, width), F32),
            jax.ShapeDtypeStruct((count, hidden, width), F32),
            jax.ShapeDtypeStruct((count, rows, 1), F32),
        ],
        compiler_params=pltpu.CompilerParams(vmem_limit_bytes=VMEM_LIMIT),
        cost_estimate=pl.CostEstimate(
            flops=18 * count * rows * width * hidden,
            bytes_accessed=count * (8 * rows * width + 18 * width * hidden),
            transcendentals=count * rows * hidden,
        ),
        name="run_experts",
    )(x_slots, g_slots, gates, w_gate.transpose(0, 2, 1), w_up.transpose(0, 2, 1), w_down)
    return y, r, d_gate.transpose(0, 2, 1), d_up.transpose(0, 2, 1), d_down, dots


def combine_body(group, place_ref, slots_ref, extra_ref, weight_ref, out_ref):
    tokens = place_ref.shape[2]
    width = out_ref.shape[1]
    for block in range(group):
        rows = slice(block * tokens, (block + 1) * tokens)
        total = inner_rows(place_ref[block], slots_ref[:, block].reshape(-1, width))
        total += matmul(extra_ref[rows, :], weight_ref[...])
        out_ref[rows, :] = total.astype(BF16)


def combine_rows(place, slots, extra, weight, capacity):
    blocks, slot_count, tokens = place.shape
    local_experts, _, width = slots.shape
    group = 4 if blocks % 4 == 0 else 1
    inner = extra.shape[1]
    return pl.pallas_call(
        functools.partial(combine_body, group),
        grid=(blocks // group,),
        in_specs=[
            pl.BlockSpec((group, slot_count, tokens), lambda i: (i, 0, 0)),
            pl.BlockSpec((local_experts, group, capacity, width), lambda i: (0, i, 0, 0)),
            pl.BlockSpec((group * tokens, inner), lambda i: (i, 0)),
            pl.BlockSpec((inner, width), lambda i: (0, 0)),
        ],
        out_specs=pl.BlockSpec((group * tokens, width), lambda i: (i, 0)),
        out_shape=jax.ShapeDtypeStruct((blocks * tokens, width), BF16),
        compiler_params=pltpu.CompilerParams(vmem_limit_bytes=VMEM_LIMIT),
        cost_estimate=pl.CostEstimate(
            flops=2 * blocks * tokens * (slot_count + inner) * width,
            bytes_accessed=4 * blocks * tokens * width,
            transcendentals=0,
        ),
        name="combine_rows",
    )(place, slots.reshape(local_experts, blocks, capacity, width), extra, weight)


def on_device(
    inputs,
    segment_ids,
    routes,
    first_gain,
    query_weight,
    latent_down,
    latent_gain,
    latent_up,
    output_weight,
    second_gain,
    router_weight,
    shared_gate,
    shared_up,
    shared_down,
    expert_gate,
    expert_up,
    expert_down,
    cotangent,
):
    n_row = lax.axis_size("row")
    n_col = lax.axis_size("col")
    blocks = n_row * n_col
    own_row = lax.axis_index("row")
    own_col = lax.axis_index("col")
    own_rows = inputs.shape[1]
    width = inputs.shape[2]
    experts = router_weight.shape[1]
    local_experts = expert_gate.shape[0]
    capacity = max(2, own_rows // 8)
    stream = inputs.reshape(own_rows, width).astype(F32)
    grad_out = cotangent.reshape(own_rows, width)
    own_routes = routes.reshape(own_rows, TOPK)
    segments = segment_ids.reshape(-1)
    length = segments.shape[0]
    own_start = own_row * own_rows
    qk_dim = NOPE + ROPE
    softmax_scale = qk_dim ** (-0.5)
    cosine_table, sine_table = angle_tables(length)

    scale_one = rms_scale(stream)
    normed_one = (stream * scale_one * first_gain).astype(BF16)
    down_cols = latent_down.shape[1] // n_row
    own_down = lax.dynamic_slice_in_dim(latent_down, own_row * down_cols, down_cols, 1)
    output_rows = output_weight.shape[0]
    query_cols = query_weight.shape[1]
    query_all, output_down, expand_all, seq_normed, all_routes = gather_mixed(
        [query_weight, jnp.concatenate([output_weight, own_down.T], axis=0), latent_up],
        [0, 1, 0],
        [False, False, True],
        normed_one,
        padded_rows(own_routes.astype(F32).T),
        1,
    )
    output_all = output_down[:output_rows]
    down_all = output_down[output_rows:]

    all_routes = all_routes[:, :TOPK].astype(jnp.int32)
    grad_all = every_token(grad_out.astype(BF16))
    local_ids = own_col * local_experts + jnp.arange(local_experts)
    named = all_routes[:, :, None, :] == local_ids[None, None, :, None]
    chosen_here = jnp.max(named.astype(BF16), axis=1)
    before = (jnp.arange(own_rows)[:, None] < jnp.arange(own_rows)[None, :]).astype(BF16)
    rank = matmul(chosen_here.reshape(-1, own_rows), before).reshape(chosen_here.shape)
    slot_of = jnp.where(chosen_here > 0, rank.astype(jnp.int32), -1)
    placed = slot_of[:, :, None, :] == jnp.arange(capacity)[None, None, :, None]
    place = placed.astype(BF16).reshape(blocks, local_experts * capacity, own_rows)
    grad_slots = select_rows(place, grad_all, capacity)

    shared_cols = shared_gate.shape[1] // n_col
    shared_send = jnp.stack([shared_gate.T, shared_up.T, shared_down], axis=0)
    depth = shared_send.shape[2]
    shared_send = (
        shared_send.reshape(3, n_col, shared_cols, depth)
        .transpose(1, 0, 2, 3)
        .reshape(n_col, 3 * shared_cols, depth)
    )
    shared_own = (
        lax.all_to_all(shared_send, "col", split_axis=0, concat_axis=0, tiled=True)
        .transpose(1, 0, 2)
        .reshape(3, shared_cols, width)
    )
    gate_up_own = shared_own[:2].reshape(2 * shared_cols, width)
    down_own = shared_own[2]

    heads_local = query_cols // qk_dim
    query_raw = matmul(seq_normed, query_all).reshape(length, heads_local, qk_dim)
    queries = jnp.concatenate(
        [
            query_raw[..., :NOPE],
            rotate(query_raw[..., NOPE:], cosine_table[:, None, :], sine_table[:, None, :]),
        ],
        axis=-1,
    ).astype(BF16)
    latent_all = lax.all_gather(outer_cols(seq_normed, down_all), "row", axis=1, tiled=True)
    latent = latent_all[:, :LATENT]
    scale_latent = rms_scale(latent)
    latent_normed = (latent * scale_latent * latent_gain).astype(BF16)
    keyval = matmul(latent_normed, expand_all).reshape(length, heads_local, NOPE + VD)
    key_rope = rotate(latent_all[:, LATENT:], cosine_table, sine_table)
    attn_keys = jnp.concatenate(
        [keyval[..., :NOPE], jnp.broadcast_to(key_rope[:, None, :], (length, heads_local, ROPE))],
        axis=-1,
    ).astype(BF16)
    values = keyval[..., NOPE:].astype(BF16)
    positions = jnp.arange(length)
    allowed = (positions[:, None] >= positions[None, :]) & (segments[:, None] == segments[None, :])
    scores = masked_scores(queries, attn_keys, allowed, softmax_scale)
    highest = jnp.max(scores, axis=-1, keepdims=True)
    log_total = highest + jnp.log(jnp.sum(jnp.exp(scores - highest), axis=-1, keepdims=True))
    attn_probs = jnp.exp(scores - log_total).astype(BF16)
    heads_out = (
        jnp.einsum("hqk,khd->qhd", attn_probs, values, preferred_element_type=jnp.float32)
        .astype(BF16)
        .reshape(length, heads_local * VD)
    )
    heads_out, grad_all = lax.optimization_barrier((heads_out, grad_all))
    (attn_total,) = total_mixed([], [], [], matmul(heads_out, output_all).astype(BF16), 6)
    residual = stream + attn_total

    scale_two = rms_scale(residual)
    normed_two = (residual * scale_two * second_gain).astype(BF16)
    logits = matmul(normed_two, router_weight)
    expert_ids = jnp.arange(experts)
    chosen = own_routes[:, :, None] == expert_ids[None, None, :]
    picked = jnp.sum(jnp.where(chosen, logits[:, None, :], 0.0), axis=-1)
    gate_probs = jax.nn.softmax(picked, axis=-1)

    all_normed, all_gates = gather_every(normed_two, padded_rows(gate_probs.T), 2)
    all_gates = all_gates[:, :TOPK]
    gate_here = jnp.sum(jnp.where(named, all_gates[:, :, None, :], 0.0), axis=1)
    slot_gate = jnp.sum(jnp.where(placed, gate_here[:, :, None, :], 0.0), axis=-1)
    slot_gate = slot_gate.transpose(1, 0, 2).reshape(local_experts, blocks * capacity, 1)
    normed_slots = select_rows(place, all_normed, capacity)
    out_slots, rows_slots, expert_gate_grad, expert_up_grad, expert_down_grad, slot_dot = (
        run_experts(normed_slots, grad_slots, slot_gate, expert_gate, expert_up, expert_down)
    )

    shared_both = outer_cols(all_normed, gate_up_own)
    shared_act, shared_slope = silu_parts(shared_both[:, :shared_cols])
    shared_lin = shared_both[:, shared_cols:]
    shared_hidden = (shared_act * shared_lin).astype(BF16)
    shared_hidden_grad = outer_cols(grad_all, down_own)
    shared_both_grad = jnp.concatenate(
        [
            (shared_hidden_grad * shared_lin * shared_slope).astype(BF16),
            (shared_hidden_grad * shared_act).astype(BF16),
        ],
        axis=1,
    )
    slot_dot = slot_dot.reshape(local_experts, blocks, capacity).transpose(1, 0, 2)
    token_dot = jnp.sum(jnp.where(placed, slot_dot[:, :, :, None], 0.0), axis=2)
    out_total, rows_total, token_dot = total_every(
        [
            combine_rows(place, out_slots, shared_hidden, down_own, capacity),
            combine_rows(place, rows_slots, shared_both_grad, gate_up_own, capacity),
        ],
        token_dot,
        3,
    )
    layer_out = (residual + out_total).astype(BF16).reshape(1, own_rows, width)
    gate_up_part = inner_rows(shared_both_grad, all_normed)
    down_part = inner_rows(shared_hidden, grad_all)
    shared_back = jnp.concatenate([gate_up_part, down_part], axis=0).astype(BF16)
    shared_back = (
        shared_back.reshape(3 * shared_cols, n_col, depth).transpose(1, 0, 2)
    )
    shared_back = lax.all_to_all(shared_back, "col", split_axis=0, concat_axis=0, tiled=True)
    shared_back = (
        shared_back.reshape(n_col, 3, shared_cols, depth)
        .transpose(1, 0, 2, 3)
        .reshape(3, n_col * shared_cols, depth)
        .astype(F32)
    )
    shared_gate_grad = shared_back[0].T
    shared_up_grad = shared_back[1].T
    shared_down_grad = shared_back[2]

    token_dot = jnp.sum(token_dot.reshape(n_col, n_row, local_experts, own_rows), axis=1)
    token_dot = token_dot.reshape(experts, own_rows).T
    gate_grad = jnp.sum(jnp.where(chosen, token_dot[:, None, :], 0.0), axis=-1)
    picked_grad = gate_probs * (gate_grad - jnp.sum(gate_probs * gate_grad, axis=-1, keepdims=True))
    logit_grad = jnp.sum(jnp.where(chosen, picked_grad[:, :, None], 0.0), axis=1).astype(BF16)

    normed_two_grad = rows_total + outer_cols(logit_grad, router_weight)
    second_gain_part = jnp.sum(normed_two_grad * residual * scale_two, axis=0)
    residual_grad = grad_out + rms_back(residual, scale_two, normed_two_grad * second_gain)

    seq_resid, all_logit_grad = gather_mixed(
        [], [], [], residual_grad.astype(BF16), logit_grad, 4
    )
    router_grad = inner_rows(all_normed, all_logit_grad.reshape(-1, experts))
    output_part = inner_rows(heads_out, seq_resid)
    heads_grad = outer_cols(seq_resid, output_all).astype(BF16).reshape(length, heads_local, VD)
    recomputed = jnp.exp(masked_scores(queries, attn_keys, allowed, softmax_scale) - log_total)
    delta_rows = jnp.sum(
        heads_grad.astype(F32) * heads_out.reshape(length, heads_local, VD).astype(F32),
        axis=-1,
    )
    prob_grad = jnp.einsum("qhd,khd->hqk", heads_grad, values, preferred_element_type=jnp.float32)
    score_grad = (recomputed * (prob_grad - delta_rows.T[:, :, None]) * softmax_scale).astype(BF16)
    queries_grad = jnp.einsum(
        "hqk,khd->qhd", score_grad, attn_keys, preferred_element_type=jnp.float32
    )
    key_grad = jnp.einsum("hqk,qhd->khd", score_grad, queries, preferred_element_type=jnp.float32)
    value_grad = jnp.einsum(
        "hqk,qhd->khd",
        recomputed.astype(BF16),
        heads_grad,
        preferred_element_type=jnp.float32,
    )
    query_full = (
        jnp.concatenate(
            [
                queries_grad[..., :NOPE],
                unrotate(
                    queries_grad[..., NOPE:], cosine_table[:, None, :], sine_table[:, None, :]
                ),
            ],
            axis=-1,
        )
        .astype(BF16)
        .reshape(length, heads_local * qk_dim)
    )
    keyval_grad = (
        jnp.concatenate([key_grad[..., :NOPE], value_grad], axis=-1)
        .astype(BF16)
        .reshape(length, heads_local * (NOPE + VD))
    )
    expand_part = inner_rows(latent_normed, keyval_grad)
    latent_normed_part = outer_cols(keyval_grad, expand_all)
    rope_part = jnp.sum(key_grad[..., NOPE:], axis=1)
    latent_normed_grad, rope_raw = (
        lax.psum(latent_normed_part.astype(BF16), "row").astype(F32),
        lax.psum(rope_part.astype(BF16), "row").astype(F32),
    )
    rope_grad = unrotate(rope_raw, cosine_table, sine_table)
    latent_gain_part = jnp.sum(
        lax.dynamic_slice_in_dim(
            latent_normed_grad * latent * scale_latent, own_start, own_rows, 0
        ),
        axis=0,
    )
    latent_grad = rms_back(latent, scale_latent, latent_normed_grad * latent_gain)
    down_grad_in = jnp.concatenate([latent_grad, rope_grad], axis=-1).astype(BF16)
    own_down_grad = lax.dynamic_slice_in_dim(down_grad_in, own_row * down_cols, down_cols, 1)
    output_down_part = jnp.concatenate(
        [output_part.astype(BF16), inner_rows(own_down_grad, seq_normed).astype(BF16)], axis=0
    )
    input_part = outer_cols(query_full, query_all) + matmul(own_down_grad, down_all)
    query_grad, output_down_grad, latent_up_grad, normed_one_grad = total_mixed(
        [inner_rows(seq_normed, query_full).astype(BF16), output_down_part, expand_part.astype(BF16)],
        [0, 1, 0],
        [False, False, True],
        input_part.astype(BF16),
        7,
    )
    output_grad = output_down_grad[:output_rows]
    first_gain_part = jnp.sum(normed_one_grad * stream * scale_one, axis=0)
    input_grad = (
        residual_grad + rms_back(stream, scale_one, normed_one_grad * first_gain)
    ).reshape(1, own_rows, width)

    gains = jnp.concatenate([first_gain_part, latent_gain_part, second_gain_part])
    gains = padded_rows(gains.reshape(-1, LATENT // 4))
    down_total, all_gains = gather_mixed(
        [], [], [], output_down_grad[output_rows:].astype(BF16), gains, 5
    )
    latent_down_grad = down_total.astype(F32).T
    gains = jnp.sum(all_gains, axis=0).reshape(-1)
    first_gain_grad = gains[:width]
    latent_gain_grad = gains[width : width + LATENT]
    second_gain_grad = gains[width + LATENT : 2 * width + LATENT]
    return (
        layer_out,
        input_grad,
        first_gain_grad,
        query_grad,
        latent_down_grad,
        latent_gain_grad,
        latent_up_grad,
        output_grad,
        second_gain_grad,
        router_grad,
        shared_gate_grad,
        shared_up_grad,
        shared_down_grad,
        expert_gate_grad,
        expert_up_grad,
        expert_down_grad,
    )


def solution(mesh):
    return jax.shard_map(
        on_device,
        mesh=mesh,
        in_specs=(
            P("col", "row", None),
            P("col", None),
            P("col", "row", None),
            P(),
            P("col", "row"),
            P("col", None),
            P(),
            P("col", "row"),
            P("row", "col"),
            P(),
            P(),
            P("col", "row"),
            P("col", "row"),
            P("row", "col"),
            P("col", None, "row"),
            P("col", None, "row"),
            P("col", "row", None),
            P("col", "row", None),
        ),
        out_specs=(
            P("col", "row", None),
            P("col", "row", None),
            P(),
            P("col", "row"),
            P("col", None),
            P(),
            P("col", "row"),
            P("row", "col"),
            P(),
            P(),
            P("col", "row"),
            P("col", "row"),
            P("row", "col"),
            P("col", None, "row"),
            P("col", None, "row"),
            P("col", "row", None),
        ),
        check_vma=False,
    )
```

```python
import functools

import jax
import jax.numpy as jnp
from jax import lax
from jax.experimental import pallas as pl
from jax.experimental.pallas import tpu as pltpu
from jax.sharding import PartitionSpec as P

NOPE = 128
ROPE = 64
LATENT = 512
VD = 128
TOPK = 6


EPS = 1e-06
ROWS_CONTRACT = (((0,), (0,)), ((), ()))
COLS_CONTRACT = (((1,), (1,)), ((), ()))


def matmul(left_side, right_side):
    return jnp.dot(left_side, right_side, preferred_element_type=jnp.float32)


def inner_rows(left_side, right_side):
    return lax.dot_general(left_side, right_side, ROWS_CONTRACT, preferred_element_type=jnp.float32)


def outer_cols(left_side, right_side):
    return lax.dot_general(left_side, right_side, COLS_CONTRACT, preferred_element_type=jnp.float32)


def rms_scale(values):
    return lax.rsqrt(jnp.mean(values * values, axis=-1, keepdims=True) + EPS)


def rms_back(values, scaling, gradient):
    return scaling * gradient - values * scaling**3 * jnp.mean(
        gradient * values, axis=-1, keepdims=True
    )


def silu_parts(preact):
    logistic = jax.nn.sigmoid(preact)
    return (preact * logistic, logistic * (1.0 + preact * (1.0 - logistic)))


def angle_tables(length):
    halfway = ROPE // 2
    frequency = 10000.0 ** (-2.0 * jnp.arange(halfway, dtype=jnp.float32) / ROPE)
    angles = jnp.arange(length, dtype=jnp.float32)[:, None] * frequency[None, :]
    return (jnp.cos(angles), jnp.sin(angles))


def rotate(values, cosine_in, sine_in):
    halfway = values.shape[-1] // 2
    leading = values[..., :halfway]
    trailing = values[..., halfway:]
    return jnp.concatenate(
        [leading * cosine_in - trailing * sine_in, leading * sine_in + trailing * cosine_in],
        axis=-1,
    )


def unrotate(values, cosine_in, sine_in):
    halfway = values.shape[-1] // 2
    leading = values[..., :halfway]
    trailing = values[..., halfway:]
    return jnp.concatenate(
        [leading * cosine_in + trailing * sine_in, trailing * cosine_in - leading * sine_in],
        axis=-1,
    )


F32 = jnp.float32
BF16 = jnp.bfloat16
EVERY = ("col", "row")
VMEM_LIMIT = 63 * 1024 * 1024


def token_rows(values):
    return lax.all_gather(values, "row", axis=0, tiled=True)


def every_token(values):
    return lax.all_gather(values, EVERY, axis=0, tiled=True)


def row_total(partial_value):
    return lax.psum_scatter(
        partial_value.astype(BF16), "row", scatter_dimension=0, tiled=True
    ).astype(F32)


def every_total(partial_value):
    return lax.psum_scatter(partial_value, EVERY, scatter_dimension=0, tiled=True).astype(F32)


def col_gather(values):
    return lax.all_gather(values, "col", axis=0, tiled=True)


def col_total(partial_value, dim):
    return lax.psum_scatter(
        partial_value.astype(BF16), "col", scatter_dimension=dim, tiled=True
    ).astype(F32)


MESH_ID = pl.DeviceIdType.MESH


def places():
    row, col = lax.axis_index("row"), lax.axis_index("col")
    return row // 2, lax.rem(row, 2), col // 2, lax.rem(col, 2)


def to_place(wide, core, line, side):
    return {"row": wide * 2 + core, "col": line * 2 + side}


def greet(partners, everyone):
    barrier = pltpu.get_barrier_semaphore()
    if everyone:
        n_row, n_col = lax.axis_size("row"), lax.axis_size("col")
        total = n_row * n_col
        me = lax.axis_index("col") * n_row + lax.axis_index("row")

        @pl.loop(1, total)
        def _(step):
            other = lax.rem(me + step, total)
            pl.semaphore_signal(
                barrier,
                inc=1,
                device_id={"row": lax.rem(other, n_row), "col": other // n_row},
                device_id_type=MESH_ID,
            )

        pl.semaphore_wait(barrier, total - 1)
        return
    for there, partner in partners:

        @pl.when(there)
        def _(partner=partner):
            pl.semaphore_signal(barrier, inc=1, device_id=partner, device_id_type=MESH_ID)

    pl.semaphore_wait(barrier, sum(jnp.int32(there) for there, _ in partners))


def remote(src, dst, send_sem, recv_sem, partner):
    return pltpu.make_async_remote_copy(
        src_ref=src,
        dst_ref=dst,
        send_sem=send_sem,
        recv_sem=recv_sem,
        device_id=partner,
        device_id_type=MESH_ID,
    )


def small_exchange(small_ref, small_out, send_sem, recv_sem, personal):
    n_row = lax.axis_size("row")
    total = n_row * lax.axis_size("col")
    me = lax.axis_index("col") * n_row + lax.axis_index("row")

    def copy(other, slot):
        return remote(
            small_ref.at[other] if personal else small_ref,
            small_out.at[slot],
            send_sem.at[other],
            recv_sem.at[slot],
            {"row": lax.rem(other, n_row), "col": other // n_row},
        )

    def start():
        @pl.loop(1, total)
        def _(step):
            copy(lax.rem(me + step, total), me).start()

        small_out[me] = small_ref[me] if personal else small_ref[...]

    def finish():
        @pl.loop(1, total)
        def _(step):
            other = lax.rem(me + step, total)
            copy(other, other).wait_recv()
            copy(other, me).wait_send()

    return start, finish


def line_order(lines):
    order = []
    for step in range((lines + 1) // 2):
        order.append(step)
        if lines - 1 - step != step:
            order.append(lines - 1 - step)
    return order


def scatter_body(lines, count, small, *refs):
    place_ref, refs = refs[0], refs[1:]
    slots, extras, weights = refs[:count], refs[count : 2 * count], refs[2 * count : 3 * count]
    refs = refs[3 * count :]
    if small:
        small_ref, refs = refs[0], refs[1:]
    outs, refs = refs[:count], refs[count:]
    if small:
        small_out, refs = refs[0], refs[1:]
    own, core_in, wide_in, side_in, up_in, down_in = refs[:6]
    slot_in, staged, slot_sem, credit = refs[6:10]
    core_send, core_recv, wide_send, wide_recv, side_send, side_recv = refs[10:16]
    up_send, up_recv, down_send, down_recv = refs[16:20]
    refs = refs[3:]
    wide, core, line, side = places()
    tokens, width = own.shape[1:]
    ring, core_ring = slot_in.shape[0], core_in.shape[0]
    half = tokens // 2
    core_mate = to_place(wide, 1 - core, line, side)
    wide_mate = to_place(1 - wide, core, line, side)
    side_mate = to_place(wide, core, line, 1 - side)
    above = to_place(wide, core, line + 1, side)
    below = to_place(wide, core, line - 1, side)
    has_above = line < lines - 1
    has_below = line > 0
    greet(
        [
            (core >= 0, core_mate),
            (core >= 0, wide_mate),
            (core >= 0, side_mate),
            (has_above, above),
            (has_below, below),
        ],
        small,
    )
    parts = [pl.ds(0, half), pl.ds(half, half)]

    def at(a, l, s, w):
        return ((a * lines + l) * 2 + s) * 2 + w

    items = [(a, l) for a in range(count) for l in line_order(lines)]
    blocks = []
    for a, l in items:
        blocks += [(a, 2 * (l * 4 + j) + 1 - core) for j in range(4)]
        blocks += [(a, 2 * (l * 4 + j) + core) for j in range(4)]

    def slot_copy(q):
        a, b = blocks[q]
        return pltpu.make_async_copy(
            slots[a].at[:, b], slot_in.at[q % ring], slot_sem.at[q % ring]
        )

    def summed(q):
        if q + ring - 1 < len(blocks):
            slot_copy(q + ring - 1).start()
        slot_copy(q).wait()
        a, b = blocks[q]
        rows = pl.ds(pl.multiple_of(b * tokens, tokens), tokens)
        total = inner_rows(place_ref[b], slot_in[q % ring].reshape(-1, width))
        return (total + matmul(extras[a][rows, :], weights[a][...])).astype(BF16)

    def core_copy(n):
        return remote(
            staged.at[n % ring],
            core_in.at[n % core_ring],
            core_send.at[n],
            core_recv.at[n],
            core_mate,
        )

    def wide_one(a, l, s):
        n = (a * lines + l) * 3 + s
        return remote(
            own.at[at(a, l, s, 1 - wide), parts[0]],
            wide_in.at[n],
            wide_send.at[n],
            wide_recv.at[n],
            wide_mate,
        )

    def side_one(a, l, w):
        n = (a * lines + l) * 3 + w
        return remote(
            own.at[at(a, l, 1 - side, w), parts[1]],
            side_in.at[n],
            side_send.at[n],
            side_recv.at[n],
            side_mate,
        )

    def side_two(a, l):
        n = (a * lines + l) * 3 + 2
        return remote(
            own.at[at(a, l, 1 - side, wide), parts[0]],
            side_in.at[n],
            side_send.at[n],
            side_recv.at[n],
            side_mate,
        )

    def wide_two(a, l):
        n = (a * lines + l) * 3 + 2
        return remote(
            own.at[at(a, l, side, 1 - wide), parts[1]],
            wide_in.at[n],
            wide_send.at[n],
            wide_recv.at[n],
            wide_mate,
        )

    def up_copy(a, l, h):
        n = (a * lines + l) * 2 + h
        return remote(
            own.at[at(a, l, side, wide), parts[h]],
            up_in.at[n],
            up_send.at[n],
            up_recv.at[n],
            above,
        )

    def down_copy(a, l, h):
        n = (a * lines + l) * 2 + h
        return remote(
            own.at[at(a, l, side, wide), parts[h]],
            down_in.at[n],
            down_send.at[n],
            down_recv.at[n],
            below,
        )

    def add(i, rows, other):
        own[i, rows] = (own[i, rows].astype(F32) + other[...].astype(F32)).astype(BF16)

    for q in range(ring - 1):
        slot_copy(q).start()
    if small:
        small_start, small_finish = small_exchange(small_ref, small_out, *refs[17:19], True)
        small_start()

    def stage_one(t):
        a, l = items[t]
        for j in range(4):
            n = t * 4 + j
            if n >= ring:
                core_copy(n - ring).wait_send()
            staged[n % ring] = summed(t * 8 + j)
            if n >= core_ring:
                pl.semaphore_wait(credit, 1)
            core_copy(n).start()
        for j in range(4):
            own[a * 4 * lines + l * 4 + j] = summed(t * 8 + 4 + j)
        for j in range(4):
            n = t * 4 + j
            core_copy(n).wait_recv()
            add(a * 4 * lines + l * 4 + j, pl.ds(0, tokens), core_in.at[n % core_ring])
            if n + core_ring < 4 * len(items):
                pl.semaphore_signal(
                    credit, inc=1, device_id=core_mate, device_id_type=MESH_ID
                )
        for j in range(2):
            wide_one(a, l, j).start()
            side_one(a, l, j).start()

    def stage_two(a, l):
        n = (a * lines + l) * 3
        for j in range(2):
            s = 1 - side if j == 0 else side
            wide_one(a, l, s).wait_recv()
            add(at(a, l, s, wide), parts[0], wide_in.at[n + s])
            if j == 0:
                side_two(a, l).start()
            w = 1 - wide if j == 0 else wide
            side_one(a, l, w).wait_recv()
            add(at(a, l, side, w), parts[1], side_in.at[n + w])
            if j == 0:
                wide_two(a, l).start()

    def stage_three(a, l):
        n = (a * lines + l) * 3 + 2
        i = at(a, l, side, wide)
        for h in range(2):
            if h == 0:
                side_two(a, l).wait_recv()
                add(i, parts[0], side_in.at[n])
            else:
                wide_two(a, l).wait_recv()
                add(i, parts[1], wide_in.at[n])

            @pl.when(jnp.logical_and(line == 0, l > 0))
            def _(h=h):
                up_copy(a, l, h).start()

            @pl.when(jnp.logical_and(line == lines - 1, l < lines - 1))
            def _(h=h):
                down_copy(a, l, h).start()

    def onward(a, l, up):
        @pl.when(jnp.logical_and(has_below, has_above))
        def _():
            copy, arrived = (up_copy, up_in) if up else (down_copy, down_in)
            for h in range(2):
                copy(a, l, h).wait_recv()
                add(at(a, l, side, wide), parts[h], arrived.at[(a * lines + l) * 2 + h])
                copy(a, l, h).start()

    def passing(a, j):
        high, low = lines - 1 - j, j
        lower_half = line * 2 < lines

        def go(up, when):
            l = high if up else low
            beyond = line < l if up else line > l

            @pl.when(jnp.logical_and(when, beyond))
            def _():
                onward(a, l, up)

        go(True, lower_half)
        go(False, lower_half)
        go(False, jnp.logical_not(lower_half))
        go(True, jnp.logical_not(lower_half))

    def final(a):
        for h in range(2):

            @pl.when(has_below)
            def _(h=h):
                up_copy(a, line, h).wait_recv()
                add(at(a, line, side, wide), parts[h], up_in.at[(a * lines + line) * 2 + h])

            @pl.when(has_above)
            def _(h=h):
                down_copy(a, line, h).wait_recv()
                add(at(a, line, side, wide), parts[h], down_in.at[(a * lines + line) * 2 + h])

        outs[a][...] = own[at(a, line, side, wide)].astype(F32)

    passes = {}
    for a in range(count):
        for j in range(lines - 1):
            after = a * lines + min(2 * j + 2, lines - 1) + 3
            passes.setdefault(after, []).append(functools.partial(passing, a, j))
        passes.setdefault(a * lines + lines + 3, []).append(functools.partial(final, a))
    for step in range(len(items) + 4):
        if step < len(items):
            stage_one(step)
        if 0 <= step - 1 < len(items):
            stage_two(*items[step - 1])
        if 0 <= step - 2 < len(items):
            stage_three(*items[step - 2])
        for action in passes.get(step, []):
            action()
    if small:
        small_finish()
    for n in range(4 * len(items) - ring, 4 * len(items)):
        core_copy(n).wait_send()
    for a, l in items:
        for j in range(2):
            wide_one(a, l, j).wait_send()
            side_one(a, l, j).wait_send()
        side_two(a, l).wait_send()
        wide_two(a, l).wait_send()
        for h in range(2):

            @pl.when(jnp.logical_and(has_above, line < l))
            def _(h=h):
                up_copy(a, l, h).wait_send()

            @pl.when(jnp.logical_and(has_below, line > l))
            def _(h=h):
                down_copy(a, l, h).wait_send()


def kernel_total(place, partials, small_value, number):
    n_row, n_col = lax.axis_size("row"), lax.axis_size("col")
    lines, count = n_col // 2, len(partials)
    blocks, _, tokens = place.shape
    local_experts, rows, width = partials[0][0].shape
    capacity = rows // blocks
    small = small_value is not None
    out_shape = [jax.ShapeDtypeStruct((tokens, width), F32)] * count
    hbm, vmem = pl.BlockSpec(memory_space=pl.ANY), pl.BlockSpec(memory_space=pltpu.VMEM)
    in_specs = [vmem] + [hbm] * count + [vmem] * (2 * count)
    operands = [place]
    operands += [p[0].reshape(local_experts, blocks, capacity, width) for p in partials]
    operands += [p[1] for p in partials] + [p[2] for p in partials]
    if small:
        in_specs.append(vmem)
        out_shape.append(jax.ShapeDtypeStruct(small_value.shape, small_value.dtype))
        operands.append(small_value)
    dma = pltpu.SemaphoreType.DMA
    scratch = [
        pltpu.VMEM((count * 4 * lines, tokens, width), BF16),
        pltpu.VMEM((8, tokens, width), BF16),
        pltpu.VMEM((count * 3 * lines, tokens // 2, width), BF16),
        pltpu.VMEM((count * 3 * lines, tokens // 2, width), BF16),
        pltpu.VMEM((count * 2 * lines, tokens // 2, width), BF16),
        pltpu.VMEM((count * 2 * lines, tokens // 2, width), BF16),
        pltpu.VMEM((4, local_experts, capacity, width), BF16),
        pltpu.VMEM((4, tokens, width), BF16),
        dma((4,)),
        pltpu.SemaphoreType.REGULAR,
        *[dma((count * 4 * lines,))] * 2,
        *[dma((count * 3 * lines,))] * 4,
        *[dma((count * 2 * lines,))] * 4,
    ]
    if small:
        scratch += [dma((n_row * n_col,))] * 2
    return pl.pallas_call(
        functools.partial(scatter_body, lines, count, small),
        out_shape=out_shape,
        in_specs=in_specs,
        out_specs=[pl.BlockSpec(memory_space=pltpu.VMEM)] * len(out_shape),
        scratch_shapes=scratch,
        compiler_params=pltpu.CompilerParams(
            collective_id=number, has_side_effects=True, vmem_limit_bytes=VMEM_LIMIT
        ),
        name=f"scatter_{number}",
    )(*operands)


def kernel_fits(rows, width, count):
    n_row, n_col = lax.axis_size("row"), lax.axis_size("col")
    tokens = rows // (n_row * n_col)
    held = count * n_col * 2 * width * tokens * 13 // 4
    return n_row == 4 and n_col % 2 == 0 and tokens % 32 == 0 and held < 58 * 1024 * 1024


def row_mates(wide, core, line, side):
    return to_place(wide, 1 - core, line, side), to_place(1 - wide, core, line, side)


def strip(ref, dim, index, size):
    start = pl.multiple_of(index * size, size)
    return ref.at[pl.ds(start, size)] if dim == 0 else ref.at[:, pl.ds(start, size)]


def cols_plan(lines, dims, flips, spots, cols, outs, sems):
    wide, core, line, side = spots
    side_mate = to_place(wide, core, line, 1 - side)
    above = to_place(wide, core, line + 1, side)
    below = to_place(wide, core, line - 1, side)
    has_above, has_below = line < lines - 1, line > 0
    local_sem, side_send, side_recv, up_send, up_recv, down_send, down_recv = sems
    count = len(dims)

    def spot(m, l, s):
        return strip(outs[m], dims[m], l * 2 + s, cols[m].shape[dims[m]])

    def line_copy(m, l, s, up, here=False):
        n = (m * lines + l) * 2 + s
        return remote(
            cols[m] if here else spot(m, l, s),
            spot(m, l, s),
            (up_send if up else down_send).at[n],
            (up_recv if up else down_recv).at[n],
            above if up else below,
        )

    def side_copy(m, l, here=False):
        n = m * lines + l
        return remote(
            cols[m] if here else spot(m, l, side),
            spot(m, l, side),
            side_send.at[n],
            side_recv.at[n],
            side_mate,
        )

    def to_line(m, s, here):
        @pl.when(has_above)
        def _():
            line_copy(m, line, s, True, here).start()

        @pl.when(has_below)
        def _():
            line_copy(m, line, s, False, here).start()

    def local(m):
        return pltpu.make_async_copy(cols[m], spot(m, line, side), local_sem.at[m])

    def start():
        for m in range(count):
            to_line(m, side, True)
            side_copy(m, line, True).start()
        for m in range(count):
            local(m).start()

    def from_line(m, dist, up):
        l = line - dist if up else line + dist

        @pl.when(l >= 0 if up else l < lines)
        def _():
            for s in (side, 1 - side) if flips[m] else (side,):
                line_copy(m, l, s, up).wait_recv()

                @pl.when(has_above if up else has_below)
                def _(s=s):
                    line_copy(m, l, s, up).start()

            if not flips[m]:
                side_copy(m, l).start()

    def step(dist):
        if dist == 1:
            for m in range(count):
                if flips[m]:
                    side_copy(m, line).wait_recv()
                    to_line(m, 1 - side, False)
        if dist < lines:
            for m in range(count):
                from_line(m, dist, True)
                from_line(m, dist, False)

    def finish():
        for m in range(count):
            local(m).wait()
            if flips[m]:
                side_copy(m, line).wait_send()
            for l in range(lines):
                if not flips[m]:
                    side_copy(m, l).wait()
                for s in range(2) if flips[m] else (side,):

                    @pl.when(jnp.logical_and(has_above, line >= l))
                    def _(m=m, l=l, s=s):
                        line_copy(m, l, s, True).wait_send()

                    @pl.when(jnp.logical_and(has_below, line <= l))
                    def _(m=m, l=l, s=s):
                        line_copy(m, l, s, False).wait_send()

    return start, step, finish


def row_plan(spots, row_ref, out_ref, sems):
    wide, core, line, side = spots
    core_mate, wide_mate = row_mates(wide, core, line, side)
    local_sem, core_send, core_recv, wide_send, wide_recv = sems
    tokens = row_ref.shape[0]

    def spot(w, k):
        return strip(out_ref, 0, w * 2 + k, tokens)

    def core_copy(n):
        src = row_ref if n == 0 else spot(1 - wide, core)
        dst = spot(wide if n == 0 else 1 - wide, core)
        return remote(src, dst, core_send.at[n], core_recv.at[n], core_mate)

    wide_copy = remote(row_ref, spot(wide, core), wide_send.at[0], wide_recv.at[0], wide_mate)
    local = pltpu.make_async_copy(row_ref, spot(wide, core), local_sem.at[0])

    def start():
        wide_copy.start()
        core_copy(0).start()
        local.start()

    def step(dist):
        if dist == 1:
            wide_copy.wait_recv()
            core_copy(1).start()

    def finish():
        local.wait()
        wide_copy.wait_send()
        for n in range(2):
            core_copy(n).wait()

    return start, step, finish


def every_plan(lines, ways, spots, own_ref, out_ref, sems):
    wide, core, line, side = spots
    core_mate, wide_mate = row_mates(wide, core, line, side)
    side_mate = to_place(wide, core, line, 1 - side)
    above = to_place(wide, core, line + 1, side)
    below = to_place(wide, core, line - 1, side)
    has_above, has_below = line < lines - 1, line > 0
    local_sem, core_send, core_recv, wide_send, wide_recv, side_send, side_recv = sems[:7]
    up_send, up_recv, down_send, down_recv = sems[7:]
    tokens = own_ref.shape[0]
    half = tokens // 2

    def spot(l, s, w, k, h):
        return out_ref.at[pl.ds((((l * 2 + s) * 2 + w) * 2 + k) * tokens + h * half, half)]

    def source(l, s, w, h, here):
        return own_ref.at[pl.ds(h * half, half)] if here else spot(l, s, w, core, h)

    def core_copy(l, s, w, h, here=False):
        n = ((l * 2 + s) * 2 + w) * 2 + h
        return remote(
            source(l, s, w, h, here),
            spot(l, s, w, core, h),
            core_send.at[n],
            core_recv.at[n],
            core_mate,
        )

    def wide_copy(l, s, h, here=False):
        n = (l * 2 + h) * 2 + (0 if ways[h] else s)
        return remote(
            source(l, s, wide, h, here),
            spot(l, s, wide, core, h),
            wide_send.at[n],
            wide_recv.at[n],
            wide_mate,
        )

    def side_copy(l, w, h, here=False):
        n = (l * 2 + h) * 2 + (w if ways[h] else 0)
        return remote(
            source(l, side, w, h, here),
            spot(l, side, w, core, h),
            side_send.at[n],
            side_recv.at[n],
            side_mate,
        )

    def line_copy(l, h, up, here=False):
        n = l * 2 + h
        return remote(
            source(l, side, wide, h, here),
            spot(l, side, wide, core, h),
            (up_send if up else down_send).at[n],
            (up_recv if up else down_recv).at[n],
            above if up else below,
        )

    def local(h):
        return pltpu.make_async_copy(
            own_ref.at[pl.ds(h * half, half)], spot(line, side, wide, core, h), local_sem.at[h]
        )

    def spread(l, h, here=False):
        if ways[h]:
            wide_copy(l, side, h, here).start()
            side_copy(l, wide, h, here).start()
        else:
            side_copy(l, wide, h, here).start()
            wide_copy(l, side, h, here).start()
        core_copy(l, side, wide, h, here).start()

    def second(l):
        for h in range(2):
            if ways[h]:
                wide_copy(l, side, h).wait_recv()
                side_copy(l, 1 - wide, h).start()
                core_copy(l, side, 1 - wide, h).start()
            else:
                side_copy(l, wide, h).wait_recv()
                wide_copy(l, 1 - side, h).start()
                core_copy(l, 1 - side, wide, h).start()

    def third(l):
        for j in range(2):
            for h in range(2):
                if ways[h]:
                    w = 1 - wide if j else wide
                    side_copy(l, w, h).wait_recv()
                    core_copy(l, 1 - side, w, h).start()
                else:
                    s = 1 - side if j else side
                    wide_copy(l, s, h).wait_recv()
                    core_copy(l, s, 1 - wide, h).start()

    def start():
        for h in range(2):

            @pl.when(has_above)
            def _(h=h):
                line_copy(line, h, True, True).start()

            @pl.when(has_below)
            def _(h=h):
                line_copy(line, h, False, True).start()

            spread(line, h, True)
        for h in range(2):
            local(h).start()

    def from_line(dist, up):
        l = line - dist if up else line + dist

        @pl.when(l >= 0 if up else l < lines)
        def _():
            for h in range(2):
                line_copy(l, h, up).wait_recv()

                @pl.when(has_above if up else has_below)
                def _(h=h):
                    line_copy(l, h, up).start()

                spread(l, h)

    def stage(action, dist):
        if dist == 0:
            action(line)
            return

        @pl.when(line - dist >= 0)
        def _():
            action(line - dist)

        @pl.when(line + dist < lines)
        def _():
            action(line + dist)

    def step(dist):
        if dist < lines:
            from_line(dist, True)
            from_line(dist, False)
        if dist - 1 < lines:
            stage(second, dist - 1)
        if 0 <= dist - 2 < lines:
            stage(third, dist - 2)

    def finish():
        for h in range(2):
            local(h).wait()
        for l in range(lines):
            for s in range(2):
                for w in range(2):
                    for h in range(2):
                        core_copy(l, s, w, h).wait()
            for h in range(2):
                for j in range(1 if ways[h] else 2):
                    wide_copy(l, side if ways[h] else j, h).wait_send()
                for j in range(2 if ways[h] else 1):
                    side_copy(l, j if ways[h] else wide, h).wait_send()

                @pl.when(jnp.logical_and(has_above, line >= l))
                def _(h=h, l=l):
                    line_copy(l, h, True).wait_send()

                @pl.when(jnp.logical_and(has_below, line <= l))
                def _(h=h, l=l):
                    line_copy(l, h, False).wait_send()

    return start, step, finish


def gather_body(lines, dims, flips, ways, kinds, *refs):
    has_row, has_every, has_small = kinds
    count = len(dims)
    outputs = count + has_row + has_every + has_small
    ins, outs, sems = refs[:outputs], refs[outputs : 2 * outputs], list(refs[2 * outputs :])
    spots = places()
    wide, core, line, side = spots
    core_mate, wide_mate = row_mates(*spots)
    partners = [(core >= 0, core_mate), (core >= 0, wide_mate)]
    if count or has_every:
        partners += [
            (core >= 0, to_place(wide, core, line, 1 - side)),
            (line < lines - 1, to_place(wide, core, line + 1, side)),
            (line > 0, to_place(wide, core, line - 1, side)),
        ]
    greet(partners, has_small)

    def take(n):
        taken, sems[:] = sems[:n], sems[n:]
        return taken

    plans, at = [], count
    if count:
        plans.append(cols_plan(lines, dims, flips, spots, ins[:count], outs[:count], take(7)))
    if has_row:
        plans.append(row_plan(spots, ins[at], outs[at], take(5)))
        at += 1
    if has_every:
        plans.append(every_plan(lines, ways, spots, ins[at], outs[at], take(11)))
        at += 1
    if has_small:
        small_start, small_finish = small_exchange(ins[at], outs[at], *take(2), False)
        small_start()
    for start, _, _ in plans:
        start()
    for dist in range(1, lines + 2):
        for _, step, _ in plans:
            step(dist)
    if has_small:
        small_finish()
    for _, _, finish in plans:
        finish()


def kernel_gather(col_values, dims, flips, row_value, every_value, ways, small_value, number):
    n_row, n_col = lax.axis_size("row"), lax.axis_size("col")
    lines, count, total = n_col // 2, len(dims), n_row * n_col
    hbm, vmem = pl.BlockSpec(memory_space=pl.ANY), pl.BlockSpec(memory_space=pltpu.VMEM)
    dma = pltpu.SemaphoreType.DMA
    operands, in_specs, out_specs, out_shape = list(col_values), [hbm] * count, [hbm] * count, []
    scratch = []
    for value, dim in zip(col_values, dims):
        shape = list(value.shape)
        shape[dim] *= n_col
        out_shape.append(jax.ShapeDtypeStruct(tuple(shape), value.dtype))
    if count:
        scratch += [dma((count,))] + [dma((count * lines,))] * 2
        scratch += [dma((2 * count * lines,))] * 4
    if row_value is not None:
        scratch += [dma((1,)), dma((2,)), dma((2,)), dma((1,)), dma((1,))]
    if every_value is not None:
        scratch += [dma((2,)), *[dma((8 * lines,))] * 2, *[dma((4 * lines,))] * 4]
        scratch += [dma((2 * lines,))] * 4
    for value, times in ((row_value, n_row), (every_value, total)):
        if value is not None:
            operands.append(value)
            in_specs.append(vmem)
            out_specs.append(hbm)
            shape = (times * value.shape[0], *value.shape[1:])
            out_shape.append(jax.ShapeDtypeStruct(shape, value.dtype))
    if small_value is not None:
        operands.append(small_value)
        in_specs.append(vmem)
        out_specs.append(vmem)
        out_shape.append(jax.ShapeDtypeStruct((total, *small_value.shape), small_value.dtype))
        scratch += [dma((total,))] * 2
    kinds = tuple(value is not None for value in (row_value, every_value, small_value))
    return pl.pallas_call(
        functools.partial(gather_body, lines, tuple(dims), tuple(flips), ways, kinds),
        out_shape=out_shape,
        in_specs=in_specs,
        out_specs=out_specs,
        scratch_shapes=scratch,
        compiler_params=pltpu.CompilerParams(collective_id=number, has_side_effects=True),
        name=f"gather_{number}",
    )(*operands)


def mixed_total_body(lines, dims, flips, *refs):
    count = len(dims)
    cols, row_ref, refs = refs[:count], refs[count], refs[count + 1 :]
    col_outs, row_out, refs = refs[:count], refs[count], refs[count + 1 :]
    row_own, row_core, row_wide, refs = refs[0], refs[1], refs[2], refs[3:]
    owns, refs = refs[:count], refs[count:]
    side_ins, refs = refs[:count], refs[count:]
    up_ins, refs = refs[:count], refs[count:]
    down_ins, refs = refs[:count], refs[count:]
    row_load, core_send, core_recv, wide_send, wide_recv = refs[:5]
    if count:
        load_sem, side_send, side_recv, up_send, up_recv, down_send, down_recv = refs[5:12]
    wide, core, line, side = places()
    core_mate, wide_mate = row_mates(wide, core, line, side)
    side_mate = to_place(wide, core, line, 1 - side)
    above = to_place(wide, core, line + 1, side)
    below = to_place(wide, core, line - 1, side)
    has_above = line < lines - 1
    has_below = line > 0
    partners = [(core >= 0, core_mate), (core >= 0, wide_mate)]
    if count:
        partners += [(core >= 0, side_mate), (has_above, above), (has_below, below)]
    greet(partners, False)
    tokens = row_out.shape[0]

    def core_copy(w):
        return remote(
            strip(row_ref, 0, w * 2 + 1 - core, tokens),
            row_core.at[w],
            core_send.at[w],
            core_recv.at[w],
            core_mate,
        )

    def row_loaded(w):
        return pltpu.make_async_copy(
            strip(row_ref, 0, w * 2 + core, tokens), row_own.at[w], row_load.at[w]
        )

    wide_copy = remote(row_own.at[1 - wide], row_wide, wide_send.at[0], wide_recv.at[0], wide_mate)

    def source(m, l, s):
        return strip(cols[m], dims[m], l * 2 + s, col_outs[m].shape[dims[m]])

    def side_copy(m, l):
        n = m * lines + l
        return remote(
            owns[m].at[l, 1 - side] if flips[m] else source(m, l, 1 - side),
            side_ins[m].at[0 if flips[m] else l],
            side_send.at[n],
            side_recv.at[n],
            side_mate,
        )

    def own_at(m, l, s):
        return owns[m].at[l, s] if flips[m] else owns[m].at[l]

    def loaded(m, l, s):
        return pltpu.make_async_copy(
            source(m, l, s), own_at(m, l, s), load_sem.at[(m * lines + l) * 2 + s]
        )

    def line_copy(m, l, s, up):
        n = (m * lines + l) * 2 + s
        into = (up_ins if up else down_ins)[m]
        return remote(
            own_at(m, l, s),
            into.at[l, s] if flips[m] else into.at[l],
            (up_send if up else down_send).at[n],
            (up_recv if up else down_recv).at[n],
            above if up else below,
        )

    def sides(m):
        return (1 - side, side) if flips[m] else (side,)

    for w in range(2):
        core_copy(w).start()
        row_loaded(w).start()
    items = [(m, l) for l in (line_order(lines) if count else []) for m in range(count)]
    for m, l in items:
        for s in sides(m):
            loaded(m, l, s).start()
        if not flips[m]:
            side_copy(m, l).start()
    for j in range(2):
        w = wide if j else 1 - wide
        row_loaded(w).wait()
        core_copy(w).wait_recv()
        row_own[w] = (row_own[w].astype(F32) + row_core[w].astype(F32)).astype(BF16)
        if j == 0:
            wide_copy.start()

    def add(m, l, s, other):
        mine = own_at(m, l, s)
        mine[...] = (mine[...].astype(F32) + other.astype(F32)).astype(BF16)

    def near(m, l):
        for s in sides(m):
            loaded(m, l, s).wait()
            if not flips[m]:
                side_copy(m, l).wait_recv()
                add(m, l, s, side_ins[m][l])

            @pl.when(jnp.logical_and(line == 0, l > 0))
            def _(s=s):
                line_copy(m, l, s, True).start()

            @pl.when(jnp.logical_and(line == lines - 1, l < lines - 1))
            def _(s=s):
                line_copy(m, l, s, False).start()

    def onward(m, l, up):
        @pl.when(jnp.logical_and(has_below, has_above))
        def _():
            for s in sides(m):
                where = (l, s) if flips[m] else (l,)
                line_copy(m, l, s, up).wait_recv()
                add(m, l, s, (up_ins if up else down_ins)[m][where])
                line_copy(m, l, s, up).start()

    def passing(m, j):
        high, low = lines - 1 - j, j
        lower_half = line * 2 < lines

        def go(up, when):
            l = high if up else low
            beyond = line < l if up else line > l

            @pl.when(jnp.logical_and(when, beyond))
            def _():
                onward(m, l, up)

        go(True, lower_half)
        go(False, lower_half)
        go(False, jnp.logical_not(lower_half))
        go(True, jnp.logical_not(lower_half))

    def final(m):
        for s in sides(m):
            where = (line, s) if flips[m] else (line,)

            @pl.when(has_below)
            def _(s=s, where=where):
                line_copy(m, line, s, True).wait_recv()
                add(m, line, s, up_ins[m][where])

            @pl.when(has_above)
            def _(s=s, where=where):
                line_copy(m, line, s, False).wait_recv()
                add(m, line, s, down_ins[m][where])

        if flips[m]:
            side_copy(m, line).start()

    flipped = [m for m in range(count) if flips[m]]
    straight = [m for m in range(count) if not flips[m]]
    order = line_order(lines)
    for l in order:
        for m in flipped:
            near(m, l)
    if count:
        for step in range(lines + 2):
            if step < lines:
                for m in straight:
                    near(m, order[step])
            if step < lines - 1:
                for m in flipped:
                    passing(m, step)
            if step == lines - 1:
                for m in flipped:
                    final(m)
            if 2 <= step < lines + 1:
                for m in straight:
                    passing(m, step - 2)
            if step == lines + 1:
                for m in straight:
                    final(m)
    wide_copy.wait()
    row_out[...] = row_own[wide].astype(F32) + row_wide[...].astype(F32)
    for w in range(2):
        core_copy(w).wait_send()
    for m in range(count):
        if flips[m]:
            side_copy(m, line).wait()
            add(m, line, side, side_ins[m][0])
        col_outs[m][...] = own_at(m, line, side)[...].astype(F32)
        for l in range(lines):
            if not flips[m]:
                side_copy(m, l).wait_send()
            for s in sides(m):

                @pl.when(jnp.logical_and(has_above, line < l))
                def _(m=m, l=l, s=s):
                    line_copy(m, l, s, True).wait_send()

                @pl.when(jnp.logical_and(has_below, line > l))
                def _(m=m, l=l, s=s):
                    line_copy(m, l, s, False).wait_send()


def mixed_total(col_values, dims, flips, row_value, number):
    n_row, n_col = lax.axis_size("row"), lax.axis_size("col")
    lines, count = n_col // 2, len(dims)
    tokens, width = row_value.shape[0] // n_row, row_value.shape[1]
    hbm, vmem = pl.BlockSpec(memory_space=pl.ANY), pl.BlockSpec(memory_space=pltpu.VMEM)
    blocks = []
    for value, dim in zip(col_values, dims):
        shape = list(value.shape)
        shape[dim] //= n_col
        blocks.append(tuple(shape))
    dma = pltpu.SemaphoreType.DMA
    scratch = [
        pltpu.VMEM((2, tokens, width), BF16),
        pltpu.VMEM((2, tokens, width), BF16),
        pltpu.VMEM((tokens, width), BF16),
    ]
    doubled = [(lines, 2) if flip else (lines,) for flip in flips]
    side_held = [(1,) if flip else (lines,) for flip in flips]
    for lead in (doubled, side_held, doubled, doubled):
        scratch += [pltpu.VMEM((*d, *shape), BF16) for d, shape in zip(lead, blocks)]
    scratch += [dma((2,)), dma((2,)), dma((2,)), dma((1,)), dma((1,))]
    if count:
        scratch += [dma((2 * count * lines,))] + [dma((count * lines,))] * 2
        scratch += [dma((2 * count * lines,))] * 4
    return pl.pallas_call(
        functools.partial(mixed_total_body, lines, tuple(dims), tuple(flips)),
        out_shape=[jax.ShapeDtypeStruct(shape, F32) for shape in blocks]
        + [jax.ShapeDtypeStruct((tokens, width), F32)],
        in_specs=[hbm] * (count + 1),
        out_specs=[vmem] * (count + 1),
        scratch_shapes=scratch,
        compiler_params=pltpu.CompilerParams(
            collective_id=number, has_side_effects=True, vmem_limit_bytes=VMEM_LIMIT
        ),
        name=f"mixed_total_{number}",
    )(*col_values, row_value)


def row_sum_body(value_ref, out_ref, held, core_in, wide_in, *sems):
    one_send, one_recv, two_send, two_recv, core_send, core_recv, wide_send, wide_recv = sems
    wide, core, line, side = places()
    core_mate, wide_mate = row_mates(wide, core, line, side)
    greet([(core >= 0, core_mate), (core >= 0, wide_mate)], False)
    tokens = wide_in.shape[0]

    def block(ref, w, k):
        return strip(ref, 0, w * 2 + k, tokens)

    ones = [
        remote(block(value_ref, w, 1 - core), core_in.at[w], one_send.at[w], one_recv.at[w], core_mate)
        for w in range(2)
    ]
    two = remote(held.at[1 - wide], wide_in, two_send.at[0], two_recv.at[0], wide_mate)
    for copy in ones:
        copy.start()
    for w in range(2):
        ones[w].wait_recv()
        held[w] = (block(value_ref, w, core)[...].astype(F32) + core_in[w].astype(F32)).astype(BF16)
    two.start()
    two.wait_recv()
    held[wide] = (held[wide].astype(F32) + wide_in[...].astype(F32)).astype(BF16)

    def to_core(n):
        w = wide if n == 0 else 1 - wide
        src = held.at[wide] if n == 0 else block(out_ref, w, core)
        return remote(src, block(out_ref, w, core), core_send.at[n], core_recv.at[n], core_mate)

    to_wide = remote(
        held.at[wide], block(out_ref, wide, core), wide_send.at[0], wide_recv.at[0], wide_mate
    )
    to_wide.start()
    to_core(0).start()
    block(out_ref, wide, core)[...] = held[wide]
    to_wide.wait_recv()
    to_core(1).start()
    for n in range(2):
        to_core(n).wait()
    to_wide.wait_send()
    two.wait_send()
    for copy in ones:
        copy.wait_send()


def row_sum(value, number):
    n_row = lax.axis_size("row")
    if n_row != 4:
        return lax.psum(value, "row")
    tokens, width = value.shape[0] // n_row, value.shape[1]
    dma = pltpu.SemaphoreType.DMA
    return pl.pallas_call(
        row_sum_body,
        out_shape=jax.ShapeDtypeStruct(value.shape, value.dtype),
        in_specs=[pl.BlockSpec(memory_space=pltpu.VMEM)],
        out_specs=pl.BlockSpec(memory_space=pltpu.VMEM),
        scratch_shapes=[
            pltpu.VMEM((2, tokens, width), value.dtype),
            pltpu.VMEM((2, tokens, width), value.dtype),
            pltpu.VMEM((tokens, width), value.dtype),
            dma((2,)),
            dma((2,)),
            dma((1,)),
            dma((1,)),
            dma((2,)),
            dma((2,)),
            dma((1,)),
            dma((1,)),
        ],
        compiler_params=pltpu.CompilerParams(collective_id=number, has_side_effects=True),
        name=f"row_sum_{number}",
    )(value)


def finish_body(value_ref, gains_ref, out_ref, sums_ref, row_in, held, *sems):
    local_sem, value_send, value_recv, row_send, row_recv, col_send, col_recv = sems
    n_row, n_col = lax.axis_size("row"), lax.axis_size("col")
    row, col = lax.axis_index("row"), lax.axis_index("col")
    rows = [{"row": lax.rem(row + d, n_row), "col": col} for d in range(1, n_row)]
    cols = [{"row": row, "col": lax.rem(col + d, n_col)} for d in range(1, n_col)]
    greet([(row >= 0, partner) for partner in rows + cols], False)
    tokens = value_ref.shape[0]

    def value_copy(d, source):
        return remote(
            value_ref,
            strip(out_ref, 0, source, tokens),
            value_send.at[d],
            value_recv.at[source],
            rows[d],
        )

    def row_copy(d, source):
        return remote(gains_ref, row_in.at[source], row_send.at[d], row_recv.at[source], rows[d])

    def col_copy(d, source):
        return remote(held, sums_ref.at[source], col_send.at[d], col_recv.at[source], cols[d])

    for d in range(n_row - 1):
        row_copy(d, row).start()
    for d in range(n_row - 1):
        value_copy(d, row).start()
    local = pltpu.make_async_copy(value_ref, strip(out_ref, 0, row, tokens), local_sem)
    local.start()
    total = gains_ref[...]
    for d in range(n_row - 1):
        source = rows[d]["row"]
        row_copy(d, source).wait_recv()
        total = total + row_in[source]
    held[...] = total
    for d in range(n_col - 1):
        col_copy(d, col).start()
    sums_ref[col] = total
    for d in range(n_row - 1):
        value_copy(d, rows[d]["row"]).wait_recv()
        value_copy(d, row).wait_send()
        row_copy(d, row).wait_send()
    for d in range(n_col - 1):
        col_copy(d, cols[d]["col"]).wait_recv()
        col_copy(d, col).wait_send()
    local.wait()


def kernel_finish(value, gains, number):
    n_row, n_col = lax.axis_size("row"), lax.axis_size("col")
    dma = pltpu.SemaphoreType.DMA
    vmem = pl.BlockSpec(memory_space=pltpu.VMEM)
    return pl.pallas_call(
        finish_body,
        out_shape=[
            jax.ShapeDtypeStruct((n_row * value.shape[0], value.shape[1]), value.dtype),
            jax.ShapeDtypeStruct((n_col, *gains.shape), gains.dtype),
        ],
        in_specs=[vmem, vmem],
        out_specs=[vmem, vmem],
        scratch_shapes=[
            pltpu.VMEM((n_row, *gains.shape), gains.dtype),
            pltpu.VMEM(gains.shape, gains.dtype),
            dma,
            dma((n_row - 1,)),
            dma((n_row,)),
            dma((n_row - 1,)),
            dma((n_row,)),
            dma((n_col - 1,)),
            dma((n_col,)),
        ],
        compiler_params=pltpu.CompilerParams(collective_id=number, has_side_effects=True),
        name=f"finish_{number}",
    )(value, gains)


def total_every(place, partials, small_value, number):
    blocks, slot_count, tokens = place.shape
    if kernel_fits(blocks * tokens, partials[0][0].shape[2], len(partials)):
        return kernel_total(place, partials, small_value, number)
    capacity = partials[0][0].shape[1] // blocks
    exchanged = lax.all_to_all(small_value, EVERY, split_axis=0, concat_axis=0, tiled=True)
    return *[every_total(combine_rows(place, *p, capacity)) for p in partials], exchanged


def mixed_fits(col_values):
    n_row, lines = lax.axis_size("row"), lax.axis_size("col") // 2
    return n_row == 4 and (not col_values or (lax.axis_size("col") % 2 == 0 and lines <= 8))


def gather(col_values, dims, flips, row_value, every_value, ways, small_value, number):
    fits = not col_values and every_value is None or lax.axis_size("col") in (4, 6, 8, 10)
    if lax.axis_size("row") == 4 and fits:
        return kernel_gather(
            col_values, dims, flips, row_value, every_value, ways, small_value, number
        )
    out = [lax.all_gather(v, "col", axis=d, tiled=True) for v, d in zip(col_values, dims)]
    if row_value is not None:
        out.append(token_rows(row_value))
    if every_value is not None:
        out.append(every_token(every_value))
    if small_value is not None:
        out.append(every_token(small_value[None]))
    return out


def total_mixed(col_values, dims, flips, row_value, number):
    if mixed_fits(col_values):
        return mixed_total(col_values, dims, flips, row_value, number)
    return *[col_total(v, d) for v, d in zip(col_values, dims)], row_total(row_value)


def padded_rows(values):
    return jnp.pad(values, ((0, -values.shape[0] % 8), (0, 0)))


def masked_scores(queries, attn_keys, allowed, softmax_scale):
    scores = (
        jnp.einsum("qhd,khd->hqk", queries, attn_keys, preferred_element_type=jnp.float32)
        * softmax_scale
    )
    return jnp.where(allowed[None], scores, -1e30)


def tokens_body(
    group,
    capacity,
    place_ref,
    x_ref,
    g_ref,
    both_ref,
    down_ref,
    xs_ref,
    gs_ref,
    hidden_ref,
    grad_ref,
    dboth_ref,
    ddown_ref,
):
    tokens = place_ref.shape[2]
    for block in range(group):
        rows = slice(block * tokens, (block + 1) * tokens)
        for source, slots in ((x_ref, xs_ref), (g_ref, gs_ref)):
            picked = matmul(place_ref[block], source[rows, :])
            slots[:, block] = picked.astype(BF16).reshape(-1, capacity, picked.shape[-1])
    half = down_ref.shape[0]
    both = outer_cols(x_ref[...], both_ref[...])
    act, slope = silu_parts(both[:, :half])
    lin = both[:, half:]
    hidden = (act * lin).astype(BF16)
    back = outer_cols(g_ref[...], down_ref[...])
    grads = jnp.concatenate([back * lin * slope, back * act], axis=1).astype(BF16)
    hidden_ref[...] = hidden
    grad_ref[...] = grads
    dboth = inner_rows(grads, x_ref[...])
    ddown = inner_rows(hidden, g_ref[...])

    @pl.when(pl.program_id(0) == 0)
    def _():
        dboth_ref[...] = dboth
        ddown_ref[...] = ddown

    @pl.when(pl.program_id(0) > 0)
    def _():
        dboth_ref[...] += dboth
        ddown_ref[...] += ddown


def run_tokens(place, x_all, g_all, both_weight, down_weight, local_experts):
    blocks, slots, tokens = place.shape
    capacity = slots // local_experts
    width = x_all.shape[1]
    half = down_weight.shape[0]
    group = 4 if blocks % 4 == 0 else 1
    row_block = pl.BlockSpec((group * tokens, width), lambda i: (i, 0))
    slot_block = pl.BlockSpec((local_experts, group, capacity, width), lambda i: (0, i, 0, 0))
    slot_shape = jax.ShapeDtypeStruct((local_experts, blocks, capacity, width), BF16)

    def whole(size):
        return pl.BlockSpec((size, width), lambda i: (0, 0))

    def hidden_block(size):
        return pl.BlockSpec((group * tokens, size), lambda i: (i, 0))

    rows = blocks * tokens
    xs, gs, hidden, grads, dboth, ddown = pl.pallas_call(
        functools.partial(tokens_body, group, capacity),
        grid=(blocks // group,),
        in_specs=[
            pl.BlockSpec((group, slots, tokens), lambda i: (i, 0, 0)),
            row_block,
            row_block,
            whole(2 * half),
            whole(half),
        ],
        out_specs=[
            slot_block,
            slot_block,
            hidden_block(half),
            hidden_block(2 * half),
            whole(2 * half),
            whole(half),
        ],
        out_shape=[
            slot_shape,
            slot_shape,
            jax.ShapeDtypeStruct((rows, half), BF16),
            jax.ShapeDtypeStruct((rows, 2 * half), BF16),
            jax.ShapeDtypeStruct((2 * half, width), F32),
            jax.ShapeDtypeStruct((half, width), F32),
        ],
        compiler_params=pltpu.CompilerParams(vmem_limit_bytes=VMEM_LIMIT),
        cost_estimate=pl.CostEstimate(
            flops=2 * rows * width * (2 * slots + 6 * half),
            bytes_accessed=8 * rows * width,
            transcendentals=rows * half,
        ),
        name="run_tokens",
    )(place, x_all, g_all, both_weight, down_weight)
    shape = (local_experts, blocks * capacity, width)
    return xs.reshape(shape), gs.reshape(shape), hidden, grads, dboth, ddown


def experts_body(
    x_ref, g_ref, gate_ref, wg_ref, wu_ref, wd_ref, y_ref, r_ref, dg_ref, du_ref, dd_ref, gg_ref
):
    first = pl.program_id(1) == 0
    x = x_ref[0]
    g = g_ref[0]
    gate = gate_ref[0]
    pre = outer_cols(x, wg_ref[0])
    lin = outer_cols(x, wu_ref[0])
    back = outer_cols(g, wd_ref[0])
    act, slope = silu_parts(pre)
    hidden = act * lin
    gg_ref[0] = jnp.sum(hidden * back, axis=-1, keepdims=True)
    hidden = (hidden * gate).astype(BF16)
    back = back * gate
    pre_grad = (back * lin * slope).astype(BF16)
    lin_grad = (back * act).astype(BF16)
    width = x_ref.shape[2]
    chunk = 512 if width % 512 == 0 else width
    for start in range(0, width, chunk):
        cols = slice(start, start + chunk)
        y_ref[0, :, cols] = matmul(hidden, wd_ref[0, :, cols]).astype(BF16)
        r_ref[0, :, cols] = (
            matmul(pre_grad, wg_ref[0, :, cols]) + matmul(lin_grad, wu_ref[0, :, cols])
        ).astype(BF16)
        d_gate = inner_rows(pre_grad, x_ref[0, :, cols])
        d_up = inner_rows(lin_grad, x_ref[0, :, cols])
        d_down = inner_rows(hidden, g_ref[0, :, cols])

        @pl.when(first)
        def _():
            dg_ref[0, :, cols] = d_gate
            du_ref[0, :, cols] = d_up
            dd_ref[0, :, cols] = d_down

        @pl.when(jnp.logical_not(first))
        def _():
            dg_ref[0, :, cols] += d_gate
            du_ref[0, :, cols] += d_up
            dd_ref[0, :, cols] += d_down


def run_experts(x_slots, g_slots, gates, w_gate, w_up, w_down):
    count, rows, width = x_slots.shape
    hidden = w_down.shape[1]
    chunk = 512 if rows % 512 == 0 else rows
    row_block = pl.BlockSpec((1, chunk, width), lambda e, r: (e, r, 0))
    col_block = pl.BlockSpec((1, chunk, 1), lambda e, r: (e, r, 0))
    out_block = pl.BlockSpec((1, hidden, width), lambda e, r: (e, 0, 0))
    y, r, d_gate, d_up, d_down, dots = pl.pallas_call(
        experts_body,
        grid=(count, rows // chunk),
        in_specs=[row_block, row_block, col_block, out_block, out_block, out_block],
        out_specs=[row_block, row_block, out_block, out_block, out_block, col_block],
        out_shape=[
            jax.ShapeDtypeStruct((count, rows, width), BF16),
            jax.ShapeDtypeStruct((count, rows, width), BF16),
            jax.ShapeDtypeStruct((count, hidden, width), F32),
            jax.ShapeDtypeStruct((count, hidden, width), F32),
            jax.ShapeDtypeStruct((count, hidden, width), F32),
            jax.ShapeDtypeStruct((count, rows, 1), F32),
        ],
        compiler_params=pltpu.CompilerParams(vmem_limit_bytes=VMEM_LIMIT),
        cost_estimate=pl.CostEstimate(
            flops=18 * count * rows * width * hidden,
            bytes_accessed=count * (8 * rows * width + 18 * width * hidden),
            transcendentals=count * rows * hidden,
        ),
        name="run_experts",
    )(x_slots, g_slots, gates, w_gate.transpose(0, 2, 1), w_up.transpose(0, 2, 1), w_down)
    return y, r, d_gate.transpose(0, 2, 1), d_up.transpose(0, 2, 1), d_down, dots


def combine_body(group, place_ref, slots_ref, extra_ref, weight_ref, out_ref):
    tokens = place_ref.shape[2]
    width = out_ref.shape[1]
    for block in range(group):
        rows = slice(block * tokens, (block + 1) * tokens)
        total = inner_rows(place_ref[block], slots_ref[:, block].reshape(-1, width))
        total += matmul(extra_ref[rows, :], weight_ref[...])
        out_ref[rows, :] = total.astype(BF16)


def combine_rows(place, slots, extra, weight, capacity):
    blocks, slot_count, tokens = place.shape
    local_experts, _, width = slots.shape
    group = 4 if blocks % 4 == 0 else 1
    inner = extra.shape[1]
    return pl.pallas_call(
        functools.partial(combine_body, group),
        grid=(blocks // group,),
        in_specs=[
            pl.BlockSpec((group, slot_count, tokens), lambda i: (i, 0, 0)),
            pl.BlockSpec((local_experts, group, capacity, width), lambda i: (0, i, 0, 0)),
            pl.BlockSpec((group * tokens, inner), lambda i: (i, 0)),
            pl.BlockSpec((inner, width), lambda i: (0, 0)),
        ],
        out_specs=pl.BlockSpec((group * tokens, width), lambda i: (i, 0)),
        out_shape=jax.ShapeDtypeStruct((blocks * tokens, width), BF16),
        compiler_params=pltpu.CompilerParams(vmem_limit_bytes=VMEM_LIMIT),
        cost_estimate=pl.CostEstimate(
            flops=2 * blocks * tokens * (slot_count + inner) * width,
            bytes_accessed=4 * blocks * tokens * width,
            transcendentals=0,
        ),
        name="combine_rows",
    )(place, slots.reshape(local_experts, blocks, capacity, width), extra, weight)


def on_device(
    inputs,
    segment_ids,
    routes,
    first_gain,
    query_weight,
    latent_down,
    latent_gain,
    latent_up,
    output_weight,
    second_gain,
    router_weight,
    shared_gate,
    shared_up,
    shared_down,
    expert_gate,
    expert_up,
    expert_down,
    cotangent,
):
    n_row = lax.axis_size("row")
    n_col = lax.axis_size("col")
    blocks = n_row * n_col
    own_row = lax.axis_index("row")
    own_col = lax.axis_index("col")
    own_rows = inputs.shape[1]
    width = inputs.shape[2]
    experts = router_weight.shape[1]
    local_experts = expert_gate.shape[0]
    capacity = max(2, own_rows // 8)
    stream = inputs.reshape(own_rows, width).astype(F32)
    grad_out = cotangent.reshape(own_rows, width)
    own_routes = routes.reshape(own_rows, TOPK)
    segments = segment_ids.reshape(-1)
    length = segments.shape[0]
    own_start = own_row * own_rows
    qk_dim = NOPE + ROPE
    softmax_scale = qk_dim ** (-0.5)
    cosine_table, sine_table = angle_tables(length)

    scale_one = rms_scale(stream)
    normed_one = (stream * scale_one * first_gain).astype(BF16)
    down_cols = latent_down.shape[1] // n_row
    own_down = lax.dynamic_slice_in_dim(latent_down, own_row * down_cols, down_cols, 1)
    output_rows = output_weight.shape[0]
    query_cols = query_weight.shape[1]
    query_all, output_down, expand_all, seq_normed, grad_all, all_routes = gather(
        [query_weight, jnp.concatenate([output_weight, own_down.T], axis=0), latent_up],
        [0, 1, 0],
        [False, False, True],
        normed_one,
        grad_out.astype(BF16),
        (0, 0),
        padded_rows(own_routes.astype(F32).T),
        1,
    )
    output_all = output_down[:output_rows]
    down_all = output_down[output_rows:]

    all_routes = all_routes[:, :TOPK].astype(jnp.int32)
    local_ids = own_col * local_experts + jnp.arange(local_experts)
    named = all_routes[:, :, None, :] == local_ids[None, None, :, None]
    chosen_here = jnp.max(named.astype(BF16), axis=1)
    before = (jnp.arange(own_rows)[:, None] < jnp.arange(own_rows)[None, :]).astype(BF16)
    rank = matmul(chosen_here.reshape(-1, own_rows), before).reshape(chosen_here.shape)
    slot_of = jnp.where(chosen_here > 0, rank.astype(jnp.int32), -1)
    placed = slot_of[:, :, None, :] == jnp.arange(capacity)[None, None, :, None]
    place = placed.astype(BF16).reshape(blocks, local_experts * capacity, own_rows)

    shared_cols = shared_gate.shape[1] // n_col
    shared_send = jnp.stack([shared_gate.T, shared_up.T, shared_down], axis=0)
    depth = shared_send.shape[2]
    shared_send = (
        shared_send.reshape(3, n_col, shared_cols, depth)
        .transpose(1, 0, 2, 3)
        .reshape(n_col, 3 * shared_cols, depth)
    )
    shared_send, all_routes = lax.optimization_barrier((shared_send, all_routes))
    shared_own = (
        lax.all_to_all(shared_send, "col", split_axis=0, concat_axis=0, tiled=True)
        .transpose(1, 0, 2)
        .reshape(3, shared_cols, width)
    )
    shared_own = jnp.pad(shared_own, ((0, 0), (0, -shared_cols % 128), (0, 0)))
    shared_held = shared_own.shape[1]
    gate_up_own = shared_own[:2].reshape(2 * shared_held, width)
    down_own = shared_own[2]

    heads_local = query_cols // qk_dim
    query_raw = matmul(seq_normed, query_all).reshape(length, heads_local, qk_dim)
    queries = jnp.concatenate(
        [
            query_raw[..., :NOPE],
            rotate(query_raw[..., NOPE:], cosine_table[:, None, :], sine_table[:, None, :]),
        ],
        axis=-1,
    ).astype(BF16)
    (latent_all,) = gather(
        [], [], [], outer_cols(down_all, seq_normed), None, None, None, 8
    )
    latent_all = latent_all.T
    latent = latent_all[:, :LATENT]
    scale_latent = rms_scale(latent)
    latent_normed = (latent * scale_latent * latent_gain).astype(BF16)
    keyval = matmul(latent_normed, expand_all).reshape(length, heads_local, NOPE + VD)
    key_rope = rotate(latent_all[:, LATENT:], cosine_table, sine_table)
    attn_keys = jnp.concatenate(
        [keyval[..., :NOPE], jnp.broadcast_to(key_rope[:, None, :], (length, heads_local, ROPE))],
        axis=-1,
    ).astype(BF16)
    values = keyval[..., NOPE:].astype(BF16)
    positions = jnp.arange(length)
    allowed = (positions[:, None] >= positions[None, :]) & (segments[:, None] == segments[None, :])
    scores = masked_scores(queries, attn_keys, allowed, softmax_scale)
    highest = jnp.max(scores, axis=-1, keepdims=True)
    log_total = highest + jnp.log(jnp.sum(jnp.exp(scores - highest), axis=-1, keepdims=True))
    attn_probs = jnp.exp(scores - log_total).astype(BF16)
    heads_out = (
        jnp.einsum("hqk,khd->qhd", attn_probs, values, preferred_element_type=jnp.float32)
        .astype(BF16)
        .reshape(length, heads_local * VD)
    )
    (attn_total,) = total_mixed([], [], [], matmul(heads_out, output_all).astype(BF16), 6)
    residual = stream + attn_total

    scale_two = rms_scale(residual)
    normed_two = (residual * scale_two * second_gain).astype(BF16)
    logits = matmul(normed_two, router_weight)
    expert_ids = jnp.arange(experts)
    chosen = own_routes[:, :, None] == expert_ids[None, None, :]
    picked = jnp.sum(jnp.where(chosen, logits[:, None, :], 0.0), axis=-1)
    gate_probs = jax.nn.softmax(picked, axis=-1)

    all_normed, all_gates = gather(
        [], [], [], None, normed_two, (0, 1), padded_rows(gate_probs.T), 2
    )
    all_gates = all_gates[:, :TOPK]
    gate_here = jnp.sum(jnp.where(named, all_gates[:, :, None, :], 0.0), axis=1)
    slot_gate = jnp.sum(jnp.where(placed, gate_here[:, :, None, :], 0.0), axis=-1)
    slot_gate = slot_gate.transpose(1, 0, 2).reshape(local_experts, blocks * capacity, 1)
    normed_slots, grad_slots, shared_hidden, shared_both_grad, gate_up_part, down_part = run_tokens(
        place, all_normed, grad_all, gate_up_own, down_own, local_experts
    )
    out_slots, rows_slots, expert_gate_grad, expert_up_grad, expert_down_grad, slot_dot = (
        run_experts(normed_slots, grad_slots, slot_gate, expert_gate, expert_up, expert_down)
    )

    slot_dot = slot_dot.reshape(local_experts, blocks, capacity).transpose(1, 0, 2)
    token_dot = jnp.sum(jnp.where(placed, slot_dot[:, :, :, None], 0.0), axis=2)
    out_total, rows_total, token_dot = total_every(
        place,
        [
            (out_slots, shared_hidden, down_own),
            (rows_slots, shared_both_grad, gate_up_own),
        ],
        token_dot,
        3,
    )
    layer_out = (residual + out_total).astype(BF16).reshape(1, own_rows, width)
    shared_back = jnp.concatenate(
        [gate_up_part.reshape(2, shared_held, width), down_part[None]], axis=0
    )[:, :shared_cols].astype(BF16)
    shared_back = (
        shared_back.reshape(3 * shared_cols, n_col, depth).transpose(1, 0, 2)
    )
    shared_back = lax.all_to_all(shared_back, "col", split_axis=0, concat_axis=0, tiled=True)
    token_dot = jnp.sum(token_dot.reshape(n_col, n_row, local_experts, own_rows), axis=1)
    token_dot = token_dot.reshape(experts, own_rows).T
    gate_grad = jnp.sum(jnp.where(chosen, token_dot[:, None, :], 0.0), axis=-1)
    picked_grad = gate_probs * (gate_grad - jnp.sum(gate_probs * gate_grad, axis=-1, keepdims=True))
    logit_grad = jnp.sum(jnp.where(chosen, picked_grad[:, :, None], 0.0), axis=1).astype(BF16)

    normed_two_grad = rows_total + outer_cols(logit_grad, router_weight)
    second_gain_part = jnp.sum(normed_two_grad * residual * scale_two, axis=0)
    residual_grad = grad_out + rms_back(residual, scale_two, normed_two_grad * second_gain)

    seq_resid, all_picked = gather(
        [], [], [], residual_grad.astype(BF16), None, None, padded_rows(picked_grad.T), 4
    )
    all_named = all_routes[:, :, :, None] == expert_ids
    all_logit_grad = jnp.sum(jnp.where(all_named, all_picked[:, :TOPK, :, None], 0.0), axis=1)
    router_grad = inner_rows(all_normed, all_logit_grad.astype(BF16).reshape(-1, experts))
    output_part = inner_rows(heads_out, seq_resid)
    heads_grad = outer_cols(seq_resid, output_all).astype(BF16).reshape(length, heads_local, VD)
    recomputed = jnp.exp(masked_scores(queries, attn_keys, allowed, softmax_scale) - log_total)
    delta_rows = jnp.sum(
        heads_grad.astype(F32) * heads_out.reshape(length, heads_local, VD).astype(F32),
        axis=-1,
    )
    prob_grad = jnp.einsum("qhd,khd->hqk", heads_grad, values, preferred_element_type=jnp.float32)
    score_grad = (recomputed * (prob_grad - delta_rows.T[:, :, None]) * softmax_scale).astype(BF16)
    queries_grad = jnp.einsum(
        "hqk,khd->qhd", score_grad, attn_keys, preferred_element_type=jnp.float32
    )
    key_grad = jnp.einsum("hqk,qhd->khd", score_grad, queries, preferred_element_type=jnp.float32)
    value_grad = jnp.einsum(
        "hqk,qhd->khd",
        recomputed.astype(BF16),
        heads_grad,
        preferred_element_type=jnp.float32,
    )
    query_full = (
        jnp.concatenate(
            [
                queries_grad[..., :NOPE],
                unrotate(
                    queries_grad[..., NOPE:], cosine_table[:, None, :], sine_table[:, None, :]
                ),
            ],
            axis=-1,
        )
        .astype(BF16)
        .reshape(length, heads_local * qk_dim)
    )
    keyval_grad = (
        jnp.concatenate([key_grad[..., :NOPE], value_grad], axis=-1)
        .astype(BF16)
        .reshape(length, heads_local * (NOPE + VD))
    )
    expand_part = inner_rows(latent_normed, keyval_grad)
    latent_normed_part = outer_cols(keyval_grad, expand_all)
    rope_part = jnp.sum(key_grad[..., NOPE:], axis=1)
    latent_total = row_sum(
        jnp.concatenate([latent_normed_part, rope_part], axis=1).astype(BF16), 9
    ).astype(F32)
    latent_normed_grad, rope_raw = latent_total[:, :LATENT], latent_total[:, LATENT:]
    rope_grad = unrotate(rope_raw, cosine_table, sine_table)
    latent_gain_part = jnp.sum(
        lax.dynamic_slice_in_dim(
            latent_normed_grad * latent * scale_latent, own_start, own_rows, 0
        ),
        axis=0,
    )
    latent_grad = rms_back(latent, scale_latent, latent_normed_grad * latent_gain)
    down_grad_in = jnp.concatenate([latent_grad, rope_grad], axis=-1).astype(BF16)
    own_down_grad = lax.dynamic_slice_in_dim(down_grad_in, own_row * down_cols, down_cols, 1)
    output_down_part = jnp.concatenate(
        [output_part.astype(BF16), inner_rows(own_down_grad, seq_normed).astype(BF16)], axis=0
    )
    input_part = outer_cols(query_full, query_all) + matmul(own_down_grad, down_all)
    input_part, shared_back = lax.optimization_barrier((input_part, shared_back))
    query_grad, output_down_grad, latent_up_grad, normed_one_grad = total_mixed(
        [inner_rows(seq_normed, query_full).astype(BF16), output_down_part, expand_part.astype(BF16)],
        [0, 1, 0],
        [False, False, True],
        input_part.astype(BF16),
        7,
    )
    output_grad = output_down_grad[:output_rows]
    first_gain_part = jnp.sum(normed_one_grad * stream * scale_one, axis=0)
    input_grad = (
        residual_grad + rms_back(stream, scale_one, normed_one_grad * first_gain)
    ).reshape(1, own_rows, width)

    shared_back = (
        shared_back.reshape(n_col, 3, shared_cols, depth)
        .transpose(1, 0, 2, 3)
        .reshape(3, n_col * shared_cols, depth)
        .astype(F32)
    )
    shared_gate_grad = shared_back[0].T
    shared_up_grad = shared_back[1].T
    shared_down_grad = shared_back[2]

    gains = jnp.concatenate([first_gain_part, latent_gain_part, second_gain_part])
    gains = padded_rows(gains.reshape(-1, LATENT // 4))
    down_total, all_gains = kernel_finish(output_down_grad[output_rows:].astype(BF16), gains, 5)
    latent_down_grad = down_total.astype(F32).T
    gains = jnp.sum(all_gains, axis=0).reshape(-1)
    first_gain_grad = gains[:width]
    latent_gain_grad = gains[width : width + LATENT]
    second_gain_grad = gains[width + LATENT : 2 * width + LATENT]
    return (
        layer_out,
        input_grad,
        first_gain_grad,
        query_grad,
        latent_down_grad,
        latent_gain_grad,
        latent_up_grad,
        output_grad,
        second_gain_grad,
        router_grad,
        shared_gate_grad,
        shared_up_grad,
        shared_down_grad,
        expert_gate_grad,
        expert_up_grad,
        expert_down_grad,
    )


def solution(mesh):
    return jax.shard_map(
        on_device,
        mesh=mesh,
        in_specs=(
            P("col", "row", None),
            P("col", None),
            P("col", "row", None),
            P(),
            P("col", "row"),
            P("col", None),
            P(),
            P("col", "row"),
            P("row", "col"),
            P(),
            P(),
            P("col", "row"),
            P("col", "row"),
            P("row", "col"),
            P("col", None, "row"),
            P("col", None, "row"),
            P("col", "row", None),
            P("col", "row", None),
        ),
        out_specs=(
            P("col", "row", None),
            P("col", "row", None),
            P(),
            P("col", "row"),
            P("col", None),
            P(),
            P("col", "row"),
            P("row", "col"),
            P(),
            P(),
            P("col", "row"),
            P("col", "row"),
            P("row", "col"),
            P("col", None, "row"),
            P("col", None, "row"),
            P("col", "row", None),
        ),
        check_vma=False,
    )
```

```python
import functools

import jax
import jax.numpy as jnp
from jax import lax
from jax.experimental import pallas as pl
from jax.experimental.pallas import tpu as pltpu
from jax.sharding import PartitionSpec as P

NOPE = 128
ROPE = 64
LATENT = 512
VD = 128
TOPK = 6


EPS = 1e-06
ROWS_CONTRACT = (((0,), (0,)), ((), ()))
COLS_CONTRACT = (((1,), (1,)), ((), ()))


def matmul(left_side, right_side):
    return jnp.dot(left_side, right_side, preferred_element_type=jnp.float32)


def inner_rows(left_side, right_side):
    return lax.dot_general(left_side, right_side, ROWS_CONTRACT, preferred_element_type=jnp.float32)


def outer_cols(left_side, right_side):
    return lax.dot_general(left_side, right_side, COLS_CONTRACT, preferred_element_type=jnp.float32)


def rms_scale(values):
    return lax.rsqrt(jnp.mean(values * values, axis=-1, keepdims=True) + EPS)


def rms_back(values, scaling, gradient):
    return scaling * gradient - values * scaling**3 * jnp.mean(
        gradient * values, axis=-1, keepdims=True
    )


def silu_parts(preact):
    logistic = jax.nn.sigmoid(preact)
    return (preact * logistic, logistic * (1.0 + preact * (1.0 - logistic)))


def angle_tables(length):
    halfway = ROPE // 2
    frequency = 10000.0 ** (-2.0 * jnp.arange(halfway, dtype=jnp.float32) / ROPE)
    angles = jnp.arange(length, dtype=jnp.float32)[:, None] * frequency[None, :]
    return (jnp.cos(angles), jnp.sin(angles))


def rotate(values, cosine_in, sine_in):
    halfway = values.shape[-1] // 2
    leading = values[..., :halfway]
    trailing = values[..., halfway:]
    return jnp.concatenate(
        [leading * cosine_in - trailing * sine_in, leading * sine_in + trailing * cosine_in],
        axis=-1,
    )


def unrotate(values, cosine_in, sine_in):
    halfway = values.shape[-1] // 2
    leading = values[..., :halfway]
    trailing = values[..., halfway:]
    return jnp.concatenate(
        [leading * cosine_in + trailing * sine_in, trailing * cosine_in - leading * sine_in],
        axis=-1,
    )


F32 = jnp.float32
BF16 = jnp.bfloat16
EVERY = ("col", "row")
VMEM_LIMIT = 63 * 1024 * 1024


def token_rows(values):
    return lax.all_gather(values, "row", axis=0, tiled=True)


def every_token(values):
    return lax.all_gather(values, EVERY, axis=0, tiled=True)


def row_total(partial_value):
    return lax.psum_scatter(
        partial_value.astype(BF16), "row", scatter_dimension=0, tiled=True
    ).astype(F32)


def every_total(partial_value):
    return lax.psum_scatter(partial_value, EVERY, scatter_dimension=0, tiled=True).astype(F32)


def col_gather(values):
    return lax.all_gather(values, "col", axis=0, tiled=True)


def col_total(partial_value, dim):
    return lax.psum_scatter(
        partial_value.astype(BF16), "col", scatter_dimension=dim, tiled=True
    ).astype(F32)


MESH_ID = pl.DeviceIdType.MESH


def places():
    row, col = lax.axis_index("row"), lax.axis_index("col")
    return row // 2, lax.rem(row, 2), col // 2, lax.rem(col, 2)


def to_place(wide, core, line, side):
    return {"row": wide * 2 + core, "col": line * 2 + side}


def greet(partners, everyone):
    barrier = pltpu.get_barrier_semaphore()
    if everyone:
        n_row, n_col = lax.axis_size("row"), lax.axis_size("col")
        total = n_row * n_col
        me = lax.axis_index("col") * n_row + lax.axis_index("row")

        @pl.loop(1, total)
        def _(step):
            other = lax.rem(me + step, total)
            pl.semaphore_signal(
                barrier,
                inc=1,
                device_id={"row": lax.rem(other, n_row), "col": other // n_row},
                device_id_type=MESH_ID,
            )

        pl.semaphore_wait(barrier, total - 1)
        return
    for there, partner in partners:

        @pl.when(there)
        def _(partner=partner):
            pl.semaphore_signal(barrier, inc=1, device_id=partner, device_id_type=MESH_ID)

    pl.semaphore_wait(barrier, sum(jnp.int32(there) for there, _ in partners))


def remote(src, dst, send_sem, recv_sem, partner):
    return pltpu.make_async_remote_copy(
        src_ref=src,
        dst_ref=dst,
        send_sem=send_sem,
        recv_sem=recv_sem,
        device_id=partner,
        device_id_type=MESH_ID,
    )


def small_exchange(small_ref, small_out, send_sem, recv_sem, personal):
    n_row = lax.axis_size("row")
    total = n_row * lax.axis_size("col")
    me = lax.axis_index("col") * n_row + lax.axis_index("row")

    def copy(other, slot):
        return remote(
            small_ref.at[other] if personal else small_ref,
            small_out.at[slot],
            send_sem.at[other],
            recv_sem.at[slot],
            {"row": lax.rem(other, n_row), "col": other // n_row},
        )

    def start():
        @pl.loop(1, total)
        def _(step):
            copy(lax.rem(me + step, total), me).start()

        small_out[me] = small_ref[me] if personal else small_ref[...]

    def finish():
        @pl.loop(1, total)
        def _(step):
            other = lax.rem(me + step, total)
            copy(other, other).wait_recv()
            copy(other, me).wait_send()

    return start, finish


def line_order(lines):
    order = []
    for step in range((lines + 1) // 2):
        order.append(step)
        if lines - 1 - step != step:
            order.append(lines - 1 - step)
    return order


def every_total_plan(lines, ways, spots, place_ref, slots, extras, weights, outs, scratch):
    count = 1
    slots, extras, weights, outs = [slots], [extras], [weights], [outs]
    own, core_in, wide_in, side_in, up_in, down_in = scratch[:6]
    slot_in, staged, slot_sem, credit = scratch[6:10]
    core_send, core_recv, wide_send, wide_recv, side_send, side_recv = scratch[10:16]
    up_send, up_recv, down_send, down_recv = scratch[16:20]
    wide, core, line, side = spots
    tokens, width = own.shape[1:]
    ring, core_ring = slot_in.shape[0], core_in.shape[0]
    half = tokens // 2
    core_mate = to_place(wide, 1 - core, line, side)
    wide_mate = to_place(1 - wide, core, line, side)
    side_mate = to_place(wide, core, line, 1 - side)
    above = to_place(wide, core, line + 1, side)
    below = to_place(wide, core, line - 1, side)
    has_above = line < lines - 1
    has_below = line > 0
    parts = [pl.ds(0, half), pl.ds(half, half)]

    def at(a, l, s, w):
        return ((a * lines + l) * 2 + s) * 2 + w

    items = [(a, l) for a in range(count) for l in line_order(lines)]
    corners = [(1 - side, 1 - wide), (1 - side, wide), (side, 1 - wide), (side, wide)]
    blocks = []
    for a, l in items:
        for s, w in corners:
            blocks += [(a, 2 * at(0, l, s, w) + 1 - core), (a, 2 * at(0, l, s, w) + core)]

    def slot_copy(q):
        a, b = blocks[q]
        return pltpu.make_async_copy(
            slots[a].at[:, b], slot_in.at[q % ring], slot_sem.at[q % ring]
        )

    def summed(q):
        if q + ring - 1 < len(blocks):
            slot_copy(q + ring - 1).start()
        slot_copy(q).wait()
        a, b = blocks[q]
        rows = pl.ds(pl.multiple_of(b * tokens, tokens), tokens)
        total = inner_rows(place_ref[b], slot_in[q % ring].reshape(-1, width))
        return (total + matmul(extras[a][rows, :], weights[a][...])).astype(BF16)

    def core_copy(n):
        return remote(
            staged.at[n % ring],
            core_in.at[n % core_ring],
            core_send.at[n],
            core_recv.at[n],
            core_mate,
        )

    def spot(a, l, h, j):
        return ((a * lines + l) * 2 + h) * 2 + j

    def wide_copy(a, l, s, h):
        n = spot(a, l, h, 0 if ways[h] else s)
        return remote(
            own.at[at(a, l, s, 1 - wide), parts[h]],
            wide_in.at[n],
            wide_send.at[n],
            wide_recv.at[n],
            wide_mate,
        )

    def side_copy(a, l, w, h):
        n = spot(a, l, h, w if ways[h] else 0)
        return remote(
            own.at[at(a, l, 1 - side, w), parts[h]],
            side_in.at[n],
            side_send.at[n],
            side_recv.at[n],
            side_mate,
        )

    def up_copy(a, l, h):
        n = (a * lines + l) * 2 + h
        return remote(
            own.at[at(a, l, side, wide), parts[h]],
            up_in.at[n],
            up_send.at[n],
            up_recv.at[n],
            above,
        )

    def down_copy(a, l, h):
        n = (a * lines + l) * 2 + h
        return remote(
            own.at[at(a, l, side, wide), parts[h]],
            down_in.at[n],
            down_send.at[n],
            down_recv.at[n],
            below,
        )

    def add(i, rows, other):
        own[i, rows] = (own[i, rows].astype(F32) + other[...].astype(F32)).astype(BF16)

    def start():
        for q in range(ring - 1):
            slot_copy(q).start()

    def stage_one(t):
        a, l = items[t]
        for j, (s, w) in enumerate(corners):
            n = t * 4 + j
            if n >= ring:
                core_copy(n - ring).wait_send()
            staged[n % ring] = summed(t * 8 + 2 * j)
            if n >= core_ring:
                pl.semaphore_wait(credit, 1)
            core_copy(n).start()
            own[at(a, l, s, w)] = summed(t * 8 + 2 * j + 1)
            core_copy(n).wait_recv()
            add(at(a, l, s, w), pl.ds(0, tokens), core_in.at[n % core_ring])
            if n + core_ring < 4 * len(items):
                pl.semaphore_signal(
                    credit, inc=1, device_id=core_mate, device_id_type=MESH_ID
                )
            for h in range(2):
                if ways[h] and j in (0, 1):
                    side_copy(a, l, w, h).start()
                if not ways[h] and j in (0, 2):
                    wide_copy(a, l, s, h).start()

    def stage_two(a, l):
        for j in range(2):
            s = side if j else 1 - side
            w = wide if j else 1 - wide
            for h in range(2):
                if ways[h]:
                    side_copy(a, l, w, h).wait_recv()
                    add(at(a, l, side, w), parts[h], side_in.at[spot(a, l, h, w)])
                    if j == 0:
                        wide_copy(a, l, side, h).start()
                else:
                    wide_copy(a, l, s, h).wait_recv()
                    add(at(a, l, s, wide), parts[h], wide_in.at[spot(a, l, h, s)])
                    if j == 0:
                        side_copy(a, l, wide, h).start()

    def stage_three(a, l):
        i = at(a, l, side, wide)
        for h in range(2):
            if ways[h]:
                wide_copy(a, l, side, h).wait_recv()
                add(i, parts[h], wide_in.at[spot(a, l, h, 0)])
            else:
                side_copy(a, l, wide, h).wait_recv()
                add(i, parts[h], side_in.at[spot(a, l, h, 0)])

            @pl.when(jnp.logical_and(line == 0, l > 0))
            def _(h=h):
                up_copy(a, l, h).start()

            @pl.when(jnp.logical_and(line == lines - 1, l < lines - 1))
            def _(h=h):
                down_copy(a, l, h).start()

    def onward(a, l, up):
        @pl.when(jnp.logical_and(has_below, has_above))
        def _():
            copy, arrived = (up_copy, up_in) if up else (down_copy, down_in)
            for h in range(2):
                copy(a, l, h).wait_recv()
                add(at(a, l, side, wide), parts[h], arrived.at[(a * lines + l) * 2 + h])
                copy(a, l, h).start()

    def passing(a, j):
        high, low = lines - 1 - j, j
        lower_half = line * 2 < lines

        def go(up, when):
            l = high if up else low
            beyond = line < l if up else line > l

            @pl.when(jnp.logical_and(when, beyond))
            def _():
                onward(a, l, up)

        go(True, lower_half)
        go(False, lower_half)
        go(False, jnp.logical_not(lower_half))
        go(True, jnp.logical_not(lower_half))

    def final(a):
        for h in range(2):

            @pl.when(has_below)
            def _(h=h):
                up_copy(a, line, h).wait_recv()
                add(at(a, line, side, wide), parts[h], up_in.at[(a * lines + line) * 2 + h])

            @pl.when(has_above)
            def _(h=h):
                down_copy(a, line, h).wait_recv()
                add(at(a, line, side, wide), parts[h], down_in.at[(a * lines + line) * 2 + h])

        outs[a][...] = own[at(a, line, side, wide)].astype(F32)

    def one(t):
        stage_one(t)

    def two(t):
        stage_two(*items[t])

    def three(t):
        stage_three(*items[t])

    def along(j):
        passing(0, j)

    def last(_):
        final(0)

    def finish():
        for n in range(4 * len(items) - ring, 4 * len(items)):
            core_copy(n).wait_send()
        for a, l in items:
            for h in range(2):
                for j in range(1 if ways[h] else 2):
                    wide_copy(a, l, side if ways[h] else j, h).wait_send()
                for j in range(2 if ways[h] else 1):
                    side_copy(a, l, j if ways[h] else wide, h).wait_send()

                @pl.when(jnp.logical_and(has_above, line < l))
                def _(h=h, a=a, l=l):
                    up_copy(a, l, h).wait_send()

                @pl.when(jnp.logical_and(has_below, line > l))
                def _(h=h, a=a, l=l):
                    down_copy(a, l, h).wait_send()

    return start, (one, two, three, along, last), finish


def kernel_fits(place_shape, width):
    blocks, _, tokens = place_shape
    return tokens % 32 == 0 and 4 * blocks * tokens * width <= 40 * 1024 * 1024


def row_mates(wide, core, line, side):
    return to_place(wide, 1 - core, line, side), to_place(1 - wide, core, line, side)


def strip(ref, dim, index, size):
    start = pl.multiple_of(index * size, size)
    return ref.at[pl.ds(start, size)] if dim == 0 else ref.at[:, pl.ds(start, size)]


def cols_plan(lines, dims, flips, spots, cols, outs, sems):
    wide, core, line, side = spots
    side_mate = to_place(wide, core, line, 1 - side)
    above = to_place(wide, core, line + 1, side)
    below = to_place(wide, core, line - 1, side)
    has_above, has_below = line < lines - 1, line > 0
    local_sem, side_send, side_recv, up_send, up_recv, down_send, down_recv = sems
    count = len(dims)

    def spot(m, l, s):
        return strip(outs[m], dims[m], l * 2 + s, cols[m].shape[dims[m]])

    def line_copy(m, l, s, up, here=False):
        n = (m * lines + l) * 2 + s
        return remote(
            cols[m] if here else spot(m, l, s),
            spot(m, l, s),
            (up_send if up else down_send).at[n],
            (up_recv if up else down_recv).at[n],
            above if up else below,
        )

    def side_copy(m, l, here=False):
        n = m * lines + l
        return remote(
            cols[m] if here else spot(m, l, side),
            spot(m, l, side),
            side_send.at[n],
            side_recv.at[n],
            side_mate,
        )

    def to_line(m, s, here):
        @pl.when(has_above)
        def _():
            line_copy(m, line, s, True, here).start()

        @pl.when(has_below)
        def _():
            line_copy(m, line, s, False, here).start()

    def local(m):
        return pltpu.make_async_copy(cols[m], spot(m, line, side), local_sem.at[m])

    def start():
        for m in range(count):
            to_line(m, side, True)
            side_copy(m, line, True).start()
        for m in range(count):
            local(m).start()

    def from_line(m, dist, up):
        l = line - dist if up else line + dist

        @pl.when(l >= 0 if up else l < lines)
        def _():
            for s in (side, 1 - side) if flips[m] else (side,):
                line_copy(m, l, s, up).wait_recv()

                @pl.when(has_above if up else has_below)
                def _(s=s):
                    line_copy(m, l, s, up).start()

            if not flips[m]:
                side_copy(m, l).start()

    def step(dist):
        if dist == 1:
            for m in range(count):
                if flips[m]:
                    side_copy(m, line).wait_recv()
                    to_line(m, 1 - side, False)
        if dist < lines:
            for m in range(count):
                from_line(m, dist, True)
                from_line(m, dist, False)

    def finish():
        for m in range(count):
            local(m).wait()
            if flips[m]:
                side_copy(m, line).wait_send()
            for l in range(lines):
                if not flips[m]:
                    side_copy(m, l).wait()
                for s in range(2) if flips[m] else (side,):

                    @pl.when(jnp.logical_and(has_above, line >= l))
                    def _(m=m, l=l, s=s):
                        line_copy(m, l, s, True).wait_send()

                    @pl.when(jnp.logical_and(has_below, line <= l))
                    def _(m=m, l=l, s=s):
                        line_copy(m, l, s, False).wait_send()

    return start, step, finish


def row_plan(spots, row_ref, out_ref, sems):
    wide, core, line, side = spots
    core_mate, wide_mate = row_mates(wide, core, line, side)
    local_sem, core_send, core_recv, wide_send, wide_recv = sems
    tokens = row_ref.shape[0]

    def spot(w, k):
        return strip(out_ref, 0, w * 2 + k, tokens)

    def core_copy(n):
        src = row_ref if n == 0 else spot(1 - wide, core)
        dst = spot(wide if n == 0 else 1 - wide, core)
        return remote(src, dst, core_send.at[n], core_recv.at[n], core_mate)

    wide_copy = remote(row_ref, spot(wide, core), wide_send.at[0], wide_recv.at[0], wide_mate)
    local = pltpu.make_async_copy(row_ref, spot(wide, core), local_sem.at[0])

    def start():
        wide_copy.start()
        core_copy(0).start()
        local.start()

    def step(dist):
        if dist == 1:
            wide_copy.wait_recv()
            core_copy(1).start()

    def finish():
        local.wait()
        wide_copy.wait_send()
        for n in range(2):
            core_copy(n).wait()

    return start, step, finish


def every_plan(lines, ways, spots, own_ref, out_ref, sems):
    wide, core, line, side = spots
    core_mate, wide_mate = row_mates(wide, core, line, side)
    side_mate = to_place(wide, core, line, 1 - side)
    above = to_place(wide, core, line + 1, side)
    below = to_place(wide, core, line - 1, side)
    has_above, has_below = line < lines - 1, line > 0
    local_sem, core_send, core_recv, wide_send, wide_recv, side_send, side_recv = sems[:7]
    up_send, up_recv, down_send, down_recv = sems[7:]
    tokens = own_ref.shape[0]
    half = tokens // 2

    def spot(l, s, w, k, h):
        return out_ref.at[pl.ds((((l * 2 + s) * 2 + w) * 2 + k) * tokens + h * half, half)]

    def source(l, s, w, h, here):
        return own_ref.at[pl.ds(h * half, half)] if here else spot(l, s, w, core, h)

    def core_copy(l, s, w, h, here=False):
        n = ((l * 2 + s) * 2 + w) * 2 + h
        return remote(
            source(l, s, w, h, here),
            spot(l, s, w, core, h),
            core_send.at[n],
            core_recv.at[n],
            core_mate,
        )

    def wide_copy(l, s, h, here=False):
        n = (l * 2 + h) * 2 + (0 if ways[h] else s)
        return remote(
            source(l, s, wide, h, here),
            spot(l, s, wide, core, h),
            wide_send.at[n],
            wide_recv.at[n],
            wide_mate,
        )

    def side_copy(l, w, h, here=False):
        n = (l * 2 + h) * 2 + (w if ways[h] else 0)
        return remote(
            source(l, side, w, h, here),
            spot(l, side, w, core, h),
            side_send.at[n],
            side_recv.at[n],
            side_mate,
        )

    def line_copy(l, h, up, here=False):
        n = l * 2 + h
        return remote(
            source(l, side, wide, h, here),
            spot(l, side, wide, core, h),
            (up_send if up else down_send).at[n],
            (up_recv if up else down_recv).at[n],
            above if up else below,
        )

    def local(h):
        return pltpu.make_async_copy(
            own_ref.at[pl.ds(h * half, half)], spot(line, side, wide, core, h), local_sem.at[h]
        )

    def spread(l, h, here=False):
        if ways[h]:
            wide_copy(l, side, h, here).start()
            side_copy(l, wide, h, here).start()
        else:
            side_copy(l, wide, h, here).start()
            wide_copy(l, side, h, here).start()
        core_copy(l, side, wide, h, here).start()

    def second(l):
        for h in range(2):
            if ways[h]:
                wide_copy(l, side, h).wait_recv()
                side_copy(l, 1 - wide, h).start()
                core_copy(l, side, 1 - wide, h).start()
            else:
                side_copy(l, wide, h).wait_recv()
                wide_copy(l, 1 - side, h).start()
                core_copy(l, 1 - side, wide, h).start()

    def third(l):
        for j in range(2):
            for h in range(2):
                if ways[h]:
                    w = 1 - wide if j else wide
                    side_copy(l, w, h).wait_recv()
                    core_copy(l, 1 - side, w, h).start()
                else:
                    s = 1 - side if j else side
                    wide_copy(l, s, h).wait_recv()
                    core_copy(l, s, 1 - wide, h).start()

    def start():
        for h in range(2):

            @pl.when(has_above)
            def _(h=h):
                line_copy(line, h, True, True).start()

            @pl.when(has_below)
            def _(h=h):
                line_copy(line, h, False, True).start()

            spread(line, h, True)
        for h in range(2):
            local(h).start()

    def from_line(dist, up):
        l = line - dist if up else line + dist

        @pl.when(l >= 0 if up else l < lines)
        def _():
            for h in range(2):
                line_copy(l, h, up).wait_recv()

                @pl.when(has_above if up else has_below)
                def _(h=h):
                    line_copy(l, h, up).start()

                spread(l, h)

    def stage(action, dist):
        if dist == 0:
            action(line)
            return

        @pl.when(line - dist >= 0)
        def _():
            action(line - dist)

        @pl.when(line + dist < lines)
        def _():
            action(line + dist)

    def step(dist):
        if dist < lines:
            from_line(dist, True)
            from_line(dist, False)
        if dist - 1 < lines:
            stage(second, dist - 1)
        if 0 <= dist - 2 < lines:
            stage(third, dist - 2)

    def finish():
        for h in range(2):
            local(h).wait()
        for l in range(lines):
            for s in range(2):
                for w in range(2):
                    for h in range(2):
                        core_copy(l, s, w, h).wait()
            for h in range(2):
                for j in range(1 if ways[h] else 2):
                    wide_copy(l, side if ways[h] else j, h).wait_send()
                for j in range(2 if ways[h] else 1):
                    side_copy(l, j if ways[h] else wide, h).wait_send()

                @pl.when(jnp.logical_and(has_above, line >= l))
                def _(h=h, l=l):
                    line_copy(l, h, True).wait_send()

                @pl.when(jnp.logical_and(has_below, line <= l))
                def _(h=h, l=l):
                    line_copy(l, h, False).wait_send()

    return start, step, finish


def pick_plan(lines, place_ref, rows_ref, slots_ref, rows_in, slots_out, load_sem, store_sem):
    ring, tokens = rows_in.shape[:2]
    blocks = place_ref.shape[0]
    chunks = lines + 1
    per_step = -(-blocks // chunks)

    def load(b):
        return pltpu.make_async_copy(
            rows_ref.at[pl.ds(pl.multiple_of(b * tokens, tokens), tokens)],
            rows_in.at[lax.rem(b, ring)],
            load_sem.at[lax.rem(b, ring)],
        )

    def store(b):
        return pltpu.make_async_copy(
            slots_out.at[lax.rem(b, ring)], slots_ref.at[:, b], store_sem.at[lax.rem(b, ring)]
        )

    def start():
        for b in range(ring - 1):
            load(b).start()

    def step(dist):
        @pl.loop((dist - 1) * per_step, min(dist * per_step, blocks))
        def _(b):
            @pl.when(b + ring - 1 < blocks)
            def _():
                load(b + ring - 1).start()

            load(b).wait()

            @pl.when(b >= ring)
            def _():
                store(b - ring).wait()

            slot = lax.rem(b, ring)
            picked = matmul(place_ref[b], rows_in[slot])
            slots_out[slot] = picked.astype(BF16).reshape(slots_out.shape[1:])
            store(b).start()

    def finish():
        for b in range(blocks - ring, blocks):
            store(b).wait()

    return start, step, finish


def gather_body(lines, dims, flips, ways, kinds, *refs):
    has_row, has_every, has_small, has_pick = kinds
    count = len(dims)
    outputs = count + has_row + has_every + has_small
    if has_pick:
        pick_refs = refs[outputs : outputs + 2]
        pick_refs += refs[2 * outputs + 2 : 2 * outputs + 3] + refs[-4:]
        refs = refs[:outputs] + refs[outputs + 2 : 2 * outputs + 2] + refs[2 * outputs + 3 : -4]
    ins, outs, sems = refs[:outputs], refs[outputs : 2 * outputs], list(refs[2 * outputs :])
    spots = places()
    wide, core, line, side = spots
    core_mate, wide_mate = row_mates(*spots)
    partners = [(core >= 0, core_mate), (core >= 0, wide_mate)]
    if count or has_every:
        partners += [
            (core >= 0, to_place(wide, core, line, 1 - side)),
            (line < lines - 1, to_place(wide, core, line + 1, side)),
            (line > 0, to_place(wide, core, line - 1, side)),
        ]
    greet(partners, has_small)

    def take(n):
        taken, sems[:] = sems[:n], sems[n:]
        return taken

    plans, at = [], count
    if count:
        plans.append(cols_plan(lines, dims, flips, spots, ins[:count], outs[:count], take(7)))
    if has_row:
        plans.append(row_plan(spots, ins[at], outs[at], take(5)))
        at += 1
    if has_every:
        plans.append(every_plan(lines, ways, spots, ins[at], outs[at], take(11)))
        at += 1
    if has_small:
        small_start, small_finish = small_exchange(ins[at], outs[at], *take(2), False)
        small_start()
    if has_pick:
        plans.append(pick_plan(lines, *pick_refs))
    for start, _, _ in plans:
        start()
    for dist in range(1, lines + 2):
        for _, step, _ in plans:
            step(dist)
    if has_small:
        small_finish()
    for _, _, finish in plans:
        finish()


def kernel_gather(
    col_values, dims, flips, row_value, every_value, ways, small_value, number, pick=None
):
    n_row, n_col = lax.axis_size("row"), lax.axis_size("col")
    lines, count, total = n_col // 2, len(dims), n_row * n_col
    hbm, vmem = pl.BlockSpec(memory_space=pl.ANY), pl.BlockSpec(memory_space=pltpu.VMEM)
    dma = pltpu.SemaphoreType.DMA
    operands, in_specs, out_specs, out_shape = list(col_values), [hbm] * count, [hbm] * count, []
    scratch = []
    for value, dim in zip(col_values, dims):
        shape = list(value.shape)
        shape[dim] *= n_col
        out_shape.append(jax.ShapeDtypeStruct(tuple(shape), value.dtype))
    if count:
        scratch += [dma((count,))] + [dma((count * lines,))] * 2
        scratch += [dma((2 * count * lines,))] * 4
    if row_value is not None:
        scratch += [dma((1,)), dma((2,)), dma((2,)), dma((1,)), dma((1,))]
    if every_value is not None:
        scratch += [dma((2,)), *[dma((8 * lines,))] * 2, *[dma((4 * lines,))] * 4]
        scratch += [dma((2 * lines,))] * 4
    for value, times in ((row_value, n_row), (every_value, total)):
        if value is not None:
            operands.append(value)
            in_specs.append(vmem)
            out_specs.append(hbm)
            shape = (times * value.shape[0], *value.shape[1:])
            out_shape.append(jax.ShapeDtypeStruct(shape, value.dtype))
    if small_value is not None:
        operands.append(small_value)
        in_specs.append(vmem)
        out_specs.append(vmem)
        out_shape.append(jax.ShapeDtypeStruct((total, *small_value.shape), small_value.dtype))
        scratch += [dma((total,))] * 2
    if pick is not None:
        place, rows, local_experts = pick
        blocks, slots, tokens = place.shape
        shape = (local_experts, slots // local_experts, rows.shape[1])
        operands += [place, rows]
        in_specs += [vmem, hbm]
        out_specs.append(hbm)
        out_shape.append(jax.ShapeDtypeStruct((shape[0], blocks, *shape[1:]), BF16))
        scratch += [
            pltpu.VMEM((4, tokens, rows.shape[1]), BF16),
            pltpu.VMEM((4, *shape), BF16),
            dma((4,)),
            dma((4,)),
        ]
    kinds = tuple(value is not None for value in (row_value, every_value, small_value, pick))
    return pl.pallas_call(
        functools.partial(gather_body, lines, tuple(dims), tuple(flips), ways, kinds),
        out_shape=out_shape,
        in_specs=in_specs,
        out_specs=out_specs,
        scratch_shapes=scratch,
        compiler_params=pltpu.CompilerParams(collective_id=number, has_side_effects=True),
        name=f"gather_{number}",
    )(*operands)


def mixed_total_plan(lines, dims, flips, spots, refs):
    count = len(dims)
    cols, row_ref, refs = refs[:count], refs[count], refs[count + 1 :]
    col_outs, row_out, refs = refs[:count], refs[count], refs[count + 1 :]
    row_own, row_core, row_wide, refs = refs[0], refs[1], refs[2], refs[3:]
    owns, refs = refs[:count], refs[count:]
    side_ins, refs = refs[:count], refs[count:]
    up_ins, refs = refs[:count], refs[count:]
    down_ins, refs = refs[:count], refs[count:]
    row_load, core_send, core_recv, wide_send, wide_recv = refs[:5]
    if count:
        load_sem, side_send, side_recv, up_send, up_recv, down_send, down_recv = refs[5:12]
    wide, core, line, side = spots
    core_mate, wide_mate = row_mates(wide, core, line, side)
    side_mate = to_place(wide, core, line, 1 - side)
    above = to_place(wide, core, line + 1, side)
    below = to_place(wide, core, line - 1, side)
    has_above = line < lines - 1
    has_below = line > 0
    tokens = row_out.shape[0]

    def core_copy(w):
        return remote(
            strip(row_ref, 0, w * 2 + 1 - core, tokens),
            row_core.at[w],
            core_send.at[w],
            core_recv.at[w],
            core_mate,
        )

    def row_loaded(w):
        return pltpu.make_async_copy(
            strip(row_ref, 0, w * 2 + core, tokens), row_own.at[w], row_load.at[w]
        )

    wide_copy = remote(row_own.at[1 - wide], row_wide, wide_send.at[0], wide_recv.at[0], wide_mate)

    def source(m, l, s):
        return strip(cols[m], dims[m], l * 2 + s, col_outs[m].shape[dims[m]])

    def side_copy(m, l):
        n = m * lines + l
        return remote(
            owns[m].at[l, 1 - side] if flips[m] else source(m, l, 1 - side),
            side_ins[m].at[0 if flips[m] else l],
            side_send.at[n],
            side_recv.at[n],
            side_mate,
        )

    def own_at(m, l, s):
        return owns[m].at[l, s] if flips[m] else owns[m].at[l]

    def loaded(m, l, s):
        return pltpu.make_async_copy(
            source(m, l, s), own_at(m, l, s), load_sem.at[(m * lines + l) * 2 + s]
        )

    def line_copy(m, l, s, up):
        n = (m * lines + l) * 2 + s
        into = (up_ins if up else down_ins)[m]
        return remote(
            own_at(m, l, s),
            into.at[l, s] if flips[m] else into.at[l],
            (up_send if up else down_send).at[n],
            (up_recv if up else down_recv).at[n],
            above if up else below,
        )

    def sides(m):
        return (1 - side, side) if flips[m] else (side,)

    def add(m, l, s, other):
        mine = own_at(m, l, s)
        mine[...] = (mine[...].astype(F32) + other.astype(F32)).astype(BF16)

    def near(m, l):
        for s in sides(m):
            loaded(m, l, s).wait()
            if not flips[m]:
                side_copy(m, l).wait_recv()
                add(m, l, s, side_ins[m][l])

            @pl.when(jnp.logical_and(line == 0, l > 0))
            def _(s=s):
                line_copy(m, l, s, True).start()

            @pl.when(jnp.logical_and(line == lines - 1, l < lines - 1))
            def _(s=s):
                line_copy(m, l, s, False).start()

    def onward(m, l, up):
        @pl.when(jnp.logical_and(has_below, has_above))
        def _():
            for s in sides(m):
                where = (l, s) if flips[m] else (l,)
                line_copy(m, l, s, up).wait_recv()
                add(m, l, s, (up_ins if up else down_ins)[m][where])
                line_copy(m, l, s, up).start()

    def passing(m, j):
        high, low = lines - 1 - j, j
        lower_half = line * 2 < lines

        def go(up, when):
            l = high if up else low
            beyond = line < l if up else line > l

            @pl.when(jnp.logical_and(when, beyond))
            def _():
                onward(m, l, up)

        go(True, lower_half)
        go(False, lower_half)
        go(False, jnp.logical_not(lower_half))
        go(True, jnp.logical_not(lower_half))

    def final(m):
        for s in sides(m):
            where = (line, s) if flips[m] else (line,)

            @pl.when(has_below)
            def _(s=s, where=where):
                line_copy(m, line, s, True).wait_recv()
                add(m, line, s, up_ins[m][where])

            @pl.when(has_above)
            def _(s=s, where=where):
                line_copy(m, line, s, False).wait_recv()
                add(m, line, s, down_ins[m][where])

        if flips[m]:
            side_copy(m, line).start()

    flipped = [m for m in range(count) if flips[m]]
    straight = [m for m in range(count) if not flips[m]]
    order = line_order(lines)
    def start():
        for w in range(2):
            core_copy(w).start()
            row_loaded(w).start()
        items = [(m, l) for l in (line_order(lines) if count else []) for m in range(count)]
        for m, l in items:
            for s in sides(m):
                loaded(m, l, s).start()
            if not flips[m]:
                side_copy(m, l).start()

    def step_on(step):
        if step == 0:
            for j in range(2):
                w = wide if j else 1 - wide
                row_loaded(w).wait()
                core_copy(w).wait_recv()
                row_own[w] = (row_own[w].astype(F32) + row_core[w].astype(F32)).astype(BF16)
                if j == 0:
                    wide_copy.start()
            for l in order:
                for m in flipped:
                    near(m, l)
        if step == 1:
            wide_copy.wait_recv()
            row_out[...] = row_own[wide].astype(F32) + row_wide[...].astype(F32)
        if not count:
            return
        if step < lines:
            for m in straight:
                near(m, order[step])
        if step < lines - 1:
            for m in flipped:
                passing(m, step)
        if step == lines - 1:
            for m in flipped:
                final(m)
        if 2 <= step < lines + 1:
            for m in straight:
                passing(m, step - 2)
        if step == lines + 1:
            for m in straight:
                final(m)

    def finish():
        wide_copy.wait_send()
        for w in range(2):
            core_copy(w).wait_send()
        for m in range(count):
            if flips[m]:
                side_copy(m, line).wait()
                add(m, line, side, side_ins[m][0])
            col_outs[m][...] = own_at(m, line, side)[...].astype(F32)
            for l in range(lines):
                if not flips[m]:
                    side_copy(m, l).wait_send()
                for s in sides(m):

                    @pl.when(jnp.logical_and(has_above, line < l))
                    def _(m=m, l=l, s=s):
                        line_copy(m, l, s, True).wait_send()

                    @pl.when(jnp.logical_and(has_below, line > l))
                    def _(m=m, l=l, s=s):
                        line_copy(m, l, s, False).wait_send()

    def own_rows(m, rows):
        return own_at(m, line, side).at[rows]

    return start, step_on, finish, lines + 2, own_rows


def total_order(lines, stages, mixed_step):
    one, two, three, along, last = stages
    order = []
    lag = 3 if mixed_step else 2
    late_two = [(two, lines - 1)]
    for k in range(lines):
        order.append((one, k))
        if mixed_step:
            order.append((mixed_step, k))
        if k >= lag and lag == 3:
            order.append((three, k - lag))
        if k >= 1:
            order.append((two, k - 1))
        if k >= lag and lag == 2:
            order.append((three, k - lag))
    rest = [(three, k) for k in range(max(0, lines - lag), lines)]
    if mixed_step:
        order += rest[:-2] + [(mixed_step, lines)]
        if lines >= 4:
            order.append((along, 0))
        order += rest[-2:-1] + late_two + [(mixed_step, lines + 1)] + rest[-1:]
    else:
        order += late_two
        if lines >= 4:
            order.append((along, 0))
        order += rest
    order += [(along, j) for j in range(1 if lines >= 4 else 0, lines - 1)]
    return order + [(last, 0)]


def last_plan(row_out, scaled_ref, gains_ref, sums_ref, down_ref, scratch):
    row_in, held, summed = scratch[:3]
    row_send, row_recv, col_send, col_recv, down_send, down_recv, local_sem = scratch[3:]
    n_row, n_col = lax.axis_size("row"), lax.axis_size("col")
    row, col = lax.axis_index("row"), lax.axis_index("col")
    rows = [{"row": lax.rem(row + d, n_row), "col": col} for d in range(1, n_row)]
    cols = [{"row": row, "col": lax.rem(col + d, n_col)} for d in range(1, n_col)]
    size = down_ref.shape[0] // n_row

    def row_copy(d, source):
        return remote(held, row_in.at[source], row_send.at[d], row_recv.at[source], rows[d])

    def col_copy(d, source):
        return remote(summed, sums_ref.at[source], col_send.at[d], col_recv.at[source], cols[d])

    def down_copy(d, source, value):
        return remote(
            value,
            strip(down_ref, 0, source, size),
            down_send.at[d],
            down_recv.at[source],
            rows[d],
        )

    def first():
        held[...] = gains_ref[...]
        held[0:1, :] = jnp.sum(row_out[...] * scaled_ref[...], axis=0, keepdims=True)
        for d in range(n_row - 1):
            row_copy(d, row).start()

    def second():
        total = held[...]
        for d in range(n_row - 1):
            source = rows[d]["row"]
            row_copy(d, source).wait_recv()
            total = total + row_in[source]
        summed[...] = total
        sums_ref[col] = total
        for d in range(n_col - 1):
            col_copy(d, col).start()

    def finish(value):
        local = pltpu.make_async_copy(value, strip(down_ref, 0, row, size), local_sem)
        local.start()
        for d in range(n_row - 1):
            down_copy(d, row, value).start()
        for d in range(n_col - 1):
            col_copy(d, cols[d]["col"]).wait_recv()
            col_copy(d, col).wait_send()
        for d in range(n_row - 1):
            row_copy(d, row).wait_send()
            down_copy(d, rows[d]["row"], value).wait_recv()
            down_copy(d, row, value).wait_send()
        local.wait()

    return rows + cols, first, second, finish


def total_body(lines, dims, flips, ways, kinds, *refs):
    has_mixed, has_every, has_small, has_last = kinds
    count = len(dims)
    spots = places()
    wide, core, line, side = spots
    core_mate, wide_mate = row_mates(*spots)
    partners = [(core >= 0, core_mate), (core >= 0, wide_mate)]
    if count or has_every:
        partners += [
            (core >= 0, to_place(wide, core, line, 1 - side)),
            (line < lines - 1, to_place(wide, core, line + 1, side)),
            (line > 0, to_place(wide, core, line - 1, side)),
        ]
    refs = list(refs)

    def take(n):
        taken, refs[:] = refs[:n], refs[n:]
        return taken

    mixed = (count + 1) * has_mixed
    mixed_ins, every_ins, small_ins = take(mixed), take(4 * has_every), take(has_small)
    last_ins = take(2 * has_last)
    mixed_outs, every_outs, small_outs = take(mixed), take(has_every), take(has_small)
    if has_last:
        last_outs = take(2)
        down_rows = last_outs[1].shape[0] // lax.axis_size("row")
        peers, last_first, last_second, last_finish = last_plan(
            mixed_outs[-1], *last_ins, *last_outs, take(10)
        )
        partners = [(core >= 0, peer) for peer in peers]
    greet(partners, has_small)
    if has_small:
        small_start, small_finish = small_exchange(*small_ins, *small_outs, *take(2), True)
        small_start()
    mixed_step = None
    if has_every:
        every_start, stages, every_finish = every_total_plan(
            lines, ways, spots, *every_ins, *every_outs, take(20)
        )
        every_start()
    if has_mixed:
        mixed_start, mixed_go, mixed_finish, mixed_steps, own_rows = mixed_total_plan(
            lines, dims, flips, spots, mixed_ins + mixed_outs + refs
        )
        mixed_start()

        def mixed_step(step):
            mixed_go(step)
            if has_last and step == 1:
                last_first()
            if has_last and step == lines:
                last_second()

    if has_every:
        for action, index in total_order(lines, stages, mixed_step):
            action(index)
    else:
        for step in range(mixed_steps):
            mixed_step(step)
    if has_last:
        last_finish(own_rows(1, pl.ds(mixed_outs[1].shape[0] - down_rows, down_rows)))
    if has_mixed:
        mixed_finish()
    if has_every:
        every_finish()
    if has_small:
        small_finish()


def kernel_total(
    col_values, dims, flips, row_value, every_value, ways, small_value, number, last_value=None
):
    n_row, n_col = lax.axis_size("row"), lax.axis_size("col")
    lines, count = n_col // 2, len(dims)
    hbm, vmem = pl.BlockSpec(memory_space=pl.ANY), pl.BlockSpec(memory_space=pltpu.VMEM)
    dma = pltpu.SemaphoreType.DMA
    operands, in_specs, out_shape, scratch = [], [], [], []
    if row_value is not None:
        operands += [*col_values, row_value]
        in_specs += [hbm] * (count + 1)
        blocks = []
        for value, dim in zip(col_values, dims):
            shape = list(value.shape)
            shape[dim] //= n_col
            blocks.append(tuple(shape))
        tokens, width = row_value.shape[0] // n_row, row_value.shape[1]
        out_shape += [jax.ShapeDtypeStruct(shape, F32) for shape in blocks]
        out_shape.append(jax.ShapeDtypeStruct((tokens, width), F32))
    every_scratch, small_scratch = [], []
    if every_value is not None:
        place, slots, extra, weight = every_value
        n_blocks, _, tokens = place.shape
        local_experts, rows, width = slots.shape
        capacity = rows // n_blocks
        operands += [place, slots.reshape(local_experts, n_blocks, capacity, width), extra, weight]
        in_specs += [vmem, hbm, vmem, vmem]
        out_shape.append(jax.ShapeDtypeStruct((tokens, width), F32))
        half = (tokens // 2, width)
        every_scratch = [
            pltpu.VMEM((4 * lines, tokens, width), BF16),
            pltpu.VMEM((8, tokens, width), BF16),
            pltpu.VMEM((4 * lines, *half), BF16),
            pltpu.VMEM((4 * lines, *half), BF16),
            pltpu.VMEM((2 * lines, *half), BF16),
            pltpu.VMEM((2 * lines, *half), BF16),
            pltpu.VMEM((4, local_experts, capacity, width), BF16),
            pltpu.VMEM((4, tokens, width), BF16),
            dma((4,)),
            pltpu.SemaphoreType.REGULAR,
            *[dma((4 * lines,))] * 6,
            *[dma((2 * lines,))] * 4,
        ]
    if small_value is not None:
        operands.append(small_value)
        in_specs.append(vmem)
        out_shape.append(jax.ShapeDtypeStruct(small_value.shape, small_value.dtype))
        small_scratch = [dma((n_row * n_col,))] * 2
    if last_value is not None:
        scaled, gains, down_rows = last_value
        operands += [scaled, gains]
        in_specs += [vmem, vmem]
        out_shape += [
            jax.ShapeDtypeStruct((n_col, *gains.shape), F32),
            jax.ShapeDtypeStruct((n_row * down_rows, blocks[1][1]), BF16),
        ]
        scratch += [
            pltpu.VMEM((n_row, *gains.shape), F32),
            pltpu.VMEM(gains.shape, F32),
            pltpu.VMEM(gains.shape, F32),
            dma((n_row - 1,)),
            dma((n_row,)),
            dma((n_col - 1,)),
            dma((n_col,)),
            dma((n_row - 1,)),
            dma((n_row,)),
            dma,
        ]
    scratch += small_scratch + every_scratch
    if row_value is not None:
        tokens, width = row_value.shape[0] // n_row, row_value.shape[1]
        scratch += [
            pltpu.VMEM((2, tokens, width), BF16),
            pltpu.VMEM((2, tokens, width), BF16),
            pltpu.VMEM((tokens, width), BF16),
        ]
        doubled = [(lines, 2) if flip else (lines,) for flip in flips]
        side_held = [(1,) if flip else (lines,) for flip in flips]
        for lead in (doubled, side_held, doubled, doubled):
            scratch += [pltpu.VMEM((*d, *shape), BF16) for d, shape in zip(lead, blocks)]
        scratch += [dma((2,)), dma((2,)), dma((2,)), dma((1,)), dma((1,))]
        if count:
            scratch += [dma((2 * count * lines,))] + [dma((count * lines,))] * 2
            scratch += [dma((2 * count * lines,))] * 4
    kinds = tuple(v is not None for v in (row_value, every_value, small_value, last_value))
    return pl.pallas_call(
        functools.partial(total_body, lines, tuple(dims), tuple(flips), ways, kinds),
        out_shape=out_shape,
        in_specs=in_specs,
        out_specs=[vmem] * len(out_shape),
        scratch_shapes=scratch,
        compiler_params=pltpu.CompilerParams(
            collective_id=number, has_side_effects=True, vmem_limit_bytes=VMEM_LIMIT
        ),
        name=f"total_{number}",
    )(*operands)


def row_sum_body(value_ref, out_ref, held, core_in, wide_in, *sems):
    one_send, one_recv, two_send, two_recv, core_send, core_recv, wide_send, wide_recv = sems
    wide, core, line, side = places()
    core_mate, wide_mate = row_mates(wide, core, line, side)
    greet([(core >= 0, core_mate), (core >= 0, wide_mate)], False)
    tokens = wide_in.shape[0]

    def block(ref, w, k):
        return strip(ref, 0, w * 2 + k, tokens)

    ones = [
        remote(block(value_ref, w, 1 - core), core_in.at[w], one_send.at[w], one_recv.at[w], core_mate)
        for w in range(2)
    ]
    two = remote(held.at[1 - wide], wide_in, two_send.at[0], two_recv.at[0], wide_mate)
    for copy in ones:
        copy.start()
    for w in range(2):
        ones[w].wait_recv()
        held[w] = (block(value_ref, w, core)[...].astype(F32) + core_in[w].astype(F32)).astype(BF16)
    two.start()
    two.wait_recv()
    held[wide] = (held[wide].astype(F32) + wide_in[...].astype(F32)).astype(BF16)

    def to_core(n):
        w = wide if n == 0 else 1 - wide
        src = held.at[wide] if n == 0 else block(out_ref, w, core)
        return remote(src, block(out_ref, w, core), core_send.at[n], core_recv.at[n], core_mate)

    to_wide = remote(
        held.at[wide], block(out_ref, wide, core), wide_send.at[0], wide_recv.at[0], wide_mate
    )
    to_wide.start()
    to_core(0).start()
    block(out_ref, wide, core)[...] = held[wide]
    to_wide.wait_recv()
    to_core(1).start()
    for n in range(2):
        to_core(n).wait()
    to_wide.wait_send()
    two.wait_send()
    for copy in ones:
        copy.wait_send()


def row_sum(value, number):
    n_row = lax.axis_size("row")
    if n_row != 4:
        return lax.psum(value, "row")
    tokens, width = value.shape[0] // n_row, value.shape[1]
    dma = pltpu.SemaphoreType.DMA
    return pl.pallas_call(
        row_sum_body,
        out_shape=jax.ShapeDtypeStruct(value.shape, value.dtype),
        in_specs=[pl.BlockSpec(memory_space=pltpu.VMEM)],
        out_specs=pl.BlockSpec(memory_space=pltpu.VMEM),
        scratch_shapes=[
            pltpu.VMEM((2, tokens, width), value.dtype),
            pltpu.VMEM((2, tokens, width), value.dtype),
            pltpu.VMEM((tokens, width), value.dtype),
            dma((2,)),
            dma((2,)),
            dma((1,)),
            dma((1,)),
            dma((2,)),
            dma((2,)),
            dma((1,)),
            dma((1,)),
        ],
        compiler_params=pltpu.CompilerParams(collective_id=number, has_side_effects=True),
        name=f"row_sum_{number}",
    )(value)


def gather(
    col_values, dims, flips, row_value, every_value, ways, small_value, number, pick=None
):
    fits = not col_values and every_value is None or lax.axis_size("col") in (4, 6, 8, 10)
    if lax.axis_size("row") == 4 and fits:
        return kernel_gather(
            col_values, dims, flips, row_value, every_value, ways, small_value, number, pick
        )
    out = [lax.all_gather(v, "col", axis=d, tiled=True) for v, d in zip(col_values, dims)]
    if row_value is not None:
        out.append(token_rows(row_value))
    if every_value is not None:
        out.append(every_token(every_value))
    if small_value is not None:
        out.append(every_token(small_value[None]))
    if pick is not None:
        out.append(pick_rows(*pick))
    return out


def pick_body(capacity, place_ref, rows_ref, slots_ref):
    picked = matmul(place_ref[0], rows_ref[...]).astype(BF16)
    slots_ref[:, 0] = picked.reshape(-1, capacity, picked.shape[-1])


def pick_rows(place, rows, local_experts):
    blocks, slots, tokens = place.shape
    capacity, width = slots // local_experts, rows.shape[1]
    return pl.pallas_call(
        functools.partial(pick_body, capacity),
        grid=(blocks,),
        in_specs=[
            pl.BlockSpec((1, slots, tokens), lambda i: (i, 0, 0)),
            pl.BlockSpec((tokens, width), lambda i: (i, 0)),
        ],
        out_specs=pl.BlockSpec((local_experts, 1, capacity, width), lambda i: (0, i, 0, 0)),
        out_shape=jax.ShapeDtypeStruct((local_experts, blocks, capacity, width), BF16),
        name="pick_rows",
    )(place, rows)


def total(
    col_values, dims, flips, row_value, every_value, ways, small_value, number, last_value=None
):
    fits = lax.axis_size("row") == 4
    if col_values or every_value is not None:
        fits = fits and lax.axis_size("col") in (4, 6, 8, 10)
    if every_value is not None:
        fits = fits and kernel_fits(every_value[0].shape, every_value[1].shape[2])
    if fits:
        return kernel_total(
            col_values,
            dims,
            flips,
            row_value,
            every_value,
            ways,
            small_value,
            number,
            last_value,
        )
    out = [col_total(v, d) for v, d in zip(col_values, dims)]
    if row_value is not None:
        out.append(row_total(row_value))
    if every_value is not None:
        capacity = every_value[1].shape[1] // every_value[0].shape[0]
        out.append(every_total(combine_rows(*every_value, capacity)))
    if small_value is not None:
        out.append(lax.all_to_all(small_value, EVERY, split_axis=0, concat_axis=0, tiled=True))
    if last_value is not None:
        scaled, gains, down_rows = last_value
        part = jnp.sum(out[len(dims)] * scaled, axis=0)
        out.append(lax.psum(gains.at[0].set(part), EVERY)[None])
        out.append(token_rows(out[1][-down_rows:].astype(BF16)))
    return out


def padded_rows(values):
    return jnp.pad(values, ((0, -values.shape[0] % 8), (0, 0)))


def masked_scores(queries, attn_keys, allowed, softmax_scale):
    scores = (
        jnp.einsum("qhd,khd->hqk", queries, attn_keys, preferred_element_type=jnp.float32)
        * softmax_scale
    )
    return jnp.where(allowed[None], scores, -1e30)


def tokens_body(
    group,
    capacity,
    place_ref,
    x_ref,
    g_ref,
    both_ref,
    down_ref,
    xs_ref,
    hidden_ref,
    grad_ref,
    dboth_ref,
    ddown_ref,
):
    tokens = place_ref.shape[2]
    for block in range(group):
        rows = slice(block * tokens, (block + 1) * tokens)
        picked = matmul(place_ref[block], x_ref[rows, :])
        xs_ref[:, block] = picked.astype(BF16).reshape(-1, capacity, picked.shape[-1])
    half = down_ref.shape[0]
    both = outer_cols(x_ref[...], both_ref[...])
    act, slope = silu_parts(both[:, :half])
    lin = both[:, half:]
    hidden = (act * lin).astype(BF16)
    back = outer_cols(g_ref[...], down_ref[...])
    grads = jnp.concatenate([back * lin * slope, back * act], axis=1).astype(BF16)
    hidden_ref[...] = hidden
    grad_ref[...] = grads
    dboth = inner_rows(grads, x_ref[...])
    ddown = inner_rows(hidden, g_ref[...])

    @pl.when(pl.program_id(0) == 0)
    def _():
        dboth_ref[...] = dboth
        ddown_ref[...] = ddown

    @pl.when(pl.program_id(0) > 0)
    def _():
        dboth_ref[...] += dboth
        ddown_ref[...] += ddown


def run_tokens(place, x_all, g_all, both_weight, down_weight, local_experts):
    blocks, slots, tokens = place.shape
    capacity = slots // local_experts
    width = x_all.shape[1]
    half = down_weight.shape[0]
    group = 4 if blocks % 4 == 0 else 1
    row_block = pl.BlockSpec((group * tokens, width), lambda i: (i, 0))
    slot_block = pl.BlockSpec((local_experts, group, capacity, width), lambda i: (0, i, 0, 0))
    slot_shape = jax.ShapeDtypeStruct((local_experts, blocks, capacity, width), BF16)

    def whole(size):
        return pl.BlockSpec((size, width), lambda i: (0, 0))

    def hidden_block(size):
        return pl.BlockSpec((group * tokens, size), lambda i: (i, 0))

    rows = blocks * tokens
    xs, hidden, grads, dboth, ddown = pl.pallas_call(
        functools.partial(tokens_body, group, capacity),
        grid=(blocks // group,),
        in_specs=[
            pl.BlockSpec((group, slots, tokens), lambda i: (i, 0, 0)),
            row_block,
            row_block,
            whole(2 * half),
            whole(half),
        ],
        out_specs=[
            slot_block,
            hidden_block(half),
            hidden_block(2 * half),
            whole(2 * half),
            whole(half),
        ],
        out_shape=[
            slot_shape,
            jax.ShapeDtypeStruct((rows, half), BF16),
            jax.ShapeDtypeStruct((rows, 2 * half), BF16),
            jax.ShapeDtypeStruct((2 * half, width), F32),
            jax.ShapeDtypeStruct((half, width), F32),
        ],
        compiler_params=pltpu.CompilerParams(vmem_limit_bytes=VMEM_LIMIT),
        cost_estimate=pl.CostEstimate(
            flops=2 * rows * width * (slots + 6 * half),
            bytes_accessed=8 * rows * width,
            transcendentals=rows * half,
        ),
        name="run_tokens",
    )(place, x_all, g_all, both_weight, down_weight)
    xs = xs.reshape(local_experts, blocks * capacity, width)
    return xs, hidden, grads, dboth, ddown


def experts_body(
    x_ref,
    g_ref,
    gate_ref,
    wg_ref,
    wu_ref,
    wd_ref,
    y_ref,
    r_ref,
    dg_ref,
    du_ref,
    dd_ref,
    gg_ref,
    both,
    down,
    load_sem,
):
    expert, part = pl.program_id(0), pl.program_id(1)
    size = wd_ref.shape[1]
    held = down.shape[1]
    width = x_ref.shape[2]
    slot = lax.rem(expert, 2)

    def loads(e):
        into = lax.rem(e, 2)
        return [
            pltpu.make_async_copy(wg_ref.at[e], both.at[into, pl.ds(0, size)], load_sem.at[into, 0]),
            pltpu.make_async_copy(
                wu_ref.at[e], both.at[into, pl.ds(held, size)], load_sem.at[into, 1]
            ),
            pltpu.make_async_copy(wd_ref.at[e], down.at[into, pl.ds(0, size)], load_sem.at[into, 2]),
        ]

    @pl.when(jnp.logical_and(expert == 0, part == 0))
    def _():
        if held > size:
            gap = jnp.zeros((2, held - size, width), BF16)
            both[:, size:held] = gap
            both[:, held + size :] = gap
            down[:, size:] = gap
        for copy in loads(expert):
            copy.start()

    @pl.when(part == 0)
    def _():
        for copy in loads(expert):
            copy.wait()

        @pl.when(expert + 1 < pl.num_programs(0))
        def _():
            for copy in loads(expert + 1):
                copy.start()

    x = x_ref[0]
    g = g_ref[0]
    gate = gate_ref[0]
    pre_lin = outer_cols(x, both[slot])
    pre, lin = pre_lin[:, :held], pre_lin[:, held:]
    back = outer_cols(g, down[slot])
    act, slope = silu_parts(pre)
    hidden = act * lin
    gg_ref[0] = jnp.sum(hidden * back, axis=-1, keepdims=True)
    hidden = (hidden * gate).astype(BF16)
    back = back * gate
    pre_grad = (back * lin * slope).astype(BF16)
    lin_grad = (back * act).astype(BF16)
    grads = jnp.concatenate([pre_grad, lin_grad], axis=1)
    first = part == 0
    chunk = 512 if width % 512 == 0 else width
    for start in range(0, width, chunk):
        cols = slice(start, start + chunk)
        y_ref[0, :, cols] = matmul(hidden, down[slot, :, cols]).astype(BF16)
        r_ref[0, :, cols] = matmul(grads, both[slot, :, cols]).astype(BF16)
        d_gate = inner_rows(pre_grad[:, :size], x_ref[0, :, cols])
        d_up = inner_rows(lin_grad[:, :size], x_ref[0, :, cols])
        d_down = inner_rows(hidden[:, :size], g_ref[0, :, cols])

        @pl.when(first)
        def _():
            dg_ref[0, :, cols] = d_gate
            du_ref[0, :, cols] = d_up
            dd_ref[0, :, cols] = d_down

        @pl.when(jnp.logical_not(first))
        def _():
            dg_ref[0, :, cols] += d_gate
            du_ref[0, :, cols] += d_up
            dd_ref[0, :, cols] += d_down


def run_experts(x_slots, g_slots, gates, w_gate, w_up, w_down):
    count, rows, width = x_slots.shape
    hidden = w_down.shape[1]
    held = hidden + -hidden % 128
    chunk = 512 if rows % 512 == 0 else rows
    hbm = pl.BlockSpec(memory_space=pl.ANY)
    row_block = pl.BlockSpec((1, chunk, width), lambda e, r: (e, r, 0))
    col_block = pl.BlockSpec((1, chunk, 1), lambda e, r: (e, r, 0))
    out_block = pl.BlockSpec((1, hidden, width), lambda e, r: (e, 0, 0))
    y, r, d_gate, d_up, d_down, dots = pl.pallas_call(
        experts_body,
        grid=(count, rows // chunk),
        in_specs=[row_block, row_block, col_block, hbm, hbm, hbm],
        out_specs=[row_block, row_block, out_block, out_block, out_block, col_block],
        out_shape=[
            jax.ShapeDtypeStruct((count, rows, width), BF16),
            jax.ShapeDtypeStruct((count, rows, width), BF16),
            jax.ShapeDtypeStruct((count, hidden, width), F32),
            jax.ShapeDtypeStruct((count, hidden, width), F32),
            jax.ShapeDtypeStruct((count, hidden, width), F32),
            jax.ShapeDtypeStruct((count, rows, 1), F32),
        ],
        scratch_shapes=[
            pltpu.VMEM((2, 2 * held, width), BF16),
            pltpu.VMEM((2, held, width), BF16),
            pltpu.SemaphoreType.DMA((2, 3)),
        ],
        compiler_params=pltpu.CompilerParams(vmem_limit_bytes=VMEM_LIMIT),
        cost_estimate=pl.CostEstimate(
            flops=18 * count * rows * width * hidden,
            bytes_accessed=count * (8 * rows * width + 18 * width * hidden),
            transcendentals=count * rows * hidden,
        ),
        name="run_experts",
    )(x_slots, g_slots, gates, w_gate.transpose(0, 2, 1), w_up.transpose(0, 2, 1), w_down)
    return y, r, d_gate.transpose(0, 2, 1), d_up.transpose(0, 2, 1), d_down, dots


def combine_body(group, place_ref, slots_ref, extra_ref, weight_ref, out_ref):
    tokens = place_ref.shape[2]
    width = out_ref.shape[1]
    for block in range(group):
        rows = slice(block * tokens, (block + 1) * tokens)
        total = inner_rows(place_ref[block], slots_ref[:, block].reshape(-1, width))
        total += matmul(extra_ref[rows, :], weight_ref[...])
        out_ref[rows, :] = total.astype(BF16)


def combine_rows(place, slots, extra, weight, capacity):
    blocks, slot_count, tokens = place.shape
    local_experts, _, width = slots.shape
    group = 4 if blocks % 4 == 0 else 1
    inner = extra.shape[1]
    return pl.pallas_call(
        functools.partial(combine_body, group),
        grid=(blocks // group,),
        in_specs=[
            pl.BlockSpec((group, slot_count, tokens), lambda i: (i, 0, 0)),
            pl.BlockSpec((local_experts, group, capacity, width), lambda i: (0, i, 0, 0)),
            pl.BlockSpec((group * tokens, inner), lambda i: (i, 0)),
            pl.BlockSpec((inner, width), lambda i: (0, 0)),
        ],
        out_specs=pl.BlockSpec((group * tokens, width), lambda i: (i, 0)),
        out_shape=jax.ShapeDtypeStruct((blocks * tokens, width), BF16),
        compiler_params=pltpu.CompilerParams(vmem_limit_bytes=VMEM_LIMIT),
        cost_estimate=pl.CostEstimate(
            flops=2 * blocks * tokens * (slot_count + inner) * width,
            bytes_accessed=4 * blocks * tokens * width,
            transcendentals=0,
        ),
        name="combine_rows",
    )(place, slots.reshape(local_experts, blocks, capacity, width), extra, weight)


def on_device(
    inputs,
    segment_ids,
    routes,
    first_gain,
    query_weight,
    latent_down,
    latent_gain,
    latent_up,
    output_weight,
    second_gain,
    router_weight,
    shared_gate,
    shared_up,
    shared_down,
    expert_gate,
    expert_up,
    expert_down,
    cotangent,
):
    n_row = lax.axis_size("row")
    n_col = lax.axis_size("col")
    blocks = n_row * n_col
    own_row = lax.axis_index("row")
    own_col = lax.axis_index("col")
    own_rows = inputs.shape[1]
    width = inputs.shape[2]
    experts = router_weight.shape[1]
    local_experts = expert_gate.shape[0]
    capacity = max(2, own_rows // 8)
    stream = inputs.reshape(own_rows, width).astype(F32)
    grad_out = cotangent.reshape(own_rows, width)
    own_routes = routes.reshape(own_rows, TOPK)
    segments = segment_ids.reshape(-1)
    length = segments.shape[0]
    own_start = own_row * own_rows
    qk_dim = NOPE + ROPE
    softmax_scale = qk_dim ** (-0.5)
    cosine_table, sine_table = angle_tables(length)

    scale_one = rms_scale(stream)
    normed_one = (stream * scale_one * first_gain).astype(BF16)
    down_cols = latent_down.shape[1] // n_row
    own_down = lax.dynamic_slice_in_dim(latent_down, own_row * down_cols, down_cols, 1)
    output_rows = output_weight.shape[0]
    query_cols = query_weight.shape[1]
    query_all, output_down, expand_all, seq_normed, grad_all, all_routes = gather(
        [query_weight, jnp.concatenate([output_weight, own_down.T], axis=0), latent_up],
        [0, 1, 0],
        [False, False, True],
        normed_one,
        grad_out.astype(BF16),
        (0, 0),
        padded_rows(own_routes.astype(F32).T),
        1,
    )
    output_all = output_down[:output_rows]
    down_all = output_down[output_rows:]

    all_routes = all_routes[:, :TOPK].astype(jnp.int32)
    local_ids = own_col * local_experts + jnp.arange(local_experts)
    named = all_routes[:, :, None, :] == local_ids[None, None, :, None]
    chosen_here = jnp.max(named.astype(BF16), axis=1)
    before = (jnp.arange(own_rows)[:, None] < jnp.arange(own_rows)[None, :]).astype(BF16)
    rank = matmul(chosen_here.reshape(-1, own_rows), before).reshape(chosen_here.shape)
    slot_of = jnp.where(chosen_here > 0, rank.astype(jnp.int32), -1)
    placed = slot_of[:, :, None, :] == jnp.arange(capacity)[None, None, :, None]
    place = placed.astype(BF16).reshape(blocks, local_experts * capacity, own_rows)

    shared_cols = shared_gate.shape[1] // n_col
    shared_send = jnp.stack([shared_gate.T, shared_up.T, shared_down], axis=0)
    depth = shared_send.shape[2]
    shared_send = (
        shared_send.reshape(3, n_col, shared_cols, depth)
        .transpose(1, 0, 2, 3)
        .reshape(n_col, 3 * shared_cols, depth)
    )
    shared_send, all_routes = lax.optimization_barrier((shared_send, all_routes))
    shared_own = (
        lax.all_to_all(shared_send, "col", split_axis=0, concat_axis=0, tiled=True)
        .transpose(1, 0, 2)
        .reshape(3, shared_cols, width)
    )
    shared_own = jnp.pad(shared_own, ((0, 0), (0, -shared_cols % 128), (0, 0)))
    shared_held = shared_own.shape[1]
    gate_up_own = shared_own[:2].reshape(2 * shared_held, width)
    down_own = shared_own[2]

    heads_local = query_cols // qk_dim
    query_raw = matmul(seq_normed, query_all).reshape(length, heads_local, qk_dim)
    queries = jnp.concatenate(
        [
            query_raw[..., :NOPE],
            rotate(query_raw[..., NOPE:], cosine_table[:, None, :], sine_table[:, None, :]),
        ],
        axis=-1,
    ).astype(BF16)
    (latent_all,) = gather(
        [], [], [], outer_cols(down_all, seq_normed), None, None, None, 8
    )
    latent_all = latent_all.T
    latent = latent_all[:, :LATENT]
    scale_latent = rms_scale(latent)
    latent_normed = (latent * scale_latent * latent_gain).astype(BF16)
    keyval = matmul(latent_normed, expand_all).reshape(length, heads_local, NOPE + VD)
    key_rope = rotate(latent_all[:, LATENT:], cosine_table, sine_table)
    attn_keys = jnp.concatenate(
        [keyval[..., :NOPE], jnp.broadcast_to(key_rope[:, None, :], (length, heads_local, ROPE))],
        axis=-1,
    ).astype(BF16)
    values = keyval[..., NOPE:].astype(BF16)
    positions = jnp.arange(length)
    allowed = (positions[:, None] >= positions[None, :]) & (segments[:, None] == segments[None, :])
    scores = masked_scores(queries, attn_keys, allowed, softmax_scale)
    highest = jnp.max(scores, axis=-1, keepdims=True)
    log_total = highest + jnp.log(jnp.sum(jnp.exp(scores - highest), axis=-1, keepdims=True))
    attn_probs = jnp.exp(scores - log_total).astype(BF16)
    heads_out = (
        jnp.einsum("hqk,khd->qhd", attn_probs, values, preferred_element_type=jnp.float32)
        .astype(BF16)
        .reshape(length, heads_local * VD)
    )
    (attn_total,) = total(
        [], [], [], matmul(heads_out, output_all).astype(BF16), None, None, None, 6
    )
    residual = stream + attn_total

    scale_two = rms_scale(residual)
    normed_two = (residual * scale_two * second_gain).astype(BF16)
    logits = matmul(normed_two, router_weight)
    expert_ids = jnp.arange(experts)
    chosen = own_routes[:, :, None] == expert_ids[None, None, :]
    picked = jnp.sum(jnp.where(chosen, logits[:, None, :], 0.0), axis=-1)
    gate_probs = jax.nn.softmax(picked, axis=-1)

    all_normed, all_gates, grad_slots = gather(
        [],
        [],
        [],
        None,
        normed_two,
        (0, 1),
        padded_rows(gate_probs.T),
        2,
        (place, grad_all, local_experts),
    )
    grad_slots = grad_slots.reshape(local_experts, blocks * capacity, width)
    all_gates = all_gates[:, :TOPK]
    gate_here = jnp.sum(jnp.where(named, all_gates[:, :, None, :], 0.0), axis=1)
    slot_gate = jnp.sum(jnp.where(placed, gate_here[:, :, None, :], 0.0), axis=-1)
    slot_gate = slot_gate.transpose(1, 0, 2).reshape(local_experts, blocks * capacity, 1)
    normed_slots, shared_hidden, shared_both_grad, gate_up_part, down_part = run_tokens(
        place, all_normed, grad_all, gate_up_own, down_own, local_experts
    )
    out_slots, rows_slots, expert_gate_grad, expert_up_grad, expert_down_grad, slot_dot = (
        run_experts(normed_slots, grad_slots, slot_gate, expert_gate, expert_up, expert_down)
    )

    slot_dot = slot_dot.reshape(local_experts, blocks, capacity).transpose(1, 0, 2)
    token_dot = jnp.sum(jnp.where(placed, slot_dot[:, :, :, None], 0.0), axis=2)
    rows_total, token_dot = total(
        [],
        [],
        [],
        None,
        (place, rows_slots, shared_both_grad, gate_up_own),
        (0, 1),
        token_dot,
        3,
    )
    shared_back = jnp.concatenate(
        [gate_up_part.reshape(2, shared_held, width), down_part[None]], axis=0
    )[:, :shared_cols].astype(BF16)
    shared_back = (
        shared_back.reshape(3 * shared_cols, n_col, depth).transpose(1, 0, 2)
    )
    shared_back = lax.all_to_all(shared_back, "col", split_axis=0, concat_axis=0, tiled=True)
    token_dot = jnp.sum(token_dot.reshape(n_col, n_row, local_experts, own_rows), axis=1)
    token_dot = token_dot.reshape(experts, own_rows).T
    gate_grad = jnp.sum(jnp.where(chosen, token_dot[:, None, :], 0.0), axis=-1)
    picked_grad = gate_probs * (gate_grad - jnp.sum(gate_probs * gate_grad, axis=-1, keepdims=True))
    logit_grad = jnp.sum(jnp.where(chosen, picked_grad[:, :, None], 0.0), axis=1).astype(BF16)

    normed_two_grad = rows_total + outer_cols(logit_grad, router_weight)
    second_gain_part = jnp.sum(normed_two_grad * residual * scale_two, axis=0)
    residual_grad = grad_out + rms_back(residual, scale_two, normed_two_grad * second_gain)

    seq_resid, all_picked = gather(
        [], [], [], residual_grad.astype(BF16), None, None, padded_rows(picked_grad.T), 4
    )
    all_named = all_routes[:, :, :, None] == expert_ids
    all_logit_grad = jnp.sum(jnp.where(all_named, all_picked[:, :TOPK, :, None], 0.0), axis=1)
    router_grad = inner_rows(all_normed, all_logit_grad.astype(BF16).reshape(-1, experts))
    output_part = inner_rows(heads_out, seq_resid)
    heads_grad = outer_cols(seq_resid, output_all).astype(BF16).reshape(length, heads_local, VD)
    recomputed = jnp.exp(masked_scores(queries, attn_keys, allowed, softmax_scale) - log_total)
    delta_rows = jnp.sum(
        heads_grad.astype(F32) * heads_out.reshape(length, heads_local, VD).astype(F32),
        axis=-1,
    )
    prob_grad = jnp.einsum("qhd,khd->hqk", heads_grad, values, preferred_element_type=jnp.float32)
    score_grad = (recomputed * (prob_grad - delta_rows.T[:, :, None]) * softmax_scale).astype(BF16)
    queries_grad = jnp.einsum(
        "hqk,khd->qhd", score_grad, attn_keys, preferred_element_type=jnp.float32
    )
    key_grad = jnp.einsum("hqk,qhd->khd", score_grad, queries, preferred_element_type=jnp.float32)
    value_grad = jnp.einsum(
        "hqk,qhd->khd",
        recomputed.astype(BF16),
        heads_grad,
        preferred_element_type=jnp.float32,
    )
    query_full = (
        jnp.concatenate(
            [
                queries_grad[..., :NOPE],
                unrotate(
                    queries_grad[..., NOPE:], cosine_table[:, None, :], sine_table[:, None, :]
                ),
            ],
            axis=-1,
        )
        .astype(BF16)
        .reshape(length, heads_local * qk_dim)
    )
    keyval_grad = (
        jnp.concatenate([key_grad[..., :NOPE], value_grad], axis=-1)
        .astype(BF16)
        .reshape(length, heads_local * (NOPE + VD))
    )
    expand_part = inner_rows(latent_normed, keyval_grad)
    latent_normed_part = outer_cols(keyval_grad, expand_all)
    rope_part = jnp.sum(key_grad[..., NOPE:], axis=1)
    latent_total = row_sum(
        jnp.concatenate([latent_normed_part, rope_part], axis=1).astype(BF16), 9
    ).astype(F32)
    latent_normed_grad, rope_raw = latent_total[:, :LATENT], latent_total[:, LATENT:]
    rope_grad = unrotate(rope_raw, cosine_table, sine_table)
    latent_gain_part = jnp.sum(
        lax.dynamic_slice_in_dim(
            latent_normed_grad * latent * scale_latent, own_start, own_rows, 0
        ),
        axis=0,
    )
    latent_grad = rms_back(latent, scale_latent, latent_normed_grad * latent_gain)
    down_grad_in = jnp.concatenate([latent_grad, rope_grad], axis=-1).astype(BF16)
    own_down_grad = lax.dynamic_slice_in_dim(down_grad_in, own_row * down_cols, down_cols, 1)
    output_down_part = jnp.concatenate(
        [output_part.astype(BF16), inner_rows(own_down_grad, seq_normed).astype(BF16)], axis=0
    )
    input_part = outer_cols(query_full, query_all) + matmul(own_down_grad, down_all)
    input_part, shared_back = lax.optimization_barrier((input_part, shared_back))
    gains = jnp.stack(
        [
            jnp.zeros_like(second_gain_part),
            second_gain_part,
            jnp.pad(latent_gain_part, (0, width - LATENT)),
        ]
    )
    gains = padded_rows(gains)
    (
        query_grad,
        output_down_grad,
        latent_up_grad,
        normed_one_grad,
        out_total,
        all_gains,
        down_total,
    ) = total(
        [inner_rows(seq_normed, query_full).astype(BF16), output_down_part, expand_part.astype(BF16)],
        [0, 1, 0],
        [False, False, True],
        input_part.astype(BF16),
        (place, out_slots, shared_hidden, down_own),
        (0, 0),
        None,
        7,
        (stream * scale_one, gains, down_cols),
    )
    layer_out = (residual + out_total).astype(BF16).reshape(1, own_rows, width)
    output_grad = output_down_grad[:output_rows]
    input_grad = (
        residual_grad + rms_back(stream, scale_one, normed_one_grad * first_gain)
    ).reshape(1, own_rows, width)

    shared_back = (
        shared_back.reshape(n_col, 3, shared_cols, depth)
        .transpose(1, 0, 2, 3)
        .reshape(3, n_col * shared_cols, depth)
        .astype(F32)
    )
    shared_gate_grad = shared_back[0].T
    shared_up_grad = shared_back[1].T
    shared_down_grad = shared_back[2]

    latent_down_grad = down_total.astype(F32).T
    gains = jnp.sum(all_gains, axis=0)
    first_gain_grad, second_gain_grad = gains[0], gains[1]
    latent_gain_grad = gains[2, :LATENT]
    return (
        layer_out,
        input_grad,
        first_gain_grad,
        query_grad,
        latent_down_grad,
        latent_gain_grad,
        latent_up_grad,
        output_grad,
        second_gain_grad,
        router_grad,
        shared_gate_grad,
        shared_up_grad,
        shared_down_grad,
        expert_gate_grad,
        expert_up_grad,
        expert_down_grad,
    )


def solution(mesh):
    return jax.shard_map(
        on_device,
        mesh=mesh,
        in_specs=(
            P("col", "row", None),
            P("col", None),
            P("col", "row", None),
            P(),
            P("col", "row"),
            P("col", None),
            P(),
            P("col", "row"),
            P("row", "col"),
            P(),
            P(),
            P("col", "row"),
            P("col", "row"),
            P("row", "col"),
            P("col", None, "row"),
            P("col", None, "row"),
            P("col", "row", None),
            P("col", "row", None),
        ),
        out_specs=(
            P("col", "row", None),
            P("col", "row", None),
            P(),
            P("col", "row"),
            P("col", None),
            P(),
            P("col", "row"),
            P("row", "col"),
            P(),
            P(),
            P("col", "row"),
            P("col", "row"),
            P("row", "col"),
            P("col", None, "row"),
            P("col", None, "row"),
            P("col", "row", None),
        ),
        check_vma=False,
    )
```

```python
import functools

import jax
import jax.numpy as jnp
from jax import lax
from jax.experimental import pallas as pl
from jax.experimental.pallas import tpu as pltpu
from jax.sharding import PartitionSpec as P

NOPE = 128
ROPE = 64
LATENT = 512
VD = 128
TOPK = 6


EPS = 1e-06
ROWS_CONTRACT = (((0,), (0,)), ((), ()))
COLS_CONTRACT = (((1,), (1,)), ((), ()))


def matmul(left_side, right_side):
    return jnp.dot(left_side, right_side, preferred_element_type=jnp.float32)


def inner_rows(left_side, right_side):
    return lax.dot_general(left_side, right_side, ROWS_CONTRACT, preferred_element_type=jnp.float32)


def outer_cols(left_side, right_side):
    return lax.dot_general(left_side, right_side, COLS_CONTRACT, preferred_element_type=jnp.float32)


def rms_scale(values):
    return lax.rsqrt(jnp.mean(values * values, axis=-1, keepdims=True) + EPS)


def rms_back(values, scaling, gradient):
    return scaling * gradient - values * scaling**3 * jnp.mean(
        gradient * values, axis=-1, keepdims=True
    )


def silu_parts(preact):
    logistic = jax.nn.sigmoid(preact)
    return (preact * logistic, logistic * (1.0 + preact * (1.0 - logistic)))


def angle_tables(length):
    halfway = ROPE // 2
    frequency = 10000.0 ** (-2.0 * jnp.arange(halfway, dtype=jnp.float32) / ROPE)
    angles = jnp.arange(length, dtype=jnp.float32)[:, None] * frequency[None, :]
    return (jnp.cos(angles), jnp.sin(angles))


def rotate(values, cosine_in, sine_in):
    halfway = values.shape[-1] // 2
    leading = values[..., :halfway]
    trailing = values[..., halfway:]
    return jnp.concatenate(
        [leading * cosine_in - trailing * sine_in, leading * sine_in + trailing * cosine_in],
        axis=-1,
    )


def unrotate(values, cosine_in, sine_in):
    halfway = values.shape[-1] // 2
    leading = values[..., :halfway]
    trailing = values[..., halfway:]
    return jnp.concatenate(
        [leading * cosine_in + trailing * sine_in, trailing * cosine_in - leading * sine_in],
        axis=-1,
    )


F32 = jnp.float32
BF16 = jnp.bfloat16
EVERY = ("col", "row")
VMEM_LIMIT = 63 * 1024 * 1024


def token_rows(values):
    return lax.all_gather(values, "row", axis=0, tiled=True)


def every_token(values):
    return lax.all_gather(values, EVERY, axis=0, tiled=True)


def row_total(partial_value):
    return lax.psum_scatter(
        partial_value.astype(BF16), "row", scatter_dimension=0, tiled=True
    ).astype(F32)


def every_total(partial_value):
    return lax.psum_scatter(partial_value, EVERY, scatter_dimension=0, tiled=True).astype(F32)


def col_gather(values):
    return lax.all_gather(values, "col", axis=0, tiled=True)


def col_total(partial_value, dim):
    return lax.psum_scatter(
        partial_value.astype(BF16), "col", scatter_dimension=dim, tiled=True
    ).astype(F32)


MESH_ID = pl.DeviceIdType.MESH


def places():
    row, col = lax.axis_index("row"), lax.axis_index("col")
    return row // 2, lax.rem(row, 2), col // 2, lax.rem(col, 2)


def to_place(wide, core, line, side):
    return {"row": wide * 2 + core, "col": line * 2 + side}


def greet(partners, everyone):
    barrier = pltpu.get_barrier_semaphore()
    if everyone:
        n_row, n_col = lax.axis_size("row"), lax.axis_size("col")
        total = n_row * n_col
        me = lax.axis_index("col") * n_row + lax.axis_index("row")

        @pl.loop(1, total)
        def _(step):
            other = lax.rem(me + step, total)
            pl.semaphore_signal(
                barrier,
                inc=1,
                device_id={"row": lax.rem(other, n_row), "col": other // n_row},
                device_id_type=MESH_ID,
            )

        pl.semaphore_wait(barrier, total - 1)
        return
    for there, partner in partners:

        @pl.when(there)
        def _(partner=partner):
            pl.semaphore_signal(barrier, inc=1, device_id=partner, device_id_type=MESH_ID)

    pl.semaphore_wait(barrier, sum(jnp.int32(there) for there, _ in partners))


def remote(src, dst, send_sem, recv_sem, partner):
    return pltpu.make_async_remote_copy(
        src_ref=src,
        dst_ref=dst,
        send_sem=send_sem,
        recv_sem=recv_sem,
        device_id=partner,
        device_id_type=MESH_ID,
    )


def small_exchange(small_ref, small_out, send_sem, recv_sem, personal):
    n_row = lax.axis_size("row")
    total = n_row * lax.axis_size("col")
    me = lax.axis_index("col") * n_row + lax.axis_index("row")

    def copy(other, slot):
        return remote(
            small_ref.at[other] if personal else small_ref,
            small_out.at[slot],
            send_sem.at[other],
            recv_sem.at[slot],
            {"row": lax.rem(other, n_row), "col": other // n_row},
        )

    def start():
        @pl.loop(1, total)
        def _(step):
            copy(lax.rem(me + step, total), me).start()

        small_out[me] = small_ref[me] if personal else small_ref[...]

    def finish():
        @pl.loop(1, total)
        def _(step):
            other = lax.rem(me + step, total)
            copy(other, other).wait_recv()
            copy(other, me).wait_send()

    return start, finish


def line_order(lines):
    order = []
    for step in range((lines + 1) // 2):
        order.append(step)
        if lines - 1 - step != step:
            order.append(lines - 1 - step)
    return order


def every_total_plan(lines, ways, spots, place_ref, slots, extras, weights, outs, scratch):
    count = 1
    slots, extras, weights, outs = [slots], [extras], [weights], [outs]
    own, core_in, wide_in, side_in, up_in, down_in = scratch[:6]
    slot_in, staged, slot_sem, credit = scratch[6:10]
    core_send, core_recv, wide_send, wide_recv, side_send, side_recv = scratch[10:16]
    up_send, up_recv, down_send, down_recv = scratch[16:20]
    wide, core, line, side = spots
    tokens, width = own.shape[1:]
    ring, core_ring = slot_in.shape[0], core_in.shape[0]
    half = tokens // 2
    core_mate = to_place(wide, 1 - core, line, side)
    wide_mate = to_place(1 - wide, core, line, side)
    side_mate = to_place(wide, core, line, 1 - side)
    above = to_place(wide, core, line + 1, side)
    below = to_place(wide, core, line - 1, side)
    has_above = line < lines - 1
    has_below = line > 0
    parts = [pl.ds(0, half), pl.ds(half, half)]

    def at(a, l, s, w):
        return ((a * lines + l) * 2 + s) * 2 + w

    items = [(a, l) for a in range(count) for l in line_order(lines)]
    corners = [(1 - side, 1 - wide), (1 - side, wide), (side, 1 - wide), (side, wide)]
    blocks = []
    for a, l in items:
        for s, w in corners:
            blocks += [(a, 2 * at(0, l, s, w) + 1 - core), (a, 2 * at(0, l, s, w) + core)]

    def slot_copy(q):
        a, b = blocks[q]
        return pltpu.make_async_copy(
            slots[a].at[:, b], slot_in.at[q % ring], slot_sem.at[q % ring]
        )

    def summed(q):
        if q + ring - 1 < len(blocks):
            slot_copy(q + ring - 1).start()
        slot_copy(q).wait()
        a, b = blocks[q]
        rows = pl.ds(pl.multiple_of(b * tokens, tokens), tokens)
        total = inner_rows(place_ref[b], slot_in[q % ring].reshape(-1, width))
        return (total + matmul(extras[a][rows, :], weights[a][...])).astype(BF16)

    def core_copy(n):
        return remote(
            staged.at[n % ring],
            core_in.at[n % core_ring],
            core_send.at[n],
            core_recv.at[n],
            core_mate,
        )

    def spot(a, l, h, j):
        return ((a * lines + l) * 2 + h) * 2 + j

    def wide_copy(a, l, s, h):
        n = spot(a, l, h, 0 if ways[h] else s)
        return remote(
            own.at[at(a, l, s, 1 - wide), parts[h]],
            wide_in.at[n],
            wide_send.at[n],
            wide_recv.at[n],
            wide_mate,
        )

    def side_copy(a, l, w, h):
        n = spot(a, l, h, w if ways[h] else 0)
        return remote(
            own.at[at(a, l, 1 - side, w), parts[h]],
            side_in.at[n],
            side_send.at[n],
            side_recv.at[n],
            side_mate,
        )

    def up_copy(a, l, h):
        n = (a * lines + l) * 2 + h
        return remote(
            own.at[at(a, l, side, wide), parts[h]],
            up_in.at[n],
            up_send.at[n],
            up_recv.at[n],
            above,
        )

    def down_copy(a, l, h):
        n = (a * lines + l) * 2 + h
        return remote(
            own.at[at(a, l, side, wide), parts[h]],
            down_in.at[n],
            down_send.at[n],
            down_recv.at[n],
            below,
        )

    def add(i, rows, other):
        own[i, rows] = (own[i, rows].astype(F32) + other[...].astype(F32)).astype(BF16)

    def start():
        for q in range(ring - 1):
            slot_copy(q).start()

    def stage_one(t):
        a, l = items[t]
        for j, (s, w) in enumerate(corners):
            n = t * 4 + j
            if n >= ring:
                core_copy(n - ring).wait_send()
            staged[n % ring] = summed(t * 8 + 2 * j)
            if n >= core_ring:
                pl.semaphore_wait(credit, 1)
            core_copy(n).start()
            own[at(a, l, s, w)] = summed(t * 8 + 2 * j + 1)
            core_copy(n).wait_recv()
            add(at(a, l, s, w), pl.ds(0, tokens), core_in.at[n % core_ring])
            if n + core_ring < 4 * len(items):
                pl.semaphore_signal(
                    credit, inc=1, device_id=core_mate, device_id_type=MESH_ID
                )
            for h in range(2):
                if ways[h] and j in (0, 1):
                    side_copy(a, l, w, h).start()
                if not ways[h] and j in (0, 2):
                    wide_copy(a, l, s, h).start()

    def stage_two(a, l):
        for j in range(2):
            s = side if j else 1 - side
            w = wide if j else 1 - wide
            for h in range(2):
                if ways[h]:
                    side_copy(a, l, w, h).wait_recv()
                    add(at(a, l, side, w), parts[h], side_in.at[spot(a, l, h, w)])
                    if j == 0:
                        wide_copy(a, l, side, h).start()
                else:
                    wide_copy(a, l, s, h).wait_recv()
                    add(at(a, l, s, wide), parts[h], wide_in.at[spot(a, l, h, s)])
                    if j == 0:
                        side_copy(a, l, wide, h).start()

    def stage_three(a, l):
        i = at(a, l, side, wide)
        for h in range(2):
            if ways[h]:
                wide_copy(a, l, side, h).wait_recv()
                add(i, parts[h], wide_in.at[spot(a, l, h, 0)])
            else:
                side_copy(a, l, wide, h).wait_recv()
                add(i, parts[h], side_in.at[spot(a, l, h, 0)])

            @pl.when(jnp.logical_and(line == 0, l > 0))
            def _(h=h):
                up_copy(a, l, h).start()

            @pl.when(jnp.logical_and(line == lines - 1, l < lines - 1))
            def _(h=h):
                down_copy(a, l, h).start()

    def onward(a, l, up):
        @pl.when(jnp.logical_and(has_below, has_above))
        def _():
            copy, arrived = (up_copy, up_in) if up else (down_copy, down_in)
            for h in range(2):
                copy(a, l, h).wait_recv()
                add(at(a, l, side, wide), parts[h], arrived.at[(a * lines + l) * 2 + h])
                copy(a, l, h).start()

    def passing(a, j):
        high, low = lines - 1 - j, j
        lower_half = line * 2 < lines

        def go(up, when):
            l = high if up else low
            beyond = line < l if up else line > l

            @pl.when(jnp.logical_and(when, beyond))
            def _():
                onward(a, l, up)

        go(True, lower_half)
        go(False, lower_half)
        go(False, jnp.logical_not(lower_half))
        go(True, jnp.logical_not(lower_half))

    def final(a):
        for h in range(2):

            @pl.when(has_below)
            def _(h=h):
                up_copy(a, line, h).wait_recv()
                add(at(a, line, side, wide), parts[h], up_in.at[(a * lines + line) * 2 + h])

            @pl.when(has_above)
            def _(h=h):
                down_copy(a, line, h).wait_recv()
                add(at(a, line, side, wide), parts[h], down_in.at[(a * lines + line) * 2 + h])

        outs[a][...] = own[at(a, line, side, wide)].astype(F32)

    def one(t):
        stage_one(t)

    def two(t):
        stage_two(*items[t])

    def three(t):
        stage_three(*items[t])

    def along(j):
        passing(0, j)

    def last(_):
        final(0)

    def finish():
        for n in range(4 * len(items) - ring, 4 * len(items)):
            core_copy(n).wait_send()
        for a, l in items:
            for h in range(2):
                for j in range(1 if ways[h] else 2):
                    wide_copy(a, l, side if ways[h] else j, h).wait_send()
                for j in range(2 if ways[h] else 1):
                    side_copy(a, l, j if ways[h] else wide, h).wait_send()

                @pl.when(jnp.logical_and(has_above, line < l))
                def _(h=h, a=a, l=l):
                    up_copy(a, l, h).wait_send()

                @pl.when(jnp.logical_and(has_below, line > l))
                def _(h=h, a=a, l=l):
                    down_copy(a, l, h).wait_send()

    return start, (one, two, three, along, last), finish


def kernel_fits(place_shape, width):
    blocks, _, tokens = place_shape
    return tokens % 32 == 0 and 4 * blocks * tokens * width <= 40 * 1024 * 1024


def row_mates(wide, core, line, side):
    return to_place(wide, 1 - core, line, side), to_place(1 - wide, core, line, side)


def strip(ref, dim, index, size):
    start = pl.multiple_of(index * size, size)
    return ref.at[pl.ds(start, size)] if dim == 0 else ref.at[:, pl.ds(start, size)]


def cols_plan(lines, dims, flips, spots, cols, outs, sems):
    wide, core, line, side = spots
    side_mate = to_place(wide, core, line, 1 - side)
    above = to_place(wide, core, line + 1, side)
    below = to_place(wide, core, line - 1, side)
    has_above, has_below = line < lines - 1, line > 0
    local_sem, side_send, side_recv, up_send, up_recv, down_send, down_recv = sems
    count = len(dims)

    def spot(m, l, s):
        return strip(outs[m], dims[m], l * 2 + s, cols[m].shape[dims[m]])

    def line_copy(m, l, s, up, here=False):
        n = (m * lines + l) * 2 + s
        return remote(
            cols[m] if here else spot(m, l, s),
            spot(m, l, s),
            (up_send if up else down_send).at[n],
            (up_recv if up else down_recv).at[n],
            above if up else below,
        )

    def side_copy(m, l, here=False):
        n = m * lines + l
        return remote(
            cols[m] if here else spot(m, l, side),
            spot(m, l, side),
            side_send.at[n],
            side_recv.at[n],
            side_mate,
        )

    def to_line(m, s, here):
        @pl.when(has_above)
        def _():
            line_copy(m, line, s, True, here).start()

        @pl.when(has_below)
        def _():
            line_copy(m, line, s, False, here).start()

    def local(m):
        return pltpu.make_async_copy(cols[m], spot(m, line, side), local_sem.at[m])

    def start():
        for m in range(count):
            to_line(m, side, True)
            side_copy(m, line, True).start()
        for m in range(count):
            local(m).start()

    def from_line(m, dist, up):
        l = line - dist if up else line + dist

        @pl.when(l >= 0 if up else l < lines)
        def _():
            for s in (side, 1 - side) if flips[m] else (side,):
                line_copy(m, l, s, up).wait_recv()

                @pl.when(has_above if up else has_below)
                def _(s=s):
                    line_copy(m, l, s, up).start()

            if not flips[m]:
                side_copy(m, l).start()

    def step(dist):
        if dist == 1:
            for m in range(count):
                if flips[m]:
                    side_copy(m, line).wait_recv()
                    to_line(m, 1 - side, False)
        if dist < lines:
            for m in range(count):
                from_line(m, dist, True)
                from_line(m, dist, False)

    def finish():
        for m in range(count):
            local(m).wait()
            if flips[m]:
                side_copy(m, line).wait_send()
            for l in range(lines):
                if not flips[m]:
                    side_copy(m, l).wait()
                for s in range(2) if flips[m] else (side,):

                    @pl.when(jnp.logical_and(has_above, line >= l))
                    def _(m=m, l=l, s=s):
                        line_copy(m, l, s, True).wait_send()

                    @pl.when(jnp.logical_and(has_below, line <= l))
                    def _(m=m, l=l, s=s):
                        line_copy(m, l, s, False).wait_send()

    return start, step, finish


def row_plan(spots, row_ref, out_ref, sems):
    wide, core, line, side = spots
    core_mate, wide_mate = row_mates(wide, core, line, side)
    local_sem, core_send, core_recv, wide_send, wide_recv = sems
    tokens = row_ref.shape[0]

    def spot(w, k):
        return strip(out_ref, 0, w * 2 + k, tokens)

    def core_copy(n):
        src = row_ref if n == 0 else spot(1 - wide, core)
        dst = spot(wide if n == 0 else 1 - wide, core)
        return remote(src, dst, core_send.at[n], core_recv.at[n], core_mate)

    wide_copy = remote(row_ref, spot(wide, core), wide_send.at[0], wide_recv.at[0], wide_mate)
    local = pltpu.make_async_copy(row_ref, spot(wide, core), local_sem.at[0])

    def start():
        wide_copy.start()
        core_copy(0).start()
        local.start()

    def step(dist):
        if dist == 1:
            wide_copy.wait_recv()
            core_copy(1).start()

    def finish():
        local.wait()
        wide_copy.wait_send()
        for n in range(2):
            core_copy(n).wait()

    return start, step, finish


def every_plan(lines, ways, spots, own_ref, out_ref, sems):
    wide, core, line, side = spots
    core_mate, wide_mate = row_mates(wide, core, line, side)
    side_mate = to_place(wide, core, line, 1 - side)
    above = to_place(wide, core, line + 1, side)
    below = to_place(wide, core, line - 1, side)
    has_above, has_below = line < lines - 1, line > 0
    local_sem, core_send, core_recv, wide_send, wide_recv, side_send, side_recv = sems[:7]
    up_send, up_recv, down_send, down_recv = sems[7:]
    tokens = own_ref.shape[0]
    half = tokens // 2

    def spot(l, s, w, k, h):
        return out_ref.at[pl.ds((((l * 2 + s) * 2 + w) * 2 + k) * tokens + h * half, half)]

    def source(l, s, w, h, here):
        return own_ref.at[pl.ds(h * half, half)] if here else spot(l, s, w, core, h)

    def core_copy(l, s, w, h, here=False):
        n = ((l * 2 + s) * 2 + w) * 2 + h
        return remote(
            source(l, s, w, h, here),
            spot(l, s, w, core, h),
            core_send.at[n],
            core_recv.at[n],
            core_mate,
        )

    def wide_copy(l, s, h, here=False):
        n = (l * 2 + h) * 2 + (0 if ways[h] else s)
        return remote(
            source(l, s, wide, h, here),
            spot(l, s, wide, core, h),
            wide_send.at[n],
            wide_recv.at[n],
            wide_mate,
        )

    def side_copy(l, w, h, here=False):
        n = (l * 2 + h) * 2 + (w if ways[h] else 0)
        return remote(
            source(l, side, w, h, here),
            spot(l, side, w, core, h),
            side_send.at[n],
            side_recv.at[n],
            side_mate,
        )

    def line_copy(l, h, up, here=False):
        n = l * 2 + h
        return remote(
            source(l, side, wide, h, here),
            spot(l, side, wide, core, h),
            (up_send if up else down_send).at[n],
            (up_recv if up else down_recv).at[n],
            above if up else below,
        )

    def local(h):
        return pltpu.make_async_copy(
            own_ref.at[pl.ds(h * half, half)], spot(line, side, wide, core, h), local_sem.at[h]
        )

    def spread(l, h, here=False):
        if ways[h]:
            wide_copy(l, side, h, here).start()
            side_copy(l, wide, h, here).start()
        else:
            side_copy(l, wide, h, here).start()
            wide_copy(l, side, h, here).start()
        core_copy(l, side, wide, h, here).start()

    def second(l):
        for h in range(2):
            if ways[h]:
                wide_copy(l, side, h).wait_recv()
                side_copy(l, 1 - wide, h).start()
                core_copy(l, side, 1 - wide, h).start()
            else:
                side_copy(l, wide, h).wait_recv()
                wide_copy(l, 1 - side, h).start()
                core_copy(l, 1 - side, wide, h).start()

    def third(l):
        for j in range(2):
            for h in range(2):
                if ways[h]:
                    w = 1 - wide if j else wide
                    side_copy(l, w, h).wait_recv()
                    core_copy(l, 1 - side, w, h).start()
                else:
                    s = 1 - side if j else side
                    wide_copy(l, s, h).wait_recv()
                    core_copy(l, s, 1 - wide, h).start()

    def start():
        for h in range(2):

            @pl.when(has_above)
            def _(h=h):
                line_copy(line, h, True, True).start()

            @pl.when(has_below)
            def _(h=h):
                line_copy(line, h, False, True).start()

            spread(line, h, True)
        for h in range(2):
            local(h).start()

    def from_line(dist, up):
        l = line - dist if up else line + dist

        @pl.when(l >= 0 if up else l < lines)
        def _():
            for h in range(2):
                line_copy(l, h, up).wait_recv()

                @pl.when(has_above if up else has_below)
                def _(h=h):
                    line_copy(l, h, up).start()

                spread(l, h)

    def stage(action, dist):
        if dist == 0:
            action(line)
            return

        @pl.when(line - dist >= 0)
        def _():
            action(line - dist)

        @pl.when(line + dist < lines)
        def _():
            action(line + dist)

    def step(dist):
        if dist < lines:
            from_line(dist, True)
            from_line(dist, False)
        if dist - 1 < lines:
            stage(second, dist - 1)
        if 0 <= dist - 2 < lines:
            stage(third, dist - 2)

    def finish():
        for h in range(2):
            local(h).wait()
        for l in range(lines):
            for s in range(2):
                for w in range(2):
                    for h in range(2):
                        core_copy(l, s, w, h).wait()
            for h in range(2):
                for j in range(1 if ways[h] else 2):
                    wide_copy(l, side if ways[h] else j, h).wait_send()
                for j in range(2 if ways[h] else 1):
                    side_copy(l, j if ways[h] else wide, h).wait_send()

                @pl.when(jnp.logical_and(has_above, line >= l))
                def _(h=h, l=l):
                    line_copy(l, h, True).wait_send()

                @pl.when(jnp.logical_and(has_below, line <= l))
                def _(h=h, l=l):
                    line_copy(l, h, False).wait_send()

    return start, step, finish


def pick_plan(lines, place_ref, rows_ref, slots_ref, rows_in, slots_out, load_sem, store_sem):
    ring, tokens = rows_in.shape[:2]
    blocks = place_ref.shape[0]
    chunks = lines + 1
    per_step = -(-blocks // chunks)

    def load(b):
        return pltpu.make_async_copy(
            rows_ref.at[pl.ds(pl.multiple_of(b * tokens, tokens), tokens)],
            rows_in.at[lax.rem(b, ring)],
            load_sem.at[lax.rem(b, ring)],
        )

    def store(b):
        return pltpu.make_async_copy(
            slots_out.at[lax.rem(b, ring)], slots_ref.at[:, b], store_sem.at[lax.rem(b, ring)]
        )

    def start():
        for b in range(ring - 1):
            load(b).start()

    def step(dist):
        @pl.loop((dist - 1) * per_step, min(dist * per_step, blocks))
        def _(b):
            @pl.when(b + ring - 1 < blocks)
            def _():
                load(b + ring - 1).start()

            load(b).wait()

            @pl.when(b >= ring)
            def _():
                store(b - ring).wait()

            slot = lax.rem(b, ring)
            picked = matmul(place_ref[b], rows_in[slot])
            slots_out[slot] = picked.astype(BF16).reshape(slots_out.shape[1:])
            store(b).start()

    def finish():
        for b in range(blocks - ring, blocks):
            store(b).wait()

    return start, step, finish


def gather_body(lines, dims, flips, ways, kinds, *refs):
    has_row, has_every, has_small, has_pick = kinds
    count = len(dims)
    outputs = count + has_row + has_every + has_small
    if has_pick:
        pick_refs = refs[outputs : outputs + 2]
        pick_refs += refs[2 * outputs + 2 : 2 * outputs + 3] + refs[-4:]
        refs = refs[:outputs] + refs[outputs + 2 : 2 * outputs + 2] + refs[2 * outputs + 3 : -4]
    ins, outs, sems = refs[:outputs], refs[outputs : 2 * outputs], list(refs[2 * outputs :])
    spots = places()
    wide, core, line, side = spots
    core_mate, wide_mate = row_mates(*spots)
    partners = [(core >= 0, core_mate), (core >= 0, wide_mate)]
    if count or has_every:
        partners += [
            (core >= 0, to_place(wide, core, line, 1 - side)),
            (line < lines - 1, to_place(wide, core, line + 1, side)),
            (line > 0, to_place(wide, core, line - 1, side)),
        ]
    greet(partners, has_small)

    def take(n):
        taken, sems[:] = sems[:n], sems[n:]
        return taken

    plans, at = [], count
    if count:
        plans.append(cols_plan(lines, dims, flips, spots, ins[:count], outs[:count], take(7)))
    if has_row:
        plans.append(row_plan(spots, ins[at], outs[at], take(5)))
        at += 1
    if has_every:
        plans.append(every_plan(lines, ways, spots, ins[at], outs[at], take(11)))
        at += 1
    if has_small:
        small_start, small_finish = small_exchange(ins[at], outs[at], *take(2), False)
    if has_pick:
        plans.append(pick_plan(lines, *pick_refs))
    for start, _, _ in plans:
        start()
    if has_small:
        small_start()
    for dist in range(1, lines + 2):
        for _, step, _ in plans:
            step(dist)
    if has_small:
        small_finish()
    for _, _, finish in plans:
        finish()


def kernel_gather(
    col_values, dims, flips, row_value, every_value, ways, small_value, number, pick=None
):
    n_row, n_col = lax.axis_size("row"), lax.axis_size("col")
    lines, count, total = n_col // 2, len(dims), n_row * n_col
    hbm, vmem = pl.BlockSpec(memory_space=pl.ANY), pl.BlockSpec(memory_space=pltpu.VMEM)
    dma = pltpu.SemaphoreType.DMA
    operands, in_specs, out_specs, out_shape = list(col_values), [hbm] * count, [hbm] * count, []
    scratch = []
    for value, dim in zip(col_values, dims):
        shape = list(value.shape)
        shape[dim] *= n_col
        out_shape.append(jax.ShapeDtypeStruct(tuple(shape), value.dtype))
    if count:
        scratch += [dma((count,))] + [dma((count * lines,))] * 2
        scratch += [dma((2 * count * lines,))] * 4
    if row_value is not None:
        scratch += [dma((1,)), dma((2,)), dma((2,)), dma((1,)), dma((1,))]
    if every_value is not None:
        scratch += [dma((2,)), *[dma((8 * lines,))] * 2, *[dma((4 * lines,))] * 4]
        scratch += [dma((2 * lines,))] * 4
    for value, times in ((row_value, n_row), (every_value, total)):
        if value is not None:
            operands.append(value)
            in_specs.append(vmem)
            out_specs.append(hbm)
            shape = (times * value.shape[0], *value.shape[1:])
            out_shape.append(jax.ShapeDtypeStruct(shape, value.dtype))
    if small_value is not None:
        operands.append(small_value)
        in_specs.append(vmem)
        out_specs.append(vmem)
        out_shape.append(jax.ShapeDtypeStruct((total, *small_value.shape), small_value.dtype))
        scratch += [dma((total,))] * 2
    if pick is not None:
        place, rows, local_experts = pick
        blocks, slots, tokens = place.shape
        shape = (local_experts, slots // local_experts, rows.shape[1])
        operands += [place, rows]
        in_specs += [vmem, hbm]
        out_specs.append(hbm)
        out_shape.append(jax.ShapeDtypeStruct((shape[0], blocks, *shape[1:]), BF16))
        scratch += [
            pltpu.VMEM((4, tokens, rows.shape[1]), BF16),
            pltpu.VMEM((4, *shape), BF16),
            dma((4,)),
            dma((4,)),
        ]
    kinds = tuple(value is not None for value in (row_value, every_value, small_value, pick))
    return pl.pallas_call(
        functools.partial(gather_body, lines, tuple(dims), tuple(flips), ways, kinds),
        out_shape=out_shape,
        in_specs=in_specs,
        out_specs=out_specs,
        scratch_shapes=scratch,
        compiler_params=pltpu.CompilerParams(collective_id=number, has_side_effects=True),
        name=f"gather_{number}",
    )(*operands)


def mixed_total_plan(lines, dims, flips, spots, refs):
    count = len(dims)
    cols, row_ref, refs = refs[:count], refs[count], refs[count + 1 :]
    col_outs, row_out, refs = refs[:count], refs[count], refs[count + 1 :]
    row_own, row_core, row_wide, refs = refs[0], refs[1], refs[2], refs[3:]
    owns, refs = refs[:count], refs[count:]
    side_ins, refs = refs[:count], refs[count:]
    up_ins, refs = refs[:count], refs[count:]
    down_ins, refs = refs[:count], refs[count:]
    row_load, core_send, core_recv, wide_send, wide_recv = refs[:5]
    if count:
        load_sem, side_send, side_recv, up_send, up_recv, down_send, down_recv = refs[5:12]
    wide, core, line, side = spots
    core_mate, wide_mate = row_mates(wide, core, line, side)
    side_mate = to_place(wide, core, line, 1 - side)
    above = to_place(wide, core, line + 1, side)
    below = to_place(wide, core, line - 1, side)
    has_above = line < lines - 1
    has_below = line > 0
    tokens = row_out.shape[0]

    def core_copy(w):
        return remote(
            strip(row_ref, 0, w * 2 + 1 - core, tokens),
            row_core.at[w],
            core_send.at[w],
            core_recv.at[w],
            core_mate,
        )

    def row_loaded(w):
        return pltpu.make_async_copy(
            strip(row_ref, 0, w * 2 + core, tokens), row_own.at[w], row_load.at[w]
        )

    wide_copy = remote(row_own.at[1 - wide], row_wide, wide_send.at[0], wide_recv.at[0], wide_mate)

    def source(m, l, s):
        return strip(cols[m], dims[m], l * 2 + s, col_outs[m].shape[dims[m]])

    def side_copy(m, l):
        n = m * lines + l
        return remote(
            owns[m].at[l, 1 - side] if flips[m] else source(m, l, 1 - side),
            side_ins[m].at[0 if flips[m] else l],
            side_send.at[n],
            side_recv.at[n],
            side_mate,
        )

    def own_at(m, l, s):
        return owns[m].at[l, s] if flips[m] else owns[m].at[l]

    def loaded(m, l, s):
        return pltpu.make_async_copy(
            source(m, l, s), own_at(m, l, s), load_sem.at[(m * lines + l) * 2 + s]
        )

    def line_copy(m, l, s, up):
        n = (m * lines + l) * 2 + s
        into = (up_ins if up else down_ins)[m]
        return remote(
            own_at(m, l, s),
            into.at[l, s] if flips[m] else into.at[l],
            (up_send if up else down_send).at[n],
            (up_recv if up else down_recv).at[n],
            above if up else below,
        )

    def sides(m):
        return (1 - side, side) if flips[m] else (side,)

    def add(m, l, s, other):
        mine = own_at(m, l, s)
        mine[...] = (mine[...].astype(F32) + other.astype(F32)).astype(BF16)

    def near(m, l):
        for s in sides(m):
            loaded(m, l, s).wait()
            if not flips[m]:
                side_copy(m, l).wait_recv()
                add(m, l, s, side_ins[m][l])

            @pl.when(jnp.logical_and(line == 0, l > 0))
            def _(s=s):
                line_copy(m, l, s, True).start()

            @pl.when(jnp.logical_and(line == lines - 1, l < lines - 1))
            def _(s=s):
                line_copy(m, l, s, False).start()

    def onward(m, l, up):
        @pl.when(jnp.logical_and(has_below, has_above))
        def _():
            for s in sides(m):
                where = (l, s) if flips[m] else (l,)
                line_copy(m, l, s, up).wait_recv()
                add(m, l, s, (up_ins if up else down_ins)[m][where])
                line_copy(m, l, s, up).start()

    def passing(m, j):
        high, low = lines - 1 - j, j
        lower_half = line * 2 < lines

        def go(up, when):
            l = high if up else low
            beyond = line < l if up else line > l

            @pl.when(jnp.logical_and(when, beyond))
            def _():
                onward(m, l, up)

        go(True, lower_half)
        go(False, lower_half)
        go(False, jnp.logical_not(lower_half))
        go(True, jnp.logical_not(lower_half))

    def final(m):
        for s in sides(m):
            where = (line, s) if flips[m] else (line,)

            @pl.when(has_below)
            def _(s=s, where=where):
                line_copy(m, line, s, True).wait_recv()
                add(m, line, s, up_ins[m][where])

            @pl.when(has_above)
            def _(s=s, where=where):
                line_copy(m, line, s, False).wait_recv()
                add(m, line, s, down_ins[m][where])

        if flips[m]:
            side_copy(m, line).start()

    flipped = [m for m in range(count) if flips[m]]
    straight = [m for m in range(count) if not flips[m]]
    order = line_order(lines)
    def start():
        for w in range(2):
            core_copy(w).start()
            row_loaded(w).start()
        items = [(m, l) for l in (line_order(lines) if count else []) for m in range(count)]
        for m, l in items:
            for s in sides(m):
                loaded(m, l, s).start()
            if not flips[m]:
                side_copy(m, l).start()

    def step_on(step):
        if step == 0:
            for j in range(2):
                w = wide if j else 1 - wide
                row_loaded(w).wait()
                core_copy(w).wait_recv()
                row_own[w] = (row_own[w].astype(F32) + row_core[w].astype(F32)).astype(BF16)
                if j == 0:
                    wide_copy.start()
            for l in order:
                for m in flipped:
                    near(m, l)
        if step == 1:
            wide_copy.wait_recv()
            row_out[...] = row_own[wide].astype(F32) + row_wide[...].astype(F32)
        if not count:
            return
        if step < lines:
            for m in straight:
                near(m, order[step])
        if step < lines - 1:
            for m in flipped:
                passing(m, step)
        if step == lines - 1:
            for m in flipped:
                final(m)
        if 2 <= step < lines + 1:
            for m in straight:
                passing(m, step - 2)
        if step == lines + 1:
            for m in straight:
                final(m)

    def finish():
        wide_copy.wait_send()
        for w in range(2):
            core_copy(w).wait_send()
        for m in range(count):
            if flips[m]:
                side_copy(m, line).wait()
                add(m, line, side, side_ins[m][0])
            col_outs[m][...] = own_at(m, line, side)[...].astype(F32)
            for l in range(lines):
                if not flips[m]:
                    side_copy(m, l).wait_send()
                for s in sides(m):

                    @pl.when(jnp.logical_and(has_above, line < l))
                    def _(m=m, l=l, s=s):
                        line_copy(m, l, s, True).wait_send()

                    @pl.when(jnp.logical_and(has_below, line > l))
                    def _(m=m, l=l, s=s):
                        line_copy(m, l, s, False).wait_send()

    def own_rows(m, rows):
        return own_at(m, line, side).at[rows]

    return start, step_on, finish, lines + 2, own_rows


def total_order(lines, stages, mixed_step):
    one, two, three, along, last = stages
    order = []
    lag = 3 if mixed_step else 2
    late_two = [(two, lines - 1)]
    for k in range(lines):
        order.append((one, k))
        if mixed_step:
            order.append((mixed_step, k))
        if k >= lag and lag == 3:
            order.append((three, k - lag))
        if k >= 1:
            order.append((two, k - 1))
        if k >= lag and lag == 2:
            order.append((three, k - lag))
    rest = [(three, k) for k in range(max(0, lines - lag), lines)]
    if mixed_step:
        order += rest[:-2] + [(mixed_step, lines)]
        if lines >= 4:
            order.append((along, 0))
        order += rest[-2:-1] + late_two + [(mixed_step, lines + 1)] + rest[-1:]
    else:
        order += late_two
        if lines >= 4:
            order.append((along, 0))
        order += rest
    order += [(along, j) for j in range(1 if lines >= 4 else 0, lines - 1)]
    return order + [(last, 0)]


def last_plan(row_out, scaled_ref, gains_ref, sums_ref, down_ref, scratch):
    row_in, held, summed = scratch[:3]
    row_send, row_recv, col_send, col_recv, down_send, down_recv, local_sem = scratch[3:]
    n_row, n_col = lax.axis_size("row"), lax.axis_size("col")
    row, col = lax.axis_index("row"), lax.axis_index("col")
    rows = [{"row": lax.rem(row + d, n_row), "col": col} for d in range(1, n_row)]
    cols = [{"row": row, "col": lax.rem(col + d, n_col)} for d in range(1, n_col)]
    size = down_ref.shape[0] // n_row

    def row_copy(d, source):
        return remote(held, row_in.at[source], row_send.at[d], row_recv.at[source], rows[d])

    def col_copy(d, source):
        return remote(summed, sums_ref.at[source], col_send.at[d], col_recv.at[source], cols[d])

    def down_copy(d, source, value):
        return remote(
            value,
            strip(down_ref, 0, source, size),
            down_send.at[d],
            down_recv.at[source],
            rows[d],
        )

    def first():
        held[...] = gains_ref[...]
        part = jnp.sum(row_out[...] * scaled_ref[...], axis=0, keepdims=True)
        piece = part.shape[1] // 4
        for i in range(4):
            held[i : i + 1, 0:piece] = part[:, i * piece : (i + 1) * piece]
        for d in range(n_row - 1):
            row_copy(d, row).start()

    def second():
        total = held[...]
        for d in range(n_row - 1):
            source = rows[d]["row"]
            row_copy(d, source).wait_recv()
            total = total + row_in[source]
        summed[...] = total
        sums_ref[col] = total
        for d in range(n_col - 1):
            col_copy(d, col).start()

    def local(value):
        return pltpu.make_async_copy(value, strip(down_ref, 0, row, size), local_sem)

    def third(value):
        local(value).start()
        for d in range(n_row - 1):
            down_copy(d, row, value).start()

    def finish(value):
        for d in range(n_col - 1):
            col_copy(d, cols[d]["col"]).wait_recv()
            col_copy(d, col).wait_send()
        for d in range(n_row - 1):
            row_copy(d, row).wait_send()
            down_copy(d, rows[d]["row"], value).wait_recv()
            down_copy(d, row, value).wait_send()
        local(value).wait()

    return rows + cols, first, second, third, finish


def total_body(lines, dims, flips, ways, kinds, *refs):
    has_mixed, has_every, has_small, has_last = kinds
    count = len(dims)
    spots = places()
    wide, core, line, side = spots
    core_mate, wide_mate = row_mates(*spots)
    partners = [(core >= 0, core_mate), (core >= 0, wide_mate)]
    if count or has_every:
        partners += [
            (core >= 0, to_place(wide, core, line, 1 - side)),
            (line < lines - 1, to_place(wide, core, line + 1, side)),
            (line > 0, to_place(wide, core, line - 1, side)),
        ]
    refs = list(refs)

    def take(n):
        taken, refs[:] = refs[:n], refs[n:]
        return taken

    mixed = (count + 1) * has_mixed
    mixed_ins, every_ins, small_ins = take(mixed), take(4 * has_every), take(has_small)
    last_ins = take(2 * has_last)
    mixed_outs, every_outs, small_outs = take(mixed), take(has_every), take(has_small)
    if has_last:
        last_outs = take(2)
        down_rows = last_outs[1].shape[0] // lax.axis_size("row")
        peers, last_first, last_second, last_third, last_finish = last_plan(
            mixed_outs[-1], *last_ins, *last_outs, take(10)
        )
        partners = [(core >= 0, peer) for peer in peers]
    greet(partners, has_small)
    if has_small:
        small_start, small_finish = small_exchange(*small_ins, *small_outs, *take(2), True)
    mixed_step = None
    if has_every:
        every_start, stages, every_finish = every_total_plan(
            lines, ways, spots, *every_ins, *every_outs, take(20)
        )
        every_start()
    if has_mixed:
        mixed_start, mixed_go, mixed_finish, mixed_steps, own_rows = mixed_total_plan(
            lines, dims, flips, spots, mixed_ins + mixed_outs + refs
        )
        mixed_start()

        def down_value():
            return own_rows(1, pl.ds(mixed_outs[1].shape[0] - down_rows, down_rows))

        def mixed_step(step):
            mixed_go(step)
            if has_last and step == 1:
                last_first()
            if has_last and step == lines:
                last_second()
            if has_last and step == lines + 1:
                last_third(down_value())

    if has_every:
        for number, (action, index) in enumerate(total_order(lines, stages, mixed_step)):
            action(index)
            if has_small and number == 0:
                small_start()
    else:
        if has_small:
            small_start()
        for step in range(mixed_steps):
            mixed_step(step)
    if has_last:
        last_finish(down_value())
    if has_mixed:
        mixed_finish()
    if has_every:
        every_finish()
    if has_small:
        small_finish()


def kernel_total(
    col_values, dims, flips, row_value, every_value, ways, small_value, number, last_value=None
):
    n_row, n_col = lax.axis_size("row"), lax.axis_size("col")
    lines, count = n_col // 2, len(dims)
    hbm, vmem = pl.BlockSpec(memory_space=pl.ANY), pl.BlockSpec(memory_space=pltpu.VMEM)
    dma = pltpu.SemaphoreType.DMA
    operands, in_specs, out_shape, scratch = [], [], [], []
    if row_value is not None:
        operands += [*col_values, row_value]
        in_specs += [hbm] * (count + 1)
        blocks = []
        for value, dim in zip(col_values, dims):
            shape = list(value.shape)
            shape[dim] //= n_col
            blocks.append(tuple(shape))
        tokens, width = row_value.shape[0] // n_row, row_value.shape[1]
        out_shape += [jax.ShapeDtypeStruct(shape, F32) for shape in blocks]
        out_shape.append(jax.ShapeDtypeStruct((tokens, width), F32))
    every_scratch, small_scratch = [], []
    if every_value is not None:
        place, slots, extra, weight = every_value
        n_blocks, _, tokens = place.shape
        local_experts, rows, width = slots.shape
        capacity = rows // n_blocks
        operands += [place, slots.reshape(local_experts, n_blocks, capacity, width), extra, weight]
        in_specs += [vmem, hbm, vmem, vmem]
        out_shape.append(jax.ShapeDtypeStruct((tokens, width), F32))
        half = (tokens // 2, width)
        every_scratch = [
            pltpu.VMEM((4 * lines, tokens, width), BF16),
            pltpu.VMEM((8, tokens, width), BF16),
            pltpu.VMEM((4 * lines, *half), BF16),
            pltpu.VMEM((4 * lines, *half), BF16),
            pltpu.VMEM((2 * lines, *half), BF16),
            pltpu.VMEM((2 * lines, *half), BF16),
            pltpu.VMEM((4, local_experts, capacity, width), BF16),
            pltpu.VMEM((4, tokens, width), BF16),
            dma((4,)),
            pltpu.SemaphoreType.REGULAR,
            *[dma((4 * lines,))] * 6,
            *[dma((2 * lines,))] * 4,
        ]
    if small_value is not None:
        operands.append(small_value)
        in_specs.append(vmem)
        out_shape.append(jax.ShapeDtypeStruct(small_value.shape, small_value.dtype))
        small_scratch = [dma((n_row * n_col,))] * 2
    if last_value is not None:
        scaled, gains, down_rows = last_value
        operands += [scaled, gains]
        in_specs += [vmem, vmem]
        out_shape += [
            jax.ShapeDtypeStruct((n_col, *gains.shape), F32),
            jax.ShapeDtypeStruct((n_row * down_rows, blocks[1][1]), BF16),
        ]
        scratch += [
            pltpu.VMEM((n_row, *gains.shape), F32),
            pltpu.VMEM(gains.shape, F32),
            pltpu.VMEM(gains.shape, F32),
            dma((n_row - 1,)),
            dma((n_row,)),
            dma((n_col - 1,)),
            dma((n_col,)),
            dma((n_row - 1,)),
            dma((n_row,)),
            dma,
        ]
    scratch += small_scratch + every_scratch
    if row_value is not None:
        tokens, width = row_value.shape[0] // n_row, row_value.shape[1]
        scratch += [
            pltpu.VMEM((2, tokens, width), BF16),
            pltpu.VMEM((2, tokens, width), BF16),
            pltpu.VMEM((tokens, width), BF16),
        ]
        doubled = [(lines, 2) if flip else (lines,) for flip in flips]
        side_held = [(1,) if flip else (lines,) for flip in flips]
        for lead in (doubled, side_held, doubled, doubled):
            scratch += [pltpu.VMEM((*d, *shape), BF16) for d, shape in zip(lead, blocks)]
        scratch += [dma((2,)), dma((2,)), dma((2,)), dma((1,)), dma((1,))]
        if count:
            scratch += [dma((2 * count * lines,))] + [dma((count * lines,))] * 2
            scratch += [dma((2 * count * lines,))] * 4
    kinds = tuple(v is not None for v in (row_value, every_value, small_value, last_value))
    return pl.pallas_call(
        functools.partial(total_body, lines, tuple(dims), tuple(flips), ways, kinds),
        out_shape=out_shape,
        in_specs=in_specs,
        out_specs=[vmem] * len(out_shape),
        scratch_shapes=scratch,
        compiler_params=pltpu.CompilerParams(
            collective_id=number, has_side_effects=True, vmem_limit_bytes=VMEM_LIMIT
        ),
        name=f"total_{number}",
    )(*operands)


def row_sum_body(value_ref, out_ref, held, core_in, wide_in, *sems):
    one_send, one_recv, two_send, two_recv, core_send, core_recv, wide_send, wide_recv = sems
    wide, core, line, side = places()
    core_mate, wide_mate = row_mates(wide, core, line, side)
    greet([(core >= 0, core_mate), (core >= 0, wide_mate)], False)
    tokens = wide_in.shape[0]

    def block(ref, w, k):
        return strip(ref, 0, w * 2 + k, tokens)

    ones = [
        remote(block(value_ref, w, 1 - core), core_in.at[w], one_send.at[w], one_recv.at[w], core_mate)
        for w in range(2)
    ]
    two = remote(held.at[1 - wide], wide_in, two_send.at[0], two_recv.at[0], wide_mate)
    for copy in ones:
        copy.start()
    for w in range(2):
        ones[w].wait_recv()
        held[w] = (block(value_ref, w, core)[...].astype(F32) + core_in[w].astype(F32)).astype(BF16)
    two.start()
    two.wait_recv()
    held[wide] = (held[wide].astype(F32) + wide_in[...].astype(F32)).astype(BF16)

    def to_core(n):
        w = wide if n == 0 else 1 - wide
        src = held.at[wide] if n == 0 else block(out_ref, w, core)
        return remote(src, block(out_ref, w, core), core_send.at[n], core_recv.at[n], core_mate)

    to_wide = remote(
        held.at[wide], block(out_ref, wide, core), wide_send.at[0], wide_recv.at[0], wide_mate
    )
    to_wide.start()
    to_core(0).start()
    block(out_ref, wide, core)[...] = held[wide]
    to_wide.wait_recv()
    to_core(1).start()
    for n in range(2):
        to_core(n).wait()
    to_wide.wait_send()
    two.wait_send()
    for copy in ones:
        copy.wait_send()


def row_sum(value, number):
    n_row = lax.axis_size("row")
    if n_row != 4:
        return lax.psum(value, "row")
    tokens, width = value.shape[0] // n_row, value.shape[1]
    dma = pltpu.SemaphoreType.DMA
    return pl.pallas_call(
        row_sum_body,
        out_shape=jax.ShapeDtypeStruct(value.shape, value.dtype),
        in_specs=[pl.BlockSpec(memory_space=pltpu.VMEM)],
        out_specs=pl.BlockSpec(memory_space=pltpu.VMEM),
        scratch_shapes=[
            pltpu.VMEM((2, tokens, width), value.dtype),
            pltpu.VMEM((2, tokens, width), value.dtype),
            pltpu.VMEM((tokens, width), value.dtype),
            dma((2,)),
            dma((2,)),
            dma((1,)),
            dma((1,)),
            dma((2,)),
            dma((2,)),
            dma((1,)),
            dma((1,)),
        ],
        compiler_params=pltpu.CompilerParams(collective_id=number, has_side_effects=True),
        name=f"row_sum_{number}",
    )(value)


def gather(
    col_values, dims, flips, row_value, every_value, ways, small_value, number, pick=None
):
    fits = not col_values and every_value is None or lax.axis_size("col") in (4, 6, 8, 10)
    if lax.axis_size("row") == 4 and fits:
        return kernel_gather(
            col_values, dims, flips, row_value, every_value, ways, small_value, number, pick
        )
    out = [lax.all_gather(v, "col", axis=d, tiled=True) for v, d in zip(col_values, dims)]
    if row_value is not None:
        out.append(token_rows(row_value))
    if every_value is not None:
        out.append(every_token(every_value))
    if small_value is not None:
        out.append(every_token(small_value[None]))
    if pick is not None:
        out.append(pick_rows(*pick))
    return out


def pick_body(capacity, place_ref, rows_ref, slots_ref):
    picked = matmul(place_ref[0], rows_ref[...]).astype(BF16)
    slots_ref[:, 0] = picked.reshape(-1, capacity, picked.shape[-1])


def pick_rows(place, rows, local_experts):
    blocks, slots, tokens = place.shape
    capacity, width = slots // local_experts, rows.shape[1]
    return pl.pallas_call(
        functools.partial(pick_body, capacity),
        grid=(blocks,),
        in_specs=[
            pl.BlockSpec((1, slots, tokens), lambda i: (i, 0, 0)),
            pl.BlockSpec((tokens, width), lambda i: (i, 0)),
        ],
        out_specs=pl.BlockSpec((local_experts, 1, capacity, width), lambda i: (0, i, 0, 0)),
        out_shape=jax.ShapeDtypeStruct((local_experts, blocks, capacity, width), BF16),
        name="pick_rows",
    )(place, rows)


def total(
    col_values, dims, flips, row_value, every_value, ways, small_value, number, last_value=None
):
    fits = lax.axis_size("row") == 4
    if col_values or every_value is not None:
        fits = fits and lax.axis_size("col") in (4, 6, 8, 10)
    if every_value is not None:
        fits = fits and kernel_fits(every_value[0].shape, every_value[1].shape[2])
    if fits:
        return kernel_total(
            col_values,
            dims,
            flips,
            row_value,
            every_value,
            ways,
            small_value,
            number,
            last_value,
        )
    out = [col_total(v, d) for v, d in zip(col_values, dims)]
    if row_value is not None:
        out.append(row_total(row_value))
    if every_value is not None:
        capacity = every_value[1].shape[1] // every_value[0].shape[0]
        out.append(every_total(combine_rows(*every_value, capacity)))
    if small_value is not None:
        out.append(lax.all_to_all(small_value, EVERY, split_axis=0, concat_axis=0, tiled=True))
    if last_value is not None:
        scaled, gains, down_rows = last_value
        part = jnp.sum(out[len(dims)] * scaled, axis=0).reshape(4, -1)
        part = jnp.pad(part, ((0, 4), (0, gains.shape[1] - part.shape[1])))
        out.append(lax.psum(gains + part, EVERY)[None])
        out.append(token_rows(out[1][-down_rows:].astype(BF16)))
    return out


def padded_rows(values):
    return jnp.pad(values, ((0, -values.shape[0] % 8), (0, 0)))


def masked_scores(queries, attn_keys, allowed, softmax_scale):
    scores = (
        jnp.einsum("qhd,khd->hqk", queries, attn_keys, preferred_element_type=jnp.float32)
        * softmax_scale
    )
    return jnp.where(allowed[None], scores, -1e30)


def tokens_body(
    group,
    capacity,
    place_ref,
    x_ref,
    g_ref,
    both_ref,
    down_ref,
    xs_ref,
    hidden_ref,
    grad_ref,
    dboth_ref,
    ddown_ref,
):
    tokens = place_ref.shape[2]
    for block in range(group):
        rows = slice(block * tokens, (block + 1) * tokens)
        picked = matmul(place_ref[block], x_ref[rows, :])
        xs_ref[:, block] = picked.astype(BF16).reshape(-1, capacity, picked.shape[-1])
    half = down_ref.shape[0]
    both = outer_cols(x_ref[...], both_ref[...])
    act, slope = silu_parts(both[:, :half])
    lin = both[:, half:]
    hidden = (act * lin).astype(BF16)
    back = outer_cols(g_ref[...], down_ref[...])
    grads = jnp.concatenate([back * lin * slope, back * act], axis=1).astype(BF16)
    hidden_ref[...] = hidden
    grad_ref[...] = grads
    dboth = inner_rows(grads, x_ref[...])
    ddown = inner_rows(hidden, g_ref[...])

    @pl.when(pl.program_id(0) == 0)
    def _():
        dboth_ref[...] = dboth
        ddown_ref[...] = ddown

    @pl.when(pl.program_id(0) > 0)
    def _():
        dboth_ref[...] += dboth
        ddown_ref[...] += ddown


def run_tokens(place, x_all, g_all, both_weight, down_weight, local_experts):
    blocks, slots, tokens = place.shape
    capacity = slots // local_experts
    width = x_all.shape[1]
    half = down_weight.shape[0]
    group = 4 if blocks % 4 == 0 else 1
    row_block = pl.BlockSpec((group * tokens, width), lambda i: (i, 0))
    slot_block = pl.BlockSpec((local_experts, group, capacity, width), lambda i: (0, i, 0, 0))
    slot_shape = jax.ShapeDtypeStruct((local_experts, blocks, capacity, width), BF16)

    def whole(size):
        return pl.BlockSpec((size, width), lambda i: (0, 0))

    def hidden_block(size):
        return pl.BlockSpec((group * tokens, size), lambda i: (i, 0))

    rows = blocks * tokens
    xs, hidden, grads, dboth, ddown = pl.pallas_call(
        functools.partial(tokens_body, group, capacity),
        grid=(blocks // group,),
        in_specs=[
            pl.BlockSpec((group, slots, tokens), lambda i: (i, 0, 0)),
            row_block,
            row_block,
            whole(2 * half),
            whole(half),
        ],
        out_specs=[
            slot_block,
            hidden_block(half),
            hidden_block(2 * half),
            whole(2 * half),
            whole(half),
        ],
        out_shape=[
            slot_shape,
            jax.ShapeDtypeStruct((rows, half), BF16),
            jax.ShapeDtypeStruct((rows, 2 * half), BF16),
            jax.ShapeDtypeStruct((2 * half, width), F32),
            jax.ShapeDtypeStruct((half, width), F32),
        ],
        compiler_params=pltpu.CompilerParams(vmem_limit_bytes=VMEM_LIMIT),
        cost_estimate=pl.CostEstimate(
            flops=2 * rows * width * (slots + 6 * half),
            bytes_accessed=8 * rows * width,
            transcendentals=rows * half,
        ),
        name="run_tokens",
    )(place, x_all, g_all, both_weight, down_weight)
    xs = xs.reshape(local_experts, blocks * capacity, width)
    return xs, hidden, grads, dboth, ddown


def experts_body(
    x_ref,
    g_ref,
    gate_ref,
    wg_ref,
    wu_ref,
    wd_ref,
    y_ref,
    r_ref,
    dg_ref,
    du_ref,
    dd_ref,
    gg_ref,
    both,
    down,
    load_sem,
):
    expert, part = pl.program_id(0), pl.program_id(1)
    size = wd_ref.shape[1]
    held = down.shape[1]
    width = x_ref.shape[2]
    slot = lax.rem(expert, 2)

    def loads(e):
        into = lax.rem(e, 2)
        return [
            pltpu.make_async_copy(wg_ref.at[e], both.at[into, pl.ds(0, size)], load_sem.at[into, 0]),
            pltpu.make_async_copy(
                wu_ref.at[e], both.at[into, pl.ds(held, size)], load_sem.at[into, 1]
            ),
            pltpu.make_async_copy(wd_ref.at[e], down.at[into, pl.ds(0, size)], load_sem.at[into, 2]),
        ]

    @pl.when(jnp.logical_and(expert == 0, part == 0))
    def _():
        if held > size:
            gap = jnp.zeros((2, held - size, width), BF16)
            both[:, size:held] = gap
            both[:, held + size :] = gap
            down[:, size:] = gap
        for copy in loads(expert):
            copy.start()

    @pl.when(part == 0)
    def _():
        for copy in loads(expert):
            copy.wait()

        @pl.when(expert + 1 < pl.num_programs(0))
        def _():
            for copy in loads(expert + 1):
                copy.start()

    x = x_ref[0]
    g = g_ref[0]
    gate = gate_ref[0]
    pre_lin = outer_cols(x, both[slot])
    pre, lin = pre_lin[:, :held], pre_lin[:, held:]
    back = outer_cols(g, down[slot])
    act, slope = silu_parts(pre)
    hidden = act * lin
    gg_ref[0] = jnp.sum(hidden * back, axis=-1, keepdims=True)
    hidden = (hidden * gate).astype(BF16)
    back = back * gate
    pre_grad = (back * lin * slope).astype(BF16)
    lin_grad = (back * act).astype(BF16)
    grads = jnp.concatenate([pre_grad, lin_grad], axis=1)
    first = part == 0
    chunk = 512 if width % 512 == 0 else width
    for start in range(0, width, chunk):
        cols = slice(start, start + chunk)
        y_ref[0, :, cols] = matmul(hidden, down[slot, :, cols]).astype(BF16)
        r_ref[0, :, cols] = matmul(grads, both[slot, :, cols]).astype(BF16)
        d_gate = inner_rows(pre_grad[:, :size], x_ref[0, :, cols])
        d_up = inner_rows(lin_grad[:, :size], x_ref[0, :, cols])
        d_down = inner_rows(hidden[:, :size], g_ref[0, :, cols])

        @pl.when(first)
        def _():
            dg_ref[0, :, cols] = d_gate
            du_ref[0, :, cols] = d_up
            dd_ref[0, :, cols] = d_down

        @pl.when(jnp.logical_not(first))
        def _():
            dg_ref[0, :, cols] += d_gate
            du_ref[0, :, cols] += d_up
            dd_ref[0, :, cols] += d_down


def run_experts(x_slots, g_slots, gates, w_gate, w_up, w_down):
    count, rows, width = x_slots.shape
    hidden = w_down.shape[1]
    held = hidden + -hidden % 128
    chunk = 512 if rows % 512 == 0 else rows
    hbm = pl.BlockSpec(memory_space=pl.ANY)
    row_block = pl.BlockSpec((1, chunk, width), lambda e, r: (e, r, 0))
    col_block = pl.BlockSpec((1, chunk, 1), lambda e, r: (e, r, 0))
    out_block = pl.BlockSpec((1, hidden, width), lambda e, r: (e, 0, 0))
    y, r, d_gate, d_up, d_down, dots = pl.pallas_call(
        experts_body,
        grid=(count, rows // chunk),
        in_specs=[row_block, row_block, col_block, hbm, hbm, hbm],
        out_specs=[row_block, row_block, out_block, out_block, out_block, col_block],
        out_shape=[
            jax.ShapeDtypeStruct((count, rows, width), BF16),
            jax.ShapeDtypeStruct((count, rows, width), BF16),
            jax.ShapeDtypeStruct((count, hidden, width), F32),
            jax.ShapeDtypeStruct((count, hidden, width), F32),
            jax.ShapeDtypeStruct((count, hidden, width), F32),
            jax.ShapeDtypeStruct((count, rows, 1), F32),
        ],
        scratch_shapes=[
            pltpu.VMEM((2, 2 * held, width), BF16),
            pltpu.VMEM((2, held, width), BF16),
            pltpu.SemaphoreType.DMA((2, 3)),
        ],
        compiler_params=pltpu.CompilerParams(vmem_limit_bytes=VMEM_LIMIT),
        cost_estimate=pl.CostEstimate(
            flops=18 * count * rows * width * hidden,
            bytes_accessed=count * (8 * rows * width + 18 * width * hidden),
            transcendentals=count * rows * hidden,
        ),
        name="run_experts",
    )(x_slots, g_slots, gates, w_gate.transpose(0, 2, 1), w_up.transpose(0, 2, 1), w_down)
    return y, r, d_gate.transpose(0, 2, 1), d_up.transpose(0, 2, 1), d_down, dots


def combine_body(group, place_ref, slots_ref, extra_ref, weight_ref, out_ref):
    tokens = place_ref.shape[2]
    width = out_ref.shape[1]
    for block in range(group):
        rows = slice(block * tokens, (block + 1) * tokens)
        total = inner_rows(place_ref[block], slots_ref[:, block].reshape(-1, width))
        total += matmul(extra_ref[rows, :], weight_ref[...])
        out_ref[rows, :] = total.astype(BF16)


def combine_rows(place, slots, extra, weight, capacity):
    blocks, slot_count, tokens = place.shape
    local_experts, _, width = slots.shape
    group = 4 if blocks % 4 == 0 else 1
    inner = extra.shape[1]
    return pl.pallas_call(
        functools.partial(combine_body, group),
        grid=(blocks // group,),
        in_specs=[
            pl.BlockSpec((group, slot_count, tokens), lambda i: (i, 0, 0)),
            pl.BlockSpec((local_experts, group, capacity, width), lambda i: (0, i, 0, 0)),
            pl.BlockSpec((group * tokens, inner), lambda i: (i, 0)),
            pl.BlockSpec((inner, width), lambda i: (0, 0)),
        ],
        out_specs=pl.BlockSpec((group * tokens, width), lambda i: (i, 0)),
        out_shape=jax.ShapeDtypeStruct((blocks * tokens, width), BF16),
        compiler_params=pltpu.CompilerParams(vmem_limit_bytes=VMEM_LIMIT),
        cost_estimate=pl.CostEstimate(
            flops=2 * blocks * tokens * (slot_count + inner) * width,
            bytes_accessed=4 * blocks * tokens * width,
            transcendentals=0,
        ),
        name="combine_rows",
    )(place, slots.reshape(local_experts, blocks, capacity, width), extra, weight)


def on_device(
    inputs,
    segment_ids,
    routes,
    first_gain,
    query_weight,
    latent_down,
    latent_gain,
    latent_up,
    output_weight,
    second_gain,
    router_weight,
    shared_gate,
    shared_up,
    shared_down,
    expert_gate,
    expert_up,
    expert_down,
    cotangent,
):
    n_row = lax.axis_size("row")
    n_col = lax.axis_size("col")
    blocks = n_row * n_col
    own_row = lax.axis_index("row")
    own_col = lax.axis_index("col")
    own_rows = inputs.shape[1]
    width = inputs.shape[2]
    experts = router_weight.shape[1]
    local_experts = expert_gate.shape[0]
    capacity = max(2, own_rows // 8)
    stream = inputs.reshape(own_rows, width).astype(F32)
    grad_out = cotangent.reshape(own_rows, width)
    own_routes = routes.reshape(own_rows, TOPK)
    segments = segment_ids.reshape(-1)
    length = segments.shape[0]
    own_start = own_row * own_rows
    qk_dim = NOPE + ROPE
    softmax_scale = qk_dim ** (-0.5)
    cosine_table, sine_table = angle_tables(length)

    scale_one = rms_scale(stream)
    normed_one = (stream * scale_one * first_gain).astype(BF16)
    down_cols = latent_down.shape[1] // n_row
    own_down = lax.dynamic_slice_in_dim(latent_down, own_row * down_cols, down_cols, 1)
    output_rows = output_weight.shape[0]
    query_cols = query_weight.shape[1]
    query_all, output_down, expand_all, seq_normed, grad_all, all_routes = gather(
        [query_weight, jnp.concatenate([output_weight, own_down.T], axis=0), latent_up],
        [0, 1, 0],
        [False, False, True],
        normed_one,
        grad_out.astype(BF16),
        (0, 0),
        padded_rows(own_routes.astype(F32).T),
        1,
    )
    output_all = output_down[:output_rows]
    down_all = output_down[output_rows:]

    all_routes = all_routes[:, :TOPK].astype(jnp.int32)
    local_ids = own_col * local_experts + jnp.arange(local_experts)
    named = all_routes[:, :, None, :] == local_ids[None, None, :, None]
    chosen_here = jnp.max(named.astype(BF16), axis=1)
    before = (jnp.arange(own_rows)[:, None] < jnp.arange(own_rows)[None, :]).astype(BF16)
    rank = matmul(chosen_here.reshape(-1, own_rows), before).reshape(chosen_here.shape)
    slot_of = jnp.where(chosen_here > 0, rank.astype(jnp.int32), -1)
    placed = slot_of[:, :, None, :] == jnp.arange(capacity)[None, None, :, None]
    place = placed.astype(BF16).reshape(blocks, local_experts * capacity, own_rows)

    shared_cols = shared_gate.shape[1] // n_col
    shared_send = jnp.stack([shared_gate.T, shared_up.T, shared_down], axis=0)
    depth = shared_send.shape[2]
    shared_send = (
        shared_send.reshape(3, n_col, shared_cols, depth)
        .transpose(1, 0, 2, 3)
        .reshape(n_col, 3 * shared_cols, depth)
    )
    shared_send, all_routes = lax.optimization_barrier((shared_send, all_routes))
    shared_own = (
        lax.all_to_all(shared_send, "col", split_axis=0, concat_axis=0, tiled=True)
        .transpose(1, 0, 2)
        .reshape(3, shared_cols, width)
    )
    shared_own = jnp.pad(shared_own, ((0, 0), (0, -shared_cols % 128), (0, 0)))
    shared_held = shared_own.shape[1]
    gate_up_own = shared_own[:2].reshape(2 * shared_held, width)
    down_own = shared_own[2]

    heads_local = query_cols // qk_dim
    query_raw = matmul(seq_normed, query_all).reshape(length, heads_local, qk_dim)
    queries = jnp.concatenate(
        [
            query_raw[..., :NOPE],
            rotate(query_raw[..., NOPE:], cosine_table[:, None, :], sine_table[:, None, :]),
        ],
        axis=-1,
    ).astype(BF16)
    (latent_all,) = gather(
        [], [], [], outer_cols(down_all, seq_normed), None, None, None, 8
    )
    latent_all = latent_all.T
    latent = latent_all[:, :LATENT]
    scale_latent = rms_scale(latent)
    latent_normed = (latent * scale_latent * latent_gain).astype(BF16)
    keyval = matmul(latent_normed, expand_all).reshape(length, heads_local, NOPE + VD)
    key_rope = rotate(latent_all[:, LATENT:], cosine_table, sine_table)
    attn_keys = jnp.concatenate(
        [keyval[..., :NOPE], jnp.broadcast_to(key_rope[:, None, :], (length, heads_local, ROPE))],
        axis=-1,
    ).astype(BF16)
    values = keyval[..., NOPE:].astype(BF16)
    positions = jnp.arange(length)
    allowed = (positions[:, None] >= positions[None, :]) & (segments[:, None] == segments[None, :])
    scores = masked_scores(queries, attn_keys, allowed, softmax_scale)
    highest = jnp.max(scores, axis=-1, keepdims=True)
    log_total = highest + jnp.log(jnp.sum(jnp.exp(scores - highest), axis=-1, keepdims=True))
    attn_probs = jnp.exp(scores - log_total).astype(BF16)
    heads_out = (
        jnp.einsum("hqk,khd->qhd", attn_probs, values, preferred_element_type=jnp.float32)
        .astype(BF16)
        .reshape(length, heads_local * VD)
    )
    (attn_total,) = total(
        [], [], [], matmul(heads_out, output_all).astype(BF16), None, None, None, 6
    )
    residual = stream + attn_total

    scale_two = rms_scale(residual)
    normed_two = (residual * scale_two * second_gain).astype(BF16)
    logits = matmul(normed_two, router_weight)
    expert_ids = jnp.arange(experts)
    chosen = own_routes[:, :, None] == expert_ids[None, None, :]
    picked = jnp.sum(jnp.where(chosen, logits[:, None, :], 0.0), axis=-1)
    gate_probs = jax.nn.softmax(picked, axis=-1)

    all_normed, all_gates, grad_slots = gather(
        [],
        [],
        [],
        None,
        normed_two,
        (0, 1),
        padded_rows(gate_probs.T),
        2,
        (place, grad_all, local_experts),
    )
    grad_slots = grad_slots.reshape(local_experts, blocks * capacity, width)
    all_gates = all_gates[:, :TOPK]
    gate_here = jnp.sum(jnp.where(named, all_gates[:, :, None, :], 0.0), axis=1)
    slot_gate = jnp.sum(jnp.where(placed, gate_here[:, :, None, :], 0.0), axis=-1)
    slot_gate = slot_gate.transpose(1, 0, 2).reshape(local_experts, blocks * capacity, 1)
    normed_slots, shared_hidden, shared_both_grad, gate_up_part, down_part = run_tokens(
        place, all_normed, grad_all, gate_up_own, down_own, local_experts
    )
    out_slots, rows_slots, expert_gate_grad, expert_up_grad, expert_down_grad, slot_dot = (
        run_experts(normed_slots, grad_slots, slot_gate, expert_gate, expert_up, expert_down)
    )

    slot_dot = slot_dot.reshape(local_experts, blocks, capacity).transpose(1, 0, 2)
    token_dot = jnp.sum(jnp.where(placed, slot_dot[:, :, :, None], 0.0), axis=2)
    rows_total, token_dot = total(
        [],
        [],
        [],
        None,
        (place, rows_slots, shared_both_grad, gate_up_own),
        (0, 1),
        token_dot,
        3,
    )
    shared_back = jnp.concatenate(
        [gate_up_part.reshape(2, shared_held, width), down_part[None]], axis=0
    )[:, :shared_cols].astype(BF16)
    shared_back = (
        shared_back.reshape(3 * shared_cols, n_col, depth).transpose(1, 0, 2)
    )
    shared_back = lax.all_to_all(shared_back, "col", split_axis=0, concat_axis=0, tiled=True)
    token_dot = jnp.sum(token_dot.reshape(n_col, n_row, local_experts, own_rows), axis=1)
    token_dot = token_dot.reshape(experts, own_rows).T
    gate_grad = jnp.sum(jnp.where(chosen, token_dot[:, None, :], 0.0), axis=-1)
    picked_grad = gate_probs * (gate_grad - jnp.sum(gate_probs * gate_grad, axis=-1, keepdims=True))
    logit_grad = jnp.sum(jnp.where(chosen, picked_grad[:, :, None], 0.0), axis=1).astype(BF16)

    normed_two_grad = rows_total + outer_cols(logit_grad, router_weight)
    second_gain_part = jnp.sum(normed_two_grad * residual * scale_two, axis=0)
    residual_grad = grad_out + rms_back(residual, scale_two, normed_two_grad * second_gain)

    seq_resid, all_picked = gather(
        [], [], [], residual_grad.astype(BF16), None, None, padded_rows(picked_grad.T), 4
    )
    all_named = all_routes[:, :, :, None] == expert_ids
    all_logit_grad = jnp.sum(jnp.where(all_named, all_picked[:, :TOPK, :, None], 0.0), axis=1)
    router_grad = inner_rows(all_normed, all_logit_grad.astype(BF16).reshape(-1, experts))
    output_part = inner_rows(heads_out, seq_resid)
    heads_grad = outer_cols(seq_resid, output_all).astype(BF16).reshape(length, heads_local, VD)
    recomputed = jnp.exp(masked_scores(queries, attn_keys, allowed, softmax_scale) - log_total)
    delta_rows = jnp.sum(
        heads_grad.astype(F32) * heads_out.reshape(length, heads_local, VD).astype(F32),
        axis=-1,
    )
    prob_grad = jnp.einsum("qhd,khd->hqk", heads_grad, values, preferred_element_type=jnp.float32)
    score_grad = (recomputed * (prob_grad - delta_rows.T[:, :, None]) * softmax_scale).astype(BF16)
    queries_grad = jnp.einsum(
        "hqk,khd->qhd", score_grad, attn_keys, preferred_element_type=jnp.float32
    )
    key_grad = jnp.einsum("hqk,qhd->khd", score_grad, queries, preferred_element_type=jnp.float32)
    value_grad = jnp.einsum(
        "hqk,qhd->khd",
        recomputed.astype(BF16),
        heads_grad,
        preferred_element_type=jnp.float32,
    )
    query_full = (
        jnp.concatenate(
            [
                queries_grad[..., :NOPE],
                unrotate(
                    queries_grad[..., NOPE:], cosine_table[:, None, :], sine_table[:, None, :]
                ),
            ],
            axis=-1,
        )
        .astype(BF16)
        .reshape(length, heads_local * qk_dim)
    )
    keyval_grad = (
        jnp.concatenate([key_grad[..., :NOPE], value_grad], axis=-1)
        .astype(BF16)
        .reshape(length, heads_local * (NOPE + VD))
    )
    expand_part = inner_rows(latent_normed, keyval_grad)
    latent_normed_part = outer_cols(keyval_grad, expand_all)
    rope_part = jnp.sum(key_grad[..., NOPE:], axis=1)
    latent_total = row_sum(
        jnp.concatenate([latent_normed_part, rope_part], axis=1).astype(BF16), 9
    ).astype(F32)
    latent_normed_grad, rope_raw = latent_total[:, :LATENT], latent_total[:, LATENT:]
    rope_grad = unrotate(rope_raw, cosine_table, sine_table)
    latent_gain_part = jnp.sum(
        lax.dynamic_slice_in_dim(
            latent_normed_grad * latent * scale_latent, own_start, own_rows, 0
        ),
        axis=0,
    )
    latent_grad = rms_back(latent, scale_latent, latent_normed_grad * latent_gain)
    down_grad_in = jnp.concatenate([latent_grad, rope_grad], axis=-1).astype(BF16)
    own_down_grad = lax.dynamic_slice_in_dim(down_grad_in, own_row * down_cols, down_cols, 1)
    output_down_part = jnp.concatenate(
        [output_part.astype(BF16), inner_rows(own_down_grad, seq_normed).astype(BF16)], axis=0
    )
    input_part = outer_cols(query_full, query_all) + matmul(own_down_grad, down_all)
    input_part, shared_back = lax.optimization_barrier((input_part, shared_back))
    gains = jnp.concatenate(
        [
            jnp.pad(second_gain_part.reshape(4, -1), ((4, 0), (0, 0))),
            jnp.pad(latent_gain_part.reshape(4, -1), ((0, 4), (0, 0))),
        ],
        axis=1,
    )
    (
        query_grad,
        output_down_grad,
        latent_up_grad,
        normed_one_grad,
        out_total,
        all_gains,
        down_total,
    ) = total(
        [inner_rows(seq_normed, query_full).astype(BF16), output_down_part, expand_part.astype(BF16)],
        [0, 1, 0],
        [False, False, True],
        input_part.astype(BF16),
        (place, out_slots, shared_hidden, down_own),
        (0, 0),
        None,
        7,
        (stream * scale_one, gains, down_cols),
    )
    layer_out = (residual + out_total).astype(BF16).reshape(1, own_rows, width)
    output_grad = output_down_grad[:output_rows]
    input_grad = (
        residual_grad + rms_back(stream, scale_one, normed_one_grad * first_gain)
    ).reshape(1, own_rows, width)

    shared_back = (
        shared_back.reshape(n_col, 3, shared_cols, depth)
        .transpose(1, 0, 2, 3)
        .reshape(3, n_col * shared_cols, depth)
        .astype(F32)
    )
    shared_gate_grad = shared_back[0].T
    shared_up_grad = shared_back[1].T
    shared_down_grad = shared_back[2]

    latent_down_grad = down_total.astype(F32).T
    gains = jnp.sum(all_gains, axis=0)
    first_gain_grad = gains[:4, : width // 4].reshape(-1)
    second_gain_grad = gains[4:, : width // 4].reshape(-1)
    latent_gain_grad = gains[:4, width // 4 :].reshape(-1)
    return (
        layer_out,
        input_grad,
        first_gain_grad,
        query_grad,
        latent_down_grad,
        latent_gain_grad,
        latent_up_grad,
        output_grad,
        second_gain_grad,
        router_grad,
        shared_gate_grad,
        shared_up_grad,
        shared_down_grad,
        expert_gate_grad,
        expert_up_grad,
        expert_down_grad,
    )


def solution(mesh):
    return jax.shard_map(
        on_device,
        mesh=mesh,
        in_specs=(
            P("col", "row", None),
            P("col", None),
            P("col", "row", None),
            P(),
            P("col", "row"),
            P("col", None),
            P(),
            P("col", "row"),
            P("row", "col"),
            P(),
            P(),
            P("col", "row"),
            P("col", "row"),
            P("row", "col"),
            P("col", None, "row"),
            P("col", None, "row"),
            P("col", "row", None),
            P("col", "row", None),
        ),
        out_specs=(
            P("col", "row", None),
            P("col", "row", None),
            P(),
            P("col", "row"),
            P("col", None),
            P(),
            P("col", "row"),
            P("row", "col"),
            P(),
            P(),
            P("col", "row"),
            P("col", "row"),
            P("row", "col"),
            P("col", None, "row"),
            P("col", None, "row"),
            P("col", "row", None),
        ),
        check_vma=False,
    )
```

```python
import functools

import jax
import jax.numpy as jnp
from jax import lax
from jax.experimental import pallas as pl
from jax.experimental.pallas import tpu as pltpu
from jax.sharding import PartitionSpec as P

NOPE = 128
ROPE = 64
LATENT = 512
VD = 128
TOPK = 6


EPS = 1e-06
ROWS_CONTRACT = (((0,), (0,)), ((), ()))
COLS_CONTRACT = (((1,), (1,)), ((), ()))


def matmul(left_side, right_side):
    return jnp.dot(left_side, right_side, preferred_element_type=jnp.float32)


def inner_rows(left_side, right_side):
    return lax.dot_general(left_side, right_side, ROWS_CONTRACT, preferred_element_type=jnp.float32)


def outer_cols(left_side, right_side):
    return lax.dot_general(left_side, right_side, COLS_CONTRACT, preferred_element_type=jnp.float32)


def rms_scale(values):
    return lax.rsqrt(jnp.mean(values * values, axis=-1, keepdims=True) + EPS)


def rms_back(values, scaling, gradient):
    return scaling * gradient - values * scaling**3 * jnp.mean(
        gradient * values, axis=-1, keepdims=True
    )


def silu_parts(preact):
    logistic = jax.nn.sigmoid(preact)
    return (preact * logistic, logistic * (1.0 + preact * (1.0 - logistic)))


def angle_tables(length):
    halfway = ROPE // 2
    frequency = 10000.0 ** (-2.0 * jnp.arange(halfway, dtype=jnp.float32) / ROPE)
    angles = jnp.arange(length, dtype=jnp.float32)[:, None] * frequency[None, :]
    return (jnp.cos(angles), jnp.sin(angles))


def rotate(values, cosine_in, sine_in):
    halfway = values.shape[-1] // 2
    leading = values[..., :halfway]
    trailing = values[..., halfway:]
    return jnp.concatenate(
        [leading * cosine_in - trailing * sine_in, leading * sine_in + trailing * cosine_in],
        axis=-1,
    )


def unrotate(values, cosine_in, sine_in):
    halfway = values.shape[-1] // 2
    leading = values[..., :halfway]
    trailing = values[..., halfway:]
    return jnp.concatenate(
        [leading * cosine_in + trailing * sine_in, trailing * cosine_in - leading * sine_in],
        axis=-1,
    )


F32 = jnp.float32
BF16 = jnp.bfloat16
EVERY = ("col", "row")
VMEM_LIMIT = 63 * 1024 * 1024


def token_rows(values):
    return lax.all_gather(values, "row", axis=0, tiled=True)


def every_token(values):
    return lax.all_gather(values, EVERY, axis=0, tiled=True)


def row_total(partial_value):
    return lax.psum_scatter(
        partial_value.astype(BF16), "row", scatter_dimension=0, tiled=True
    ).astype(F32)


def every_total(partial_value):
    return lax.psum_scatter(partial_value, EVERY, scatter_dimension=0, tiled=True).astype(F32)


def col_gather(values):
    return lax.all_gather(values, "col", axis=0, tiled=True)


def col_total(partial_value, dim):
    return lax.psum_scatter(
        partial_value.astype(BF16), "col", scatter_dimension=dim, tiled=True
    ).astype(F32)


MESH_ID = pl.DeviceIdType.MESH


def places():
    row, col = lax.axis_index("row"), lax.axis_index("col")
    return row // 2, lax.rem(row, 2), col // 2, lax.rem(col, 2)


def to_place(wide, core, line, side):
    return {"row": wide * 2 + core, "col": line * 2 + side}


def greet(partners, everyone):
    barrier = pltpu.get_barrier_semaphore()
    if everyone:
        n_row, n_col = lax.axis_size("row"), lax.axis_size("col")
        total = n_row * n_col
        me = lax.axis_index("col") * n_row + lax.axis_index("row")

        @pl.loop(1, total)
        def _(step):
            other = lax.rem(me + step, total)
            pl.semaphore_signal(
                barrier,
                inc=1,
                device_id={"row": lax.rem(other, n_row), "col": other // n_row},
                device_id_type=MESH_ID,
            )

        pl.semaphore_wait(barrier, total - 1)
        return
    for there, partner in partners:

        @pl.when(there)
        def _(partner=partner):
            pl.semaphore_signal(barrier, inc=1, device_id=partner, device_id_type=MESH_ID)

    pl.semaphore_wait(barrier, sum(jnp.int32(there) for there, _ in partners))


def remote(src, dst, send_sem, recv_sem, partner):
    return pltpu.make_async_remote_copy(
        src_ref=src,
        dst_ref=dst,
        send_sem=send_sem,
        recv_sem=recv_sem,
        device_id=partner,
        device_id_type=MESH_ID,
    )


def small_exchange(small_ref, small_out, send_sem, recv_sem, personal):
    n_row = lax.axis_size("row")
    total = n_row * lax.axis_size("col")
    me = lax.axis_index("col") * n_row + lax.axis_index("row")

    def copy(other, slot):
        return remote(
            small_ref.at[other] if personal else small_ref,
            small_out.at[slot],
            send_sem.at[other],
            recv_sem.at[slot],
            {"row": lax.rem(other, n_row), "col": other // n_row},
        )

    def start():
        @pl.loop(1, total)
        def _(step):
            copy(lax.rem(me + step, total), me).start()

        small_out[me] = small_ref[me] if personal else small_ref[...]

    def finish():
        @pl.loop(1, total)
        def _(step):
            other = lax.rem(me + step, total)
            copy(other, other).wait_recv()
            copy(other, me).wait_send()

    return start, finish


def line_order(lines):
    order = []
    for step in range((lines + 1) // 2):
        order.append(step)
        if lines - 1 - step != step:
            order.append(lines - 1 - step)
    return order


def every_total_plan(lines, ways, spots, place_ref, slots, extras, weights, outs, scratch):
    count = 1
    slots, extras, weights, outs = [slots], [extras], [weights], [outs]
    own, core_in, wide_in, side_in, up_in, down_in = scratch[:6]
    slot_in, staged, slot_sem, credit = scratch[6:10]
    core_send, core_recv, wide_send, wide_recv, side_send, side_recv = scratch[10:16]
    up_send, up_recv, down_send, down_recv = scratch[16:20]
    wide, core, line, side = spots
    tokens, width = own.shape[1:]
    ring, core_ring = slot_in.shape[0], core_in.shape[0]
    half = tokens // 2
    core_mate = to_place(wide, 1 - core, line, side)
    wide_mate = to_place(1 - wide, core, line, side)
    side_mate = to_place(wide, core, line, 1 - side)
    above = to_place(wide, core, line + 1, side)
    below = to_place(wide, core, line - 1, side)
    has_above = line < lines - 1
    has_below = line > 0
    parts = [pl.ds(0, half), pl.ds(half, half)]

    def at(a, l, s, w):
        return ((a * lines + l) * 2 + s) * 2 + w

    items = [(a, l) for a in range(count) for l in line_order(lines)]
    corners = [(1 - side, 1 - wide), (1 - side, wide), (side, 1 - wide), (side, wide)]
    blocks = []
    for a, l in items:
        for s, w in corners:
            blocks += [(a, 2 * at(0, l, s, w) + 1 - core), (a, 2 * at(0, l, s, w) + core)]

    def slot_copy(q):
        a, b = blocks[q]
        return pltpu.make_async_copy(
            slots[a].at[:, b], slot_in.at[q % ring], slot_sem.at[q % ring]
        )

    def summed(q):
        if q + ring - 1 < len(blocks):
            slot_copy(q + ring - 1).start()
        slot_copy(q).wait()
        a, b = blocks[q]
        rows = pl.ds(pl.multiple_of(b * tokens, tokens), tokens)
        total = inner_rows(place_ref[b], slot_in[q % ring].reshape(-1, width))
        return (total + matmul(extras[a][rows, :], weights[a][...])).astype(BF16)

    def core_copy(n):
        return remote(
            staged.at[n % ring],
            core_in.at[n % core_ring],
            core_send.at[n],
            core_recv.at[n],
            core_mate,
        )

    def spot(a, l, h, j):
        return ((a * lines + l) * 2 + h) * 2 + j

    def wide_copy(a, l, s, h):
        n = spot(a, l, h, 0 if ways[h] else s)
        return remote(
            own.at[at(a, l, s, 1 - wide), parts[h]],
            wide_in.at[n],
            wide_send.at[n],
            wide_recv.at[n],
            wide_mate,
        )

    def side_copy(a, l, w, h):
        n = spot(a, l, h, w if ways[h] else 0)
        return remote(
            own.at[at(a, l, 1 - side, w), parts[h]],
            side_in.at[n],
            side_send.at[n],
            side_recv.at[n],
            side_mate,
        )

    def up_copy(a, l, h):
        n = (a * lines + l) * 2 + h
        return remote(
            own.at[at(a, l, side, wide), parts[h]],
            up_in.at[n],
            up_send.at[n],
            up_recv.at[n],
            above,
        )

    def down_copy(a, l, h):
        n = (a * lines + l) * 2 + h
        return remote(
            own.at[at(a, l, side, wide), parts[h]],
            down_in.at[n],
            down_send.at[n],
            down_recv.at[n],
            below,
        )

    def add(i, rows, other):
        own[i, rows] = (own[i, rows].astype(F32) + other[...].astype(F32)).astype(BF16)

    def start():
        for q in range(ring - 1):
            slot_copy(q).start()

    def stage_one(t):
        a, l = items[t]
        for j, (s, w) in enumerate(corners):
            n = t * 4 + j
            if n >= ring:
                core_copy(n - ring).wait_send()
            staged[n % ring] = summed(t * 8 + 2 * j)
            if n >= core_ring:
                pl.semaphore_wait(credit, 1)
            core_copy(n).start()
            own[at(a, l, s, w)] = summed(t * 8 + 2 * j + 1)
            core_copy(n).wait_recv()
            add(at(a, l, s, w), pl.ds(0, tokens), core_in.at[n % core_ring])
            if n + core_ring < 4 * len(items):
                pl.semaphore_signal(
                    credit, inc=1, device_id=core_mate, device_id_type=MESH_ID
                )
            for h in range(2):
                if ways[h] and j in (0, 1):
                    side_copy(a, l, w, h).start()
                if not ways[h] and j in (0, 2):
                    wide_copy(a, l, s, h).start()

    def stage_two(a, l):
        for j in range(2):
            s = side if j else 1 - side
            w = wide if j else 1 - wide
            for h in range(2):
                if ways[h]:
                    side_copy(a, l, w, h).wait_recv()
                    add(at(a, l, side, w), parts[h], side_in.at[spot(a, l, h, w)])
                    if j == 0:
                        wide_copy(a, l, side, h).start()
                else:
                    wide_copy(a, l, s, h).wait_recv()
                    add(at(a, l, s, wide), parts[h], wide_in.at[spot(a, l, h, s)])
                    if j == 0:
                        side_copy(a, l, wide, h).start()

    def stage_three(a, l):
        i = at(a, l, side, wide)
        for h in range(2):
            if ways[h]:
                wide_copy(a, l, side, h).wait_recv()
                add(i, parts[h], wide_in.at[spot(a, l, h, 0)])
            else:
                side_copy(a, l, wide, h).wait_recv()
                add(i, parts[h], side_in.at[spot(a, l, h, 0)])

            @pl.when(jnp.logical_and(line == 0, l > 0))
            def _(h=h):
                up_copy(a, l, h).start()

            @pl.when(jnp.logical_and(line == lines - 1, l < lines - 1))
            def _(h=h):
                down_copy(a, l, h).start()

    def onward(a, l, up):
        @pl.when(jnp.logical_and(has_below, has_above))
        def _():
            copy, arrived = (up_copy, up_in) if up else (down_copy, down_in)
            for h in range(2):
                copy(a, l, h).wait_recv()
                add(at(a, l, side, wide), parts[h], arrived.at[(a * lines + l) * 2 + h])
                copy(a, l, h).start()

    def passing(a, j):
        high, low = lines - 1 - j, j
        lower_half = line * 2 < lines

        def go(up, when):
            l = high if up else low
            beyond = line < l if up else line > l

            @pl.when(jnp.logical_and(when, beyond))
            def _():
                onward(a, l, up)

        go(True, lower_half)
        go(False, lower_half)
        go(False, jnp.logical_not(lower_half))
        go(True, jnp.logical_not(lower_half))

    def final(a):
        for h in range(2):

            @pl.when(has_below)
            def _(h=h):
                up_copy(a, line, h).wait_recv()
                add(at(a, line, side, wide), parts[h], up_in.at[(a * lines + line) * 2 + h])

            @pl.when(has_above)
            def _(h=h):
                down_copy(a, line, h).wait_recv()
                add(at(a, line, side, wide), parts[h], down_in.at[(a * lines + line) * 2 + h])

        outs[a][...] = own[at(a, line, side, wide)].astype(F32)

    def one(t):
        stage_one(t)

    def two(t):
        stage_two(*items[t])

    def three(t):
        stage_three(*items[t])

    def along(j):
        passing(0, j)

    def last(_):
        final(0)

    def finish():
        for n in range(4 * len(items) - ring, 4 * len(items)):
            core_copy(n).wait_send()
        for a, l in items:
            for h in range(2):
                for j in range(1 if ways[h] else 2):
                    wide_copy(a, l, side if ways[h] else j, h).wait_send()
                for j in range(2 if ways[h] else 1):
                    side_copy(a, l, j if ways[h] else wide, h).wait_send()

                @pl.when(jnp.logical_and(has_above, line < l))
                def _(h=h, a=a, l=l):
                    up_copy(a, l, h).wait_send()

                @pl.when(jnp.logical_and(has_below, line > l))
                def _(h=h, a=a, l=l):
                    down_copy(a, l, h).wait_send()

    return start, (one, two, three, along, last), finish


def kernel_fits(place_shape, width):
    blocks, _, tokens = place_shape
    return tokens % 32 == 0 and 4 * blocks * tokens * width <= 40 * 1024 * 1024


def row_mates(wide, core, line, side):
    return to_place(wide, 1 - core, line, side), to_place(1 - wide, core, line, side)


def strip(ref, dim, index, size):
    start = pl.multiple_of(index * size, size)
    return ref.at[pl.ds(start, size)] if dim == 0 else ref.at[:, pl.ds(start, size)]


def cols_plan(lines, dims, flips, spots, cols, outs, sems):
    wide, core, line, side = spots
    side_mate = to_place(wide, core, line, 1 - side)
    above = to_place(wide, core, line + 1, side)
    below = to_place(wide, core, line - 1, side)
    has_above, has_below = line < lines - 1, line > 0
    local_sem, side_send, side_recv, up_send, up_recv, down_send, down_recv = sems
    count = len(dims)

    def spot(m, l, s):
        return strip(outs[m], dims[m], l * 2 + s, cols[m].shape[dims[m]])

    def line_copy(m, l, s, up, here=False):
        n = (m * lines + l) * 2 + s
        return remote(
            cols[m] if here else spot(m, l, s),
            spot(m, l, s),
            (up_send if up else down_send).at[n],
            (up_recv if up else down_recv).at[n],
            above if up else below,
        )

    def side_copy(m, l, here=False):
        n = m * lines + l
        return remote(
            cols[m] if here else spot(m, l, side),
            spot(m, l, side),
            side_send.at[n],
            side_recv.at[n],
            side_mate,
        )

    def to_line(m, s, here):
        @pl.when(has_above)
        def _():
            line_copy(m, line, s, True, here).start()

        @pl.when(has_below)
        def _():
            line_copy(m, line, s, False, here).start()

    def local(m):
        return pltpu.make_async_copy(cols[m], spot(m, line, side), local_sem.at[m])

    def start():
        for m in range(count):
            to_line(m, side, True)
            side_copy(m, line, True).start()
        for m in range(count):
            local(m).start()

    def from_line(m, dist, up):
        l = line - dist if up else line + dist

        @pl.when(l >= 0 if up else l < lines)
        def _():
            for s in (side, 1 - side) if flips[m] else (side,):
                line_copy(m, l, s, up).wait_recv()

                @pl.when(has_above if up else has_below)
                def _(s=s):
                    line_copy(m, l, s, up).start()

            if not flips[m]:
                side_copy(m, l).start()

    def step(dist):
        if dist == 1:
            for m in range(count):
                if flips[m]:
                    side_copy(m, line).wait_recv()
                    to_line(m, 1 - side, False)
        if dist < lines:
            for m in range(count):
                from_line(m, dist, True)
                from_line(m, dist, False)

    def finish():
        for m in range(count):
            local(m).wait()
            if flips[m]:
                side_copy(m, line).wait_send()
            for l in range(lines):
                if not flips[m]:
                    side_copy(m, l).wait()
                for s in range(2) if flips[m] else (side,):

                    @pl.when(jnp.logical_and(has_above, line >= l))
                    def _(m=m, l=l, s=s):
                        line_copy(m, l, s, True).wait_send()

                    @pl.when(jnp.logical_and(has_below, line <= l))
                    def _(m=m, l=l, s=s):
                        line_copy(m, l, s, False).wait_send()

    return start, step, finish


def row_plan(spots, row_ref, out_ref, sems):
    wide, core, line, side = spots
    core_mate, wide_mate = row_mates(wide, core, line, side)
    local_sem, core_send, core_recv, wide_send, wide_recv = sems
    tokens = row_ref.shape[0]

    def spot(w, k):
        return strip(out_ref, 0, w * 2 + k, tokens)

    def core_copy(n):
        src = row_ref if n == 0 else spot(1 - wide, core)
        dst = spot(wide if n == 0 else 1 - wide, core)
        return remote(src, dst, core_send.at[n], core_recv.at[n], core_mate)

    wide_copy = remote(row_ref, spot(wide, core), wide_send.at[0], wide_recv.at[0], wide_mate)
    local = pltpu.make_async_copy(row_ref, spot(wide, core), local_sem.at[0])

    def start():
        wide_copy.start()
        core_copy(0).start()
        local.start()

    def step(dist):
        if dist == 1:
            wide_copy.wait_recv()
            core_copy(1).start()

    def finish():
        local.wait()
        wide_copy.wait_send()
        for n in range(2):
            core_copy(n).wait()

    return start, step, finish


def every_plan(lines, ways, spots, own_ref, out_ref, sems):
    wide, core, line, side = spots
    core_mate, wide_mate = row_mates(wide, core, line, side)
    side_mate = to_place(wide, core, line, 1 - side)
    above = to_place(wide, core, line + 1, side)
    below = to_place(wide, core, line - 1, side)
    has_above, has_below = line < lines - 1, line > 0
    local_sem, core_send, core_recv, wide_send, wide_recv, side_send, side_recv = sems[:7]
    up_send, up_recv, down_send, down_recv = sems[7:]
    tokens = own_ref.shape[0]
    half = tokens // 2

    def spot(l, s, w, k, h):
        return out_ref.at[pl.ds((((l * 2 + s) * 2 + w) * 2 + k) * tokens + h * half, half)]

    def source(l, s, w, h, here):
        return own_ref.at[pl.ds(h * half, half)] if here else spot(l, s, w, core, h)

    def core_copy(l, s, w, h, here=False):
        n = ((l * 2 + s) * 2 + w) * 2 + h
        return remote(
            source(l, s, w, h, here),
            spot(l, s, w, core, h),
            core_send.at[n],
            core_recv.at[n],
            core_mate,
        )

    def wide_copy(l, s, h, here=False):
        n = (l * 2 + h) * 2 + (0 if ways[h] else s)
        return remote(
            source(l, s, wide, h, here),
            spot(l, s, wide, core, h),
            wide_send.at[n],
            wide_recv.at[n],
            wide_mate,
        )

    def side_copy(l, w, h, here=False):
        n = (l * 2 + h) * 2 + (w if ways[h] else 0)
        return remote(
            source(l, side, w, h, here),
            spot(l, side, w, core, h),
            side_send.at[n],
            side_recv.at[n],
            side_mate,
        )

    def line_copy(l, h, up, here=False):
        n = l * 2 + h
        return remote(
            source(l, side, wide, h, here),
            spot(l, side, wide, core, h),
            (up_send if up else down_send).at[n],
            (up_recv if up else down_recv).at[n],
            above if up else below,
        )

    def local(h):
        return pltpu.make_async_copy(
            own_ref.at[pl.ds(h * half, half)], spot(line, side, wide, core, h), local_sem.at[h]
        )

    def spread(l, h, here=False):
        if ways[h]:
            wide_copy(l, side, h, here).start()
            side_copy(l, wide, h, here).start()
        else:
            side_copy(l, wide, h, here).start()
            wide_copy(l, side, h, here).start()
        core_copy(l, side, wide, h, here).start()

    def second(l):
        for h in range(2):
            if ways[h]:
                wide_copy(l, side, h).wait_recv()
                side_copy(l, 1 - wide, h).start()
                core_copy(l, side, 1 - wide, h).start()
            else:
                side_copy(l, wide, h).wait_recv()
                wide_copy(l, 1 - side, h).start()
                core_copy(l, 1 - side, wide, h).start()

    def third(l):
        for j in range(2):
            for h in range(2):
                if ways[h]:
                    w = 1 - wide if j else wide
                    side_copy(l, w, h).wait_recv()
                    core_copy(l, 1 - side, w, h).start()
                else:
                    s = 1 - side if j else side
                    wide_copy(l, s, h).wait_recv()
                    core_copy(l, s, 1 - wide, h).start()

    def start():
        for h in range(2):

            @pl.when(has_above)
            def _(h=h):
                line_copy(line, h, True, True).start()

            @pl.when(has_below)
            def _(h=h):
                line_copy(line, h, False, True).start()

            spread(line, h, True)
        for h in range(2):
            local(h).start()

    def from_line(dist, up):
        l = line - dist if up else line + dist

        @pl.when(l >= 0 if up else l < lines)
        def _():
            for h in range(2):
                line_copy(l, h, up).wait_recv()

                @pl.when(has_above if up else has_below)
                def _(h=h):
                    line_copy(l, h, up).start()

                spread(l, h)

    def stage(action, dist):
        if dist == 0:
            action(line)
            return

        @pl.when(line - dist >= 0)
        def _():
            action(line - dist)

        @pl.when(line + dist < lines)
        def _():
            action(line + dist)

    def step(dist):
        if dist < lines:
            from_line(dist, True)
            from_line(dist, False)
        if dist - 1 < lines:
            stage(second, dist - 1)
        if 0 <= dist - 2 < lines:
            stage(third, dist - 2)

    def finish():
        for h in range(2):
            local(h).wait()
        for l in range(lines):
            for s in range(2):
                for w in range(2):
                    for h in range(2):
                        core_copy(l, s, w, h).wait()
            for h in range(2):
                for j in range(1 if ways[h] else 2):
                    wide_copy(l, side if ways[h] else j, h).wait_send()
                for j in range(2 if ways[h] else 1):
                    side_copy(l, j if ways[h] else wide, h).wait_send()

                @pl.when(jnp.logical_and(has_above, line >= l))
                def _(h=h, l=l):
                    line_copy(l, h, True).wait_send()

                @pl.when(jnp.logical_and(has_below, line <= l))
                def _(h=h, l=l):
                    line_copy(l, h, False).wait_send()

    return start, step, finish


def pick_plan(lines, place_ref, rows_ref, slots_ref, rows_in, slots_out, load_sem, store_sem):
    ring, tokens = rows_in.shape[:2]
    blocks = place_ref.shape[0]
    chunks = lines + 1
    per_step = -(-blocks // chunks)

    def load(b):
        return pltpu.make_async_copy(
            rows_ref.at[pl.ds(pl.multiple_of(b * tokens, tokens), tokens)],
            rows_in.at[lax.rem(b, ring)],
            load_sem.at[lax.rem(b, ring)],
        )

    def store(b):
        return pltpu.make_async_copy(
            slots_out.at[lax.rem(b, ring)], slots_ref.at[:, b], store_sem.at[lax.rem(b, ring)]
        )

    def start():
        for b in range(ring - 1):
            load(b).start()

    def step(dist):
        @pl.loop((dist - 1) * per_step, min(dist * per_step, blocks))
        def _(b):
            @pl.when(b + ring - 1 < blocks)
            def _():
                load(b + ring - 1).start()

            load(b).wait()

            @pl.when(b >= ring)
            def _():
                store(b - ring).wait()

            slot = lax.rem(b, ring)
            picked = matmul(place_ref[b], rows_in[slot])
            slots_out[slot] = picked.astype(BF16).reshape(slots_out.shape[1:])
            store(b).start()

    def finish():
        for b in range(blocks - ring, blocks):
            store(b).wait()

    return start, step, finish


def gather_body(lines, dims, flips, ways, kinds, *refs):
    has_row, has_every, has_small, has_pick = kinds
    count = len(dims)
    outputs = count + has_row + has_every + has_small
    if has_pick:
        pick_refs = refs[outputs : outputs + 2]
        pick_refs += refs[2 * outputs + 2 : 2 * outputs + 3] + refs[-4:]
        refs = refs[:outputs] + refs[outputs + 2 : 2 * outputs + 2] + refs[2 * outputs + 3 : -4]
    ins, outs, sems = refs[:outputs], refs[outputs : 2 * outputs], list(refs[2 * outputs :])
    spots = places()
    wide, core, line, side = spots
    core_mate, wide_mate = row_mates(*spots)
    partners = [(core >= 0, core_mate), (core >= 0, wide_mate)]
    if count or has_every:
        partners += [
            (core >= 0, to_place(wide, core, line, 1 - side)),
            (line < lines - 1, to_place(wide, core, line + 1, side)),
            (line > 0, to_place(wide, core, line - 1, side)),
        ]
    greet(partners, has_small)

    def take(n):
        taken, sems[:] = sems[:n], sems[n:]
        return taken

    plans, at = [], count
    if count:
        plans.append(cols_plan(lines, dims, flips, spots, ins[:count], outs[:count], take(7)))
    if has_row:
        plans.append(row_plan(spots, ins[at], outs[at], take(5)))
        at += 1
    if has_every:
        plans.append(every_plan(lines, ways, spots, ins[at], outs[at], take(11)))
        at += 1
    if has_small:
        small_start, small_finish = small_exchange(ins[at], outs[at], *take(2), False)
    if has_pick:
        plans.append(pick_plan(lines, *pick_refs))
    for start, _, _ in plans:
        start()
    if has_small:
        small_start()
    for dist in range(1, lines + 2):
        for _, step, _ in plans:
            step(dist)
    if has_small:
        small_finish()
    for _, _, finish in plans:
        finish()


def kernel_gather(
    col_values, dims, flips, row_value, every_value, ways, small_value, number, pick=None
):
    n_row, n_col = lax.axis_size("row"), lax.axis_size("col")
    lines, count, total = n_col // 2, len(dims), n_row * n_col
    hbm, vmem = pl.BlockSpec(memory_space=pl.ANY), pl.BlockSpec(memory_space=pltpu.VMEM)
    dma = pltpu.SemaphoreType.DMA
    operands, in_specs, out_specs, out_shape = list(col_values), [hbm] * count, [hbm] * count, []
    scratch = []
    for value, dim in zip(col_values, dims):
        shape = list(value.shape)
        shape[dim] *= n_col
        out_shape.append(jax.ShapeDtypeStruct(tuple(shape), value.dtype))
    if count:
        scratch += [dma((count,))] + [dma((count * lines,))] * 2
        scratch += [dma((2 * count * lines,))] * 4
    if row_value is not None:
        scratch += [dma((1,)), dma((2,)), dma((2,)), dma((1,)), dma((1,))]
    if every_value is not None:
        scratch += [dma((2,)), *[dma((8 * lines,))] * 2, *[dma((4 * lines,))] * 4]
        scratch += [dma((2 * lines,))] * 4
    for value, times in ((row_value, n_row), (every_value, total)):
        if value is not None:
            operands.append(value)
            in_specs.append(vmem)
            out_specs.append(hbm)
            shape = (times * value.shape[0], *value.shape[1:])
            out_shape.append(jax.ShapeDtypeStruct(shape, value.dtype))
    if small_value is not None:
        operands.append(small_value)
        in_specs.append(vmem)
        out_specs.append(vmem)
        out_shape.append(jax.ShapeDtypeStruct((total, *small_value.shape), small_value.dtype))
        scratch += [dma((total,))] * 2
    if pick is not None:
        place, rows, local_experts = pick
        blocks, slots, tokens = place.shape
        shape = (local_experts, slots // local_experts, rows.shape[1])
        operands += [place, rows]
        in_specs += [vmem, hbm]
        out_specs.append(hbm)
        out_shape.append(jax.ShapeDtypeStruct((shape[0], blocks, *shape[1:]), BF16))
        scratch += [
            pltpu.VMEM((4, tokens, rows.shape[1]), BF16),
            pltpu.VMEM((4, *shape), BF16),
            dma((4,)),
            dma((4,)),
        ]
    kinds = tuple(value is not None for value in (row_value, every_value, small_value, pick))
    return pl.pallas_call(
        functools.partial(gather_body, lines, tuple(dims), tuple(flips), ways, kinds),
        out_shape=out_shape,
        in_specs=in_specs,
        out_specs=out_specs,
        scratch_shapes=scratch,
        compiler_params=pltpu.CompilerParams(collective_id=number, has_side_effects=True),
        name=f"gather_{number}",
    )(*operands)


def mixed_total_plan(lines, dims, flips, spots, refs):
    count = len(dims)
    cols, row_ref, refs = refs[:count], refs[count], refs[count + 1 :]
    col_outs, row_out, refs = refs[:count], refs[count], refs[count + 1 :]
    row_own, row_core, row_wide, refs = refs[0], refs[1], refs[2], refs[3:]
    owns, refs = refs[:count], refs[count:]
    side_ins, refs = refs[:count], refs[count:]
    up_ins, refs = refs[:count], refs[count:]
    down_ins, refs = refs[:count], refs[count:]
    row_load, core_send, core_recv, wide_send, wide_recv = refs[:5]
    if count:
        load_sem, side_send, side_recv, up_send, up_recv, down_send, down_recv = refs[5:12]
    wide, core, line, side = spots
    core_mate, wide_mate = row_mates(wide, core, line, side)
    side_mate = to_place(wide, core, line, 1 - side)
    above = to_place(wide, core, line + 1, side)
    below = to_place(wide, core, line - 1, side)
    has_above = line < lines - 1
    has_below = line > 0
    tokens = row_out.shape[0]

    def core_copy(w):
        return remote(
            strip(row_ref, 0, w * 2 + 1 - core, tokens),
            row_core.at[w],
            core_send.at[w],
            core_recv.at[w],
            core_mate,
        )

    def row_loaded(w):
        return pltpu.make_async_copy(
            strip(row_ref, 0, w * 2 + core, tokens), row_own.at[w], row_load.at[w]
        )

    wide_copy = remote(row_own.at[1 - wide], row_wide, wide_send.at[0], wide_recv.at[0], wide_mate)

    def source(m, l, s):
        return strip(cols[m], dims[m], l * 2 + s, col_outs[m].shape[dims[m]])

    def side_copy(m, l):
        n = m * lines + l
        return remote(
            owns[m].at[l, 1 - side] if flips[m] else source(m, l, 1 - side),
            side_ins[m].at[0 if flips[m] else l],
            side_send.at[n],
            side_recv.at[n],
            side_mate,
        )

    def own_at(m, l, s):
        return owns[m].at[l, s] if flips[m] else owns[m].at[l]

    def loaded(m, l, s):
        return pltpu.make_async_copy(
            source(m, l, s), own_at(m, l, s), load_sem.at[(m * lines + l) * 2 + s]
        )

    def line_copy(m, l, s, up):
        n = (m * lines + l) * 2 + s
        into = (up_ins if up else down_ins)[m]
        return remote(
            own_at(m, l, s),
            into.at[l, s] if flips[m] else into.at[l],
            (up_send if up else down_send).at[n],
            (up_recv if up else down_recv).at[n],
            above if up else below,
        )

    def sides(m):
        return (1 - side, side) if flips[m] else (side,)

    def add(m, l, s, other):
        mine = own_at(m, l, s)
        mine[...] = (mine[...].astype(F32) + other.astype(F32)).astype(BF16)

    def near(m, l):
        for s in sides(m):
            loaded(m, l, s).wait()
            if not flips[m]:
                side_copy(m, l).wait_recv()
                add(m, l, s, side_ins[m][l])

            @pl.when(jnp.logical_and(line == 0, l > 0))
            def _(s=s):
                line_copy(m, l, s, True).start()

            @pl.when(jnp.logical_and(line == lines - 1, l < lines - 1))
            def _(s=s):
                line_copy(m, l, s, False).start()

    def onward(m, l, up):
        @pl.when(jnp.logical_and(has_below, has_above))
        def _():
            for s in sides(m):
                where = (l, s) if flips[m] else (l,)
                line_copy(m, l, s, up).wait_recv()
                add(m, l, s, (up_ins if up else down_ins)[m][where])
                line_copy(m, l, s, up).start()

    def passing(m, j):
        high, low = lines - 1 - j, j
        lower_half = line * 2 < lines

        def go(up, when):
            l = high if up else low
            beyond = line < l if up else line > l

            @pl.when(jnp.logical_and(when, beyond))
            def _():
                onward(m, l, up)

        go(True, lower_half)
        go(False, lower_half)
        go(False, jnp.logical_not(lower_half))
        go(True, jnp.logical_not(lower_half))

    def final(m):
        for s in sides(m):
            where = (line, s) if flips[m] else (line,)

            @pl.when(has_below)
            def _(s=s, where=where):
                line_copy(m, line, s, True).wait_recv()
                add(m, line, s, up_ins[m][where])

            @pl.when(has_above)
            def _(s=s, where=where):
                line_copy(m, line, s, False).wait_recv()
                add(m, line, s, down_ins[m][where])

        if flips[m]:
            side_copy(m, line).start()

    flipped = [m for m in range(count) if flips[m]]
    straight = [m for m in range(count) if not flips[m]]
    order = line_order(lines)
    def start():
        for w in range(2):
            core_copy(w).start()
            row_loaded(w).start()
        items = [(m, l) for l in (line_order(lines) if count else []) for m in range(count)]
        for m, l in items:
            for s in sides(m):
                loaded(m, l, s).start()
            if not flips[m]:
                side_copy(m, l).start()

    def step_on(step):
        if step == 0:
            for j in range(2):
                w = wide if j else 1 - wide
                row_loaded(w).wait()
                core_copy(w).wait_recv()
                row_own[w] = (row_own[w].astype(F32) + row_core[w].astype(F32)).astype(BF16)
                if j == 0:
                    wide_copy.start()
            for l in order:
                for m in flipped:
                    near(m, l)
        if step == 1:
            wide_copy.wait_recv()
            row_out[...] = row_own[wide].astype(F32) + row_wide[...].astype(F32)
        if not count:
            return
        if step < lines:
            for m in straight:
                near(m, order[step])
        if step < lines - 1:
            for m in flipped:
                passing(m, step)
        if step == lines - 1:
            for m in flipped:
                final(m)
        if 2 <= step < lines + 1:
            for m in straight:
                passing(m, step - 2)
        if step == lines + 1:
            for m in straight:
                final(m)

    def finish():
        wide_copy.wait_send()
        for w in range(2):
            core_copy(w).wait_send()
        for m in range(count):
            if flips[m]:
                side_copy(m, line).wait()
                add(m, line, side, side_ins[m][0])
            col_outs[m][...] = own_at(m, line, side)[...].astype(F32)
            for l in range(lines):
                if not flips[m]:
                    side_copy(m, l).wait_send()
                for s in sides(m):

                    @pl.when(jnp.logical_and(has_above, line < l))
                    def _(m=m, l=l, s=s):
                        line_copy(m, l, s, True).wait_send()

                    @pl.when(jnp.logical_and(has_below, line > l))
                    def _(m=m, l=l, s=s):
                        line_copy(m, l, s, False).wait_send()

    def own_rows(m, rows):
        return own_at(m, line, side).at[rows]

    return start, step_on, finish, lines + 2, own_rows


def total_order(lines, stages, mixed_step):
    one, two, three, along, last = stages
    order = []
    lag = 3 if mixed_step else 2
    late_two = [(two, lines - 1)]
    for k in range(lines):
        order.append((one, k))
        if mixed_step:
            order.append((mixed_step, k))
        if k >= lag and lag == 3:
            order.append((three, k - lag))
        if k >= 1:
            order.append((two, k - 1))
        if k >= lag and lag == 2:
            order.append((three, k - lag))
    rest = [(three, k) for k in range(max(0, lines - lag), lines)]
    if mixed_step:
        order += rest[:-2] + [(mixed_step, lines)]
        if lines >= 4:
            order.append((along, 0))
        order += rest[-2:-1] + late_two + [(mixed_step, lines + 1)] + rest[-1:]
    else:
        order += late_two
        if lines >= 4:
            order.append((along, 0))
        order += rest
    order += [(along, j) for j in range(1 if lines >= 4 else 0, lines - 1)]
    return order + [(last, 0)]


def last_plan(row_out, scaled_ref, gains_ref, sums_ref, down_ref, scratch):
    row_in, held, summed = scratch[:3]
    row_send, row_recv, col_send, col_recv, down_send, down_recv, local_sem = scratch[3:]
    n_row, n_col = lax.axis_size("row"), lax.axis_size("col")
    row, col = lax.axis_index("row"), lax.axis_index("col")
    rows = [{"row": lax.rem(row + d, n_row), "col": col} for d in range(1, n_row)]
    cols = [{"row": row, "col": lax.rem(col + d, n_col)} for d in range(1, n_col)]
    size = down_ref.shape[0] // n_row

    def row_copy(d, source):
        return remote(held, row_in.at[source], row_send.at[d], row_recv.at[source], rows[d])

    def col_copy(d, source):
        return remote(summed, sums_ref.at[source], col_send.at[d], col_recv.at[source], cols[d])

    def down_copy(d, source, value):
        return remote(
            value,
            strip(down_ref, 0, source, size),
            down_send.at[d],
            down_recv.at[source],
            rows[d],
        )

    def first():
        held[...] = gains_ref[...]
        part = jnp.sum(row_out[...] * scaled_ref[...], axis=0, keepdims=True)
        piece = part.shape[1] // 4
        for i in range(4):
            held[i : i + 1, 0:piece] = part[:, i * piece : (i + 1) * piece]
        for d in range(n_row - 1):
            row_copy(d, row).start()

    def second():
        total = held[...]
        for d in range(n_row - 1):
            source = rows[d]["row"]
            row_copy(d, source).wait_recv()
            total = total + row_in[source]
        summed[...] = total
        sums_ref[col] = total
        for d in range(n_col - 1):
            col_copy(d, col).start()

    def local(value):
        return pltpu.make_async_copy(value, strip(down_ref, 0, row, size), local_sem)

    def third(value):
        local(value).start()
        for d in range(n_row - 1):
            down_copy(d, row, value).start()

    def finish(value):
        for d in range(n_col - 1):
            col_copy(d, cols[d]["col"]).wait_recv()
            col_copy(d, col).wait_send()
        for d in range(n_row - 1):
            row_copy(d, row).wait_send()
            down_copy(d, rows[d]["row"], value).wait_recv()
            down_copy(d, row, value).wait_send()
        local(value).wait()

    return rows + cols, first, second, third, finish


def total_body(lines, dims, flips, ways, kinds, *refs):
    has_mixed, has_every, has_small, has_last = kinds
    count = len(dims)
    spots = places()
    wide, core, line, side = spots
    core_mate, wide_mate = row_mates(*spots)
    partners = [(core >= 0, core_mate), (core >= 0, wide_mate)]
    if count or has_every:
        partners += [
            (core >= 0, to_place(wide, core, line, 1 - side)),
            (line < lines - 1, to_place(wide, core, line + 1, side)),
            (line > 0, to_place(wide, core, line - 1, side)),
        ]
    refs = list(refs)

    def take(n):
        taken, refs[:] = refs[:n], refs[n:]
        return taken

    mixed = (count + 1) * has_mixed
    mixed_ins, every_ins, small_ins = take(mixed), take(4 * has_every), take(has_small)
    last_ins = take(2 * has_last)
    mixed_outs, every_outs, small_outs = take(mixed), take(has_every), take(has_small)
    if has_last:
        last_outs = take(2)
        down_rows = last_outs[1].shape[0] // lax.axis_size("row")
        peers, last_first, last_second, last_third, last_finish = last_plan(
            mixed_outs[-1], *last_ins, *last_outs, take(10)
        )
        partners = [(core >= 0, peer) for peer in peers]
    greet(partners, has_small)
    if has_small:
        small_start, small_finish = small_exchange(
            *small_ins, *small_outs, *take(2), len(small_ins[0].shape) == 3
        )
    mixed_step = None
    if has_every:
        every_start, stages, every_finish = every_total_plan(
            lines, ways, spots, *every_ins, *every_outs, take(20)
        )
        every_start()
    if has_mixed:
        mixed_start, mixed_go, mixed_finish, mixed_steps, own_rows = mixed_total_plan(
            lines, dims, flips, spots, mixed_ins + mixed_outs + refs
        )
        mixed_start()

        def down_value():
            return own_rows(1, pl.ds(mixed_outs[1].shape[0] - down_rows, down_rows))

        def mixed_step(step):
            mixed_go(step)
            if has_last and step == 1:
                last_first()
            if has_last and step == lines:
                last_second()
            if has_last and step == lines + 1:
                last_third(down_value())

    if has_every:
        for number, (action, index) in enumerate(total_order(lines, stages, mixed_step)):
            action(index)
            if has_small and number == 0:
                small_start()
    else:
        if has_small:
            small_start()
        for step in range(mixed_steps):
            mixed_step(step)
    if has_last:
        last_finish(down_value())
    if has_mixed:
        mixed_finish()
    if has_every:
        every_finish()
    if has_small:
        small_finish()


def kernel_total(
    col_values, dims, flips, row_value, every_value, ways, small_value, number, last_value=None
):
    n_row, n_col = lax.axis_size("row"), lax.axis_size("col")
    lines, count = n_col // 2, len(dims)
    hbm, vmem = pl.BlockSpec(memory_space=pl.ANY), pl.BlockSpec(memory_space=pltpu.VMEM)
    dma = pltpu.SemaphoreType.DMA
    operands, in_specs, out_shape, scratch = [], [], [], []
    if row_value is not None:
        operands += [*col_values, row_value]
        in_specs += [hbm] * (count + 1)
        blocks = []
        for value, dim in zip(col_values, dims):
            shape = list(value.shape)
            shape[dim] //= n_col
            blocks.append(tuple(shape))
        tokens, width = row_value.shape[0] // n_row, row_value.shape[1]
        out_shape += [jax.ShapeDtypeStruct(shape, F32) for shape in blocks]
        out_shape.append(jax.ShapeDtypeStruct((tokens, width), F32))
    every_scratch, small_scratch = [], []
    if every_value is not None:
        place, slots, extra, weight = every_value
        n_blocks, _, tokens = place.shape
        local_experts, rows, width = slots.shape
        capacity = rows // n_blocks
        operands += [place, slots.reshape(local_experts, n_blocks, capacity, width), extra, weight]
        in_specs += [vmem, hbm, vmem, vmem]
        out_shape.append(jax.ShapeDtypeStruct((tokens, width), F32))
        half = (tokens // 2, width)
        every_scratch = [
            pltpu.VMEM((4 * lines, tokens, width), BF16),
            pltpu.VMEM((8, tokens, width), BF16),
            pltpu.VMEM((4 * lines, *half), BF16),
            pltpu.VMEM((4 * lines, *half), BF16),
            pltpu.VMEM((2 * lines, *half), BF16),
            pltpu.VMEM((2 * lines, *half), BF16),
            pltpu.VMEM((4, local_experts, capacity, width), BF16),
            pltpu.VMEM((4, tokens, width), BF16),
            dma((4,)),
            pltpu.SemaphoreType.REGULAR,
            *[dma((4 * lines,))] * 6,
            *[dma((2 * lines,))] * 4,
        ]
    if small_value is not None:
        operands.append(small_value)
        in_specs.append(vmem)
        lead = () if small_value.ndim == 3 else (n_row * n_col,)
        out_shape.append(jax.ShapeDtypeStruct((*lead, *small_value.shape), small_value.dtype))
        small_scratch = [dma((n_row * n_col,))] * 2
    if last_value is not None:
        scaled, gains, down_rows = last_value
        operands += [scaled, gains]
        in_specs += [vmem, vmem]
        out_shape += [
            jax.ShapeDtypeStruct((n_col, *gains.shape), F32),
            jax.ShapeDtypeStruct((n_row * down_rows, blocks[1][1]), BF16),
        ]
        scratch += [
            pltpu.VMEM((n_row, *gains.shape), F32),
            pltpu.VMEM(gains.shape, F32),
            pltpu.VMEM(gains.shape, F32),
            dma((n_row - 1,)),
            dma((n_row,)),
            dma((n_col - 1,)),
            dma((n_col,)),
            dma((n_row - 1,)),
            dma((n_row,)),
            dma,
        ]
    scratch += small_scratch + every_scratch
    if row_value is not None:
        tokens, width = row_value.shape[0] // n_row, row_value.shape[1]
        scratch += [
            pltpu.VMEM((2, tokens, width), BF16),
            pltpu.VMEM((2, tokens, width), BF16),
            pltpu.VMEM((tokens, width), BF16),
        ]
        doubled = [(lines, 2) if flip else (lines,) for flip in flips]
        side_held = [(1,) if flip else (lines,) for flip in flips]
        for lead in (doubled, side_held, doubled, doubled):
            scratch += [pltpu.VMEM((*d, *shape), BF16) for d, shape in zip(lead, blocks)]
        scratch += [dma((2,)), dma((2,)), dma((2,)), dma((1,)), dma((1,))]
        if count:
            scratch += [dma((2 * count * lines,))] + [dma((count * lines,))] * 2
            scratch += [dma((2 * count * lines,))] * 4
    kinds = tuple(v is not None for v in (row_value, every_value, small_value, last_value))
    return pl.pallas_call(
        functools.partial(total_body, lines, tuple(dims), tuple(flips), ways, kinds),
        out_shape=out_shape,
        in_specs=in_specs,
        out_specs=[vmem] * len(out_shape),
        scratch_shapes=scratch,
        compiler_params=pltpu.CompilerParams(
            collective_id=number, has_side_effects=True, vmem_limit_bytes=VMEM_LIMIT
        ),
        name=f"total_{number}",
    )(*operands)


def row_sum_body(value_ref, out_ref, held, core_in, wide_in, *sems):
    one_send, one_recv, two_send, two_recv, core_send, core_recv, wide_send, wide_recv = sems
    wide, core, line, side = places()
    core_mate, wide_mate = row_mates(wide, core, line, side)
    greet([(core >= 0, core_mate), (core >= 0, wide_mate)], False)
    tokens = wide_in.shape[0]

    def block(ref, w, k):
        return strip(ref, 0, w * 2 + k, tokens)

    ones = [
        remote(block(value_ref, w, 1 - core), core_in.at[w], one_send.at[w], one_recv.at[w], core_mate)
        for w in range(2)
    ]
    two = remote(held.at[1 - wide], wide_in, two_send.at[0], two_recv.at[0], wide_mate)
    for copy in ones:
        copy.start()
    for w in range(2):
        ones[w].wait_recv()
        held[w] = (block(value_ref, w, core)[...].astype(F32) + core_in[w].astype(F32)).astype(BF16)
    two.start()
    two.wait_recv()
    held[wide] = (held[wide].astype(F32) + wide_in[...].astype(F32)).astype(BF16)

    def to_core(n):
        w = wide if n == 0 else 1 - wide
        src = held.at[wide] if n == 0 else block(out_ref, w, core)
        return remote(src, block(out_ref, w, core), core_send.at[n], core_recv.at[n], core_mate)

    to_wide = remote(
        held.at[wide], block(out_ref, wide, core), wide_send.at[0], wide_recv.at[0], wide_mate
    )
    to_wide.start()
    to_core(0).start()
    block(out_ref, wide, core)[...] = held[wide]
    to_wide.wait_recv()
    to_core(1).start()
    for n in range(2):
        to_core(n).wait()
    to_wide.wait_send()
    two.wait_send()
    for copy in ones:
        copy.wait_send()


def row_sum(value, number):
    n_row = lax.axis_size("row")
    if n_row != 4:
        return lax.psum(value, "row")
    tokens, width = value.shape[0] // n_row, value.shape[1]
    dma = pltpu.SemaphoreType.DMA
    return pl.pallas_call(
        row_sum_body,
        out_shape=jax.ShapeDtypeStruct(value.shape, value.dtype),
        in_specs=[pl.BlockSpec(memory_space=pltpu.VMEM)],
        out_specs=pl.BlockSpec(memory_space=pltpu.VMEM),
        scratch_shapes=[
            pltpu.VMEM((2, tokens, width), value.dtype),
            pltpu.VMEM((2, tokens, width), value.dtype),
            pltpu.VMEM((tokens, width), value.dtype),
            dma((2,)),
            dma((2,)),
            dma((1,)),
            dma((1,)),
            dma((2,)),
            dma((2,)),
            dma((1,)),
            dma((1,)),
        ],
        compiler_params=pltpu.CompilerParams(collective_id=number, has_side_effects=True),
        name=f"row_sum_{number}",
    )(value)


def gather(
    col_values, dims, flips, row_value, every_value, ways, small_value, number, pick=None
):
    fits = not col_values and every_value is None or lax.axis_size("col") in (4, 6, 8, 10)
    if lax.axis_size("row") == 4 and fits:
        return kernel_gather(
            col_values, dims, flips, row_value, every_value, ways, small_value, number, pick
        )
    out = [lax.all_gather(v, "col", axis=d, tiled=True) for v, d in zip(col_values, dims)]
    if row_value is not None:
        out.append(token_rows(row_value))
    if every_value is not None:
        out.append(every_token(every_value))
    if small_value is not None:
        out.append(every_token(small_value[None]))
    if pick is not None:
        out.append(pick_rows(*pick))
    return out


def pick_body(capacity, place_ref, rows_ref, slots_ref):
    picked = matmul(place_ref[0], rows_ref[...]).astype(BF16)
    slots_ref[:, 0] = picked.reshape(-1, capacity, picked.shape[-1])


def pick_rows(place, rows, local_experts):
    blocks, slots, tokens = place.shape
    capacity, width = slots // local_experts, rows.shape[1]
    return pl.pallas_call(
        functools.partial(pick_body, capacity),
        grid=(blocks,),
        in_specs=[
            pl.BlockSpec((1, slots, tokens), lambda i: (i, 0, 0)),
            pl.BlockSpec((tokens, width), lambda i: (i, 0)),
        ],
        out_specs=pl.BlockSpec((local_experts, 1, capacity, width), lambda i: (0, i, 0, 0)),
        out_shape=jax.ShapeDtypeStruct((local_experts, blocks, capacity, width), BF16),
        name="pick_rows",
    )(place, rows)


def total(
    col_values, dims, flips, row_value, every_value, ways, small_value, number, last_value=None
):
    fits = lax.axis_size("row") == 4
    if col_values or every_value is not None:
        fits = fits and lax.axis_size("col") in (4, 6, 8, 10)
    if every_value is not None:
        fits = fits and kernel_fits(every_value[0].shape, every_value[1].shape[2])
    if fits:
        return kernel_total(
            col_values,
            dims,
            flips,
            row_value,
            every_value,
            ways,
            small_value,
            number,
            last_value,
        )
    out = [col_total(v, d) for v, d in zip(col_values, dims)]
    if row_value is not None:
        out.append(row_total(row_value))
    if every_value is not None:
        capacity = every_value[1].shape[1] // every_value[0].shape[0]
        out.append(every_total(combine_rows(*every_value, capacity)))
    if small_value is not None and small_value.ndim == 2:
        out.append(every_token(small_value[None]))
    elif small_value is not None:
        out.append(lax.all_to_all(small_value, EVERY, split_axis=0, concat_axis=0, tiled=True))
    if last_value is not None:
        scaled, gains, down_rows = last_value
        part = jnp.sum(out[len(dims)] * scaled, axis=0).reshape(4, -1)
        part = jnp.pad(part, ((0, 4), (0, gains.shape[1] - part.shape[1])))
        out.append(lax.psum(gains + part, EVERY)[None])
        out.append(token_rows(out[1][-down_rows:].astype(BF16)))
    return out


def padded_rows(values):
    return jnp.pad(values, ((0, -values.shape[0] % 8), (0, 0)))


def masked_scores(queries, attn_keys, allowed, softmax_scale):
    scores = (
        jnp.einsum("qhd,khd->hqk", queries, attn_keys, preferred_element_type=jnp.float32)
        * softmax_scale
    )
    return jnp.where(allowed[None], scores, -1e30)


def tokens_body(
    group,
    capacity,
    place_ref,
    x_ref,
    g_ref,
    both_ref,
    down_ref,
    xs_ref,
    hidden_ref,
    grad_ref,
    dboth_ref,
    ddown_ref,
):
    tokens = place_ref.shape[2]
    for block in range(group):
        rows = slice(block * tokens, (block + 1) * tokens)
        picked = matmul(place_ref[block], x_ref[rows, :])
        xs_ref[:, block] = picked.astype(BF16).reshape(-1, capacity, picked.shape[-1])
    half = down_ref.shape[0]
    both = outer_cols(x_ref[...], both_ref[...])
    act, slope = silu_parts(both[:, :half])
    lin = both[:, half:]
    hidden = (act * lin).astype(BF16)
    back = outer_cols(g_ref[...], down_ref[...])
    grads = jnp.concatenate([back * lin * slope, back * act], axis=1).astype(BF16)
    hidden_ref[...] = hidden
    grad_ref[...] = grads
    dboth = inner_rows(grads, x_ref[...])
    ddown = inner_rows(hidden, g_ref[...])

    @pl.when(pl.program_id(0) == 0)
    def _():
        dboth_ref[...] = dboth
        ddown_ref[...] = ddown

    @pl.when(pl.program_id(0) > 0)
    def _():
        dboth_ref[...] += dboth
        ddown_ref[...] += ddown


def run_tokens(place, x_all, g_all, both_weight, down_weight, local_experts):
    blocks, slots, tokens = place.shape
    capacity = slots // local_experts
    width = x_all.shape[1]
    half = down_weight.shape[0]
    group = 4 if blocks % 4 == 0 else 1
    row_block = pl.BlockSpec((group * tokens, width), lambda i: (i, 0))
    slot_block = pl.BlockSpec((local_experts, group, capacity, width), lambda i: (0, i, 0, 0))
    slot_shape = jax.ShapeDtypeStruct((local_experts, blocks, capacity, width), BF16)

    def whole(size):
        return pl.BlockSpec((size, width), lambda i: (0, 0))

    def hidden_block(size):
        return pl.BlockSpec((group * tokens, size), lambda i: (i, 0))

    rows = blocks * tokens
    xs, hidden, grads, dboth, ddown = pl.pallas_call(
        functools.partial(tokens_body, group, capacity),
        grid=(blocks // group,),
        in_specs=[
            pl.BlockSpec((group, slots, tokens), lambda i: (i, 0, 0)),
            row_block,
            row_block,
            whole(2 * half),
            whole(half),
        ],
        out_specs=[
            slot_block,
            hidden_block(half),
            hidden_block(2 * half),
            whole(2 * half),
            whole(half),
        ],
        out_shape=[
            slot_shape,
            jax.ShapeDtypeStruct((rows, half), BF16),
            jax.ShapeDtypeStruct((rows, 2 * half), BF16),
            jax.ShapeDtypeStruct((2 * half, width), F32),
            jax.ShapeDtypeStruct((half, width), F32),
        ],
        compiler_params=pltpu.CompilerParams(vmem_limit_bytes=VMEM_LIMIT),
        cost_estimate=pl.CostEstimate(
            flops=2 * rows * width * (slots + 6 * half),
            bytes_accessed=8 * rows * width,
            transcendentals=rows * half,
        ),
        name="run_tokens",
    )(place, x_all, g_all, both_weight, down_weight)
    xs = xs.reshape(local_experts, blocks * capacity, width)
    return xs, hidden, grads, dboth, ddown


def experts_body(
    x_ref,
    g_ref,
    gate_ref,
    wg_ref,
    wu_ref,
    wd_ref,
    y_ref,
    r_ref,
    dg_ref,
    du_ref,
    dd_ref,
    gg_ref,
    both,
    down,
    load_sem,
):
    expert, part = pl.program_id(0), pl.program_id(1)
    size = wd_ref.shape[1]
    held = down.shape[1]
    width = x_ref.shape[2]
    slot = lax.rem(expert, 2)

    def loads(e):
        into = lax.rem(e, 2)
        return [
            pltpu.make_async_copy(wg_ref.at[e], both.at[into, pl.ds(0, size)], load_sem.at[into, 0]),
            pltpu.make_async_copy(
                wu_ref.at[e], both.at[into, pl.ds(held, size)], load_sem.at[into, 1]
            ),
            pltpu.make_async_copy(wd_ref.at[e], down.at[into, pl.ds(0, size)], load_sem.at[into, 2]),
        ]

    @pl.when(jnp.logical_and(expert == 0, part == 0))
    def _():
        if held > size:
            gap = jnp.zeros((2, held - size, width), BF16)
            both[:, size:held] = gap
            both[:, held + size :] = gap
            down[:, size:] = gap
        for copy in loads(expert):
            copy.start()

    @pl.when(part == 0)
    def _():
        for copy in loads(expert):
            copy.wait()

        @pl.when(expert + 1 < pl.num_programs(0))
        def _():
            for copy in loads(expert + 1):
                copy.start()

    x = x_ref[0]
    g = g_ref[0]
    gate = gate_ref[0]
    pre_lin = outer_cols(x, both[slot])
    pre, lin = pre_lin[:, :held], pre_lin[:, held:]
    back = outer_cols(g, down[slot])
    act, slope = silu_parts(pre)
    hidden = act * lin
    gg_ref[0] = jnp.sum(hidden * back, axis=-1, keepdims=True)
    hidden = (hidden * gate).astype(BF16)
    back = back * gate
    pre_grad = (back * lin * slope).astype(BF16)
    lin_grad = (back * act).astype(BF16)
    grads = jnp.concatenate([pre_grad, lin_grad], axis=1)
    first = part == 0
    chunk = 512 if width % 512 == 0 else width
    for start in range(0, width, chunk):
        cols = slice(start, start + chunk)
        y_ref[0, :, cols] = matmul(hidden, down[slot, :, cols]).astype(BF16)
        r_ref[0, :, cols] = matmul(grads, both[slot, :, cols]).astype(BF16)
        d_gate = inner_rows(pre_grad[:, :size], x_ref[0, :, cols])
        d_up = inner_rows(lin_grad[:, :size], x_ref[0, :, cols])
        d_down = inner_rows(hidden[:, :size], g_ref[0, :, cols])

        @pl.when(first)
        def _():
            dg_ref[0, :, cols] = d_gate
            du_ref[0, :, cols] = d_up
            dd_ref[0, :, cols] = d_down

        @pl.when(jnp.logical_not(first))
        def _():
            dg_ref[0, :, cols] += d_gate
            du_ref[0, :, cols] += d_up
            dd_ref[0, :, cols] += d_down


def run_experts(x_slots, g_slots, gates, w_gate, w_up, w_down):
    count, rows, width = x_slots.shape
    hidden = w_down.shape[1]
    held = hidden + -hidden % 128
    chunk = 512 if rows % 512 == 0 else rows
    hbm = pl.BlockSpec(memory_space=pl.ANY)
    row_block = pl.BlockSpec((1, chunk, width), lambda e, r: (e, r, 0))
    col_block = pl.BlockSpec((1, chunk, 1), lambda e, r: (e, r, 0))
    out_block = pl.BlockSpec((1, hidden, width), lambda e, r: (e, 0, 0))
    y, r, d_gate, d_up, d_down, dots = pl.pallas_call(
        experts_body,
        grid=(count, rows // chunk),
        in_specs=[row_block, row_block, col_block, hbm, hbm, hbm],
        out_specs=[row_block, row_block, out_block, out_block, out_block, col_block],
        out_shape=[
            jax.ShapeDtypeStruct((count, rows, width), BF16),
            jax.ShapeDtypeStruct((count, rows, width), BF16),
            jax.ShapeDtypeStruct((count, hidden, width), F32),
            jax.ShapeDtypeStruct((count, hidden, width), F32),
            jax.ShapeDtypeStruct((count, hidden, width), F32),
            jax.ShapeDtypeStruct((count, rows, 1), F32),
        ],
        scratch_shapes=[
            pltpu.VMEM((2, 2 * held, width), BF16),
            pltpu.VMEM((2, held, width), BF16),
            pltpu.SemaphoreType.DMA((2, 3)),
        ],
        compiler_params=pltpu.CompilerParams(vmem_limit_bytes=VMEM_LIMIT),
        cost_estimate=pl.CostEstimate(
            flops=18 * count * rows * width * hidden,
            bytes_accessed=count * (8 * rows * width + 18 * width * hidden),
            transcendentals=count * rows * hidden,
        ),
        name="run_experts",
    )(x_slots, g_slots, gates, w_gate.transpose(0, 2, 1), w_up.transpose(0, 2, 1), w_down)
    return y, r, d_gate.transpose(0, 2, 1), d_up.transpose(0, 2, 1), d_down, dots


def combine_body(group, place_ref, slots_ref, extra_ref, weight_ref, out_ref):
    tokens = place_ref.shape[2]
    width = out_ref.shape[1]
    for block in range(group):
        rows = slice(block * tokens, (block + 1) * tokens)
        total = inner_rows(place_ref[block], slots_ref[:, block].reshape(-1, width))
        total += matmul(extra_ref[rows, :], weight_ref[...])
        out_ref[rows, :] = total.astype(BF16)


def combine_rows(place, slots, extra, weight, capacity):
    blocks, slot_count, tokens = place.shape
    local_experts, _, width = slots.shape
    group = 4 if blocks % 4 == 0 else 1
    inner = extra.shape[1]
    return pl.pallas_call(
        functools.partial(combine_body, group),
        grid=(blocks // group,),
        in_specs=[
            pl.BlockSpec((group, slot_count, tokens), lambda i: (i, 0, 0)),
            pl.BlockSpec((local_experts, group, capacity, width), lambda i: (0, i, 0, 0)),
            pl.BlockSpec((group * tokens, inner), lambda i: (i, 0)),
            pl.BlockSpec((inner, width), lambda i: (0, 0)),
        ],
        out_specs=pl.BlockSpec((group * tokens, width), lambda i: (i, 0)),
        out_shape=jax.ShapeDtypeStruct((blocks * tokens, width), BF16),
        compiler_params=pltpu.CompilerParams(vmem_limit_bytes=VMEM_LIMIT),
        cost_estimate=pl.CostEstimate(
            flops=2 * blocks * tokens * (slot_count + inner) * width,
            bytes_accessed=4 * blocks * tokens * width,
            transcendentals=0,
        ),
        name="combine_rows",
    )(place, slots.reshape(local_experts, blocks, capacity, width), extra, weight)


def on_device(
    inputs,
    segment_ids,
    routes,
    first_gain,
    query_weight,
    latent_down,
    latent_gain,
    latent_up,
    output_weight,
    second_gain,
    router_weight,
    shared_gate,
    shared_up,
    shared_down,
    expert_gate,
    expert_up,
    expert_down,
    cotangent,
):
    n_row = lax.axis_size("row")
    n_col = lax.axis_size("col")
    blocks = n_row * n_col
    own_row = lax.axis_index("row")
    own_col = lax.axis_index("col")
    own_rows = inputs.shape[1]
    width = inputs.shape[2]
    experts = router_weight.shape[1]
    local_experts = expert_gate.shape[0]
    capacity = max(2, own_rows // 8)
    stream = inputs.reshape(own_rows, width).astype(F32)
    grad_out = cotangent.reshape(own_rows, width)
    own_routes = routes.reshape(own_rows, TOPK)
    segments = segment_ids.reshape(-1)
    length = segments.shape[0]
    own_start = own_row * own_rows
    qk_dim = NOPE + ROPE
    softmax_scale = qk_dim ** (-0.5)
    cosine_table, sine_table = angle_tables(length)

    scale_one = rms_scale(stream)
    normed_one = (stream * scale_one * first_gain).astype(BF16)
    down_cols = latent_down.shape[1] // n_row
    own_down = lax.dynamic_slice_in_dim(latent_down, own_row * down_cols, down_cols, 1)
    output_rows = output_weight.shape[0]
    query_cols = query_weight.shape[1]
    query_all, output_down, expand_all, seq_normed, grad_all, all_routes = gather(
        [query_weight, jnp.concatenate([output_weight, own_down.T], axis=0), latent_up],
        [0, 1, 0],
        [False, False, True],
        normed_one,
        grad_out.astype(BF16),
        (0, 0),
        padded_rows(own_routes.astype(F32).T),
        1,
    )
    output_all = output_down[:output_rows]
    down_all = output_down[output_rows:]

    all_routes = all_routes[:, :TOPK].astype(jnp.int32)
    local_ids = own_col * local_experts + jnp.arange(local_experts)
    named = all_routes[:, :, None, :] == local_ids[None, None, :, None]
    chosen_here = jnp.max(named.astype(BF16), axis=1)
    before = (jnp.arange(own_rows)[:, None] < jnp.arange(own_rows)[None, :]).astype(BF16)
    rank = matmul(chosen_here.reshape(-1, own_rows), before).reshape(chosen_here.shape)
    slot_of = jnp.where(chosen_here > 0, rank.astype(jnp.int32), -1)
    placed = slot_of[:, :, None, :] == jnp.arange(capacity)[None, None, :, None]
    place = placed.astype(BF16).reshape(blocks, local_experts * capacity, own_rows)

    shared_cols = shared_gate.shape[1] // n_col
    shared_send = jnp.stack([shared_gate.T, shared_up.T, shared_down], axis=0)
    depth = shared_send.shape[2]
    shared_send = (
        shared_send.reshape(3, n_col, shared_cols, depth)
        .transpose(1, 0, 2, 3)
        .reshape(n_col, 3 * shared_cols, depth)
    )
    shared_send, all_routes = lax.optimization_barrier((shared_send, all_routes))
    shared_own = (
        lax.all_to_all(shared_send, "col", split_axis=0, concat_axis=0, tiled=True)
        .transpose(1, 0, 2)
        .reshape(3, shared_cols, width)
    )
    shared_own = jnp.pad(shared_own, ((0, 0), (0, -shared_cols % 128), (0, 0)))
    shared_held = shared_own.shape[1]
    gate_up_own = shared_own[:2].reshape(2 * shared_held, width)
    down_own = shared_own[2]

    heads_local = query_cols // qk_dim
    query_raw = matmul(seq_normed, query_all).reshape(length, heads_local, qk_dim)
    queries = jnp.concatenate(
        [
            query_raw[..., :NOPE],
            rotate(query_raw[..., NOPE:], cosine_table[:, None, :], sine_table[:, None, :]),
        ],
        axis=-1,
    ).astype(BF16)
    (latent_all,) = gather(
        [], [], [], outer_cols(down_all, seq_normed), None, None, None, 8
    )
    latent_all = latent_all.T
    latent = latent_all[:, :LATENT]
    scale_latent = rms_scale(latent)
    latent_normed = (latent * scale_latent * latent_gain).astype(BF16)
    keyval = matmul(latent_normed, expand_all).reshape(length, heads_local, NOPE + VD)
    key_rope = rotate(latent_all[:, LATENT:], cosine_table, sine_table)
    attn_keys = jnp.concatenate(
        [keyval[..., :NOPE], jnp.broadcast_to(key_rope[:, None, :], (length, heads_local, ROPE))],
        axis=-1,
    ).astype(BF16)
    values = keyval[..., NOPE:].astype(BF16)
    positions = jnp.arange(length)
    allowed = (positions[:, None] >= positions[None, :]) & (segments[:, None] == segments[None, :])
    scores = masked_scores(queries, attn_keys, allowed, softmax_scale)
    highest = jnp.max(scores, axis=-1, keepdims=True)
    log_total = highest + jnp.log(jnp.sum(jnp.exp(scores - highest), axis=-1, keepdims=True))
    attn_probs = jnp.exp(scores - log_total).astype(BF16)
    heads_out = (
        jnp.einsum("hqk,khd->qhd", attn_probs, values, preferred_element_type=jnp.float32)
        .astype(BF16)
        .reshape(length, heads_local * VD)
    )
    (attn_total,) = total(
        [], [], [], matmul(heads_out, output_all).astype(BF16), None, None, None, 6
    )
    residual = stream + attn_total

    scale_two = rms_scale(residual)
    normed_two = (residual * scale_two * second_gain).astype(BF16)
    logits = matmul(normed_two, router_weight)
    expert_ids = jnp.arange(experts)
    chosen = own_routes[:, :, None] == expert_ids[None, None, :]
    picked = jnp.sum(jnp.where(chosen, logits[:, None, :], 0.0), axis=-1)
    gate_probs = jax.nn.softmax(picked, axis=-1)

    all_normed, all_gates, grad_slots = gather(
        [],
        [],
        [],
        None,
        normed_two,
        (0, 1),
        padded_rows(gate_probs.T),
        2,
        (place, grad_all, local_experts),
    )
    grad_slots = grad_slots.reshape(local_experts, blocks * capacity, width)
    all_gates = all_gates[:, :TOPK]
    gate_here = jnp.sum(jnp.where(named, all_gates[:, :, None, :], 0.0), axis=1)
    slot_gate = jnp.sum(jnp.where(placed, gate_here[:, :, None, :], 0.0), axis=-1)
    slot_gate = slot_gate.transpose(1, 0, 2).reshape(local_experts, blocks * capacity, 1)
    normed_slots, shared_hidden, shared_both_grad, gate_up_part, down_part = run_tokens(
        place, all_normed, grad_all, gate_up_own, down_own, local_experts
    )
    out_slots, rows_slots, expert_gate_grad, expert_up_grad, expert_down_grad, slot_dot = (
        run_experts(normed_slots, grad_slots, slot_gate, expert_gate, expert_up, expert_down)
    )

    slot_dot = slot_dot.reshape(local_experts, blocks, capacity).transpose(1, 0, 2)
    token_dot = jnp.sum(jnp.where(placed, slot_dot[:, :, :, None], 0.0), axis=2)
    rows_total, token_dot = total(
        [],
        [],
        [],
        None,
        (place, rows_slots, shared_both_grad, gate_up_own),
        (0, 1),
        token_dot,
        3,
    )
    shared_back = jnp.concatenate(
        [gate_up_part.reshape(2, shared_held, width), down_part[None]], axis=0
    )[:, :shared_cols].astype(BF16)
    shared_back = (
        shared_back.reshape(3 * shared_cols, n_col, depth).transpose(1, 0, 2)
    )
    shared_back = lax.all_to_all(shared_back, "col", split_axis=0, concat_axis=0, tiled=True)
    token_dot = jnp.sum(token_dot.reshape(n_col, n_row, local_experts, own_rows), axis=1)
    token_dot = token_dot.reshape(experts, own_rows).T
    gate_grad = jnp.sum(jnp.where(chosen, token_dot[:, None, :], 0.0), axis=-1)
    picked_grad = gate_probs * (gate_grad - jnp.sum(gate_probs * gate_grad, axis=-1, keepdims=True))
    logit_grad = jnp.sum(jnp.where(chosen, picked_grad[:, :, None], 0.0), axis=1).astype(BF16)

    normed_two_grad = rows_total + outer_cols(logit_grad, router_weight)
    second_gain_part = jnp.sum(normed_two_grad * residual * scale_two, axis=0)
    residual_grad = grad_out + rms_back(residual, scale_two, normed_two_grad * second_gain)

    (seq_resid,) = gather([], [], [], residual_grad.astype(BF16), None, None, None, 4)
    output_part = inner_rows(heads_out, seq_resid)
    heads_grad = outer_cols(seq_resid, output_all).astype(BF16).reshape(length, heads_local, VD)
    recomputed = jnp.exp(masked_scores(queries, attn_keys, allowed, softmax_scale) - log_total)
    delta_rows = jnp.sum(
        heads_grad.astype(F32) * heads_out.reshape(length, heads_local, VD).astype(F32),
        axis=-1,
    )
    prob_grad = jnp.einsum("qhd,khd->hqk", heads_grad, values, preferred_element_type=jnp.float32)
    score_grad = (recomputed * (prob_grad - delta_rows.T[:, :, None]) * softmax_scale).astype(BF16)
    queries_grad = jnp.einsum(
        "hqk,khd->qhd", score_grad, attn_keys, preferred_element_type=jnp.float32
    )
    key_grad = jnp.einsum("hqk,qhd->khd", score_grad, queries, preferred_element_type=jnp.float32)
    value_grad = jnp.einsum(
        "hqk,qhd->khd",
        recomputed.astype(BF16),
        heads_grad,
        preferred_element_type=jnp.float32,
    )
    query_full = (
        jnp.concatenate(
            [
                queries_grad[..., :NOPE],
                unrotate(
                    queries_grad[..., NOPE:], cosine_table[:, None, :], sine_table[:, None, :]
                ),
            ],
            axis=-1,
        )
        .astype(BF16)
        .reshape(length, heads_local * qk_dim)
    )
    keyval_grad = (
        jnp.concatenate([key_grad[..., :NOPE], value_grad], axis=-1)
        .astype(BF16)
        .reshape(length, heads_local * (NOPE + VD))
    )
    expand_part = inner_rows(latent_normed, keyval_grad)
    latent_normed_part = outer_cols(keyval_grad, expand_all)
    rope_part = jnp.sum(key_grad[..., NOPE:], axis=1)
    latent_total = row_sum(
        jnp.concatenate([latent_normed_part, rope_part], axis=1).astype(BF16), 9
    ).astype(F32)
    latent_normed_grad, rope_raw = latent_total[:, :LATENT], latent_total[:, LATENT:]
    rope_grad = unrotate(rope_raw, cosine_table, sine_table)
    latent_gain_part = jnp.sum(
        lax.dynamic_slice_in_dim(
            latent_normed_grad * latent * scale_latent, own_start, own_rows, 0
        ),
        axis=0,
    )
    latent_grad = rms_back(latent, scale_latent, latent_normed_grad * latent_gain)
    down_grad_in = jnp.concatenate([latent_grad, rope_grad], axis=-1).astype(BF16)
    own_down_grad = lax.dynamic_slice_in_dim(down_grad_in, own_row * down_cols, down_cols, 1)
    output_down_part = jnp.concatenate(
        [output_part.astype(BF16), inner_rows(own_down_grad, seq_normed).astype(BF16)], axis=0
    )
    input_part = outer_cols(query_full, query_all) + matmul(own_down_grad, down_all)
    input_part, shared_back = lax.optimization_barrier((input_part, shared_back))
    gains = jnp.concatenate(
        [
            jnp.pad(second_gain_part.reshape(4, -1), ((4, 0), (0, 0))),
            jnp.pad(latent_gain_part.reshape(4, -1), ((0, 4), (0, 0))),
        ],
        axis=1,
    )
    (
        query_grad,
        output_down_grad,
        latent_up_grad,
        normed_one_grad,
        out_total,
        all_picked,
        all_gains,
        down_total,
    ) = total(
        [inner_rows(seq_normed, query_full).astype(BF16), output_down_part, expand_part.astype(BF16)],
        [0, 1, 0],
        [False, False, True],
        input_part.astype(BF16),
        (place, out_slots, shared_hidden, down_own),
        (0, 0),
        padded_rows(picked_grad.T),
        7,
        (stream * scale_one, gains, down_cols),
    )
    layer_out = (residual + out_total).astype(BF16).reshape(1, own_rows, width)
    output_grad = output_down_grad[:output_rows]
    input_grad = (
        residual_grad + rms_back(stream, scale_one, normed_one_grad * first_gain)
    ).reshape(1, own_rows, width)

    shared_back = (
        shared_back.reshape(n_col, 3, shared_cols, depth)
        .transpose(1, 0, 2, 3)
        .reshape(3, n_col * shared_cols, depth)
        .astype(F32)
    )
    shared_gate_grad = shared_back[0].T
    shared_up_grad = shared_back[1].T
    shared_down_grad = shared_back[2]

    all_named = all_routes[:, :, :, None] == expert_ids
    all_logit_grad = jnp.sum(jnp.where(all_named, all_picked[:, :TOPK, :, None], 0.0), axis=1)
    router_grad = inner_rows(all_normed, all_logit_grad.astype(BF16).reshape(-1, experts))
    latent_down_grad = down_total.astype(F32).T
    gains = jnp.sum(all_gains, axis=0)
    first_gain_grad = gains[:4, : width // 4].reshape(-1)
    second_gain_grad = gains[4:, : width // 4].reshape(-1)
    latent_gain_grad = gains[:4, width // 4 :].reshape(-1)
    return (
        layer_out,
        input_grad,
        first_gain_grad,
        query_grad,
        latent_down_grad,
        latent_gain_grad,
        latent_up_grad,
        output_grad,
        second_gain_grad,
        router_grad,
        shared_gate_grad,
        shared_up_grad,
        shared_down_grad,
        expert_gate_grad,
        expert_up_grad,
        expert_down_grad,
    )


def solution(mesh):
    return jax.shard_map(
        on_device,
        mesh=mesh,
        in_specs=(
            P("col", "row", None),
            P("col", None),
            P("col", "row", None),
            P(),
            P("col", "row"),
            P("col", None),
            P(),
            P("col", "row"),
            P("row", "col"),
            P(),
            P(),
            P("col", "row"),
            P("col", "row"),
            P("row", "col"),
            P("col", None, "row"),
            P("col", None, "row"),
            P("col", "row", None),
            P("col", "row", None),
        ),
        out_specs=(
            P("col", "row", None),
            P("col", "row", None),
            P(),
            P("col", "row"),
            P("col", None),
            P(),
            P("col", "row"),
            P("row", "col"),
            P(),
            P(),
            P("col", "row"),
            P("col", "row"),
            P("row", "col"),
            P("col", None, "row"),
            P("col", None, "row"),
            P("col", "row", None),
        ),
        check_vma=False,
    )
```
